32 devices in a mesh: dp: 4 (over y, x), expert: 8 (over z, core).
Axes of the slice: x: 2, y: 2, z: 4, core: 2. Of those that a mesh axis runs over, the one named last changes fastest.
Arguments:
- inputs: bfloat16 [1, 4096, 2048], P(None, 'expert'), may hold values from -6 to 6
- attention_norm_gain: float32 [2048], replicated, may hold values from 0.5 to 1.5
- w_query: bfloat16 [2048, 2048], P(None, 'dp'), may hold values from -0.125 to 0.125
- w_key: bfloat16 [2048, 2048], P(None, 'dp'), may hold values from -0.125 to 0.125
- w_value: bfloat16 [2048, 2048], P(None, 'dp'), may hold values from -0.125 to 0.125
- w_out: bfloat16 [2048, 2048], P('dp'), may hold values from -1 to 1
- q_gain: float32 [2048], P('dp'), may hold values from 0.5 to 1.5
- k_gain: float32 [2048], P('dp'), may hold values from 0.5 to 1.5
- expert_norm_gain: float32 [2048], replicated, may hold values from 0.5 to 1.5
- w_router: float32 [2048, 16], replicated, may hold values from -0.125 to 0.125
- w_gate: bfloat16 [16, 2048, 1024], P('expert', None, 'dp'), may hold values from -0.125 to 0.125
- w_up: bfloat16 [16, 2048, 1024], P('expert', None, 'dp'), may hold values from -0.125 to 0.125
- w_down: bfloat16 [16, 1024, 2048], P('expert', 'dp'), may hold values from -4 to 4
- routes: int32 [4096, 1, 8], P('expert'), may hold values from 0 to 15, all different within a row; in each aligned block of 512 rows (0 to 511, 512 to 1023, ..., all dimensions but the last counted through in order) at most 512 rows name the same one
- lengths: int32 [1, 16], replicated, may hold values from 1 to 3072, 4096 in all within a row
- d_output: bfloat16 [1, 4096, 2048], P(None, 'expert'), may hold values from -6 to 6
Outputs:
- output: bfloat16 [1, 4096, 2048], P(None, 'expert')
- grad_input: float32 [1, 4096, 2048], P(None, 'expert')
- grad_attn_gain: float32 [2048], P('expert')
- grad_query: float32 [2048, 2048], P('expert', 'dp')
- grad_key: float32 [2048, 2048], P('expert', 'dp')
- grad_value: float32 [2048, 2048], P('expert', 'dp')
- grad_out: float32 [2048, 2048], P(('dp', 'expert'))
- grad_q_gain: float32 [2048], P(('dp', 'expert'))
- grad_k_gain: float32 [2048], P(('dp', 'expert'))
- grad_expert_norm_gain: float32 [2048], P('expert')
- grad_router: float32 [2048, 16], P('expert')
- grad_gate: float32 [16, 2048, 1024], P('expert', None, 'dp')
- grad_up: float32 [16, 2048, 1024], P('expert', None, 'dp')
- grad_down: float32 [16, 1024, 2048], P('expert', 'dp')
The draws below stay inside these ranges and needn't reach their ends.
Inputs may be any that keep to these rules, and one draw needn't show every extreme that they name: `routes`: each token names 8 different experts; of the rows of one index of the expert axis at most 512 name any one expert, a bound that some block reaches of them. `lengths`: each row sums to 4096; its largest entry is 3072.
All inputs are finite; a program needn't handle non-finite values.
Results may differ from the reference program's by a relative error of at most 0.025.
Values may be sent and summed in bfloat16 or wider, within the bound.
A program may use at most 576 MiB of HBM per device.

```python
import math
import jax
import jax.numpy as jnp
import numpy as np
from jax import lax

D = 2048
HEADS = 16
HD = 128
FF = 1024
TOPK = 8
PACK = 4096
NDOCS = 16
EXPERTS = 16
PACKS = 1
TOK_DEV = 512
CAP = 512
N_DP = 4
N_EXPERT = 8


def steps_of(stream_key, shape, cuts, least, largest):
    level, own = 1.0, jax.random.fold_in(stream_key, 6)
    for axis_at, parts in cuts:
        heights = jnp.exp(jax.random.uniform(jax.random.fold_in(own, axis_at), (parts,), jnp.float32, least / len(cuts), largest / len(cuts)))
        level = level * jnp.repeat(heights, shape[axis_at] // parts).reshape([-1 if axis == axis_at else 1 for axis in range(len(shape))])
    return level


def length_profile(number_of, total, limit, lean):
    weights = [(1 << 20) // math.isqrt(standing ** lean) + 1 for standing in range(2, number_of + 1)]
    rest, given = total - limit - (number_of - 1), [1] * (number_of - 1)
    while rest > 0:
        movable = [i for i in range(number_of - 1) if given[i] < limit]
        whole, remaining = sum([weights[i] for i in movable]), rest
        for i in movable:
            extra = min(limit - given[i], max(1, remaining * weights[i] // whole), rest)
            given[i] = given[i] + extra
            rest = rest - extra
    return np.array([limit] + given)


def uneven(rng, count, total, limit, lean):
    if count == 2:
        one = jax.random.randint(rng, (), max(1, total - limit), min(limit, total - 1) + 1)
        return jnp.stack([one, total - one])
    sizes = jnp.asarray(length_profile(count, total, limit, lean), jnp.int32)
    twos = (count - 1) // 2
    donor, taker = sizes[1:1 + 2 * twos:2], sizes[2:2 + 2 * twos:2]
    margin = jnp.minimum(donor - 1, limit - taker)
    passed = jax.random.randint(jax.random.fold_in(rng, 1), (twos,), 0, 1 << 20) % (margin + 1)
    sizes = sizes.at[1:1 + 2 * twos:2].set(donor - passed).at[2:2 + 2 * twos:2].set(taker + passed)
    return sizes[jax.random.permutation(jax.random.fold_in(rng, 2), count)]


def deal_out(key, own, number, rows, count, top, bound, lean):
    ranking = jax.random.permutation(key, count)
    packed, usual = portions_of(count, rows * top, bound, lean, True), portions_of(count, rows * top, bound, lean, False)
    places = jnp.arange(count)

    def named(tallies, turn):
        used = int((tallies > 0).sum())
        fixed = max(1, used // 4)
        passed = fixed + (places - fixed + turn * (used - fixed)) % max(1, count - fixed)
        return jnp.zeros((count,), jnp.int32).at[ranking[jnp.where(places < fixed, places, passed)]].set(jnp.asarray(tallies, jnp.int32))

    tallies = jnp.where(number % 4 == 0, named(packed, number // 4), named(usual, number - number // 4 - 1))
    mixed = jax.random.permutation(jax.random.fold_in(own, 3), count)
    donor, sink = mixed[0:count // 2 * 2:2], mixed[1:count // 2 * 2:2]
    room = jnp.minimum(tallies[donor] - 1, bound - tallies[sink]) // 2
    room = jnp.where((donor == ranking[0]) | (sink == ranking[0]) | (tallies[sink] == 0), 0, jnp.maximum(room, 0))
    passed = jax.random.randint(jax.random.fold_in(own, 4), (count // 2,), 0, 1 << 20) % (room + 1)
    tallies = tallies.at[donor].add(-passed).at[sink].add(passed)
    labels = jnp.searchsorted(jnp.cumsum(tallies), jnp.arange(rows * top), side="right").astype(jnp.int32)
    table = labels.reshape(top, rows).T
    table = table[jax.random.permutation(jax.random.fold_in(own, 1), rows)]
    turn = jax.random.randint(jax.random.fold_in(own, 2), (rows, 1), 0, top)
    return jnp.take_along_axis(table, (jnp.arange(top)[None, :] + turn) % top, axis=1)


def portions_of(count, total, most, skew, full):
    loads = [(1 << 20) // math.isqrt(standing ** skew) + 1 for standing in range(1, count + 1)]
    largest = most if full else min(most, max(-(-total // count), total * loads[0] // sum(loads)))
    least = 1 if total - largest >= count - 1 else 0
    given, surplus = [largest] + [least] * (count - 1), total - largest - least * (count - 1)
    while surplus > 0:
        movable = [i for i in range(1, count) if given[i] < largest] or [i for i in range(1, count) if given[i] < most]
        pool, budget = sum([loads[i] for i in movable]), surplus
        for i in movable:
            extra = min(most - given[i], max(1, budget * loads[i] // pool), surplus)
            given[i] = given[i] + extra
            surplus = surplus - extra
    return np.array(given)


def centred(stream_key, shape, scale, limit, cuts=(), kind=jnp.bfloat16):
    entries = scale * jax.random.normal(stream_key, shape, jnp.float32)
    if cuts:
        entries = entries * steps_of(stream_key, shape, cuts, -0.22, 0.18)
    return jnp.clip(entries, -limit, limit).astype(kind)


def setup_inputs(seed: int = 0) -> dict:
    key_list = jax.random.split(jax.random.key(seed), 17)
    inputs = centred(key_list[0], (PACKS, PACK, D), 1.0, 6.0, ((1, 8),))
    attention_norm_gain = jnp.clip(1.0 + 0.1 * jax.random.normal(key_list[1], (D,), jnp.float32), 0.5, 1.5)
    w_query = centred(key_list[2], (D, D), D ** -0.5, 0.125, ((1, 4),))
    w_key = centred(key_list[3], (D, D), D ** -0.5, 0.125, ((1, 4),))
    w_value = centred(key_list[4], (D, D), D ** -0.5, 0.125, ((1, 4),))
    w_out = centred(key_list[5], (D, D), (D // 64) ** -0.5, 1.0, ((0, 4),))
    q_gain = jnp.clip(1.0 + 0.1 * jax.random.normal(key_list[6], (D,), jnp.float32), 0.5, 1.5)
    k_gain = jnp.clip(1.0 + 0.1 * jax.random.normal(key_list[7], (D,), jnp.float32), 0.5, 1.5)
    expert_norm_gain = jnp.clip(1.0 + 0.1 * jax.random.normal(key_list[8], (D,), jnp.float32), 0.5, 1.5)
    w_router = centred(key_list[9], (D, EXPERTS), D ** -0.5, 0.125, (), jnp.float32)
    w_gate = centred(key_list[10], (EXPERTS, D, FF), D ** -0.5, 0.125, ((0, 8), (2, 4)))
    w_up = centred(key_list[11], (EXPERTS, D, FF), D ** -0.5, 0.125, ((0, 8), (2, 4)))
    w_down = centred(key_list[12], (EXPERTS, FF, D), (max(FF // 512, 1)) ** -0.5, 4.0, ((0, 8), (1, 4)))
    routes_keys = jax.random.split(jax.random.fold_in(key_list[13], 1), PACK * PACKS // TOK_DEV)
    routes_turns = jax.random.permutation(jax.random.fold_in(key_list[13], 3), PACK * PACKS // TOK_DEV)
    routes = jax.vmap(lambda own, number: deal_out(jax.random.fold_in(key_list[13], 2), own, number, TOK_DEV, EXPERTS, TOPK, CAP, 2))(routes_keys, routes_turns).reshape((PACK, PACKS, TOPK))
    lengths = jax.vmap(lambda own: uneven(own, NDOCS, PACK, 3 * PACK // 4, 2))(jax.random.split(key_list[14], PACKS)).reshape((PACKS, NDOCS)).astype(jnp.int32)
    d_output = centred(key_list[15], (PACKS, PACK, D), 1.0, 6.0, ((1, 8),))
    return {"inputs": inputs, "attention_norm_gain": attention_norm_gain, "w_query": w_query, "w_key": w_key, "w_value": w_value, "w_out": w_out, "q_gain": q_gain, "k_gain": k_gain, "expert_norm_gain": expert_norm_gain, "w_router": w_router, "w_gate": w_gate, "w_up": w_up, "w_down": w_down, "routes": routes, "lengths": lengths, "d_output": d_output}


epsilon = 1e-05
rope_base = 10000.0

@jax.custom_vjp
def low(v):
    return lax.optimization_barrier(v.astype(jnp.bfloat16)).astype(jnp.float32)

@jax.custom_vjp
def low_back(v):
    return v

def low_keep(v):
    return (low(v), None)

def low_pass(kept, grad):
    return (grad,)

def back_keep(v):
    return (v, None)

def back_low(kept, grad):
    return (low(grad),)
low.defvjp(low_keep, low_pass)
low_back.defvjp(back_keep, back_low)

def doc_layout(lengths, pack_span):
    doc_ends = jnp.cumsum(lengths, axis=1).astype(jnp.int32)
    starts = doc_ends - lengths
    places = jnp.arange(pack_span, dtype=jnp.int32)
    segment = lax.optimization_barrier(jnp.sum((places[None, :, None] >= doc_ends[:, None, :]).astype(jnp.int32), axis=2)).astype(jnp.int32)
    member = segment[:, :, None] == jnp.arange(lengths.shape[1], dtype=jnp.int32)[None, None, :]
    begins = lax.optimization_barrier(jnp.sum(jnp.where(member, starts[:, None, :], 0), axis=2)).astype(jnp.int32)
    return (segment, places[None, :] - begins)

def rope_tables(positions, head_size):
    half_size = head_size // 2
    frequency = rope_base ** (-2.0 * jnp.arange(half_size, dtype=jnp.float32) / head_size)
    angles = positions.astype(jnp.float32)[..., None] * frequency
    return (jnp.cos(angles), jnp.sin(angles))

def rotate(heads_in, cos_table, sin_table):
    half_size = heads_in.shape[-1] // 2
    first_half = heads_in[..., :half_size]
    second_half = heads_in[..., half_size:]
    cos_head = cos_table[..., None, :]
    sin_head = sin_table[..., None, :]
    return jnp.concatenate([first_half * cos_head - second_half * sin_head, second_half * cos_head + first_half * sin_head], axis=-1)

def rms_norm(values):
    return values * lax.rsqrt(lax.optimization_barrier(jnp.mean(values * values, axis=-1, keepdims=True)) + epsilon)

def product(left_side, right_side):
    return jnp.dot(left_side, right_side, precision=lax.Precision.HIGHEST)

def reference(inputs, attention_norm_gain, w_query, w_key, w_value, w_out, q_gain, k_gain, expert_norm_gain, w_router, w_gate, w_up, w_down, routes, lengths, d_output):
    segment, positions = doc_layout(lengths, PACK)
    cos_table, sin_table = rope_tables(positions, HD)
    chosen = jnp.transpose(routes, (1, 0, 2))
    route_ids = chosen.reshape(-1)
    sorted_routes = jnp.argsort(route_ids, stable=True).astype(jnp.int32)
    counts = lax.optimization_barrier(jnp.sum((route_ids[:, None] == jnp.arange(EXPERTS, dtype=jnp.int32)[None, :]).astype(jnp.int32), axis=0)).astype(jnp.int32)
    firsts = (jnp.cumsum(counts) - counts).astype(jnp.int32)
    most_rows = N_EXPERT * CAP
    padded_order = jnp.concatenate([sorted_routes, jnp.zeros((most_rows,), jnp.int32)])
    block_rows = min(512, PACK)
    block_count = PACK // block_rows
    slice_width = FF // N_DP
    scale_factor = HD ** (-0.5)
    expert_index = jnp.arange(EXPERTS, dtype=jnp.int32)

    def layer(inputs, attention_norm_gain, w_query, w_key, w_value, w_out, q_gain, k_gain, expert_norm_gain, w_router, w_gate, w_up, w_down):
        first_normed_input = low(rms_norm(inputs) * attention_norm_gain)
        q_raw = low_back(product(first_normed_input, w_query))
        k_raw = low_back(product(first_normed_input, w_key))
        values = low(low_back(product(first_normed_input, w_value))).reshape(PACKS, PACK, HEADS, HD)
        q_normed = (rms_norm(q_raw) * q_gain).reshape(PACKS, PACK, HEADS, HD)
        k_normed = (rms_norm(k_raw) * k_gain).reshape(PACKS, PACK, HEADS, HD)
        queries = low(rotate(q_normed, cos_table, sin_table))
        keys_all = low(rotate(k_normed, cos_table, sin_table))

        def attend(block_item):
            pack_id = block_item // block_count
            row_start = block_item % block_count * block_rows
            q_block = lax.dynamic_slice_in_dim(queries[pack_id], row_start, block_rows, 0)
            seg_keys = segment[pack_id]
            seg_block = lax.dynamic_slice_in_dim(seg_keys, row_start, block_rows, 0)
            q_places = row_start + jnp.arange(block_rows, dtype=jnp.int32)
            k_places = jnp.arange(PACK, dtype=jnp.int32)
            allowed = (seg_block[:, None] == seg_keys[None, :]) & (k_places[None, :] <= q_places[:, None])
            scores = low_back(jnp.einsum('qhd,khd->hqk', q_block, keys_all[pack_id], precision=lax.Precision.HIGHEST) * scale_factor)
            scores = jnp.where(allowed[None], scores, -1e+30)
            weights = jax.nn.softmax(scores, axis=-1)
            return jnp.einsum('hqk,khd->qhd', low(weights), values[pack_id], precision=lax.Precision.HIGHEST)
        attended = lax.map(jax.checkpoint(attend), jnp.arange(PACKS * block_count, dtype=jnp.int32))
        attended = low(low_back(attended.reshape(PACKS, PACK, D)))
        hidden_state = inputs + low_back(product(attended, w_out))
        second_normed_input = rms_norm(hidden_state) * expert_norm_gain
        router = jax.nn.softmax(product(second_normed_input, w_router), axis=-1)
        gate_flat = jnp.take_along_axis(router, chosen, axis=-1).reshape(-1)
        rows_all = low(second_normed_input).reshape(PACKS * PACK, D)

        def expert_out(gate_e, up_e, down_e, expert_id):
            picked = lax.dynamic_slice_in_dim(padded_order, firsts[expert_id], most_rows, 0)
            live_rows = jnp.arange(most_rows, dtype=jnp.int32) < counts[expert_id]
            tokens = picked // TOPK
            routed_rows = rows_all[tokens]
            scaled = jnp.where(live_rows, gate_flat[picked], 0.0)
            summed = jnp.zeros((most_rows, D), jnp.float32)
            for block_id in range(N_DP):
                first_unit = block_id * slice_width
                piece_rows = low_back(routed_rows)
                gate_pre = low_back(product(piece_rows, gate_e[:, first_unit:first_unit + slice_width]))
                up_pre = low_back(product(piece_rows, up_e[:, first_unit:first_unit + slice_width]))
                activated = low(jax.nn.silu(gate_pre) * up_pre)
                summed = summed + low(product(activated, down_e[first_unit:first_unit + slice_width, :]))
            return (scaled[:, None] * low_back(summed), tokens)

        def step_expert(moe_sum, sliced):
            gate_e, up_e, down_e, expert_id = sliced
            contribution, tokens = jax.checkpoint(expert_out)(gate_e, up_e, down_e, expert_id)
            return (moe_sum.at[tokens].add(contribution), None)
        moe_flat = lax.scan(step_expert, jnp.zeros((PACKS * PACK, D), jnp.float32), (w_gate, w_up, w_down, expert_index))[0]
        return hidden_state + moe_flat.reshape(PACKS, PACK, D)
    output, pullback = jax.vjp(layer, inputs.astype(jnp.float32), attention_norm_gain.astype(jnp.float32), w_query.astype(jnp.float32), w_key.astype(jnp.float32), w_value.astype(jnp.float32), w_out.astype(jnp.float32), q_gain.astype(jnp.float32), k_gain.astype(jnp.float32), expert_norm_gain.astype(jnp.float32), w_router.astype(jnp.float32), w_gate.astype(jnp.float32), w_up.astype(jnp.float32), w_down.astype(jnp.float32))
    gradients = pullback(d_output.astype(jnp.float32))
    return (output.astype(jnp.bfloat16), gradients[0], gradients[1], gradients[2], gradients[3], gradients[4], gradients[5], gradients[6], gradients[7], gradients[8], gradients[9], gradients[10], gradients[11], gradients[12])
```

```python
import jax
import jax.numpy as jnp
from jax import lax
from jax.sharding import PartitionSpec as P

HD = 128


epsilon = 1e-05
rope_base = 10000.0
masked_score = -1e30


def doc_layout(lengths, pack_span):
    doc_ends = jnp.cumsum(lengths, axis=1)
    starts = doc_ends - lengths
    places = jnp.arange(pack_span, dtype=jnp.int32)
    segment = jnp.sum((places[None, :, None] >= doc_ends[:, None, :]).astype(jnp.int32), axis=2)
    member = segment[:, :, None] == jnp.arange(lengths.shape[1], dtype=jnp.int32)[None, None, :]
    begins = jnp.sum(jnp.where(member, starts[:, None, :], 0), axis=2)
    return (segment, places[None, :] - begins)


def rope_tables(positions, head_size):
    half_size = head_size // 2
    frequency = rope_base ** (-2.0 * jnp.arange(half_size, dtype=jnp.float32) / head_size)
    angles = positions.astype(jnp.float32)[..., None] * frequency
    return (jnp.cos(angles), jnp.sin(angles))


def rotate(heads_in, cos_table, sin_table):
    half_size = heads_in.shape[-1] // 2
    first_half = heads_in[..., :half_size]
    second_half = heads_in[..., half_size:]
    cos_head = cos_table[..., None, :]
    sin_head = sin_table[..., None, :]
    return jnp.concatenate(
        [
            first_half * cos_head - second_half * sin_head,
            second_half * cos_head + first_half * sin_head,
        ],
        axis=-1,
    )


ALL = ("dp", "expert")


def gather_all(rows):
    return lax.all_gather(rows, ALL, axis=0, tiled=True)


def gather_dp(rows):
    return lax.all_gather(rows, "dp", axis=0, tiled=True)


def scatter_all(rows):
    return lax.psum_scatter(rows, ALL, scatter_dimension=0, tiled=True).astype(jnp.float32)


def scatter_dp(rows):
    return lax.psum_scatter(rows, "dp", scatter_dimension=0, tiled=True).astype(jnp.float32)


def scatter_sum(value):
    total = lax.psum(value.astype(jnp.bfloat16), "dp")
    return lax.psum_scatter(total, "expert", scatter_dimension=0, tiled=True).astype(jnp.float32)


def head_totals(first_sum, second_sum):
    return lax.psum((first_sum, second_sum), "dp")


def per_device(
    inputs,
    attention_norm_gain,
    w_query,
    w_key,
    w_value,
    w_out,
    q_gain,
    k_gain,
    expert_norm_gain,
    w_router,
    w_gate,
    w_up,
    w_down,
    routes,
    lengths,
    d_output,
):
    pack_count, seg_rows, model_width = inputs.shape
    local_width = w_query.shape[1]
    local_heads = local_width // HD
    experts = w_router.shape[1]
    groups = lax.axis_size("expert")
    pack_span = seg_rows * groups
    local_experts = w_gate.shape[0]
    scale_factor = HD ** (-0.5)
    offset_rows = lax.axis_index("expert") * seg_rows
    segment, positions = doc_layout(lengths, pack_span)
    seg_query = lax.dynamic_slice_in_dim(segment, offset_rows, seg_rows, 1)
    pos_query = lax.dynamic_slice_in_dim(positions, offset_rows, seg_rows, 1)
    cos_table, sin_table = rope_tables(pos_query, HD)
    key_places = jnp.arange(pack_span, dtype=jnp.int32)
    query_places = offset_rows + jnp.arange(seg_rows, dtype=jnp.int32)
    allowed = (seg_query[:, :, None] == segment[:, None, :]) & (
        key_places[None, None, :] <= query_places[None, :, None]
    )
    head_shape = (pack_count, seg_rows, local_heads, HD)
    inputs_single_float = inputs.astype(jnp.float32)
    first_inverse_norm = lax.rsqrt(
        jnp.mean(inputs_single_float * inputs_single_float, axis=-1, keepdims=True) + epsilon
    )
    first_unit_input = inputs_single_float * first_inverse_norm
    first_normed_input = (first_unit_input * attention_norm_gain).astype(jnp.bfloat16)
    q_raw = jnp.dot(first_normed_input, w_query, preferred_element_type=jnp.float32)
    k_raw = jnp.dot(first_normed_input, w_key, preferred_element_type=jnp.float32)
    value_rows = jnp.dot(first_normed_input, w_value, preferred_element_type=jnp.float32).astype(
        jnp.bfloat16
    )
    q_sum, k_sum = head_totals(jnp.sum(q_raw * q_raw, axis=-1), jnp.sum(k_raw * k_raw, axis=-1))
    q_inv = lax.rsqrt(q_sum[..., None] / model_width + epsilon)
    k_inv = lax.rsqrt(k_sum[..., None] / model_width + epsilon)
    q_hat = q_raw * q_inv
    k_hat = k_raw * k_inv
    queries = rotate((q_hat * q_gain).reshape(head_shape), cos_table, sin_table).astype(
        jnp.bfloat16
    )
    key_rows = (
        rotate((k_hat * k_gain).reshape(head_shape), cos_table, sin_table)
        .astype(jnp.bfloat16)
        .reshape(pack_count, seg_rows, local_width)
    )
    keys_all, values_all = (
        lax.all_gather(key_rows, "expert", axis=1, tiled=True),
        lax.all_gather(value_rows, "expert", axis=1, tiled=True),
    )
    keys_heads = keys_all.reshape(pack_count, pack_span, local_heads, HD)
    values_heads = values_all.reshape(pack_count, pack_span, local_heads, HD)

    def score_block(query_block):
        scores = (
            jnp.einsum(
                "pshd,plhd->phsl", query_block, keys_heads, preferred_element_type=jnp.float32
            )
            * scale_factor
        )
        return jnp.where(allowed[:, None], scores, masked_score)

    scores = score_block(queries)
    largest = jnp.max(scores, axis=-1, keepdims=True)
    log_total = largest + jnp.log(jnp.sum(jnp.exp(scores - largest), axis=-1, keepdims=True))
    weights = jnp.exp(scores - log_total)
    attended = jnp.einsum(
        "phsl,plhd->pshd",
        weights.astype(jnp.bfloat16),
        values_heads,
        preferred_element_type=jnp.float32,
    )
    attended = attended.astype(jnp.bfloat16).reshape(pack_count, seg_rows, local_width)
    attn_part = jnp.dot(
        attended.reshape(seg_rows, local_width), w_out, preferred_element_type=jnp.float32
    )
    own = lax.axis_index("dp")
    part_rows = seg_rows // lax.axis_size("dp")

    def own_rows(rows):
        return lax.dynamic_slice_in_dim(rows, own * part_rows, part_rows, 0)

    hidden_state = own_rows(inputs_single_float[0]) + scatter_dp(attn_part.astype(jnp.bfloat16))
    second_inverse_norm = lax.rsqrt(
        jnp.mean(hidden_state * hidden_state, axis=-1, keepdims=True) + epsilon
    )
    second_unit_input = hidden_state * second_inverse_norm
    second_normed_input = second_unit_input * expert_norm_gain
    router = jax.nn.softmax(
        jnp.dot(second_normed_input, w_router, precision=lax.Precision.HIGHEST), axis=-1
    )
    chosen = own_rows(routes[:, 0, :])
    expert_range = jnp.arange(experts, dtype=jnp.int32)
    named = jnp.any(chosen[:, :, None] == expert_range, axis=1)
    gate_table = gather_all(jnp.where(named, router, 0.0))
    first_expert = lax.axis_index("expert") * local_experts
    gates = lax.dynamic_slice_in_dim(gate_table, first_expert, local_experts, 1)
    xn_all = gather_all(second_normed_input.astype(jnp.bfloat16))
    top_own = own_rows(d_output[0])
    top_all = gather_all(top_own)

    gate_pre = jnp.einsum("td,jdf->tjf", xn_all, w_gate, preferred_element_type=jnp.float32)
    up_pre = jnp.einsum("td,jdf->tjf", xn_all, w_up, preferred_element_type=jnp.float32)
    top_down = jnp.einsum("td,jfd->tjf", top_all, w_down, preferred_element_type=jnp.float32)
    sigmoid_gate = jax.nn.sigmoid(gate_pre)
    silu_gate = gate_pre * sigmoid_gate
    activated = silu_gate * up_pre
    scaled = (activated * gates[:, :, None]).astype(jnp.bfloat16)
    gate_part = jnp.sum(activated * top_down, axis=-1)
    grad_act = top_down * gates[:, :, None]
    grad_gate_pre = (
        grad_act * up_pre * sigmoid_gate * (1.0 + gate_pre * (1.0 - sigmoid_gate))
    ).astype(jnp.bfloat16)
    grad_up_pre = (grad_act * silu_gate).astype(jnp.bfloat16)
    moe_part = jnp.einsum("tjf,jfd->td", scaled, w_down, preferred_element_type=jnp.float32)
    grad_rows = jnp.einsum("tjf,jdf->td", grad_gate_pre, w_gate, preferred_element_type=jnp.float32)
    grad_rows = grad_rows + jnp.einsum(
        "tjf,jdf->td", grad_up_pre, w_up, preferred_element_type=jnp.float32
    )
    grad_down = jnp.einsum("tjf,td->jfd", scaled, top_all, preferred_element_type=jnp.float32)
    grad_gate = jnp.einsum("td,tjf->jdf", xn_all, grad_gate_pre, preferred_element_type=jnp.float32)
    grad_up = jnp.einsum("td,tjf->jdf", xn_all, grad_up_pre, preferred_element_type=jnp.float32)

    moe_out = scatter_all(moe_part.astype(jnp.bfloat16))
    output = gather_dp((hidden_state + moe_out).astype(jnp.bfloat16))[None]

    gate_columns = jnp.zeros((gate_part.shape[0], experts), jnp.float32)
    gate_columns = lax.dynamic_update_slice_in_dim(gate_columns, gate_part, first_expert, 1)
    grad_router_probs = jnp.where(named, scatter_all(gate_columns), 0.0)
    grad_xn_exp = scatter_all(grad_rows.astype(jnp.bfloat16))
    grad_logits = router * (
        grad_router_probs - jnp.sum(router * grad_router_probs, axis=-1, keepdims=True)
    )
    grad_second_normed_input = grad_xn_exp + jnp.einsum(
        "se,de->sd", grad_logits, w_router, precision=lax.Precision.HIGHEST
    )
    grad_router = jnp.einsum(
        "sd,se->de", second_normed_input, grad_logits, precision=lax.Precision.HIGHEST
    )
    grad_expert_norm_gain = jnp.sum(grad_second_normed_input * second_unit_input, axis=0)
    grad_second_unit_input = grad_second_normed_input * expert_norm_gain
    grad_hidden = top_own.astype(jnp.float32) + second_inverse_norm * (
        grad_second_unit_input
        - second_unit_input
        * jnp.mean(grad_second_unit_input * second_unit_input, axis=-1, keepdims=True)
    )
    grad_attn = gather_dp(grad_hidden.astype(jnp.bfloat16))[None]
    grad_out = jnp.einsum("psk,psd->kd", attended, grad_attn, preferred_element_type=jnp.float32)
    grad_heads = (
        jnp.einsum("psd,kd->psk", grad_attn, w_out, preferred_element_type=jnp.float32)
        .astype(jnp.bfloat16)
        .reshape(head_shape)
    )
    scores = score_block(queries)
    weights = jnp.exp(scores - log_total)
    grad_weights = jnp.einsum(
        "pshd,plhd->phsl", grad_heads, values_heads, preferred_element_type=jnp.float32
    )
    row_delta = jnp.sum(weights * grad_weights, axis=-1, keepdims=True)
    grad_scores = (weights * (grad_weights - row_delta)).astype(jnp.bfloat16)
    grad_queries = (
        jnp.einsum("phsl,plhd->pshd", grad_scores, keys_heads, preferred_element_type=jnp.float32)
        * scale_factor
    )
    key_part = (
        jnp.einsum("phsl,pshd->plhd", grad_scores, queries, preferred_element_type=jnp.float32)
        * scale_factor
    )
    value_part = jnp.einsum(
        "phsl,pshd->plhd",
        weights.astype(jnp.bfloat16),
        grad_heads,
        preferred_element_type=jnp.float32,
    )
    grad_keys, grad_values = (
        lax.psum_scatter(
            key_part.reshape(pack_count, pack_span, local_width).astype(jnp.bfloat16),
            "expert",
            scatter_dimension=1,
            tiled=True,
        ).astype(jnp.float32),
        lax.psum_scatter(
            value_part.reshape(pack_count, pack_span, local_width).astype(jnp.bfloat16),
            "expert",
            scatter_dimension=1,
            tiled=True,
        ).astype(jnp.float32),
    )
    grad_q_normed = rotate(grad_queries, cos_table, -sin_table).reshape(
        pack_count, seg_rows, local_width
    )
    grad_k_normed = rotate(grad_keys.reshape(head_shape), cos_table, -sin_table).reshape(
        pack_count, seg_rows, local_width
    )
    grad_q_gain = jnp.sum(grad_q_normed * q_hat, axis=(0, 1))
    grad_k_gain = jnp.sum(grad_k_normed * k_hat, axis=(0, 1))
    grad_q_hat = grad_q_normed * q_gain
    grad_k_hat = grad_k_normed * k_gain
    q_dot, k_dot = head_totals(
        jnp.sum(grad_q_hat * q_hat, axis=-1), jnp.sum(grad_k_hat * k_hat, axis=-1)
    )
    grad_q_raw = (q_inv * (grad_q_hat - q_hat * q_dot[..., None] / model_width)).astype(
        jnp.bfloat16
    )
    grad_k_raw = (k_inv * (grad_k_hat - k_hat * k_dot[..., None] / model_width)).astype(
        jnp.bfloat16
    )
    grad_v_raw = grad_values.astype(jnp.bfloat16)
    grad_query = jnp.einsum(
        "psd,psk->dk", first_normed_input, grad_q_raw, preferred_element_type=jnp.float32
    )
    grad_key = jnp.einsum(
        "psd,psk->dk", first_normed_input, grad_k_raw, preferred_element_type=jnp.float32
    )
    grad_value = jnp.einsum(
        "psd,psk->dk", first_normed_input, grad_v_raw, preferred_element_type=jnp.float32
    )
    grad_first_normed_input = jnp.einsum(
        "psk,dk->psd", grad_q_raw, w_query, preferred_element_type=jnp.float32
    )
    grad_first_normed_input = grad_first_normed_input + jnp.einsum(
        "psk,dk->psd", grad_k_raw, w_key, preferred_element_type=jnp.float32
    )
    grad_first_normed_input = grad_first_normed_input + jnp.einsum(
        "psk,dk->psd", grad_v_raw, w_value, preferred_element_type=jnp.float32
    )
    gain_portion = jnp.sum(grad_first_normed_input * first_unit_input, axis=(0, 1))
    grad_first_unit_input = grad_first_normed_input * attention_norm_gain
    input_part = first_inverse_norm * (
        grad_first_unit_input
        - first_unit_input
        * jnp.mean(grad_first_unit_input * first_unit_input, axis=-1, keepdims=True)
    )
    input_total = scatter_dp(input_part[0].astype(jnp.bfloat16))
    grad_input = gather_dp((grad_hidden + input_total).astype(jnp.bfloat16))
    grad_input = grad_input.astype(jnp.float32)[None]
    reduced_dense = (
        lax.psum_scatter(
            grad_query.astype(jnp.bfloat16), "expert", scatter_dimension=0, tiled=True
        ).astype(jnp.float32),
        lax.psum_scatter(
            grad_key.astype(jnp.bfloat16), "expert", scatter_dimension=0, tiled=True
        ).astype(jnp.float32),
        lax.psum_scatter(
            grad_value.astype(jnp.bfloat16), "expert", scatter_dimension=0, tiled=True
        ).astype(jnp.float32),
        lax.psum_scatter(
            grad_out.astype(jnp.bfloat16), "expert", scatter_dimension=0, tiled=True
        ).astype(jnp.float32),
        lax.psum_scatter(
            grad_q_gain.astype(jnp.bfloat16), "expert", scatter_dimension=0, tiled=True
        ).astype(jnp.float32),
        lax.psum_scatter(
            grad_k_gain.astype(jnp.bfloat16), "expert", scatter_dimension=0, tiled=True
        ).astype(jnp.float32),
        scatter_sum(gain_portion),
        scatter_sum(grad_expert_norm_gain),
        scatter_sum(grad_router),
    )
    return (
        output,
        grad_input,
        reduced_dense[6],
        reduced_dense[0],
        reduced_dense[1],
        reduced_dense[2],
        reduced_dense[3],
        reduced_dense[4],
        reduced_dense[5],
        reduced_dense[7],
        reduced_dense[8],
        grad_gate,
        grad_up,
        grad_down,
    )


def solution(mesh):
    placed = (
        P(None, "expert", None),
        P(),
        P(None, "dp"),
        P(None, "dp"),
        P(None, "dp"),
        P("dp", None),
        P("dp"),
        P("dp"),
        P(),
        P(),
        P("expert", None, "dp"),
        P("expert", None, "dp"),
        P("expert", "dp", None),
        P("expert", None, None),
        P(),
        P(None, "expert", None),
    )
    return jax.shard_map(
        per_device,
        mesh=mesh,
        in_specs=placed,
        out_specs=(
            P(None, "expert", None),
            P(None, "expert", None),
            P("expert"),
            P("expert", "dp"),
            P("expert", "dp"),
            P("expert", "dp"),
            P(("dp", "expert"), None),
            P(("dp", "expert")),
            P(("dp", "expert")),
            P("expert"),
            P("expert", None),
            P("expert", None, "dp"),
            P("expert", None, "dp"),
            P("expert", "dp", None),
        ),
        check_vma=False,
    )
```

```python
import functools

import jax
import jax.numpy as jnp
from jax import lax
from jax.experimental import pallas as pl
from jax.experimental.pallas import tpu as pltpu
from jax.sharding import PartitionSpec as P

HD = 128


epsilon = 1e-05
rope_base = 10000.0
masked_score = -1e30


def doc_layout(lengths, pack_span):
    doc_ends = jnp.cumsum(lengths, axis=1)
    starts = doc_ends - lengths
    places = jnp.arange(pack_span, dtype=jnp.int32)
    segment = jnp.sum((places[None, :, None] >= doc_ends[:, None, :]).astype(jnp.int32), axis=2)
    member = segment[:, :, None] == jnp.arange(lengths.shape[1], dtype=jnp.int32)[None, None, :]
    begins = jnp.sum(jnp.where(member, starts[:, None, :], 0), axis=2)
    return (segment, places[None, :] - begins)


def rope_tables(positions, head_size):
    half_size = head_size // 2
    frequency = rope_base ** (-2.0 * jnp.arange(half_size, dtype=jnp.float32) / head_size)
    angles = positions.astype(jnp.float32)[..., None] * frequency
    return (jnp.cos(angles), jnp.sin(angles))


def rotate(heads_in, cos_table, sin_table):
    half_size = heads_in.shape[-1] // 2
    first_half = heads_in[..., :half_size]
    second_half = heads_in[..., half_size:]
    cos_head = cos_table[..., None, :]
    sin_head = sin_table[..., None, :]
    return jnp.concatenate(
        [
            first_half * cos_head - second_half * sin_head,
            second_half * cos_head + first_half * sin_head,
        ],
        axis=-1,
    )


ALL = ("dp", "expert")


DEVICES = pl.DeviceIdType.MESH


def greet(device):
    pl.semaphore_signal(
        pltpu.get_barrier_semaphore(), inc=1, device_id=device, device_id_type=DEVICES
    )


def send(source, target, send_sem, arrive_sem, device):
    return pltpu.make_async_remote_copy(
        src_ref=source,
        dst_ref=target,
        send_sem=send_sem,
        recv_sem=arrive_sem,
        device_id=device,
        device_id_type=DEVICES,
    )


def corners(dp):
    return dp + 1 - 2 * (dp % 2), (dp + 2) % 4


def gather_all_kernel(line, x_ref, g_ref, out_ref, table_ref, sent, arrived, own_sem):
    dp, place = lax.axis_index("dp"), lax.axis_index("expert")
    z, c = place // 2, place % 2
    side_x, side_y = corners(dp)
    far = 3 - dp
    devices = (
        (dp, place + 2),
        (dp, place - 2),
        (side_x, place),
        (side_y, place),
        (dp, 2 * z + 1 - c),
    )
    up, down, along_x, along_y, pair = range(5)
    has_up, has_down = z < line - 1, z > 0
    for way in (along_x, along_y, pair):
        greet(devices[way])
    pl.when(has_up)(lambda: greet(devices[up]))
    pl.when(has_down)(lambda: greet(devices[down]))
    greeted = 3 + has_up.astype(jnp.int32) + has_down.astype(jnp.int32)
    pl.semaphore_wait(pltpu.get_barrier_semaphore(), greeted)

    pieces = (0, 1, 2)

    def slot(corner, height, core):
        return corner * (2 * line) + 2 * height + core

    def part(s, p):
        return table_ref.at[s] if p == 2 else out_ref.at[s, p]

    def copy(s, p, way, source=None):
        target = part(s, p)
        return send(
            target if source is None else source,
            target,
            sent.at[s, p, way],
            arrived.at[s, p],
            devices[way],
        )

    def arrive(s, p):
        copy(s, p, pair).wait_recv()

    mine = slot(dp, z, c)
    for p in pieces:
        source = g_ref if p == 2 else x_ref.at[p]
        pltpu.make_async_copy(source, part(mine, p), own_sem.at[p]).start()
        pl.when(has_up)(lambda: copy(mine, p, up, source).start())
        pl.when(has_down)(lambda: copy(mine, p, down, source).start())
        for way in (along_x, along_y, pair):
            copy(mine, p, way, source).start()

    def spread(s, p):
        for way in (along_x, along_y, pair):
            copy(s, p, way).start()

    def column(away):
        def below():
            s = slot(dp, z - away, c)
            for p in pieces:
                arrive(s, p)
                pl.when(has_up)(lambda: copy(s, p, up).start())
                spread(s, p)

        def above():
            s = slot(dp, z + away, c)
            for p in pieces:
                arrive(s, p)
                pl.when(has_down)(lambda: copy(s, p, down).start())
                spread(s, p)

        pl.when((away > 0) & (away < line) & (z - away >= 0))(below)
        pl.when((away > 0) & (away < line) & (z + away < line))(above)

    def sides(height):
        for p in pieces:
            s = slot(side_x, height, c)
            arrive(s, p)
            if p != 1:
                copy(s, p, along_y).start()
            copy(s, p, pair).start()
            s = slot(side_y, height, c)
            arrive(s, p)
            if p == 1:
                copy(s, p, along_x).start()
            copy(s, p, pair).start()

    def opposite(height):
        for p in pieces:
            s = slot(far, height, c)
            arrive(s, p)
            copy(s, p, pair).start()

    def both(away, visit):
        pl.when((away >= 0) & (away < line) & (z - away >= 0))(lambda: visit(z - away))
        pl.when((away > 0) & (away < line) & (z + away < line))(lambda: visit(z + away))

    def step(k, carry):
        column(k)
        both(k - 1, sides)
        both(k - 2, opposite)
        return carry

    lax.fori_loop(1, line + 2, step, 0)

    def finish(height, carry):
        for p in pieces:
            for corner in range(4):
                arrive(slot(corner, height, 1 - c), p)
                copy(slot(corner, height, c), p, pair).wait_send()
            s = slot(dp, height, c)
            copy(s, p, along_x).wait_send()
            copy(s, p, along_y).wait_send()
            if p == 1:
                copy(slot(side_y, height, c), p, along_x).wait_send()
            else:
                copy(slot(side_x, height, c), p, along_y).wait_send()
            pl.when(has_up & (height <= z))(lambda: copy(s, p, up).wait_send())
            pl.when(has_down & (height >= z))(lambda: copy(s, p, down).wait_send())
        return carry

    lax.fori_loop(0, line, finish, 0)
    for p in pieces:
        source = g_ref if p == 2 else x_ref.at[p]
        pltpu.make_async_copy(source, part(mine, p), own_sem.at[p]).wait()


def gather_all(rows, table, line):
    count, width = rows.shape
    slots = 8 * line
    gathered, tables = pl.pallas_call(
        functools.partial(gather_all_kernel, line),
        out_shape=(
            jax.ShapeDtypeStruct((slots, 2, count // 2, width), rows.dtype),
            jax.ShapeDtypeStruct((slots, *table.shape), table.dtype),
        ),
        in_specs=[pl.BlockSpec(memory_space=pltpu.VMEM)] * 2,
        out_specs=[pl.BlockSpec(memory_space=pl.ANY)] * 2,
        scratch_shapes=[
            pltpu.SemaphoreType.DMA((slots, 3, 5)),
            pltpu.SemaphoreType.DMA((slots, 3)),
            pltpu.SemaphoreType.DMA((3,)),
        ],
        compiler_params=pltpu.CompilerParams(collective_id=1, has_side_effects=True),
        name="gather_all",
    )(rows.reshape(2, count // 2, width), table)
    return gathered.reshape(slots * count, width), tables


def gather_square_kernel(x_ref, out_ref, sent, arrived, own_sem):
    dp, place = lax.axis_index("dp"), lax.axis_index("expert")
    side_x, side_y = corners(dp)
    devices = ((side_x, place), (side_y, place))
    for device in devices:
        greet(device)
    pl.semaphore_wait(pltpu.get_barrier_semaphore(), 2)

    def copy(corner, p, way, source=None):
        target = out_ref.at[corner, p]
        return send(
            target if source is None else source,
            target,
            sent.at[corner, p, way],
            arrived.at[corner, p],
            devices[way],
        )

    for p in (0, 1):
        pltpu.make_async_copy(x_ref.at[p], out_ref.at[dp, p], own_sem.at[p]).start()
        for way in (0, 1):
            copy(dp, p, way, x_ref.at[p]).start()
    copy(side_x, 0, 0).wait_recv()
    copy(side_x, 0, 1).start()
    copy(side_y, 0, 0).wait_recv()
    copy(side_x, 1, 0).wait_recv()
    copy(side_y, 1, 0).wait_recv()
    copy(side_y, 1, 0).start()
    for p in (0, 1):
        copy(3 - dp, p, 0).wait_recv()
        for way in (0, 1):
            copy(dp, p, way).wait_send()
        pltpu.make_async_copy(x_ref.at[p], out_ref.at[dp, p], own_sem.at[p]).wait()
    copy(side_x, 0, 1).wait_send()
    copy(side_y, 1, 0).wait_send()


def gather_dp(rows):
    count, width = rows.shape
    gathered = pl.pallas_call(
        gather_square_kernel,
        out_shape=jax.ShapeDtypeStruct((4, 2, count // 2, width), rows.dtype),
        in_specs=[pl.BlockSpec(memory_space=pltpu.VMEM)],
        out_specs=pl.BlockSpec(memory_space=pl.ANY),
        scratch_shapes=[
            pltpu.SemaphoreType.DMA((4, 2, 2)),
            pltpu.SemaphoreType.DMA((4, 2)),
            pltpu.SemaphoreType.DMA((2,)),
        ],
        compiler_params=pltpu.CompilerParams(collective_id=2, has_side_effects=True),
        name="gather_dp",
    )(rows.reshape(2, count // 2, width))
    return gathered.reshape(4 * count, width)


def farthest(line, z, k):
    total = jnp.int32(0)
    for at in range(line):
        order = sorted(range(line), key=lambda place: (-abs(place - at), place))
        place = sum([jnp.where(k == i, order[i], 0) for i in range(line)])
        total = total + jnp.where(z == at, place, 0)
    return total


def reduce_kernel(
    square,
    line,
    paired,
    x_ref,
    out_ref,
    acc,
    got_pair,
    got_x,
    got_y,
    got_far_x,
    got_far_y,
    got_below,
    got_above,
    load_sem,
    pair_sem,
    x_sem,
    y_sem,
    far_x_sem,
    far_y_sem,
    below_sem,
    above_sem,
):
    dp, place = lax.axis_index("dp"), lax.axis_index("expert")
    z, c = place // 2, place % 2
    side_x, side_y = corners(dp)
    core = c if paired else 0
    own = dp if square else 0
    quarters = (3 - dp, side_x, side_y, dp) if square else (0,)
    to_x, to_y = (side_x, place), (side_y, place)
    to_pair, to_up, to_down = (dp, 2 * z + 1 - c), (dp, place + 2), (dp, place - 2)
    greeted = 0
    if square:
        greet(to_x)
        greet(to_y)
        greeted += 2
    if paired:
        greet(to_pair)
        greeted += 1
    if line > 1:
        pl.when(z > 0)(lambda: greet(to_down))
        pl.when(z < line - 1)(lambda: greet(to_up))
        greeted = greeted + (z > 0).astype(jnp.int32) + (z < line - 1).astype(jnp.int32)
    pl.semaphore_wait(pltpu.get_barrier_semaphore(), greeted)

    def load(q, height, p):
        return pltpu.make_async_copy(
            x_ref.at[q, height, core, p], acc.at[q, height, p], load_sem.at[q, height, p]
        )

    def hand(q, height, p):
        at = (q, height, p)
        source = x_ref.at[q, height, 1 - core, p]
        return send(source, got_pair.at[at], pair_sem.at[0, *at], pair_sem.at[1, *at], to_pair)

    def along_x(height, p):
        at = (height, p)
        return send(
            acc.at[side_x, height, p], got_x.at[at], x_sem.at[0, *at], x_sem.at[1, *at], to_x
        )

    def along_y(height, p):
        at = (height, p)
        return send(
            acc.at[side_y, height, p], got_y.at[at], y_sem.at[0, *at], y_sem.at[1, *at], to_y
        )

    def far_x(height):
        return send(
            acc.at[3 - dp, height, 0],
            got_far_x.at[height],
            far_x_sem.at[0, height],
            far_x_sem.at[1, height],
            to_x,
        )

    def far_y(height):
        return send(
            acc.at[3 - dp, height, 1],
            got_far_y.at[height],
            far_y_sem.at[0, height],
            far_y_sem.at[1, height],
            to_y,
        )

    def climb(height, p):
        at = (height, p)
        return send(
            acc.at[own, height, p], got_below.at[at], below_sem.at[0, *at], below_sem.at[1, *at], to_up
        )

    def descend(height, p):
        at = (height, p)
        return send(
            acc.at[own, height, p],
            got_above.at[at],
            above_sem.at[0, *at],
            above_sem.at[1, *at],
            to_down,
        )

    def height_of(k):
        return farthest(line, z, k) if line > 1 else 0

    def start(k, carry):
        for q in quarters:
            for p in (0, 1):
                load(q, height_of(k), p).start()
                if paired:
                    hand(q, height_of(k), p).start()
        return carry

    lax.fori_loop(0, line, start, 0)

    def step(k, carry):
        def cores():
            height = height_of(k)
            for q in quarters:
                for p in (0, 1):
                    load(q, height, p).wait()
                    if paired:
                        hand(q, height, p).wait_recv()
                        acc[q, height, p] = acc[q, height, p] + got_pair[q, height, p]
                if square and q is quarters[0]:
                    far_x(height).start()
                    far_y(height).start()

        def sides():
            height = height_of(k - 1)
            along_x(height, 0).start()
            along_y(height, 1).start()
            far_x(height).wait_recv()
            acc[side_y, height, 0] = acc[side_y, height, 0] + got_far_x[height]
            along_y(height, 0).start()
            far_y(height).wait_recv()
            acc[side_x, height, 1] = acc[side_x, height, 1] + got_far_y[height]
            along_x(height, 1).start()

        def column():
            height = height_of(k - 2)
            for p in (0, 1):
                if square:
                    along_x(height, p).wait_recv()
                    along_y(height, p).wait_recv()
                    total = acc[own, height, p].astype(jnp.float32)
                    total = total + got_x[height, p].astype(jnp.float32)
                    total = total + got_y[height, p].astype(jnp.float32)
                    acc[own, height, p] = total.astype(acc.dtype)
                if line > 1:
                    pl.when((z == 0) & (height > z))(lambda: climb(height, p).start())
                    pl.when((z == line - 1) & (height < z))(lambda: descend(height, p).start())

        def pass_on():
            height = height_of(k - 3)
            for p in (0, 1):

                def upwards():
                    climb(height, p).wait_recv()
                    acc[own, height, p] = acc[own, height, p] + got_below[height, p]
                    climb(height, p).start()

                def downwards():
                    descend(height, p).wait_recv()
                    acc[own, height, p] = acc[own, height, p] + got_above[height, p]
                    descend(height, p).start()

                pl.when((height > z) & (z > 0))(upwards)
                pl.when((height < z) & (z < line - 1))(downwards)

        pl.when(k < line)(cores)
        if square:
            pl.when((k >= 1) & (k < line + 1))(sides)
        pl.when((k >= 2) & (k < line + 2))(column)
        if line > 1:
            pl.when(k >= 3)(pass_on)
        return carry

    lax.fori_loop(0, line + (3 if line > 1 else 2), step, 0)
    home = z if line > 1 else 0
    for p in (0, 1):
        out_ref[p] = acc[own, home, p].astype(jnp.float32)
        if line > 1:

            def from_below():
                climb(z, p).wait_recv()
                out_ref[p] = out_ref[p] + got_below[z, p].astype(jnp.float32)

            def from_above():
                descend(z, p).wait_recv()
                out_ref[p] = out_ref[p] + got_above[z, p].astype(jnp.float32)

            pl.when(z > 0)(from_below)
            pl.when(z < line - 1)(from_above)

    def finish(height, carry):
        if square:
            far_x(height).wait_send()
            far_y(height).wait_send()
        for p in (0, 1):
            if paired:
                for q in quarters:
                    hand(q, height, p).wait_send()
            if square:
                along_x(height, p).wait_send()
                along_y(height, p).wait_send()
            if line > 1:
                pl.when(height > z)(lambda: climb(height, p).wait_send())
                pl.when(height < z)(lambda: descend(height, p).wait_send())
        return carry

    lax.fori_loop(0, line, finish, 0)


def reduce_to(parts, square, line, paired, name, number):
    _, rows, width = parts.shape
    quarters, cores, half = (4 if square else 1), (2 if paired else 1), rows // 2

    def space(used, *shape):
        return pltpu.VMEM((*shape, half, width) if used else (*shape, 16, 128), parts.dtype)

    sems = pltpu.SemaphoreType.DMA
    total = pl.pallas_call(
        functools.partial(reduce_kernel, square, line, paired),
        out_shape=jax.ShapeDtypeStruct((2, half, width), jnp.float32),
        in_specs=[pl.BlockSpec(memory_space=pl.ANY)],
        out_specs=pl.BlockSpec(memory_space=pltpu.VMEM),
        scratch_shapes=[
            space(True, quarters, line, 2),
            space(paired, quarters, line, 2),
            space(square, line, 2),
            space(square, line, 2),
            space(square, line),
            space(square, line),
            space(line > 1, line, 2),
            space(line > 1, line, 2),
            sems((quarters, line, 2)),
            sems((2, quarters, line, 2)),
            sems((2, line, 2)),
            sems((2, line, 2)),
            sems((2, line)),
            sems((2, line)),
            sems((2, line, 2)),
            sems((2, line, 2)),
        ],
        compiler_params=pltpu.CompilerParams(
            collective_id=number, has_side_effects=True, vmem_limit_bytes=60 << 20
        ),
        name=name,
    )(parts.reshape(quarters, line, cores, 2, half, width))
    return total.reshape(rows, width)


def scatter_dp(rows):
    return reduce_to(rows.reshape(4, -1, rows.shape[1]), True, 1, False, "scatter_dp", 3)


def scatter_all(rows, line):
    parts = rows.reshape(8 * line, -1, rows.shape[1])
    return reduce_to(parts, True, line, True, "scatter_all", 4)


def scatter_expert(parts, line):
    return reduce_to(parts, False, line, True, "scatter_expert", 5)


def head_totals(first_sum, second_sum):
    return lax.psum((first_sum, second_sum), "dp")


def per_device(
    inputs,
    attention_norm_gain,
    w_query,
    w_key,
    w_value,
    w_out,
    q_gain,
    k_gain,
    expert_norm_gain,
    w_router,
    w_gate,
    w_up,
    w_down,
    routes,
    lengths,
    d_output,
):
    pack_count, seg_rows, model_width = inputs.shape
    local_width = w_query.shape[1]
    local_heads = local_width // HD
    experts = w_router.shape[1]
    groups = lax.axis_size("expert")
    line = groups // 2
    pack_span = seg_rows * groups
    local_experts = w_gate.shape[0]
    scale_factor = HD ** (-0.5)
    offset_rows = lax.axis_index("expert") * seg_rows
    segment, positions = doc_layout(lengths, pack_span)
    seg_query = lax.dynamic_slice_in_dim(segment, offset_rows, seg_rows, 1)
    pos_query = lax.dynamic_slice_in_dim(positions, offset_rows, seg_rows, 1)
    cos_table, sin_table = rope_tables(pos_query, HD)
    key_places = jnp.arange(pack_span, dtype=jnp.int32)
    query_places = offset_rows + jnp.arange(seg_rows, dtype=jnp.int32)
    allowed = (seg_query[:, :, None] == segment[:, None, :]) & (
        key_places[None, None, :] <= query_places[None, :, None]
    )
    head_shape = (pack_count, seg_rows, local_heads, HD)
    inputs_single_float = inputs.astype(jnp.float32)
    first_inverse_norm = lax.rsqrt(
        jnp.mean(inputs_single_float * inputs_single_float, axis=-1, keepdims=True) + epsilon
    )
    first_unit_input = inputs_single_float * first_inverse_norm
    first_normed_input = (first_unit_input * attention_norm_gain).astype(jnp.bfloat16)
    q_raw = jnp.dot(first_normed_input, w_query, preferred_element_type=jnp.float32)
    k_raw = jnp.dot(first_normed_input, w_key, preferred_element_type=jnp.float32)
    value_rows = jnp.dot(first_normed_input, w_value, preferred_element_type=jnp.float32).astype(
        jnp.bfloat16
    )
    q_sum, k_sum = head_totals(jnp.sum(q_raw * q_raw, axis=-1), jnp.sum(k_raw * k_raw, axis=-1))
    q_inv = lax.rsqrt(q_sum[..., None] / model_width + epsilon)
    k_inv = lax.rsqrt(k_sum[..., None] / model_width + epsilon)
    q_hat = q_raw * q_inv
    k_hat = k_raw * k_inv
    queries = rotate((q_hat * q_gain).reshape(head_shape), cos_table, sin_table).astype(
        jnp.bfloat16
    )
    key_rows = (
        rotate((k_hat * k_gain).reshape(head_shape), cos_table, sin_table)
        .astype(jnp.bfloat16)
        .reshape(pack_count, seg_rows, local_width)
    )
    keys_all, values_all = (
        lax.all_gather(key_rows, "expert", axis=1, tiled=True),
        lax.all_gather(value_rows, "expert", axis=1, tiled=True),
    )
    keys_heads = keys_all.reshape(pack_count, pack_span, local_heads, HD)
    values_heads = values_all.reshape(pack_count, pack_span, local_heads, HD)

    def score_block(query_block):
        scores = (
            jnp.einsum(
                "pshd,plhd->phsl", query_block, keys_heads, preferred_element_type=jnp.float32
            )
            * scale_factor
        )
        return jnp.where(allowed[:, None], scores, masked_score)

    scores = score_block(queries)
    largest = jnp.max(scores, axis=-1, keepdims=True)
    log_total = largest + jnp.log(jnp.sum(jnp.exp(scores - largest), axis=-1, keepdims=True))
    weights = jnp.exp(scores - log_total)
    attended = jnp.einsum(
        "phsl,plhd->pshd",
        weights.astype(jnp.bfloat16),
        values_heads,
        preferred_element_type=jnp.float32,
    )
    attended = attended.astype(jnp.bfloat16).reshape(pack_count, seg_rows, local_width)
    attn_part = jnp.dot(
        attended.reshape(seg_rows, local_width), w_out, preferred_element_type=jnp.float32
    )
    own = lax.axis_index("dp")
    part_rows = seg_rows // lax.axis_size("dp")

    def own_rows(rows):
        return lax.dynamic_slice_in_dim(rows, own * part_rows, part_rows, 0)

    hidden_state = own_rows(inputs_single_float[0]) + scatter_dp(attn_part.astype(jnp.bfloat16))
    second_inverse_norm = lax.rsqrt(
        jnp.mean(hidden_state * hidden_state, axis=-1, keepdims=True) + epsilon
    )
    second_unit_input = hidden_state * second_inverse_norm
    second_normed_input = second_unit_input * expert_norm_gain
    router = jax.nn.softmax(
        jnp.dot(second_normed_input, w_router, precision=lax.Precision.HIGHEST), axis=-1
    )
    chosen = own_rows(routes[:, 0, :])
    expert_range = jnp.arange(experts, dtype=jnp.int32)
    named = jnp.any(chosen[:, :, None] == expert_range, axis=1)
    first_expert = lax.axis_index("expert") * local_experts
    top_own = own_rows(d_output[0])
    top_all = lax.all_gather(top_own, ALL, axis=0, tiled=True)
    xn_all, gate_table = gather_all(
        second_normed_input.astype(jnp.bfloat16), jnp.where(named, router, 0.0).T, line
    )
    gates = lax.dynamic_slice_in_dim(gate_table, first_expert, local_experts, 1)
    gates = jnp.transpose(gates, (0, 2, 1)).reshape(-1, local_experts)

    gate_pre = jnp.einsum("td,jdf->tjf", xn_all, w_gate, preferred_element_type=jnp.float32)
    up_pre = jnp.einsum("td,jdf->tjf", xn_all, w_up, preferred_element_type=jnp.float32)
    top_down = jnp.einsum("td,jfd->tjf", top_all, w_down, preferred_element_type=jnp.float32)
    sigmoid_gate = jax.nn.sigmoid(gate_pre)
    silu_gate = gate_pre * sigmoid_gate
    activated = silu_gate * up_pre
    scaled = (activated * gates[:, :, None]).astype(jnp.bfloat16)
    gate_part = jnp.sum(activated * top_down, axis=-1)
    grad_act = top_down * gates[:, :, None]
    grad_gate_pre = (
        grad_act * up_pre * sigmoid_gate * (1.0 + gate_pre * (1.0 - sigmoid_gate))
    ).astype(jnp.bfloat16)
    grad_up_pre = (grad_act * silu_gate).astype(jnp.bfloat16)
    moe_part = jnp.einsum("tjf,jfd->td", scaled, w_down, preferred_element_type=jnp.float32)
    grad_rows = jnp.einsum("tjf,jdf->td", grad_gate_pre, w_gate, preferred_element_type=jnp.float32)
    grad_rows = grad_rows + jnp.einsum(
        "tjf,jdf->td", grad_up_pre, w_up, preferred_element_type=jnp.float32
    )
    grad_down = jnp.einsum("tjf,td->jfd", scaled, top_all, preferred_element_type=jnp.float32)
    grad_gate = jnp.einsum("td,tjf->jdf", xn_all, grad_gate_pre, preferred_element_type=jnp.float32)
    grad_up = jnp.einsum("td,tjf->jdf", xn_all, grad_up_pre, preferred_element_type=jnp.float32)

    moe_out = lax.psum_scatter(
        moe_part.astype(jnp.bfloat16), ALL, scatter_dimension=0, tiled=True
    ).astype(jnp.float32)
    output = gather_dp((hidden_state + moe_out).astype(jnp.bfloat16))[None]

    gate_columns = jnp.zeros((gate_part.shape[0], experts), jnp.float32)
    gate_columns = lax.dynamic_update_slice_in_dim(gate_columns, gate_part, first_expert, 1)
    gate_sums = lax.psum_scatter(gate_columns, ALL, scatter_dimension=0, tiled=True)
    grad_router_probs = jnp.where(named, gate_sums, 0.0)
    grad_xn_exp = scatter_all(grad_rows.astype(jnp.bfloat16), line)
    grad_logits = router * (
        grad_router_probs - jnp.sum(router * grad_router_probs, axis=-1, keepdims=True)
    )
    grad_second_normed_input = grad_xn_exp + jnp.einsum(
        "se,de->sd", grad_logits, w_router, precision=lax.Precision.HIGHEST
    )
    grad_router = jnp.einsum(
        "sd,se->de", second_normed_input, grad_logits, precision=lax.Precision.HIGHEST
    )
    grad_expert_norm_gain = jnp.sum(grad_second_normed_input * second_unit_input, axis=0)
    grad_second_unit_input = grad_second_normed_input * expert_norm_gain
    grad_hidden = top_own.astype(jnp.float32) + second_inverse_norm * (
        grad_second_unit_input
        - second_unit_input
        * jnp.mean(grad_second_unit_input * second_unit_input, axis=-1, keepdims=True)
    )
    grad_attn = gather_dp(grad_hidden.astype(jnp.bfloat16))[None]
    grad_out = jnp.einsum("psk,psd->kd", attended, grad_attn, preferred_element_type=jnp.float32)
    grad_heads = (
        jnp.einsum("psd,kd->psk", grad_attn, w_out, preferred_element_type=jnp.float32)
        .astype(jnp.bfloat16)
        .reshape(head_shape)
    )
    scores = score_block(queries)
    weights = jnp.exp(scores - log_total)
    grad_weights = jnp.einsum(
        "pshd,plhd->phsl", grad_heads, values_heads, preferred_element_type=jnp.float32
    )
    row_delta = jnp.sum(weights * grad_weights, axis=-1, keepdims=True)
    grad_scores = (weights * (grad_weights - row_delta)).astype(jnp.bfloat16)
    grad_queries = (
        jnp.einsum("phsl,plhd->pshd", grad_scores, keys_heads, preferred_element_type=jnp.float32)
        * scale_factor
    )
    key_part = (
        jnp.einsum("phsl,pshd->plhd", grad_scores, queries, preferred_element_type=jnp.float32)
        * scale_factor
    )
    value_part = jnp.einsum(
        "phsl,pshd->plhd",
        weights.astype(jnp.bfloat16),
        grad_heads,
        preferred_element_type=jnp.float32,
    )
    grad_keys, grad_values = (
        lax.psum_scatter(
            key_part.reshape(pack_count, pack_span, local_width).astype(jnp.bfloat16),
            "expert",
            scatter_dimension=1,
            tiled=True,
        ).astype(jnp.float32),
        lax.psum_scatter(
            value_part.reshape(pack_count, pack_span, local_width).astype(jnp.bfloat16),
            "expert",
            scatter_dimension=1,
            tiled=True,
        ).astype(jnp.float32),
    )
    grad_q_normed = rotate(grad_queries, cos_table, -sin_table).reshape(
        pack_count, seg_rows, local_width
    )
    grad_k_normed = rotate(grad_keys.reshape(head_shape), cos_table, -sin_table).reshape(
        pack_count, seg_rows, local_width
    )
    grad_q_gain = jnp.sum(grad_q_normed * q_hat, axis=(0, 1))
    grad_k_gain = jnp.sum(grad_k_normed * k_hat, axis=(0, 1))
    grad_q_hat = grad_q_normed * q_gain
    grad_k_hat = grad_k_normed * k_gain
    q_dot, k_dot = head_totals(
        jnp.sum(grad_q_hat * q_hat, axis=-1), jnp.sum(grad_k_hat * k_hat, axis=-1)
    )
    grad_q_raw = (q_inv * (grad_q_hat - q_hat * q_dot[..., None] / model_width)).astype(
        jnp.bfloat16
    )
    grad_k_raw = (k_inv * (grad_k_hat - k_hat * k_dot[..., None] / model_width)).astype(
        jnp.bfloat16
    )
    grad_v_raw = grad_values.astype(jnp.bfloat16)
    grad_heads_raw = jnp.concatenate([grad_q_raw[0], grad_k_raw[0], grad_v_raw[0]], axis=1)
    grad_projections = jnp.einsum(
        "sd,sk->dk", first_normed_input[0], grad_heads_raw, preferred_element_type=jnp.float32
    )
    grad_first_normed_input = jnp.einsum(
        "psk,dk->psd", grad_q_raw, w_query, preferred_element_type=jnp.float32
    )
    grad_first_normed_input = grad_first_normed_input + jnp.einsum(
        "psk,dk->psd", grad_k_raw, w_key, preferred_element_type=jnp.float32
    )
    grad_first_normed_input = grad_first_normed_input + jnp.einsum(
        "psk,dk->psd", grad_v_raw, w_value, preferred_element_type=jnp.float32
    )
    grad_first = scatter_dp(grad_first_normed_input[0].astype(jnp.bfloat16))
    unit_own = own_rows(first_unit_input[0])
    grad_attn_gain = jnp.sum(grad_first * unit_own, axis=0)
    grad_first = grad_first * attention_norm_gain
    grad_input = grad_hidden + own_rows(first_inverse_norm[0]) * (
        grad_first - unit_own * jnp.mean(grad_first * unit_own, axis=-1, keepdims=True)
    )
    grad_input = gather_dp(grad_input.astype(jnp.bfloat16)).astype(jnp.float32)[None]

    wide = grad_projections.shape[1]
    small = jnp.concatenate(
        [
            grad_q_gain.reshape(groups, -1),
            grad_k_gain.reshape(groups, -1),
            grad_attn_gain.reshape(groups, -1),
            grad_expert_norm_gain.reshape(groups, -1),
            grad_router.reshape(groups, -1),
        ],
        axis=1,
    )
    small_rows = 32
    filled = small.shape[1]
    small = jnp.pad(small, ((0, 0), (0, small_rows * wide - filled)))
    parts = jnp.concatenate(
        [
            grad_projections.astype(jnp.bfloat16).reshape(groups, -1, wide),
            small.astype(jnp.bfloat16).reshape(groups, small_rows, wide),
        ],
        axis=1,
    )
    summed = scatter_expert(parts, line)
    large_rows = summed.shape[0] - small_rows
    small = summed[large_rows:].reshape(-1)
    gain_size, norm_size = local_width // groups, model_width // groups
    own_gains = small[: 2 * gain_size]
    shared = lax.psum(small[2 * gain_size : filled].astype(jnp.bfloat16), "dp")
    shared = shared.astype(jnp.float32)
    grad_out = lax.psum_scatter(
        grad_out.astype(jnp.bfloat16), "expert", scatter_dimension=0, tiled=True
    ).astype(jnp.float32)
    return (
        output,
        grad_input,
        shared[:norm_size],
        summed[:large_rows, :local_width],
        summed[:large_rows, local_width : 2 * local_width],
        summed[:large_rows, 2 * local_width :],
        grad_out,
        own_gains[:gain_size],
        own_gains[gain_size:],
        shared[norm_size : 2 * norm_size],
        shared[2 * norm_size :].reshape(norm_size, experts),
        grad_gate,
        grad_up,
        grad_down,
    )


def solution(mesh):
    placed = (
        P(None, "expert", None),
        P(),
        P(None, "dp"),
        P(None, "dp"),
        P(None, "dp"),
        P("dp", None),
        P("dp"),
        P("dp"),
        P(),
        P(),
        P("expert", None, "dp"),
        P("expert", None, "dp"),
        P("expert", "dp", None),
        P("expert", None, None),
        P(),
        P(None, "expert", None),
    )
    return jax.shard_map(
        per_device,
        mesh=mesh,
        in_specs=placed,
        out_specs=(
            P(None, "expert", None),
            P(None, "expert", None),
            P("expert"),
            P("expert", "dp"),
            P("expert", "dp"),
            P("expert", "dp"),
            P(("dp", "expert"), None),
            P(("dp", "expert")),
            P(("dp", "expert")),
            P("expert"),
            P("expert", None),
            P("expert", None, "dp"),
            P("expert", None, "dp"),
            P("expert", "dp", None),
        ),
        check_vma=False,
    )
```

```python
import functools

import jax
import jax.numpy as jnp
from jax import lax
from jax.experimental import pallas as pl
from jax.experimental.pallas import tpu as pltpu
from jax.sharding import PartitionSpec as P

HD = 128


epsilon = 1e-05
rope_base = 10000.0
masked_score = -1e30


def doc_layout(lengths, pack_span):
    doc_ends = jnp.cumsum(lengths, axis=1)
    starts = doc_ends - lengths
    places = jnp.arange(pack_span, dtype=jnp.int32)
    segment = jnp.sum((places[None, :, None] >= doc_ends[:, None, :]).astype(jnp.int32), axis=2)
    member = segment[:, :, None] == jnp.arange(lengths.shape[1], dtype=jnp.int32)[None, None, :]
    begins = jnp.sum(jnp.where(member, starts[:, None, :], 0), axis=2)
    return (segment, places[None, :] - begins)


def rope_tables(positions, head_size):
    half_size = head_size // 2
    frequency = rope_base ** (-2.0 * jnp.arange(half_size, dtype=jnp.float32) / head_size)
    angles = positions.astype(jnp.float32)[..., None] * frequency
    return (jnp.cos(angles), jnp.sin(angles))


def rotate(heads_in, cos_table, sin_table):
    half_size = heads_in.shape[-1] // 2
    first_half = heads_in[..., :half_size]
    second_half = heads_in[..., half_size:]
    cos_head = cos_table[..., None, :]
    sin_head = sin_table[..., None, :]
    return jnp.concatenate(
        [
            first_half * cos_head - second_half * sin_head,
            second_half * cos_head + first_half * sin_head,
        ],
        axis=-1,
    )


ALL = ("dp", "expert")


DEVICES = pl.DeviceIdType.MESH


def greet(device):
    pl.semaphore_signal(
        pltpu.get_barrier_semaphore(), inc=1, device_id=device, device_id_type=DEVICES
    )


def send(source, target, send_sem, arrive_sem, device):
    return pltpu.make_async_remote_copy(
        src_ref=source,
        dst_ref=target,
        send_sem=send_sem,
        recv_sem=arrive_sem,
        device_id=device,
        device_id_type=DEVICES,
    )


def corners(dp):
    return dp + 1 - 2 * (dp % 2), (dp + 2) % 4


def gather_all_kernel(line, x_ref, g_ref, out_ref, table_ref, sent, arrived, own_sem):
    dp, place = lax.axis_index("dp"), lax.axis_index("expert")
    z, c = place // 2, place % 2
    side_x, side_y = corners(dp)
    far = 3 - dp
    devices = (
        (dp, place + 2),
        (dp, place - 2),
        (side_x, place),
        (side_y, place),
        (dp, 2 * z + 1 - c),
    )
    up, down, along_x, along_y, pair = range(5)
    has_up, has_down = z < line - 1, z > 0
    for way in (along_x, along_y, pair):
        greet(devices[way])
    pl.when(has_up)(lambda: greet(devices[up]))
    pl.when(has_down)(lambda: greet(devices[down]))
    greeted = 3 + has_up.astype(jnp.int32) + has_down.astype(jnp.int32)
    pl.semaphore_wait(pltpu.get_barrier_semaphore(), greeted)

    pieces = (0, 1, 2)

    def slot(corner, height, core):
        return corner * (2 * line) + 2 * height + core

    def part(s, p):
        return table_ref.at[s] if p == 2 else out_ref.at[s, p]

    def copy(s, p, way, source=None):
        target = part(s, p)
        return send(
            target if source is None else source,
            target,
            sent.at[s, p, way],
            arrived.at[s, p],
            devices[way],
        )

    def arrive(s, p):
        copy(s, p, pair).wait_recv()

    mine = slot(dp, z, c)
    for p in pieces:
        source = g_ref if p == 2 else x_ref.at[p]
        pltpu.make_async_copy(source, part(mine, p), own_sem.at[p]).start()
        pl.when(has_up)(lambda: copy(mine, p, up, source).start())
        pl.when(has_down)(lambda: copy(mine, p, down, source).start())
        for way in (along_x, along_y, pair):
            copy(mine, p, way, source).start()

    def spread(s, p):
        for way in (along_x, along_y, pair):
            copy(s, p, way).start()

    def column(away):
        def below():
            s = slot(dp, z - away, c)
            for p in pieces:
                arrive(s, p)
                pl.when(has_up)(lambda: copy(s, p, up).start())
                spread(s, p)

        def above():
            s = slot(dp, z + away, c)
            for p in pieces:
                arrive(s, p)
                pl.when(has_down)(lambda: copy(s, p, down).start())
                spread(s, p)

        pl.when((away > 0) & (away < line) & (z - away >= 0))(below)
        pl.when((away > 0) & (away < line) & (z + away < line))(above)

    def sides(height):
        for p in pieces:
            s = slot(side_x, height, c)
            arrive(s, p)
            if p != 1:
                copy(s, p, along_y).start()
            copy(s, p, pair).start()
            s = slot(side_y, height, c)
            arrive(s, p)
            if p == 1:
                copy(s, p, along_x).start()
            copy(s, p, pair).start()

    def opposite(height):
        for p in pieces:
            s = slot(far, height, c)
            arrive(s, p)
            copy(s, p, pair).start()

    def both(away, visit):
        pl.when((away >= 0) & (away < line) & (z - away >= 0))(lambda: visit(z - away))
        pl.when((away > 0) & (away < line) & (z + away < line))(lambda: visit(z + away))

    def step(k, carry):
        column(k)
        both(k - 1, sides)
        both(k - 2, opposite)
        return carry

    lax.fori_loop(1, line + 2, step, 0)

    def finish(height, carry):
        for p in pieces:
            for corner in range(4):
                arrive(slot(corner, height, 1 - c), p)
                copy(slot(corner, height, c), p, pair).wait_send()
            s = slot(dp, height, c)
            copy(s, p, along_x).wait_send()
            copy(s, p, along_y).wait_send()
            if p == 1:
                copy(slot(side_y, height, c), p, along_x).wait_send()
            else:
                copy(slot(side_x, height, c), p, along_y).wait_send()
            pl.when(has_up & (height <= z))(lambda: copy(s, p, up).wait_send())
            pl.when(has_down & (height >= z))(lambda: copy(s, p, down).wait_send())
        return carry

    lax.fori_loop(0, line, finish, 0)
    for p in pieces:
        source = g_ref if p == 2 else x_ref.at[p]
        pltpu.make_async_copy(source, part(mine, p), own_sem.at[p]).wait()


def gather_all(rows, table, line):
    count, width = rows.shape
    slots = 8 * line
    gathered, tables = pl.pallas_call(
        functools.partial(gather_all_kernel, line),
        out_shape=(
            jax.ShapeDtypeStruct((slots, 2, count // 2, width), rows.dtype),
            jax.ShapeDtypeStruct((slots, *table.shape), table.dtype),
        ),
        in_specs=[pl.BlockSpec(memory_space=pltpu.VMEM)] * 2,
        out_specs=[pl.BlockSpec(memory_space=pl.ANY)] * 2,
        scratch_shapes=[
            pltpu.SemaphoreType.DMA((slots, 3, 5)),
            pltpu.SemaphoreType.DMA((slots, 3)),
            pltpu.SemaphoreType.DMA((3,)),
        ],
        compiler_params=pltpu.CompilerParams(collective_id=1, has_side_effects=True),
        name="gather_all",
    )(rows.reshape(2, count // 2, width), table)
    return gathered.reshape(slots * count, width), tables


def gather_square_kernel(x_ref, out_ref, sent, arrived, own_sem):
    dp, place = lax.axis_index("dp"), lax.axis_index("expert")
    side_x, side_y = corners(dp)
    devices = ((side_x, place), (side_y, place))
    for device in devices:
        greet(device)
    pl.semaphore_wait(pltpu.get_barrier_semaphore(), 2)

    def copy(corner, p, way, source=None):
        target = out_ref.at[corner, p]
        return send(
            target if source is None else source,
            target,
            sent.at[corner, p, way],
            arrived.at[corner, p],
            devices[way],
        )

    for p in (0, 1):
        pltpu.make_async_copy(x_ref.at[p], out_ref.at[dp, p], own_sem.at[p]).start()
        for way in (0, 1):
            copy(dp, p, way, x_ref.at[p]).start()
    copy(side_x, 0, 0).wait_recv()
    copy(side_x, 0, 1).start()
    copy(side_y, 0, 0).wait_recv()
    copy(side_x, 1, 0).wait_recv()
    copy(side_y, 1, 0).wait_recv()
    copy(side_y, 1, 0).start()
    for p in (0, 1):
        copy(3 - dp, p, 0).wait_recv()
        for way in (0, 1):
            copy(dp, p, way).wait_send()
        pltpu.make_async_copy(x_ref.at[p], out_ref.at[dp, p], own_sem.at[p]).wait()
    copy(side_x, 0, 1).wait_send()
    copy(side_y, 1, 0).wait_send()


def gather_dp(rows):
    count, width = rows.shape
    gathered = pl.pallas_call(
        gather_square_kernel,
        out_shape=jax.ShapeDtypeStruct((4, 2, count // 2, width), rows.dtype),
        in_specs=[pl.BlockSpec(memory_space=pltpu.VMEM)],
        out_specs=pl.BlockSpec(memory_space=pl.ANY),
        scratch_shapes=[
            pltpu.SemaphoreType.DMA((4, 2, 2)),
            pltpu.SemaphoreType.DMA((4, 2)),
            pltpu.SemaphoreType.DMA((2,)),
        ],
        compiler_params=pltpu.CompilerParams(collective_id=2, has_side_effects=True),
        name="gather_dp",
    )(rows.reshape(2, count // 2, width))
    return gathered.reshape(4 * count, width)


def farthest(line, z, k):
    total = jnp.int32(0)
    for at in range(line):
        order = sorted(range(line), key=lambda place: (-abs(place - at), place))
        place = sum([jnp.where(k == i, order[i], 0) for i in range(line)])
        total = total + jnp.where(z == at, place, 0)
    return total


def reduce_kernel(
    square,
    line,
    paired,
    x_ref,
    out_ref,
    acc,
    got_pair,
    got_x,
    got_y,
    got_far_x,
    got_far_y,
    got_below,
    got_above,
    load_sem,
    pair_sem,
    x_sem,
    y_sem,
    far_x_sem,
    far_y_sem,
    below_sem,
    above_sem,
):
    dp, place = lax.axis_index("dp"), lax.axis_index("expert")
    z, c = place // 2, place % 2
    side_x, side_y = corners(dp)
    core = c if paired else 0
    own = dp if square else 0
    quarters = (3 - dp, side_x, side_y, dp) if square else (0,)
    to_x, to_y = (side_x, place), (side_y, place)
    to_pair, to_up, to_down = (dp, 2 * z + 1 - c), (dp, place + 2), (dp, place - 2)
    greeted = 0
    if square:
        greet(to_x)
        greet(to_y)
        greeted += 2
    if paired:
        greet(to_pair)
        greeted += 1
    if line > 1:
        pl.when(z > 0)(lambda: greet(to_down))
        pl.when(z < line - 1)(lambda: greet(to_up))
        greeted = greeted + (z > 0).astype(jnp.int32) + (z < line - 1).astype(jnp.int32)
    pl.semaphore_wait(pltpu.get_barrier_semaphore(), greeted)

    def load(q, height, p):
        return pltpu.make_async_copy(
            x_ref.at[q, height, core, p], acc.at[q, height, p], load_sem.at[q, height, p]
        )

    def hand(q, height, p):
        at = (q, height, p)
        source = x_ref.at[q, height, 1 - core, p]
        return send(source, got_pair.at[at], pair_sem.at[0, *at], pair_sem.at[1, *at], to_pair)

    def along_x(height, p):
        at = (height, p)
        return send(
            acc.at[side_x, height, p], got_x.at[at], x_sem.at[0, *at], x_sem.at[1, *at], to_x
        )

    def along_y(height, p):
        at = (height, p)
        return send(
            acc.at[side_y, height, p], got_y.at[at], y_sem.at[0, *at], y_sem.at[1, *at], to_y
        )

    def far_x(height):
        return send(
            acc.at[3 - dp, height, 0],
            got_far_x.at[height],
            far_x_sem.at[0, height],
            far_x_sem.at[1, height],
            to_x,
        )

    def far_y(height):
        return send(
            acc.at[3 - dp, height, 1],
            got_far_y.at[height],
            far_y_sem.at[0, height],
            far_y_sem.at[1, height],
            to_y,
        )

    def climb(height, p):
        at = (height, p)
        return send(
            acc.at[own, height, p], got_below.at[at], below_sem.at[0, *at], below_sem.at[1, *at], to_up
        )

    def descend(height, p):
        at = (height, p)
        return send(
            acc.at[own, height, p],
            got_above.at[at],
            above_sem.at[0, *at],
            above_sem.at[1, *at],
            to_down,
        )

    def height_of(k):
        return farthest(line, z, k) if line > 1 else 0

    def start(k, carry):
        for q in quarters:
            for p in (0, 1):
                load(q, height_of(k), p).start()
                if paired:
                    hand(q, height_of(k), p).start()
        return carry

    lax.fori_loop(0, line, start, 0)

    def step(k, carry):
        def cores():
            height = height_of(k)
            for q in quarters:
                for p in (0, 1):
                    load(q, height, p).wait()
                    if paired:
                        hand(q, height, p).wait_recv()
                        acc[q, height, p] = acc[q, height, p] + got_pair[q, height, p]
                if square and q is quarters[0]:
                    far_x(height).start()
                    far_y(height).start()

        def sides():
            height = height_of(k - 1)
            along_x(height, 0).start()
            along_y(height, 1).start()
            far_x(height).wait_recv()
            acc[side_y, height, 0] = acc[side_y, height, 0] + got_far_x[height]
            along_y(height, 0).start()
            far_y(height).wait_recv()
            acc[side_x, height, 1] = acc[side_x, height, 1] + got_far_y[height]
            along_x(height, 1).start()

        def column():
            height = height_of(k - 2)
            for p in (0, 1):
                if square:
                    along_x(height, p).wait_recv()
                    along_y(height, p).wait_recv()
                    total = acc[own, height, p].astype(jnp.float32)
                    total = total + got_x[height, p].astype(jnp.float32)
                    total = total + got_y[height, p].astype(jnp.float32)
                    acc[own, height, p] = total.astype(acc.dtype)
                if line > 1:
                    pl.when((z == 0) & (height > z))(lambda: climb(height, p).start())
                    pl.when((z == line - 1) & (height < z))(lambda: descend(height, p).start())

        def pass_on():
            height = height_of(k - 3)
            for p in (0, 1):

                def upwards():
                    climb(height, p).wait_recv()
                    acc[own, height, p] = acc[own, height, p] + got_below[height, p]
                    climb(height, p).start()

                def downwards():
                    descend(height, p).wait_recv()
                    acc[own, height, p] = acc[own, height, p] + got_above[height, p]
                    descend(height, p).start()

                pl.when((height > z) & (z > 0))(upwards)
                pl.when((height < z) & (z < line - 1))(downwards)

        pl.when(k < line)(cores)
        if square:
            pl.when((k >= 1) & (k < line + 1))(sides)
        pl.when((k >= 2) & (k < line + 2))(column)
        if line > 1:
            pl.when(k >= 3)(pass_on)
        return carry

    lax.fori_loop(0, line + (3 if line > 1 else 2), step, 0)
    home = z if line > 1 else 0
    for p in (0, 1):
        out_ref[p] = acc[own, home, p].astype(jnp.float32)
        if line > 1:

            def from_below():
                climb(z, p).wait_recv()
                out_ref[p] = out_ref[p] + got_below[z, p].astype(jnp.float32)

            def from_above():
                descend(z, p).wait_recv()
                out_ref[p] = out_ref[p] + got_above[z, p].astype(jnp.float32)

            pl.when(z > 0)(from_below)
            pl.when(z < line - 1)(from_above)

    def finish(height, carry):
        if square:
            far_x(height).wait_send()
            far_y(height).wait_send()
        for p in (0, 1):
            if paired:
                for q in quarters:
                    hand(q, height, p).wait_send()
            if square:
                along_x(height, p).wait_send()
                along_y(height, p).wait_send()
            if line > 1:
                pl.when(height > z)(lambda: climb(height, p).wait_send())
                pl.when(height < z)(lambda: descend(height, p).wait_send())
        return carry

    lax.fori_loop(0, line, finish, 0)


def reduce_to(parts, square, line, paired, name, number):
    _, rows, width = parts.shape
    quarters, cores, half = (4 if square else 1), (2 if paired else 1), rows // 2

    def space(used, *shape):
        return pltpu.VMEM((*shape, half, width) if used else (*shape, 16, 128), parts.dtype)

    sems = pltpu.SemaphoreType.DMA
    total = pl.pallas_call(
        functools.partial(reduce_kernel, square, line, paired),
        out_shape=jax.ShapeDtypeStruct((2, half, width), jnp.float32),
        in_specs=[pl.BlockSpec(memory_space=pl.ANY)],
        out_specs=pl.BlockSpec(memory_space=pltpu.VMEM),
        scratch_shapes=[
            space(True, quarters, line, 2),
            space(paired, quarters, line, 2),
            space(square, line, 2),
            space(square, line, 2),
            space(square, line),
            space(square, line),
            space(line > 1, line, 2),
            space(line > 1, line, 2),
            sems((quarters, line, 2)),
            sems((2, quarters, line, 2)),
            sems((2, line, 2)),
            sems((2, line, 2)),
            sems((2, line)),
            sems((2, line)),
            sems((2, line, 2)),
            sems((2, line, 2)),
        ],
        compiler_params=pltpu.CompilerParams(
            collective_id=number, has_side_effects=True, vmem_limit_bytes=60 << 20
        ),
        name=name,
    )(parts.reshape(quarters, line, cores, 2, half, width))
    return total.reshape(rows, width)


def scatter_dp(rows):
    return reduce_to(rows.reshape(4, -1, rows.shape[1]), True, 1, False, "scatter_dp", 3)


def scatter_all(rows, line):
    parts = rows.reshape(8 * line, -1, rows.shape[1])
    return reduce_to(parts, True, line, True, "scatter_all", 4)


def scatter_expert(parts, line):
    return reduce_to(parts, False, line, True, "scatter_expert", 5)


def visit_others(line, z, visit):
    def turn(k, carry):
        visit((z + k) % line)
        return carry

    lax.fori_loop(1, line, turn, 0)


def greet_line(line, dp, z, c):
    visit_others(line, z, lambda other: greet((dp, 2 * other + c)))
    greet((dp, 2 * z + 1 - c))
    pl.semaphore_wait(pltpu.get_barrier_semaphore(), line)


def columns(z):
    return pl.ds(pl.multiple_of(z * HD, HD), HD)


def to_heads_kernel(line, shared, *refs):
    count = len(shared)
    ins, outs = refs[:count], refs[count : 2 * count]
    sent, arrived, pair_sent, pair_arrived, own_sem = refs[2 * count :]
    dp, place = lax.axis_index("dp"), lax.axis_index("expert")
    z, c = place // 2, place % 2
    pair = (dp, 2 * z + 1 - c)
    greet_line(line, dp, z, c)

    def block(i, origin):
        return outs[i].at[origin, c] if shared[i] else outs[i].at[origin]

    def out(i, other):
        source = ins[i].at[:, columns(other)]
        device = (dp, 2 * other + c)
        return send(source, block(i, z), sent.at[i, other], arrived.at[i, z], device)

    def into(i, origin):
        part = block(i, origin)
        return send(part, part, sent.at[i, origin], arrived.at[i, origin], pair)

    def share(i, origin, source=None):
        part = block(i, origin)
        return send(
            part if source is None else source,
            part,
            pair_sent.at[i, origin],
            pair_arrived.at[i, origin],
            pair,
        )

    def own(i):
        return pltpu.make_async_copy(ins[i].at[:, columns(z)], block(i, z), own_sem.at[i])

    def dispatch(other):
        for i in range(count):
            out(i, other).start()

    visit_others(line, z, dispatch)
    for i in range(count):
        own(i).start()
        if shared[i]:
            share(i, z, ins[i].at[:, columns(z)]).start()

    def receive(origin):
        for i in range(count):
            into(i, origin).wait_recv()
            if shared[i]:
                share(i, origin).start()

    visit_others(line, z, receive)

    def finish(other):
        for i in range(count):
            out(i, other).wait_send()

    visit_others(line, z, finish)
    for i in range(count):
        own(i).wait()
        if shared[i]:

            def settle(origin, carry):
                share(i, origin).wait()
                return carry

            lax.fori_loop(0, line, settle, 0)


def to_heads(arrays, shared, line, name, number):
    rows = arrays[0].shape[0]
    count = len(arrays)
    sems = pltpu.SemaphoreType.DMA
    return pl.pallas_call(
        functools.partial(to_heads_kernel, line, shared),
        out_shape=[
            jax.ShapeDtypeStruct((line, 2, rows, HD) if both else (line, rows, HD), array.dtype)
            for array, both in zip(arrays, shared)
        ],
        in_specs=[pl.BlockSpec(memory_space=pltpu.VMEM)] * count,
        out_specs=[pl.BlockSpec(memory_space=pl.ANY)] * count,
        scratch_shapes=[sems((count, line))] * 4 + [sems((count,))],
        compiler_params=pltpu.CompilerParams(collective_id=number, has_side_effects=True),
        name=name,
    )(*arrays)


def to_tokens_kernel(line, summed, *refs):
    count, sums = len(summed), sum(summed)
    ins, outs = refs[:count], refs[count : 2 * count]
    mine, theirs = refs[2 * count : 2 * count + 2]
    sent, arrived, pair_sem, load_sem, own_sem = refs[2 * count + 2 :]
    dp, place = lax.axis_index("dp"), lax.axis_index("expert")
    z, c = place // 2, place % 2
    pair = (dp, 2 * z + 1 - c)
    greet_line(line, dp, z, c)
    at_sum = [sum(summed[:i]) for i in range(count)]

    def load(i, other):
        return pltpu.make_async_copy(
            ins[i].at[other, c], mine.at[at_sum[i], other], load_sem.at[at_sum[i], other]
        )

    def hand(i, other):
        s = at_sum[i]
        return send(
            ins[i].at[other, 1 - c],
            theirs.at[s, other],
            pair_sem.at[0, s, other],
            pair_sem.at[1, s, other],
            pair,
        )

    def source(i, other):
        return mine.at[at_sum[i], other] if summed[i] else ins[i].at[other]

    def out(i, other):
        target = outs[i].at[:, columns(z)]
        device = (dp, 2 * other + c)
        return send(source(i, other), target, sent.at[i, other], arrived.at[i, z], device)

    def into(i, origin):
        part = outs[i].at[:, columns(origin)]
        return send(part, part, sent.at[i, origin], arrived.at[i, origin], pair)

    def own(i):
        return pltpu.make_async_copy(source(i, z), outs[i].at[:, columns(z)], own_sem.at[i])

    def prepare(other):
        for i in range(count):
            if summed[i]:
                load(i, other).start()
                hand(i, other).start()

    def add(i, other):
        if summed[i]:
            load(i, other).wait()
            hand(i, other).wait_recv()
            s = at_sum[i]
            mine[s, other] = mine[s, other] + theirs[s, other]

    def dispatch(other):
        for i in range(count):
            add(i, other)
            out(i, other).start()

    if sums:
        visit_others(line, z, prepare)
        prepare(z)
    visit_others(line, z, dispatch)
    for i in range(count):
        add(i, z)
        own(i).start()

    def finish(other):
        for i in range(count):
            into(i, other).wait_recv()
            out(i, other).wait_send()
            if summed[i]:
                hand(i, other).wait_send()

    visit_others(line, z, finish)
    for i in range(count):
        own(i).wait()
        if summed[i]:
            hand(i, z).wait_send()


def to_tokens(arrays, summed, line, name, number):
    rows = arrays[0].shape[-2]
    count, sums = len(arrays), max(sum(summed), 1)
    sems = pltpu.SemaphoreType.DMA
    dtype = arrays[0].dtype
    held = (sums, line, rows, HD) if sum(summed) else (1, 1, 16, HD)
    return pl.pallas_call(
        functools.partial(to_tokens_kernel, line, summed),
        out_shape=[jax.ShapeDtypeStruct((rows, line * HD), dtype)] * count,
        in_specs=[pl.BlockSpec(memory_space=pl.ANY)] * count,
        out_specs=[pl.BlockSpec(memory_space=pl.ANY)] * count,
        scratch_shapes=[pltpu.VMEM(held, dtype)] * 2
        + [
            sems((count, line)),
            sems((count, line)),
            sems((2, sums, line)),
            sems((sums, line)),
            sems((count,)),
        ],
        compiler_params=pltpu.CompilerParams(collective_id=number, has_side_effects=True),
        name=name,
    )(*arrays)


KEY_TILE = 512


def contract(a, b, a_dim, b_dim):
    return lax.dot_general(
        a, b, (((a_dim,), (b_dim,)), ((), ())), preferred_element_type=jnp.float32
    )


def masked_scores(keys, queries, tile, first, starts):
    scores = contract(keys, queries, 1, 1) * HD ** (-0.5)
    key_at = tile * KEY_TILE + lax.broadcasted_iota(jnp.int32, scores.shape, 0)
    query_at = first + lax.broadcasted_iota(jnp.int32, (1, scores.shape[1]), 1)
    return jnp.where((key_at >= starts) & (key_at <= query_at), scores, masked_score)


def attend_kernel(bounds, q_ref, k_ref, v_ref, start_ref, o_ref, total_ref):
    i = pl.program_id(0)
    queries, starts = q_ref[0], start_ref[0]
    span = queries.shape[0]

    def tile_step(tile, carry):
        largest, total, acc = carry
        rows = pl.ds(pl.multiple_of(tile * KEY_TILE, KEY_TILE), KEY_TILE)
        scores = masked_scores(k_ref[rows, :], queries, tile, bounds[2, i], starts)
        new = jnp.maximum(largest, jnp.max(scores, axis=0, keepdims=True))
        weights = jnp.exp(scores - new)
        fade = jnp.exp(largest - new)
        total = fade * total + jnp.sum(weights, axis=0, keepdims=True)
        acc = fade * acc + contract(v_ref[rows, :], weights.astype(jnp.bfloat16), 0, 0)
        return new, total, acc

    largest, total, acc = lax.fori_loop(
        bounds[0, i],
        bounds[1, i],
        tile_step,
        (
            jnp.full((1, span), masked_score, jnp.float32),
            jnp.zeros((1, span), jnp.float32),
            jnp.zeros((HD, span), jnp.float32),
        ),
    )
    o_ref[0] = (acc / total).T.astype(o_ref.dtype)
    total_ref[0] = largest + jnp.log(total)


def attend_back_kernel(
    bounds, q_ref, k_ref, v_ref, start_ref, total_ref, delta_ref, d_ref, dq_ref, dk_ref, dv_ref, dk, dv
):
    i = pl.program_id(0)
    queries, starts, grad = q_ref[0], start_ref[0], d_ref[0]
    total, delta = total_ref[0], delta_ref[0]

    @pl.when(i == 0)
    def _():
        dk[...] = jnp.zeros_like(dk)
        dv[...] = jnp.zeros_like(dv)

    def tile_step(tile, acc):
        rows = pl.ds(pl.multiple_of(tile * KEY_TILE, KEY_TILE), KEY_TILE)
        keys = k_ref[rows, :]
        scores = masked_scores(keys, queries, tile, bounds[2, i], starts)
        weights = jnp.exp(scores - total)
        grad_weights = contract(v_ref[rows, :], grad, 1, 1)
        grad_scores = (weights * (grad_weights - delta)).astype(jnp.bfloat16)
        dv[rows, :] += contract(weights.astype(jnp.bfloat16), grad, 1, 0)
        dk[rows, :] += contract(grad_scores, queries, 1, 0)
        return acc + contract(keys, grad_scores, 0, 0)

    acc = jnp.zeros((HD, queries.shape[0]), jnp.float32)
    acc = lax.fori_loop(bounds[0, i], bounds[1, i], tile_step, acc)
    dq_ref[0] = (acc * HD ** (-0.5)).T.astype(dq_ref.dtype)

    @pl.when(i == pl.num_programs(0) - 1)
    def _():
        dk_ref[...] = (dk[...] * HD ** (-0.5)).astype(dk_ref.dtype)
        dv_ref[...] = dv[...].astype(dv_ref.dtype)


def attend(bounds, queries, keys, values, starts):
    line, span, _ = queries.shape
    pack = keys.shape[0]
    block = pl.BlockSpec((1, span, HD), lambda i, _: (i, 0, 0))
    row = pl.BlockSpec((1, 1, span), lambda i, _: (i, 0, 0))
    whole = pl.BlockSpec((pack, HD), lambda i, _: (0, 0))
    return pl.pallas_call(
        attend_kernel,
        grid_spec=pltpu.PrefetchScalarGridSpec(
            num_scalar_prefetch=1,
            grid=(line,),
            in_specs=[block, whole, whole, row],
            out_specs=[block, row],
        ),
        out_shape=[
            jax.ShapeDtypeStruct(queries.shape, jnp.bfloat16),
            jax.ShapeDtypeStruct(starts.shape, jnp.float32),
        ],
        name="attend",
    )(bounds, queries, keys, values, starts)


def attend_back(bounds, queries, keys, values, starts, total, delta, grad):
    line, span, _ = queries.shape
    pack = keys.shape[0]
    block = pl.BlockSpec((1, span, HD), lambda i, _: (i, 0, 0))
    row = pl.BlockSpec((1, 1, span), lambda i, _: (i, 0, 0))
    whole = pl.BlockSpec((pack, HD), lambda i, _: (0, 0))
    return pl.pallas_call(
        attend_back_kernel,
        grid_spec=pltpu.PrefetchScalarGridSpec(
            num_scalar_prefetch=1,
            grid=(line,),
            in_specs=[block, whole, whole, row, row, row, block],
            out_specs=[block, whole, whole],
            scratch_shapes=[pltpu.VMEM((pack, HD), jnp.float32)] * 2,
        ),
        out_shape=[jax.ShapeDtypeStruct(queries.shape, jnp.bfloat16)]
        + [jax.ShapeDtypeStruct((pack, HD), jnp.bfloat16)] * 2,
        name="attend_back",
    )(bounds, queries, keys, values, starts, total, delta, grad)


def by_head(layout, line):
    positions = layout[1][0]
    pack = positions.shape[0]
    span = pack // (2 * line)
    core = lax.axis_index("expert") % 2
    starts = (jnp.arange(pack, dtype=jnp.int32) - positions).reshape(line, 2, 1, span)
    starts = lax.dynamic_index_in_dim(starts, core, 1, keepdims=False)
    first = (2 * jnp.arange(line, dtype=jnp.int32) + core) * span
    bounds = jnp.stack(
        [starts[:, 0, 0] // KEY_TILE, (first + span - 1) // KEY_TILE + 1, first]
    ).astype(jnp.int32)

    def forward(queries, keys, values):
        q, k, v = to_heads(
            [queries, keys, values], (False, True, True), line, "scatter_heads", 6
        )
        k, v = k.reshape(pack, HD), v.reshape(pack, HD)
        out, total = attend(bounds, q, k, v, starts)
        (attended,) = to_tokens([out], (False,), line, "gather_heads", 7)
        return attended, (q, k, v, out, total)

    def backward(kept, grad):
        q, k, v, out, total = kept
        (grad,) = to_heads([grad], (False,), line, "scatter_grads", 8)
        delta = jnp.sum(grad.astype(jnp.float32) * out.astype(jnp.float32), axis=-1)
        dq, dk, dv = attend_back(bounds, q, k, v, starts, total, delta[:, None, :], grad)
        shape = (line, 2, span, HD)
        return to_tokens(
            [dq, dk.reshape(shape), dv.reshape(shape)],
            (False, True, True),
            line,
            "gather_grads",
            9,
        )

    return forward, backward


def by_query(layout, offset_rows):
    segment = layout[0][0]
    pack = segment.shape[0]

    def heads(rows):
        return rows.reshape(rows.shape[0], -1, HD)

    def score_block(queries, keys):
        rows = queries.shape[0]
        scores = jnp.einsum("shd,lhd->hsl", queries, keys, preferred_element_type=jnp.float32)
        own = lax.dynamic_slice_in_dim(segment, offset_rows, rows, 0)
        query_places = offset_rows + jnp.arange(rows, dtype=jnp.int32)
        key_places = jnp.arange(pack, dtype=jnp.int32)
        allowed = (own[:, None] == segment[None, :]) & (
            key_places[None, :] <= query_places[:, None]
        )
        return jnp.where(allowed[None], scores * HD ** (-0.5), masked_score)

    def forward(queries, keys, values):
        q = heads(queries)
        k = heads(lax.all_gather(keys, "expert", axis=0, tiled=True))
        v = heads(lax.all_gather(values, "expert", axis=0, tiled=True))
        scores = score_block(q, k)
        largest = jnp.max(scores, axis=-1, keepdims=True)
        total = largest + jnp.log(jnp.sum(jnp.exp(scores - largest), axis=-1, keepdims=True))
        weights = jnp.exp(scores - total).astype(jnp.bfloat16)
        attended = jnp.einsum("hsl,lhd->shd", weights, v, preferred_element_type=jnp.float32)
        return attended.astype(jnp.bfloat16).reshape(queries.shape), (q, k, v, total)

    def backward(kept, grad):
        q, k, v, total = kept
        shape = grad.shape
        grad = heads(grad)
        weights = jnp.exp(score_block(q, k) - total)
        grad_weights = jnp.einsum("shd,lhd->hsl", grad, v, preferred_element_type=jnp.float32)
        delta = jnp.sum(weights * grad_weights, axis=-1, keepdims=True)
        grad_scores = (weights * (grad_weights - delta)).astype(jnp.bfloat16)
        dq = jnp.einsum("hsl,lhd->shd", grad_scores, k, preferred_element_type=jnp.float32)
        dk = jnp.einsum("hsl,shd->lhd", grad_scores, q, preferred_element_type=jnp.float32)
        weights = weights.astype(jnp.bfloat16)
        dv = jnp.einsum("hsl,shd->lhd", weights, grad, preferred_element_type=jnp.float32)

        def to_owner(part):
            part = part.astype(jnp.bfloat16).reshape(pack, shape[1])
            return lax.psum_scatter(part, "expert", scatter_dimension=0, tiled=True)

        scale = HD ** (-0.5)
        return (dq * scale).reshape(shape), to_owner(dk * scale), to_owner(dv)

    return forward, backward


def head_totals(first_sum, second_sum):
    return lax.psum((first_sum, second_sum), "dp")


def per_device(
    inputs,
    attention_norm_gain,
    w_query,
    w_key,
    w_value,
    w_out,
    q_gain,
    k_gain,
    expert_norm_gain,
    w_router,
    w_gate,
    w_up,
    w_down,
    routes,
    lengths,
    d_output,
):
    pack_count, seg_rows, model_width = inputs.shape
    local_width = w_query.shape[1]
    local_heads = local_width // HD
    experts = w_router.shape[1]
    groups = lax.axis_size("expert")
    line = groups // 2
    pack_span = seg_rows * groups
    local_experts = w_gate.shape[0]
    offset_rows = lax.axis_index("expert") * seg_rows
    segment, positions = doc_layout(lengths, pack_span)
    pos_query = lax.dynamic_slice_in_dim(positions, offset_rows, seg_rows, 1)
    cos_table, sin_table = rope_tables(pos_query, HD)
    head_shape = (pack_count, seg_rows, local_heads, HD)
    inputs_single_float = inputs.astype(jnp.float32)
    first_inverse_norm = lax.rsqrt(
        jnp.mean(inputs_single_float * inputs_single_float, axis=-1, keepdims=True) + epsilon
    )
    first_unit_input = inputs_single_float * first_inverse_norm
    first_normed_input = (first_unit_input * attention_norm_gain).astype(jnp.bfloat16)
    q_raw = jnp.dot(first_normed_input, w_query, preferred_element_type=jnp.float32)
    k_raw = jnp.dot(first_normed_input, w_key, preferred_element_type=jnp.float32)
    value_rows = jnp.dot(first_normed_input, w_value, preferred_element_type=jnp.float32).astype(
        jnp.bfloat16
    )
    q_sum, k_sum = head_totals(jnp.sum(q_raw * q_raw, axis=-1), jnp.sum(k_raw * k_raw, axis=-1))
    q_inv = lax.rsqrt(q_sum[..., None] / model_width + epsilon)
    k_inv = lax.rsqrt(k_sum[..., None] / model_width + epsilon)
    q_hat = q_raw * q_inv
    k_hat = k_raw * k_inv
    queries = rotate((q_hat * q_gain).reshape(head_shape), cos_table, sin_table).astype(
        jnp.bfloat16
    )
    key_rows = (
        rotate((k_hat * k_gain).reshape(head_shape), cos_table, sin_table)
        .astype(jnp.bfloat16)
        .reshape(pack_count, seg_rows, local_width)
    )
    layout = (segment, positions)
    if local_heads == line:
        attention = by_head(layout, line)
    else:
        attention = by_query(layout, offset_rows)
    attended, kept = attention[0](queries.reshape(seg_rows, local_width), key_rows[0], value_rows[0])
    attn_part = jnp.dot(
        attended, w_out, preferred_element_type=jnp.float32
    )
    own = lax.axis_index("dp")
    part_rows = seg_rows // lax.axis_size("dp")

    def own_rows(rows):
        return lax.dynamic_slice_in_dim(rows, own * part_rows, part_rows, 0)

    hidden_state = own_rows(inputs_single_float[0]) + scatter_dp(attn_part.astype(jnp.bfloat16))
    second_inverse_norm = lax.rsqrt(
        jnp.mean(hidden_state * hidden_state, axis=-1, keepdims=True) + epsilon
    )
    second_unit_input = hidden_state * second_inverse_norm
    second_normed_input = second_unit_input * expert_norm_gain
    router = jax.nn.softmax(
        jnp.dot(second_normed_input, w_router, precision=lax.Precision.HIGHEST), axis=-1
    )
    chosen = own_rows(routes[:, 0, :])
    expert_range = jnp.arange(experts, dtype=jnp.int32)
    named = jnp.any(chosen[:, :, None] == expert_range, axis=1)
    first_expert = lax.axis_index("expert") * local_experts
    top_own = own_rows(d_output[0])
    top_all = lax.all_gather(top_own, ALL, axis=0, tiled=True)
    xn_all, gate_table = gather_all(
        second_normed_input.astype(jnp.bfloat16), jnp.where(named, router, 0.0).T, line
    )
    gates = lax.dynamic_slice_in_dim(gate_table, first_expert, local_experts, 1)
    gates = jnp.transpose(gates, (0, 2, 1)).reshape(-1, local_experts)

    gate_pre = jnp.einsum("td,jdf->tjf", xn_all, w_gate, preferred_element_type=jnp.float32)
    up_pre = jnp.einsum("td,jdf->tjf", xn_all, w_up, preferred_element_type=jnp.float32)
    top_down = jnp.einsum("td,jfd->tjf", top_all, w_down, preferred_element_type=jnp.float32)
    sigmoid_gate = jax.nn.sigmoid(gate_pre)
    silu_gate = gate_pre * sigmoid_gate
    activated = silu_gate * up_pre
    scaled = (activated * gates[:, :, None]).astype(jnp.bfloat16)
    gate_part = jnp.sum(activated * top_down, axis=-1)
    grad_act = top_down * gates[:, :, None]
    grad_gate_pre = (
        grad_act * up_pre * sigmoid_gate * (1.0 + gate_pre * (1.0 - sigmoid_gate))
    ).astype(jnp.bfloat16)
    grad_up_pre = (grad_act * silu_gate).astype(jnp.bfloat16)
    moe_part = jnp.einsum("tjf,jfd->td", scaled, w_down, preferred_element_type=jnp.float32)
    grad_rows = jnp.einsum("tjf,jdf->td", grad_gate_pre, w_gate, preferred_element_type=jnp.float32)
    grad_rows = grad_rows + jnp.einsum(
        "tjf,jdf->td", grad_up_pre, w_up, preferred_element_type=jnp.float32
    )
    grad_down = jnp.einsum("tjf,td->jfd", scaled, top_all, preferred_element_type=jnp.float32)
    grad_gate = jnp.einsum("td,tjf->jdf", xn_all, grad_gate_pre, preferred_element_type=jnp.float32)
    grad_up = jnp.einsum("td,tjf->jdf", xn_all, grad_up_pre, preferred_element_type=jnp.float32)

    moe_out = lax.psum_scatter(
        moe_part.astype(jnp.bfloat16), ALL, scatter_dimension=0, tiled=True
    ).astype(jnp.float32)
    output = gather_dp((hidden_state + moe_out).astype(jnp.bfloat16))[None]

    gate_columns = jnp.zeros((gate_part.shape[0], experts), jnp.float32)
    gate_columns = lax.dynamic_update_slice_in_dim(gate_columns, gate_part, first_expert, 1)
    gate_sums = lax.psum_scatter(gate_columns, ALL, scatter_dimension=0, tiled=True)
    grad_router_probs = jnp.where(named, gate_sums, 0.0)
    grad_xn_exp = scatter_all(grad_rows.astype(jnp.bfloat16), line)
    grad_logits = router * (
        grad_router_probs - jnp.sum(router * grad_router_probs, axis=-1, keepdims=True)
    )
    grad_second_normed_input = grad_xn_exp + jnp.einsum(
        "se,de->sd", grad_logits, w_router, precision=lax.Precision.HIGHEST
    )
    grad_router = jnp.einsum(
        "sd,se->de", second_normed_input, grad_logits, precision=lax.Precision.HIGHEST
    )
    grad_expert_norm_gain = jnp.sum(grad_second_normed_input * second_unit_input, axis=0)
    grad_second_unit_input = grad_second_normed_input * expert_norm_gain
    grad_hidden = top_own.astype(jnp.float32) + second_inverse_norm * (
        grad_second_unit_input
        - second_unit_input
        * jnp.mean(grad_second_unit_input * second_unit_input, axis=-1, keepdims=True)
    )
    grad_attn = gather_dp(grad_hidden.astype(jnp.bfloat16))
    grad_out = jnp.einsum("sk,sd->kd", attended, grad_attn, preferred_element_type=jnp.float32)
    grad_heads = jnp.einsum(
        "sd,kd->sk", grad_attn, w_out, preferred_element_type=jnp.float32
    ).astype(jnp.bfloat16)
    grad_queries, grad_keys, grad_values = attention[1](kept, grad_heads)
    grad_queries = grad_queries.astype(jnp.float32).reshape(head_shape)
    grad_q_normed = rotate(grad_queries, cos_table, -sin_table).reshape(
        pack_count, seg_rows, local_width
    )
    grad_k_normed = rotate(
        grad_keys.astype(jnp.float32).reshape(head_shape), cos_table, -sin_table).reshape(
        pack_count, seg_rows, local_width
    )
    grad_q_gain = jnp.sum(grad_q_normed * q_hat, axis=(0, 1))
    grad_k_gain = jnp.sum(grad_k_normed * k_hat, axis=(0, 1))
    grad_q_hat = grad_q_normed * q_gain
    grad_k_hat = grad_k_normed * k_gain
    q_dot, k_dot = head_totals(
        jnp.sum(grad_q_hat * q_hat, axis=-1), jnp.sum(grad_k_hat * k_hat, axis=-1)
    )
    grad_q_raw = (q_inv * (grad_q_hat - q_hat * q_dot[..., None] / model_width)).astype(
        jnp.bfloat16
    )
    grad_k_raw = (k_inv * (grad_k_hat - k_hat * k_dot[..., None] / model_width)).astype(
        jnp.bfloat16
    )
    grad_v_raw = grad_values.astype(jnp.bfloat16)[None]
    grad_heads_raw = jnp.concatenate([grad_q_raw[0], grad_k_raw[0], grad_v_raw[0]], axis=1)
    grad_projections = jnp.einsum(
        "sd,sk->dk", first_normed_input[0], grad_heads_raw, preferred_element_type=jnp.float32
    )
    grad_first_normed_input = jnp.einsum(
        "psk,dk->psd", grad_q_raw, w_query, preferred_element_type=jnp.float32
    )
    grad_first_normed_input = grad_first_normed_input + jnp.einsum(
        "psk,dk->psd", grad_k_raw, w_key, preferred_element_type=jnp.float32
    )
    grad_first_normed_input = grad_first_normed_input + jnp.einsum(
        "psk,dk->psd", grad_v_raw, w_value, preferred_element_type=jnp.float32
    )
    grad_first = scatter_dp(grad_first_normed_input[0].astype(jnp.bfloat16))
    unit_own = own_rows(first_unit_input[0])
    grad_attn_gain = jnp.sum(grad_first * unit_own, axis=0)
    grad_first = grad_first * attention_norm_gain
    grad_input = grad_hidden + own_rows(first_inverse_norm[0]) * (
        grad_first - unit_own * jnp.mean(grad_first * unit_own, axis=-1, keepdims=True)
    )
    grad_input = gather_dp(grad_input.astype(jnp.bfloat16)).astype(jnp.float32)[None]

    wide = grad_projections.shape[1]
    small = jnp.concatenate(
        [
            grad_q_gain.reshape(groups, -1),
            grad_k_gain.reshape(groups, -1),
            grad_attn_gain.reshape(groups, -1),
            grad_expert_norm_gain.reshape(groups, -1),
            grad_router.reshape(groups, -1),
        ],
        axis=1,
    )
    small_rows = 32
    filled = small.shape[1]
    small = jnp.pad(small, ((0, 0), (0, small_rows * wide - filled)))
    parts = jnp.concatenate(
        [
            grad_projections.astype(jnp.bfloat16).reshape(groups, -1, wide),
            small.astype(jnp.bfloat16).reshape(groups, small_rows, wide),
        ],
        axis=1,
    )
    summed = scatter_expert(parts, line)
    large_rows = summed.shape[0] - small_rows
    small = summed[large_rows:].reshape(-1)
    gain_size, norm_size = local_width // groups, model_width // groups
    own_gains = small[: 2 * gain_size]
    shared = lax.psum(small[2 * gain_size : filled].astype(jnp.bfloat16), "dp")
    shared = shared.astype(jnp.float32)
    grad_out = lax.psum_scatter(
        grad_out.astype(jnp.bfloat16), "expert", scatter_dimension=0, tiled=True
    ).astype(jnp.float32)
    return (
        output,
        grad_input,
        shared[:norm_size],
        summed[:large_rows, :local_width],
        summed[:large_rows, local_width : 2 * local_width],
        summed[:large_rows, 2 * local_width :],
        grad_out,
        own_gains[:gain_size],
        own_gains[gain_size:],
        shared[norm_size : 2 * norm_size],
        shared[2 * norm_size :].reshape(norm_size, experts),
        grad_gate,
        grad_up,
        grad_down,
    )


def solution(mesh):
    placed = (
        P(None, "expert", None),
        P(),
        P(None, "dp"),
        P(None, "dp"),
        P(None, "dp"),
        P("dp", None),
        P("dp"),
        P("dp"),
        P(),
        P(),
        P("expert", None, "dp"),
        P("expert", None, "dp"),
        P("expert", "dp", None),
        P("expert", None, None),
        P(),
        P(None, "expert", None),
    )
    return jax.shard_map(
        per_device,
        mesh=mesh,
        in_specs=placed,
        out_specs=(
            P(None, "expert", None),
            P(None, "expert", None),
            P("expert"),
            P("expert", "dp"),
            P("expert", "dp"),
            P("expert", "dp"),
            P(("dp", "expert"), None),
            P(("dp", "expert")),
            P(("dp", "expert")),
            P("expert"),
            P("expert", None),
            P("expert", None, "dp"),
            P("expert", None, "dp"),
            P("expert", "dp", None),
        ),
        check_vma=False,
    )
```

```python
import functools

import jax
import jax.numpy as jnp
from jax import lax
from jax.experimental import pallas as pl
from jax.experimental.pallas import tpu as pltpu
from jax.sharding import PartitionSpec as P

HD = 128


epsilon = 1e-05
rope_base = 10000.0
masked_score = -1e30


def doc_layout(lengths, pack_span):
    doc_ends = jnp.cumsum(lengths, axis=1)
    starts = doc_ends - lengths
    places = jnp.arange(pack_span, dtype=jnp.int32)
    segment = jnp.sum((places[None, :, None] >= doc_ends[:, None, :]).astype(jnp.int32), axis=2)
    member = segment[:, :, None] == jnp.arange(lengths.shape[1], dtype=jnp.int32)[None, None, :]
    begins = jnp.sum(jnp.where(member, starts[:, None, :], 0), axis=2)
    return (segment, places[None, :] - begins)


def rope_tables(positions, head_size):
    half_size = head_size // 2
    frequency = rope_base ** (-2.0 * jnp.arange(half_size, dtype=jnp.float32) / head_size)
    angles = positions.astype(jnp.float32)[..., None] * frequency
    return (jnp.cos(angles), jnp.sin(angles))


def rotate(heads_in, cos_table, sin_table):
    half_size = heads_in.shape[-1] // 2
    first_half = heads_in[..., :half_size]
    second_half = heads_in[..., half_size:]
    cos_head = cos_table[..., None, :]
    sin_head = sin_table[..., None, :]
    return jnp.concatenate(
        [
            first_half * cos_head - second_half * sin_head,
            second_half * cos_head + first_half * sin_head,
        ],
        axis=-1,
    )


ALL = ("dp", "expert")


DEVICES = pl.DeviceIdType.MESH


def greet(device):
    pl.semaphore_signal(
        pltpu.get_barrier_semaphore(), inc=1, device_id=device, device_id_type=DEVICES
    )


def send(source, target, send_sem, arrive_sem, device):
    return pltpu.make_async_remote_copy(
        src_ref=source,
        dst_ref=target,
        send_sem=send_sem,
        recv_sem=arrive_sem,
        device_id=device,
        device_id_type=DEVICES,
    )


def contract(a, b, a_dim, b_dim):
    return lax.dot_general(
        a, b, (((a_dim,), (b_dim,)), ((), ())), preferred_element_type=jnp.float32
    )


def corners(dp):
    return dp + 1 - 2 * (dp % 2), (dp + 2) % 4


def gather_square_kernel(x_ref, out_ref, sent, arrived, own_sem):
    dp, place = lax.axis_index("dp"), lax.axis_index("expert")
    side_x, side_y = corners(dp)
    devices = ((side_x, place), (side_y, place))
    for device in devices:
        greet(device)
    pl.semaphore_wait(pltpu.get_barrier_semaphore(), 2)

    def copy(corner, p, way, source=None):
        target = out_ref.at[corner, p]
        return send(
            target if source is None else source,
            target,
            sent.at[corner, p, way],
            arrived.at[corner, p],
            devices[way],
        )

    for p in (0, 1):
        pltpu.make_async_copy(x_ref.at[p], out_ref.at[dp, p], own_sem.at[p]).start()
        for way in (0, 1):
            copy(dp, p, way, x_ref.at[p]).start()
    copy(side_x, 0, 0).wait_recv()
    copy(side_x, 0, 1).start()
    copy(side_y, 0, 0).wait_recv()
    copy(side_x, 1, 0).wait_recv()
    copy(side_y, 1, 0).wait_recv()
    copy(side_y, 1, 0).start()
    for p in (0, 1):
        copy(3 - dp, p, 0).wait_recv()
        for way in (0, 1):
            copy(dp, p, way).wait_send()
        pltpu.make_async_copy(x_ref.at[p], out_ref.at[dp, p], own_sem.at[p]).wait()
    copy(side_x, 0, 1).wait_send()
    copy(side_y, 1, 0).wait_send()


def gather_dp(rows):
    count, width = rows.shape
    gathered = pl.pallas_call(
        gather_square_kernel,
        out_shape=jax.ShapeDtypeStruct((4, 2, count // 2, width), rows.dtype),
        in_specs=[pl.BlockSpec(memory_space=pltpu.VMEM)],
        out_specs=pl.BlockSpec(memory_space=pl.ANY),
        scratch_shapes=[
            pltpu.SemaphoreType.DMA((4, 2, 2)),
            pltpu.SemaphoreType.DMA((4, 2)),
            pltpu.SemaphoreType.DMA((2,)),
        ],
        compiler_params=pltpu.CompilerParams(collective_id=2, has_side_effects=True),
        name="gather_dp",
    )(rows.reshape(2, count // 2, width))
    return gathered.reshape(4 * count, width)


def farthest(line, z, k):
    return ranked(line, z, k, lambda place, at: (-abs(place - at), place))


def reduce_kernel(
    square,
    line,
    paired,
    x_ref,
    out_ref,
    acc,
    got_pair,
    got_x,
    got_y,
    got_far_x,
    got_far_y,
    got_below,
    got_above,
    load_sem,
    pair_sem,
    x_sem,
    y_sem,
    far_x_sem,
    far_y_sem,
    below_sem,
    above_sem,
):
    dp, place = lax.axis_index("dp"), lax.axis_index("expert")
    z, c = place // 2, place % 2
    side_x, side_y = corners(dp)
    core = c if paired else 0
    own = dp if square else 0
    quarters = (3 - dp, side_x, side_y, dp) if square else (0,)
    to_x, to_y = (side_x, place), (side_y, place)
    to_pair, to_up, to_down = (dp, 2 * z + 1 - c), (dp, place + 2), (dp, place - 2)
    greeted = 0
    if square:
        greet(to_x)
        greet(to_y)
        greeted += 2
    if paired:
        greet(to_pair)
        greeted += 1
    if line > 1:
        pl.when(z > 0)(lambda: greet(to_down))
        pl.when(z < line - 1)(lambda: greet(to_up))
        greeted = greeted + (z > 0).astype(jnp.int32) + (z < line - 1).astype(jnp.int32)
    pl.semaphore_wait(pltpu.get_barrier_semaphore(), greeted)

    def load(q, height, p):
        return pltpu.make_async_copy(
            x_ref.at[q, height, core, p], acc.at[q, height, p], load_sem.at[q, height, p]
        )

    def hand(q, height, p):
        at = (q, height, p)
        source = x_ref.at[q, height, 1 - core, p]
        return send(source, got_pair.at[at], pair_sem.at[0, *at], pair_sem.at[1, *at], to_pair)

    def along_x(height, p):
        at = (height, p)
        return send(
            acc.at[side_x, height, p], got_x.at[at], x_sem.at[0, *at], x_sem.at[1, *at], to_x
        )

    def along_y(height, p):
        at = (height, p)
        return send(
            acc.at[side_y, height, p], got_y.at[at], y_sem.at[0, *at], y_sem.at[1, *at], to_y
        )

    def far_x(height):
        return send(
            acc.at[3 - dp, height, 0],
            got_far_x.at[height],
            far_x_sem.at[0, height],
            far_x_sem.at[1, height],
            to_x,
        )

    def far_y(height):
        return send(
            acc.at[3 - dp, height, 1],
            got_far_y.at[height],
            far_y_sem.at[0, height],
            far_y_sem.at[1, height],
            to_y,
        )

    def climb(height, p):
        at = (height, p)
        return send(
            acc.at[own, height, p], got_below.at[at], below_sem.at[0, *at], below_sem.at[1, *at], to_up
        )

    def descend(height, p):
        at = (height, p)
        return send(
            acc.at[own, height, p],
            got_above.at[at],
            above_sem.at[0, *at],
            above_sem.at[1, *at],
            to_down,
        )

    def height_of(k):
        return farthest(line, z, k) if line > 1 else 0

    def start(k, carry):
        for q in quarters:
            for p in (0, 1):
                load(q, height_of(k), p).start()
                if paired:
                    hand(q, height_of(k), p).start()
        return carry

    lax.fori_loop(0, line, start, 0)

    def step(k, carry):
        def cores():
            height = height_of(k)
            for q in quarters:
                for p in (0, 1):
                    load(q, height, p).wait()
                    if paired:
                        hand(q, height, p).wait_recv()
                        acc[q, height, p] = acc[q, height, p] + got_pair[q, height, p]
                if square and q is quarters[0]:
                    far_x(height).start()
                    far_y(height).start()

        def sides():
            height = height_of(k - 1)
            along_x(height, 0).start()
            along_y(height, 1).start()
            far_x(height).wait_recv()
            acc[side_y, height, 0] = acc[side_y, height, 0] + got_far_x[height]
            along_y(height, 0).start()
            far_y(height).wait_recv()
            acc[side_x, height, 1] = acc[side_x, height, 1] + got_far_y[height]
            along_x(height, 1).start()

        def column():
            height = height_of(k - 2)
            for p in (0, 1):
                if square:
                    along_x(height, p).wait_recv()
                    along_y(height, p).wait_recv()
                    total = acc[own, height, p].astype(jnp.float32)
                    total = total + got_x[height, p].astype(jnp.float32)
                    total = total + got_y[height, p].astype(jnp.float32)
                    acc[own, height, p] = total.astype(acc.dtype)
                if line > 1:
                    pl.when((z == 0) & (height > z))(lambda: climb(height, p).start())
                    pl.when((z == line - 1) & (height < z))(lambda: descend(height, p).start())

        def pass_on():
            height = height_of(k - 3)
            for p in (0, 1):

                def upwards():
                    climb(height, p).wait_recv()
                    acc[own, height, p] = acc[own, height, p] + got_below[height, p]
                    climb(height, p).start()

                def downwards():
                    descend(height, p).wait_recv()
                    acc[own, height, p] = acc[own, height, p] + got_above[height, p]
                    descend(height, p).start()

                pl.when((height > z) & (z > 0))(upwards)
                pl.when((height < z) & (z < line - 1))(downwards)

        pl.when(k < line)(cores)
        if square:
            pl.when((k >= 1) & (k < line + 1))(sides)
        pl.when((k >= 2) & (k < line + 2))(column)
        if line > 1:
            pl.when(k >= 3)(pass_on)
        return carry

    lax.fori_loop(0, line + (3 if line > 1 else 2), step, 0)
    home = z if line > 1 else 0
    for p in (0, 1):
        out_ref[p] = acc[own, home, p].astype(jnp.float32)
        if line > 1:

            def from_below():
                climb(z, p).wait_recv()
                out_ref[p] = out_ref[p] + got_below[z, p].astype(jnp.float32)

            def from_above():
                descend(z, p).wait_recv()
                out_ref[p] = out_ref[p] + got_above[z, p].astype(jnp.float32)

            pl.when(z > 0)(from_below)
            pl.when(z < line - 1)(from_above)

    def finish(height, carry):
        if square:
            far_x(height).wait_send()
            far_y(height).wait_send()
        for p in (0, 1):
            if paired:
                for q in quarters:
                    hand(q, height, p).wait_send()
            if square:
                along_x(height, p).wait_send()
                along_y(height, p).wait_send()
            if line > 1:
                pl.when(height > z)(lambda: climb(height, p).wait_send())
                pl.when(height < z)(lambda: descend(height, p).wait_send())
        return carry

    lax.fori_loop(0, line, finish, 0)


def reduce_to(parts, square, line, paired, name, number):
    _, rows, width = parts.shape
    quarters, cores, half = (4 if square else 1), (2 if paired else 1), rows // 2

    def space(used, *shape):
        return pltpu.VMEM((*shape, half, width) if used else (*shape, 16, 128), parts.dtype)

    sems = pltpu.SemaphoreType.DMA
    total = pl.pallas_call(
        functools.partial(reduce_kernel, square, line, paired),
        out_shape=jax.ShapeDtypeStruct((2, half, width), jnp.float32),
        in_specs=[pl.BlockSpec(memory_space=pl.ANY)],
        out_specs=pl.BlockSpec(memory_space=pltpu.VMEM),
        scratch_shapes=[
            space(True, quarters, line, 2),
            space(paired, quarters, line, 2),
            space(square, line, 2),
            space(square, line, 2),
            space(square, line),
            space(square, line),
            space(line > 1, line, 2),
            space(line > 1, line, 2),
            sems((quarters, line, 2)),
            sems((2, quarters, line, 2)),
            sems((2, line, 2)),
            sems((2, line, 2)),
            sems((2, line)),
            sems((2, line)),
            sems((2, line, 2)),
            sems((2, line, 2)),
        ],
        compiler_params=pltpu.CompilerParams(
            collective_id=number, has_side_effects=True, vmem_limit_bytes=60 << 20
        ),
        name=name,
    )(parts.reshape(quarters, line, cores, 2, half, width))
    return total.reshape(rows, width)


def scatter_dp(rows):
    return reduce_to(rows.reshape(4, -1, rows.shape[1]), True, 1, False, "scatter_dp", 3)


def scatter_expert(parts, line):
    return reduce_to(parts, False, line, True, "scatter_expert", 5)


def visit_others(line, z, visit):
    def turn(k, carry):
        visit((z + k) % line)
        return carry

    lax.fori_loop(1, line, turn, 0)


def greet_line(line, dp, z, c):
    visit_others(line, z, lambda other: greet((dp, 2 * other + c)))
    greet((dp, 2 * z + 1 - c))
    pl.semaphore_wait(pltpu.get_barrier_semaphore(), line)


def columns(z):
    return pl.ds(pl.multiple_of(z * HD, HD), HD)


def to_heads_kernel(line, shared, *refs):
    count = len(shared)
    ins, outs = refs[:count], refs[count : 2 * count]
    sent, arrived, pair_sent, pair_arrived, own_sem = refs[2 * count :]
    dp, place = lax.axis_index("dp"), lax.axis_index("expert")
    z, c = place // 2, place % 2
    pair = (dp, 2 * z + 1 - c)
    greet_line(line, dp, z, c)

    def block(i, origin):
        return outs[i].at[origin, c] if shared[i] else outs[i].at[origin]

    def out(i, other):
        source = ins[i].at[:, columns(other)]
        device = (dp, 2 * other + c)
        return send(source, block(i, z), sent.at[i, other], arrived.at[i, z], device)

    def into(i, origin):
        part = block(i, origin)
        return send(part, part, sent.at[i, origin], arrived.at[i, origin], pair)

    def share(i, origin, source=None):
        part = block(i, origin)
        return send(
            part if source is None else source,
            part,
            pair_sent.at[i, origin],
            pair_arrived.at[i, origin],
            pair,
        )

    def own(i):
        return pltpu.make_async_copy(ins[i].at[:, columns(z)], block(i, z), own_sem.at[i])

    def dispatch(other):
        for i in range(count):
            out(i, other).start()

    visit_others(line, z, dispatch)
    for i in range(count):
        own(i).start()
        if shared[i]:
            share(i, z, ins[i].at[:, columns(z)]).start()

    def receive(origin):
        for i in range(count):
            into(i, origin).wait_recv()
            if shared[i]:
                share(i, origin).start()

    visit_others(line, z, receive)

    def finish(other):
        for i in range(count):
            out(i, other).wait_send()

    visit_others(line, z, finish)
    for i in range(count):
        own(i).wait()
        if shared[i]:

            def settle(origin, carry):
                share(i, origin).wait()
                return carry

            lax.fori_loop(0, line, settle, 0)


def to_heads(arrays, shared, line, name, number):
    rows = arrays[0].shape[0]
    count = len(arrays)
    sems = pltpu.SemaphoreType.DMA
    return pl.pallas_call(
        functools.partial(to_heads_kernel, line, shared),
        out_shape=[
            jax.ShapeDtypeStruct((line, 2, rows, HD) if both else (line, rows, HD), array.dtype)
            for array, both in zip(arrays, shared)
        ],
        in_specs=[pl.BlockSpec(memory_space=pltpu.VMEM)] * count,
        out_specs=[pl.BlockSpec(memory_space=pl.ANY)] * count,
        scratch_shapes=[sems((count, line))] * 4 + [sems((count,))],
        compiler_params=pltpu.CompilerParams(collective_id=number, has_side_effects=True),
        name=name,
    )(*arrays)


def to_tokens_kernel(line, summed, *refs):
    count, sums = len(summed), sum(summed)
    ins, outs = refs[:count], refs[count : 2 * count]
    mine, theirs = refs[2 * count : 2 * count + 2]
    sent, arrived, pair_sem, load_sem, own_sem = refs[2 * count + 2 :]
    dp, place = lax.axis_index("dp"), lax.axis_index("expert")
    z, c = place // 2, place % 2
    pair = (dp, 2 * z + 1 - c)
    greet_line(line, dp, z, c)
    at_sum = [sum(summed[:i]) for i in range(count)]

    def load(i, other):
        return pltpu.make_async_copy(
            ins[i].at[other, c], mine.at[at_sum[i], other], load_sem.at[at_sum[i], other]
        )

    def hand(i, other):
        s = at_sum[i]
        return send(
            ins[i].at[other, 1 - c],
            theirs.at[s, other],
            pair_sem.at[0, s, other],
            pair_sem.at[1, s, other],
            pair,
        )

    def source(i, other):
        return mine.at[at_sum[i], other] if summed[i] else ins[i].at[other]

    def out(i, other):
        target = outs[i].at[:, columns(z)]
        device = (dp, 2 * other + c)
        return send(source(i, other), target, sent.at[i, other], arrived.at[i, z], device)

    def into(i, origin):
        part = outs[i].at[:, columns(origin)]
        return send(part, part, sent.at[i, origin], arrived.at[i, origin], pair)

    def own(i):
        return pltpu.make_async_copy(source(i, z), outs[i].at[:, columns(z)], own_sem.at[i])

    def prepare(other):
        for i in range(count):
            if summed[i]:
                load(i, other).start()
                hand(i, other).start()

    def add(i, other):
        if summed[i]:
            load(i, other).wait()
            hand(i, other).wait_recv()
            s = at_sum[i]
            mine[s, other] = mine[s, other] + theirs[s, other]

    def dispatch(other):
        for i in range(count):
            add(i, other)
            out(i, other).start()

    if sums:
        visit_others(line, z, prepare)
        prepare(z)
    visit_others(line, z, dispatch)
    for i in range(count):
        add(i, z)
        own(i).start()

    def finish(other):
        for i in range(count):
            into(i, other).wait_recv()
            out(i, other).wait_send()
            if summed[i]:
                hand(i, other).wait_send()

    visit_others(line, z, finish)
    for i in range(count):
        own(i).wait()
        if summed[i]:
            hand(i, z).wait_send()


def to_tokens(arrays, summed, line, name, number):
    rows = arrays[0].shape[-2]
    count, sums = len(arrays), max(sum(summed), 1)
    sems = pltpu.SemaphoreType.DMA
    dtype = arrays[0].dtype
    held = (sums, line, rows, HD) if sum(summed) else (1, 1, 16, HD)
    return pl.pallas_call(
        functools.partial(to_tokens_kernel, line, summed),
        out_shape=[jax.ShapeDtypeStruct((rows, line * HD), dtype)] * count,
        in_specs=[pl.BlockSpec(memory_space=pl.ANY)] * count,
        out_specs=[pl.BlockSpec(memory_space=pl.ANY)] * count,
        scratch_shapes=[pltpu.VMEM(held, dtype)] * 2
        + [
            sems((count, line)),
            sems((count, line)),
            sems((2, sums, line)),
            sems((sums, line)),
            sems((count,)),
        ],
        compiler_params=pltpu.CompilerParams(collective_id=number, has_side_effects=True),
        name=name,
    )(*arrays)


KEY_TILE = 512


def masked_scores(keys, queries, tile, first, starts):
    scores = contract(keys, queries, 1, 1) * HD ** (-0.5)
    key_at = tile * KEY_TILE + lax.broadcasted_iota(jnp.int32, scores.shape, 0)
    query_at = first + lax.broadcasted_iota(jnp.int32, (1, scores.shape[1]), 1)
    return jnp.where((key_at >= starts) & (key_at <= query_at), scores, masked_score)


def attend_kernel(bounds, q_ref, k_ref, v_ref, start_ref, o_ref, total_ref):
    i = pl.program_id(0)
    queries, starts = q_ref[0], start_ref[0]
    span = queries.shape[0]

    def tile_step(tile, carry):
        largest, total, acc = carry
        rows = pl.ds(pl.multiple_of(tile * KEY_TILE, KEY_TILE), KEY_TILE)
        scores = masked_scores(k_ref[rows, :], queries, tile, bounds[2, i], starts)
        new = jnp.maximum(largest, jnp.max(scores, axis=0, keepdims=True))
        weights = jnp.exp(scores - new)
        fade = jnp.exp(largest - new)
        total = fade * total + jnp.sum(weights, axis=0, keepdims=True)
        acc = fade * acc + contract(v_ref[rows, :], weights.astype(jnp.bfloat16), 0, 0)
        return new, total, acc

    largest, total, acc = lax.fori_loop(
        bounds[0, i],
        bounds[1, i],
        tile_step,
        (
            jnp.full((1, span), masked_score, jnp.float32),
            jnp.zeros((1, span), jnp.float32),
            jnp.zeros((HD, span), jnp.float32),
        ),
    )
    o_ref[0] = (acc / total).T.astype(o_ref.dtype)
    total_ref[0] = largest + jnp.log(total)


def attend_back_kernel(
    bounds, q_ref, k_ref, v_ref, start_ref, total_ref, delta_ref, d_ref, dq_ref, dk_ref, dv_ref, dk, dv
):
    i = pl.program_id(0)
    queries, starts, grad = q_ref[0], start_ref[0], d_ref[0]
    total, delta = total_ref[0], delta_ref[0]

    @pl.when(i == 0)
    def _():
        dk[...] = jnp.zeros_like(dk)
        dv[...] = jnp.zeros_like(dv)

    def tile_step(tile, acc):
        rows = pl.ds(pl.multiple_of(tile * KEY_TILE, KEY_TILE), KEY_TILE)
        keys = k_ref[rows, :]
        scores = masked_scores(keys, queries, tile, bounds[2, i], starts)
        weights = jnp.exp(scores - total)
        grad_weights = contract(v_ref[rows, :], grad, 1, 1)
        grad_scores = (weights * (grad_weights - delta)).astype(jnp.bfloat16)
        dv[rows, :] += contract(weights.astype(jnp.bfloat16), grad, 1, 0)
        dk[rows, :] += contract(grad_scores, queries, 1, 0)
        return acc + contract(keys, grad_scores, 0, 0)

    acc = jnp.zeros((HD, queries.shape[0]), jnp.float32)
    acc = lax.fori_loop(bounds[0, i], bounds[1, i], tile_step, acc)
    dq_ref[0] = (acc * HD ** (-0.5)).T.astype(dq_ref.dtype)

    @pl.when(i == pl.num_programs(0) - 1)
    def _():
        dk_ref[...] = (dk[...] * HD ** (-0.5)).astype(dk_ref.dtype)
        dv_ref[...] = dv[...].astype(dv_ref.dtype)


def attend(bounds, queries, keys, values, starts):
    line, span, _ = queries.shape
    pack = keys.shape[0]
    block = pl.BlockSpec((1, span, HD), lambda i, _: (i, 0, 0))
    row = pl.BlockSpec((1, 1, span), lambda i, _: (i, 0, 0))
    whole = pl.BlockSpec((pack, HD), lambda i, _: (0, 0))
    return pl.pallas_call(
        attend_kernel,
        grid_spec=pltpu.PrefetchScalarGridSpec(
            num_scalar_prefetch=1,
            grid=(line,),
            in_specs=[block, whole, whole, row],
            out_specs=[block, row],
        ),
        out_shape=[
            jax.ShapeDtypeStruct(queries.shape, jnp.bfloat16),
            jax.ShapeDtypeStruct(starts.shape, jnp.float32),
        ],
        name="attend",
    )(bounds, queries, keys, values, starts)


def attend_back(bounds, queries, keys, values, starts, total, delta, grad):
    line, span, _ = queries.shape
    pack = keys.shape[0]
    block = pl.BlockSpec((1, span, HD), lambda i, _: (i, 0, 0))
    row = pl.BlockSpec((1, 1, span), lambda i, _: (i, 0, 0))
    whole = pl.BlockSpec((pack, HD), lambda i, _: (0, 0))
    return pl.pallas_call(
        attend_back_kernel,
        grid_spec=pltpu.PrefetchScalarGridSpec(
            num_scalar_prefetch=1,
            grid=(line,),
            in_specs=[block, whole, whole, row, row, row, block],
            out_specs=[block, whole, whole],
            scratch_shapes=[pltpu.VMEM((pack, HD), jnp.float32)] * 2,
        ),
        out_shape=[jax.ShapeDtypeStruct(queries.shape, jnp.bfloat16)]
        + [jax.ShapeDtypeStruct((pack, HD), jnp.bfloat16)] * 2,
        name="attend_back",
    )(bounds, queries, keys, values, starts, total, delta, grad)


def by_head(layout, line):
    positions = layout[1][0]
    pack = positions.shape[0]
    span = pack // (2 * line)
    core = lax.axis_index("expert") % 2
    starts = (jnp.arange(pack, dtype=jnp.int32) - positions).reshape(line, 2, 1, span)
    starts = lax.dynamic_index_in_dim(starts, core, 1, keepdims=False)
    first = (2 * jnp.arange(line, dtype=jnp.int32) + core) * span
    bounds = jnp.stack(
        [starts[:, 0, 0] // KEY_TILE, (first + span - 1) // KEY_TILE + 1, first]
    ).astype(jnp.int32)

    def forward(queries, keys, values):
        q, k, v = to_heads(
            [queries, keys, values], (False, True, True), line, "scatter_heads", 6
        )
        k, v = k.reshape(pack, HD), v.reshape(pack, HD)
        out, total = attend(bounds, q, k, v, starts)
        (attended,) = to_tokens([out], (False,), line, "gather_heads", 7)
        return attended, (q, k, v, out, total)

    def backward(kept, grad):
        q, k, v, out, total = kept
        (grad,) = to_heads([grad], (False,), line, "scatter_grads", 8)
        delta = jnp.sum(grad.astype(jnp.float32) * out.astype(jnp.float32), axis=-1)
        dq, dk, dv = attend_back(bounds, q, k, v, starts, total, delta[:, None, :], grad)
        shape = (line, 2, span, HD)
        return to_tokens(
            [dq, dk.reshape(shape), dv.reshape(shape)],
            (False, True, True),
            line,
            "gather_grads",
            9,
        )

    return forward, backward


def by_query(layout, offset_rows):
    segment = layout[0][0]
    pack = segment.shape[0]

    def heads(rows):
        return rows.reshape(rows.shape[0], -1, HD)

    def score_block(queries, keys):
        rows = queries.shape[0]
        scores = jnp.einsum("shd,lhd->hsl", queries, keys, preferred_element_type=jnp.float32)
        own = lax.dynamic_slice_in_dim(segment, offset_rows, rows, 0)
        query_places = offset_rows + jnp.arange(rows, dtype=jnp.int32)
        key_places = jnp.arange(pack, dtype=jnp.int32)
        allowed = (own[:, None] == segment[None, :]) & (
            key_places[None, :] <= query_places[:, None]
        )
        return jnp.where(allowed[None], scores * HD ** (-0.5), masked_score)

    def forward(queries, keys, values):
        q = heads(queries)
        k = heads(lax.all_gather(keys, "expert", axis=0, tiled=True))
        v = heads(lax.all_gather(values, "expert", axis=0, tiled=True))
        scores = score_block(q, k)
        largest = jnp.max(scores, axis=-1, keepdims=True)
        total = largest + jnp.log(jnp.sum(jnp.exp(scores - largest), axis=-1, keepdims=True))
        weights = jnp.exp(scores - total).astype(jnp.bfloat16)
        attended = jnp.einsum("hsl,lhd->shd", weights, v, preferred_element_type=jnp.float32)
        return attended.astype(jnp.bfloat16).reshape(queries.shape), (q, k, v, total)

    def backward(kept, grad):
        q, k, v, total = kept
        shape = grad.shape
        grad = heads(grad)
        weights = jnp.exp(score_block(q, k) - total)
        grad_weights = jnp.einsum("shd,lhd->hsl", grad, v, preferred_element_type=jnp.float32)
        delta = jnp.sum(weights * grad_weights, axis=-1, keepdims=True)
        grad_scores = (weights * (grad_weights - delta)).astype(jnp.bfloat16)
        dq = jnp.einsum("hsl,lhd->shd", grad_scores, k, preferred_element_type=jnp.float32)
        dk = jnp.einsum("hsl,shd->lhd", grad_scores, q, preferred_element_type=jnp.float32)
        weights = weights.astype(jnp.bfloat16)
        dv = jnp.einsum("hsl,shd->lhd", weights, grad, preferred_element_type=jnp.float32)

        def to_owner(part):
            part = part.astype(jnp.bfloat16).reshape(pack, shape[1])
            return lax.psum_scatter(part, "expert", scatter_dimension=0, tiled=True)

        scale = HD ** (-0.5)
        return (dq * scale).reshape(shape), to_owner(dk * scale), to_owner(dv)

    return forward, backward


def nearest(line, z, k):
    return ranked(line, z, k, lambda place, at: (abs(place - at), place))


def ranked(line, z, k, rank):
    total = jnp.int32(0)
    for at in range(line):
        order = sorted(range(line), key=lambda place: rank(place, at))
        place = sum([jnp.where(k == i, order[i], 0) for i in range(line)])
        total = total + jnp.where(z == at, place, 0)
    return total


def gate_act_kernel(
    line,
    x_ref,
    top_ref,
    wg_ref,
    wu_ref,
    wd_ref,
    xn_ref,
    grads_ref,
    scaled_ref,
    gates_ref,
    xbuf,
    top_buf,
    grads_buf,
    scaled_buf,
    gates_buf,
    sent,
    arrived,
    own_sem,
    top_sem,
    xn_sem,
    grads_sem,
    scaled_sem,
    gates_sem,
):
    dp, place = lax.axis_index("dp"), lax.axis_index("expert")
    z, c = place // 2, place % 2
    side_x, side_y = corners(dp)
    far = 3 - dp
    devices = (
        (dp, place + 2),
        (dp, place - 2),
        (side_x, place),
        (side_y, place),
        (dp, 2 * z + 1 - c),
    )
    up, down, along_x, along_y, pair = range(5)
    has_up, has_down = z < line - 1, z > 0
    for way in (along_x, along_y, pair):
        greet(devices[way])
    pl.when(has_up)(lambda: greet(devices[up]))
    pl.when(has_down)(lambda: greet(devices[down]))
    greeted = 3 + has_up.astype(jnp.int32) + has_down.astype(jnp.int32)
    pl.semaphore_wait(pltpu.get_barrier_semaphore(), greeted)
    local, width, units = wg_ref.shape
    rows = top_buf.shape[1]
    first = place * local

    def slot(corner, height, core):
        return corner * (2 * line) + 2 * height + core

    def copy(s, p, way, source=None):
        target = xbuf.at[s, p]
        return send(
            target if source is None else source,
            target,
            sent.at[s, p, way],
            arrived.at[s, p],
            devices[way],
        )

    def arrive(s, p):
        copy(s, p, pair).wait_recv()

    mine = slot(dp, z, c)
    for p in (0, 1):
        pltpu.make_async_copy(x_ref.at[p], xbuf.at[mine, p], own_sem.at[p]).start()
        pl.when(has_up)(lambda: copy(mine, p, up, x_ref.at[p]).start())
        pl.when(has_down)(lambda: copy(mine, p, down, x_ref.at[p]).start())
        for way in (along_x, along_y, pair):
            copy(mine, p, way, x_ref.at[p]).start()

    def decode(i):
        turn, j = i // 4, i % 4
        k = turn - (j > 0).astype(jnp.int32) - (j == 3).astype(jnp.int32)
        valid = (i >= 0) & (k >= 0) & (k < line)
        corner = jnp.where(j == 0, dp, jnp.where(j == 1, side_x, jnp.where(j == 2, side_y, far)))
        return j, k, valid, corner, nearest(line, z, k)

    def top_load(i, corner, height):
        block = corner * line + height
        return pltpu.make_async_copy(top_ref.at[block], top_buf.at[i % 2], top_sem.at[i % 2])

    def xn_out(block):
        return pltpu.make_async_copy(
            xbuf.at[pl.ds(2 * block, 2), :, :, pl.ds(0, width)],
            xn_ref.at[pl.ds(2 * block, 2)],
            xn_sem.at[block],
        )

    def grads_out(block):
        return pltpu.make_async_copy(grads_buf.at[block], grads_ref.at[block], grads_sem.at[block])

    def scaled_out(block):
        return pltpu.make_async_copy(
            scaled_buf.at[block], scaled_ref.at[block], scaled_sem.at[block]
        )

    def gates_out(block):
        return pltpu.make_async_copy(gates_buf.at[block], gates_ref.at[block], gates_sem.at[block])

    def compute(i):
        j, k, _, corner, height = decode(i)
        block = corner * line + height
        for p in (0, 1):
            arrive(slot(corner, height, 1 - c), p)
        xn_out(block).start()
        top_load(i, corner, height).wait()
        lanes = lax.broadcasted_iota(jnp.int32, (rows, 128), 1)

        def tokens():
            return xbuf[pl.ds(2 * block, 2), :, :, pl.ds(0, width)].reshape(rows, width)

        table = xbuf[pl.ds(2 * block, 2), :, :, pl.ds(width, 128)].reshape(rows, 128)
        table = table.astype(jnp.float32)
        gate_grads = jnp.zeros((rows, 128), jnp.float32)
        for e in range(local):
            at = (lanes == first + e) | (lanes == first + e + 64)
            gate = jnp.sum(jnp.where(at, table, 0.0), axis=1, keepdims=True)
            g = contract(tokens(), wg_ref[e], 1, 0)
            u = contract(tokens(), wu_ref[e], 1, 0)
            h = contract(top_buf[i % 2], wd_ref[e], 1, 1)
            sigmoid = 1.0 / (1.0 + jnp.exp(-g))
            silu = g * sigmoid
            act = silu * u
            gate_grad = jnp.sum(act * h, axis=1, keepdims=True)
            gate_grads = gate_grads + jnp.where(lanes == first + e, gate_grad, 0.0)
            grad_act = h * gate
            dg = grad_act * u * sigmoid * (1.0 + g * (1.0 - sigmoid))
            du = grad_act * silu
            scaled_buf[block, :, e * units : (e + 1) * units] = (act * gate).astype(jnp.bfloat16)
            grads_buf[block, :, e * units : (e + 1) * units] = dg.astype(jnp.bfloat16)
            at = (local + e) * units
            grads_buf[block, :, at : at + units] = du.astype(jnp.bfloat16)
        gates_buf[block] = gate_grads.astype(jnp.bfloat16)
        grads_out(block).start()
        scaled_out(block).start()
        gates_out(block).start()

    def step(i, carry):
        j, k, valid, corner, height = decode(i)
        s = slot(corner, height, c)

        def own():
            for p in (0, 1):
                pltpu.make_async_copy(x_ref.at[p], xbuf.at[mine, p], own_sem.at[p]).wait()

        def column():
            for p in (0, 1):
                arrive(s, p)
                pl.when(has_up & (height < z))(lambda: copy(s, p, up).start())
                pl.when(has_down & (height > z))(lambda: copy(s, p, down).start())
                for way in (along_x, along_y, pair):
                    copy(s, p, way).start()

        def sides():
            for p in (0, 1):
                arrive(s, p)
                copy(s, p, pair).start()
            pl.when(j == 1)(lambda: copy(s, 0, along_y).start())
            pl.when(j == 2)(lambda: copy(s, 1, along_x).start())

        def opposite():
            for p in (0, 1):
                arrive(s, p)
                copy(s, p, pair).start()

        pl.when(valid & (j == 0) & (k == 0))(own)
        pl.when(valid & (j == 0) & (k > 0))(column)
        pl.when(valid & ((j == 1) | (j == 2)))(sides)
        pl.when(valid & (j == 3))(opposite)
        pl.when(valid)(lambda: top_load(i, corner, height).start())
        pl.when(decode(i - 1)[2])(lambda: compute(i - 1))
        return carry

    lax.fori_loop(0, 4 * (line + 2) + 1, step, 0)

    def finish(height, carry):
        for p in (0, 1):
            for corner in range(4):
                copy(slot(corner, height, c), p, pair).wait_send()
            s = slot(dp, height, c)
            copy(s, p, along_x).wait_send()
            copy(s, p, along_y).wait_send()
            pl.when(has_up & (height <= z))(lambda: copy(s, p, up).wait_send())
            pl.when(has_down & (height >= z))(lambda: copy(s, p, down).wait_send())
        copy(slot(side_x, height, c), 0, along_y).wait_send()
        copy(slot(side_y, height, c), 1, along_x).wait_send()
        for corner in range(4):
            block = corner * line + height
            xn_out(block).wait()
            grads_out(block).wait()
            scaled_out(block).wait()
            gates_out(block).wait()
        return carry

    lax.fori_loop(0, line, finish, 0)


def gate_act(own, tops, w_gate, w_up, w_down, line):
    count, wide = own.shape
    local, width, units = w_gate.shape
    slots, blocks, rows, half = 8 * line, 4 * line, 2 * count, count // 2
    sems = pltpu.SemaphoreType.DMA
    dtype = own.dtype
    xn, grads, scaled, gates = pl.pallas_call(
        functools.partial(gate_act_kernel, line),
        out_shape=[
            jax.ShapeDtypeStruct((slots, 2, half, width), dtype),
            jax.ShapeDtypeStruct((blocks, rows, 2 * local * units), dtype),
            jax.ShapeDtypeStruct((blocks, rows, local * units), dtype),
            jax.ShapeDtypeStruct((blocks, rows, 128), dtype),
        ],
        in_specs=[
            pl.BlockSpec(memory_space=pltpu.VMEM),
            pl.BlockSpec(memory_space=pl.ANY),
            pl.BlockSpec(memory_space=pltpu.VMEM),
            pl.BlockSpec(memory_space=pltpu.VMEM),
            pl.BlockSpec(memory_space=pltpu.VMEM),
        ],
        out_specs=[pl.BlockSpec(memory_space=pl.ANY)] * 4,
        scratch_shapes=[
            pltpu.VMEM((slots, 2, half, wide), dtype),
            pltpu.VMEM((2, rows, width), dtype),
            pltpu.VMEM((blocks, rows, 2 * local * units), dtype),
            pltpu.VMEM((blocks, rows, local * units), dtype),
            pltpu.VMEM((blocks, rows, 128), dtype),
            sems((slots, 2, 5)),
            sems((slots, 2)),
            sems((2,)),
            sems((2,)),
            sems((blocks,)),
            sems((blocks,)),
            sems((blocks,)),
            sems((blocks,)),
        ],
        compiler_params=pltpu.CompilerParams(
            collective_id=1, has_side_effects=True, vmem_limit_bytes=60 << 20
        ),
        name="gate_act",
    )(own.reshape(2, half, wide), tops.reshape(blocks, rows, width), w_gate, w_up, w_down)
    return xn.reshape(slots * count, width), grads, scaled, gates


def product_sum_kernel(
    line,
    flipped,
    extra,
    *refs,
):
    a_ref, w_ref = refs[0], refs[1]
    e_ref = refs[2] if extra else None
    refs = refs[3:] if extra else refs[2:]
    (
        out_ref,
        made,
        a_buf,
        e_buf,
        got_pair,
        got_x,
        got_y,
        got_far_x,
        got_far_y,
        got_below,
        got_above,
        load_sem,
        extra_sem,
        pair_sem,
        x_sem,
        y_sem,
        far_x_sem,
        far_y_sem,
        below_sem,
        above_sem,
    ) = refs
    dp, place = lax.axis_index("dp"), lax.axis_index("expert")
    z, c = place // 2, place % 2
    side_x, side_y = corners(dp)
    far = 3 - dp
    to_x, to_y, to_pair = (side_x, place), (side_y, place), (dp, 2 * z + 1 - c)
    to_up, to_down = (dp, place + 2), (dp, place - 2)
    for device in (to_x, to_y, to_pair):
        greet(device)
    pl.when(z > 0)(lambda: greet(to_down))
    pl.when(z < line - 1)(lambda: greet(to_up))
    greeted = 3 + (z > 0).astype(jnp.int32) + (z < line - 1).astype(jnp.int32)
    pl.semaphore_wait(pltpu.get_barrier_semaphore(), greeted)
    count = 4 * line
    width = w_ref.shape[0] if flipped else w_ref.shape[1]
    half = made.shape[4]
    chunk = 512

    def mine(q, height, p):
        return made.at[q, height, c, p]

    def hand(q, height, p):
        at = (q, height, p)
        source = made.at[q, height, 1 - c, p]
        return send(source, got_pair.at[at], pair_sem.at[0, *at], pair_sem.at[1, *at], to_pair)

    def along_x(height, p):
        at = (height, p)
        source = mine(side_x, height, p)
        return send(source, got_x.at[at], x_sem.at[0, *at], x_sem.at[1, *at], to_x)

    def along_y(height, p):
        at = (height, p)
        source = mine(side_y, height, p)
        return send(source, got_y.at[at], y_sem.at[0, *at], y_sem.at[1, *at], to_y)

    def far_x(height):
        source = mine(far, height, 0)
        return send(
            source, got_far_x.at[height], far_x_sem.at[0, height], far_x_sem.at[1, height], to_x
        )

    def far_y(height):
        source = mine(far, height, 1)
        return send(
            source, got_far_y.at[height], far_y_sem.at[0, height], far_y_sem.at[1, height], to_y
        )

    def climb(height, p):
        at = (height, p)
        source = mine(dp, height, p)
        return send(source, got_below.at[at], below_sem.at[0, *at], below_sem.at[1, *at], to_up)

    def descend(height, p):
        at = (height, p)
        source = mine(dp, height, p)
        return send(source, got_above.at[at], above_sem.at[0, *at], above_sem.at[1, *at], to_down)

    def decode(i):
        k, j = i // 4, i % 4
        q = jnp.where(j == 0, far, jnp.where(j == 1, side_x, jnp.where(j == 2, side_y, dp)))
        return k, j, q, farthest(line, z, k)

    def load(i):
        _, _, q, height = decode(i)
        return pltpu.make_async_copy(
            a_ref.at[q * line + height], a_buf.at[i % 2], load_sem.at[i % 2]
        )

    def load_extra(i):
        _, _, q, height = decode(i)
        return pltpu.make_async_copy(
            e_ref.at[q * line + height], e_buf.at[i % 2], extra_sem.at[i % 2]
        )

    def start_load(i):
        load(i).start()
        if extra:
            load_extra(i).start()

    def add(q, height, p, other):
        at = (q, height, c, p)
        made[at] = made[at] + other[...]

    def compute(i):
        _, _, q, height = decode(i)
        load(i).wait()
        if extra:
            load_extra(i).wait()
        pl.when(i + 1 < count)(lambda: start_load(i + 1))
        for at in range(0, width, chunk):
            if flipped:
                part = contract(a_buf[i % 2], w_ref[at : at + chunk, :], 1, 1)
            else:
                part = contract(a_buf[i % 2], w_ref[:, at : at + chunk], 1, 0)
            part = part.astype(made.dtype).reshape(2, 2, half, chunk)
            made[q, height, :, :, :, at : at + chunk] = part
        if extra:
            made[q, height, :, :, :, width : width + 128] = e_buf[i % 2].reshape(2, 2, half, 128)
        for p in (0, 1):
            hand(q, height, p).start()

    def settle(i):
        _, j, q, height = decode(i)
        for p in (0, 1):
            hand(q, height, p).wait_recv()
            add(q, height, p, got_pair.at[q, height, p])

        def opposite():
            far_x(height).start()
            far_y(height).start()

        def side_of_x():
            along_x(height, 0).start()
            far_y(height).wait_recv()
            add(side_x, height, 1, got_far_y.at[height])
            along_x(height, 1).start()

        def side_of_y():
            along_y(height, 1).start()
            far_x(height).wait_recv()
            add(side_y, height, 0, got_far_x.at[height])
            along_y(height, 0).start()

        pl.when(j == 0)(opposite)
        pl.when(j == 1)(side_of_x)
        pl.when(j == 2)(side_of_y)

    def column(height):
        for p in (0, 1):
            along_x(height, p).wait_recv()
            along_y(height, p).wait_recv()
            total = made[dp, height, c, p].astype(jnp.float32)
            total = total + got_x[height, p].astype(jnp.float32)
            total = total + got_y[height, p].astype(jnp.float32)
            made[dp, height, c, p] = total.astype(made.dtype)
            pl.when((z == 0) & (height > z))(lambda: climb(height, p).start())
            pl.when((z == line - 1) & (height < z))(lambda: descend(height, p).start())

    def pass_on(height):
        for p in (0, 1):

            def upwards():
                climb(height, p).wait_recv()
                add(dp, height, p, got_below.at[height, p])
                climb(height, p).start()

            def downwards():
                descend(height, p).wait_recv()
                add(dp, height, p, got_above.at[height, p])
                descend(height, p).start()

            pl.when((height > z) & (z > 0))(upwards)
            pl.when((height < z) & (z < line - 1))(downwards)

    start_load(0)

    def step(i, carry):
        k, j, _, _ = decode(i)
        pl.when(i < count)(lambda: compute(i))
        pl.when((i >= 1) & (i <= count))(lambda: settle(i - 1))
        late = farthest(line, z, k - 2)
        pl.when((k >= 2) & (j == 0))(lambda: column(late))
        pl.when((k >= 2) & (j == 3))(lambda: pass_on(late))
        return carry

    lax.fori_loop(0, count + 8, step, 0)
    for p in (0, 1):
        out_ref[p] = made[dp, z, c, p].astype(jnp.float32)

        def from_below():
            climb(z, p).wait_recv()
            out_ref[p] = out_ref[p] + got_below[z, p].astype(jnp.float32)

        def from_above():
            descend(z, p).wait_recv()
            out_ref[p] = out_ref[p] + got_above[z, p].astype(jnp.float32)

        pl.when(z > 0)(from_below)
        pl.when(z < line - 1)(from_above)

    def finish(height, carry):
        far_x(height).wait_send()
        far_y(height).wait_send()
        for p in (0, 1):
            for q in range(4):
                hand(q, height, p).wait_send()
            along_x(height, p).wait_send()
            along_y(height, p).wait_send()
            pl.when(height > z)(lambda: climb(height, p).wait_send())
            pl.when(height < z)(lambda: descend(height, p).wait_send())
        return carry

    lax.fori_loop(0, line, finish, 0)


def product_sum(blocks, weights, flipped, extra, line, name, number):
    count, rows, depth = blocks.shape
    width = weights.shape[0] if flipped else weights.shape[1]
    wide = width + (0 if extra is None else 128)
    half = rows // 4
    sems = pltpu.SemaphoreType.DMA
    dtype = blocks.dtype

    def space(*shape):
        return pltpu.VMEM((*shape, half, wide), dtype)

    anywhere, inside = pl.BlockSpec(memory_space=pl.ANY), pl.BlockSpec(memory_space=pltpu.VMEM)
    total = pl.pallas_call(
        functools.partial(product_sum_kernel, line, flipped, extra is not None),
        out_shape=jax.ShapeDtypeStruct((2, half, wide), jnp.float32),
        in_specs=[anywhere, inside] + ([] if extra is None else [anywhere]),
        out_specs=inside,
        scratch_shapes=[
            space(4, line, 2, 2),
            pltpu.VMEM((2, rows, depth), dtype),
            pltpu.VMEM((2, rows, 128), dtype),
            space(4, line, 2),
            space(line, 2),
            space(line, 2),
            space(line),
            space(line),
            space(line, 2),
            space(line, 2),
            sems((2,)),
            sems((2,)),
            sems((2, 4, line, 2)),
            sems((2, line, 2)),
            sems((2, line, 2)),
            sems((2, line)),
            sems((2, line)),
            sems((2, line, 2)),
            sems((2, line, 2)),
        ],
        compiler_params=pltpu.CompilerParams(
            collective_id=number, has_side_effects=True, vmem_limit_bytes=60 << 20
        ),
        name=name,
    )(blocks, weights, *([] if extra is None else [extra]))
    return total.reshape(2 * half, wide)


def head_totals(first_sum, second_sum):
    return lax.psum((first_sum, second_sum), "dp")


def per_device(
    inputs,
    attention_norm_gain,
    w_query,
    w_key,
    w_value,
    w_out,
    q_gain,
    k_gain,
    expert_norm_gain,
    w_router,
    w_gate,
    w_up,
    w_down,
    routes,
    lengths,
    d_output,
):
    pack_count, seg_rows, model_width = inputs.shape
    local_width = w_query.shape[1]
    local_heads = local_width // HD
    experts = w_router.shape[1]
    groups = lax.axis_size("expert")
    line = groups // 2
    pack_span = seg_rows * groups
    local_experts = w_gate.shape[0]
    offset_rows = lax.axis_index("expert") * seg_rows
    segment, positions = doc_layout(lengths, pack_span)
    pos_query = lax.dynamic_slice_in_dim(positions, offset_rows, seg_rows, 1)
    cos_table, sin_table = rope_tables(pos_query, HD)
    head_shape = (pack_count, seg_rows, local_heads, HD)
    inputs_single_float = inputs.astype(jnp.float32)
    first_inverse_norm = lax.rsqrt(
        jnp.mean(inputs_single_float * inputs_single_float, axis=-1, keepdims=True) + epsilon
    )
    first_unit_input = inputs_single_float * first_inverse_norm
    first_normed_input = (first_unit_input * attention_norm_gain).astype(jnp.bfloat16)
    q_raw = jnp.dot(first_normed_input, w_query, preferred_element_type=jnp.float32)
    k_raw = jnp.dot(first_normed_input, w_key, preferred_element_type=jnp.float32)
    value_rows = jnp.dot(first_normed_input, w_value, preferred_element_type=jnp.float32).astype(
        jnp.bfloat16
    )
    q_sum, k_sum = head_totals(jnp.sum(q_raw * q_raw, axis=-1), jnp.sum(k_raw * k_raw, axis=-1))
    q_inv = lax.rsqrt(q_sum[..., None] / model_width + epsilon)
    k_inv = lax.rsqrt(k_sum[..., None] / model_width + epsilon)
    q_hat = q_raw * q_inv
    k_hat = k_raw * k_inv
    queries = rotate((q_hat * q_gain).reshape(head_shape), cos_table, sin_table).astype(
        jnp.bfloat16
    )
    key_rows = (
        rotate((k_hat * k_gain).reshape(head_shape), cos_table, sin_table)
        .astype(jnp.bfloat16)
        .reshape(pack_count, seg_rows, local_width)
    )
    layout = (segment, positions)
    if local_heads == line:
        attention = by_head(layout, line)
    else:
        attention = by_query(layout, offset_rows)
    attended, kept = attention[0](queries.reshape(seg_rows, local_width), key_rows[0], value_rows[0])
    attn_part = jnp.dot(
        attended, w_out, preferred_element_type=jnp.float32
    )
    own = lax.axis_index("dp")
    part_rows = seg_rows // lax.axis_size("dp")

    def own_rows(rows):
        return lax.dynamic_slice_in_dim(rows, own * part_rows, part_rows, 0)

    hidden_state = own_rows(inputs_single_float[0]) + scatter_dp(attn_part.astype(jnp.bfloat16))
    second_inverse_norm = lax.rsqrt(
        jnp.mean(hidden_state * hidden_state, axis=-1, keepdims=True) + epsilon
    )
    second_unit_input = hidden_state * second_inverse_norm
    second_normed_input = second_unit_input * expert_norm_gain
    router = jax.nn.softmax(
        jnp.dot(second_normed_input, w_router, precision=lax.Precision.HIGHEST), axis=-1
    )
    chosen = own_rows(routes[:, 0, :])
    expert_range = jnp.arange(experts, dtype=jnp.int32)
    named = jnp.any(chosen[:, :, None] == expert_range, axis=1)
    top_own = own_rows(d_output[0])
    top_all = lax.all_gather(top_own, ALL, axis=0, tiled=True)
    gate_table = jnp.where(named, router, 0.0)
    gate_high = gate_table.astype(jnp.bfloat16)
    gate_low = (gate_table - gate_high.astype(jnp.float32)).astype(jnp.bfloat16)
    widen = ((0, 0), (0, 64 - experts))
    own_tokens = jnp.concatenate(
        [
            second_normed_input.astype(jnp.bfloat16),
            jnp.pad(gate_high, widen),
            jnp.pad(gate_low, widen),
        ],
        axis=1,
    )
    xn_all, grad_units, scaled, gate_part = gate_act(
        own_tokens, top_all, w_gate, w_up, w_down, line
    )
    token_count = pack_count * pack_span
    w_both = jnp.concatenate([*w_gate, *w_up], axis=1)
    grad_tokens = product_sum(grad_units, w_both, True, gate_part, line, "grad_tokens", 4)
    grad_units = grad_units.reshape(token_count, -1)
    scaled = scaled.reshape(token_count, -1)
    units = w_gate.shape[2]
    moe_part = jnp.dot(
        scaled, w_down.reshape(-1, model_width), preferred_element_type=jnp.float32
    )
    grad_down = contract(scaled, top_all, 0, 0).reshape(w_down.shape)
    grad_both = [
        contract(xn_all, grad_units[:, at : at + units], 0, 0)
        for at in range(0, grad_units.shape[1], units)
    ]
    grad_gate = jnp.stack(grad_both[:local_experts])
    grad_up = jnp.stack(grad_both[local_experts:])

    moe_out = lax.psum_scatter(
        moe_part.astype(jnp.bfloat16), ALL, scatter_dimension=0, tiled=True
    ).astype(jnp.float32)
    output = gather_dp((hidden_state + moe_out).astype(jnp.bfloat16))[None]

    grad_xn_exp = grad_tokens[:, :model_width]
    gate_sums = grad_tokens[:, model_width : model_width + experts]
    grad_router_probs = jnp.where(named, gate_sums, 0.0)
    grad_logits = router * (
        grad_router_probs - jnp.sum(router * grad_router_probs, axis=-1, keepdims=True)
    )
    grad_second_normed_input = grad_xn_exp + jnp.einsum(
        "se,de->sd", grad_logits, w_router, precision=lax.Precision.HIGHEST
    )
    grad_router = jnp.einsum(
        "sd,se->de", second_normed_input, grad_logits, precision=lax.Precision.HIGHEST
    )
    grad_expert_norm_gain = jnp.sum(grad_second_normed_input * second_unit_input, axis=0)
    grad_second_unit_input = grad_second_normed_input * expert_norm_gain
    grad_hidden = top_own.astype(jnp.float32) + second_inverse_norm * (
        grad_second_unit_input
        - second_unit_input
        * jnp.mean(grad_second_unit_input * second_unit_input, axis=-1, keepdims=True)
    )
    grad_attn = gather_dp(grad_hidden.astype(jnp.bfloat16))
    grad_out = jnp.einsum("sk,sd->kd", attended, grad_attn, preferred_element_type=jnp.float32)
    grad_heads = jnp.einsum(
        "sd,kd->sk", grad_attn, w_out, preferred_element_type=jnp.float32
    ).astype(jnp.bfloat16)
    grad_queries, grad_keys, grad_values = attention[1](kept, grad_heads)
    grad_queries = grad_queries.astype(jnp.float32).reshape(head_shape)
    grad_q_normed = rotate(grad_queries, cos_table, -sin_table).reshape(
        pack_count, seg_rows, local_width
    )
    grad_k_normed = rotate(
        grad_keys.astype(jnp.float32).reshape(head_shape), cos_table, -sin_table).reshape(
        pack_count, seg_rows, local_width
    )
    grad_q_gain = jnp.sum(grad_q_normed * q_hat, axis=(0, 1))
    grad_k_gain = jnp.sum(grad_k_normed * k_hat, axis=(0, 1))
    grad_q_hat = grad_q_normed * q_gain
    grad_k_hat = grad_k_normed * k_gain
    q_dot, k_dot = head_totals(
        jnp.sum(grad_q_hat * q_hat, axis=-1), jnp.sum(grad_k_hat * k_hat, axis=-1)
    )
    grad_q_raw = (q_inv * (grad_q_hat - q_hat * q_dot[..., None] / model_width)).astype(
        jnp.bfloat16
    )
    grad_k_raw = (k_inv * (grad_k_hat - k_hat * k_dot[..., None] / model_width)).astype(
        jnp.bfloat16
    )
    grad_v_raw = grad_values.astype(jnp.bfloat16)[None]
    grad_heads_raw = jnp.concatenate([grad_q_raw[0], grad_k_raw[0], grad_v_raw[0]], axis=1)
    grad_projections = jnp.einsum(
        "sd,sk->dk", first_normed_input[0], grad_heads_raw, preferred_element_type=jnp.float32
    )
    grad_first_normed_input = jnp.einsum(
        "psk,dk->psd", grad_q_raw, w_query, preferred_element_type=jnp.float32
    )
    grad_first_normed_input = grad_first_normed_input + jnp.einsum(
        "psk,dk->psd", grad_k_raw, w_key, preferred_element_type=jnp.float32
    )
    grad_first_normed_input = grad_first_normed_input + jnp.einsum(
        "psk,dk->psd", grad_v_raw, w_value, preferred_element_type=jnp.float32
    )
    grad_first = scatter_dp(grad_first_normed_input[0].astype(jnp.bfloat16))
    unit_own = own_rows(first_unit_input[0])
    grad_attn_gain = jnp.sum(grad_first * unit_own, axis=0)
    grad_first = grad_first * attention_norm_gain
    grad_input = grad_hidden + own_rows(first_inverse_norm[0]) * (
        grad_first - unit_own * jnp.mean(grad_first * unit_own, axis=-1, keepdims=True)
    )
    grad_input = gather_dp(grad_input.astype(jnp.bfloat16)).astype(jnp.float32)[None]

    wide = grad_projections.shape[1]
    small = jnp.concatenate(
        [
            grad_q_gain.reshape(groups, -1),
            grad_k_gain.reshape(groups, -1),
            grad_attn_gain.reshape(groups, -1),
            grad_expert_norm_gain.reshape(groups, -1),
            grad_router.reshape(groups, -1),
        ],
        axis=1,
    )
    small_rows = 32
    filled = small.shape[1]
    small = jnp.pad(small, ((0, 0), (0, small_rows * wide - filled)))
    parts = jnp.concatenate(
        [
            grad_projections.astype(jnp.bfloat16).reshape(groups, -1, wide),
            small.astype(jnp.bfloat16).reshape(groups, small_rows, wide),
        ],
        axis=1,
    )
    summed = scatter_expert(parts, line)
    large_rows = summed.shape[0] - small_rows
    small = summed[large_rows:].reshape(-1)
    gain_size, norm_size = local_width // groups, model_width // groups
    own_gains = small[: 2 * gain_size]
    shared = lax.psum(small[2 * gain_size : filled].astype(jnp.bfloat16), "dp")
    shared = shared.astype(jnp.float32)
    grad_out = lax.psum_scatter(
        grad_out.astype(jnp.bfloat16), "expert", scatter_dimension=0, tiled=True
    ).astype(jnp.float32)
    return (
        output,
        grad_input,
        shared[:norm_size],
        summed[:large_rows, :local_width],
        summed[:large_rows, local_width : 2 * local_width],
        summed[:large_rows, 2 * local_width :],
        grad_out,
        own_gains[:gain_size],
        own_gains[gain_size:],
        shared[norm_size : 2 * norm_size],
        shared[2 * norm_size :].reshape(norm_size, experts),
        grad_gate,
        grad_up,
        grad_down,
    )


def solution(mesh):
    placed = (
        P(None, "expert", None),
        P(),
        P(None, "dp"),
        P(None, "dp"),
        P(None, "dp"),
        P("dp", None),
        P("dp"),
        P("dp"),
        P(),
        P(),
        P("expert", None, "dp"),
        P("expert", None, "dp"),
        P("expert", "dp", None),
        P("expert", None, None),
        P(),
        P(None, "expert", None),
    )
    return jax.shard_map(
        per_device,
        mesh=mesh,
        in_specs=placed,
        out_specs=(
            P(None, "expert", None),
            P(None, "expert", None),
            P("expert"),
            P("expert", "dp"),
            P("expert", "dp"),
            P("expert", "dp"),
            P(("dp", "expert"), None),
            P(("dp", "expert")),
            P(("dp", "expert")),
            P("expert"),
            P("expert", None),
            P("expert", None, "dp"),
            P("expert", None, "dp"),
            P("expert", "dp", None),
        ),
        check_vma=False,
    )
```

```python
import functools

import jax
import jax.numpy as jnp
from jax import lax
from jax.experimental import pallas as pl
from jax.experimental.pallas import tpu as pltpu
from jax.sharding import PartitionSpec as P

HD = 128


epsilon = 1e-05
rope_base = 10000.0
masked_score = -1e30


def doc_layout(lengths, pack_span):
    doc_ends = jnp.cumsum(lengths, axis=1)
    starts = doc_ends - lengths
    places = jnp.arange(pack_span, dtype=jnp.int32)
    segment = jnp.sum((places[None, :, None] >= doc_ends[:, None, :]).astype(jnp.int32), axis=2)
    member = segment[:, :, None] == jnp.arange(lengths.shape[1], dtype=jnp.int32)[None, None, :]
    begins = jnp.sum(jnp.where(member, starts[:, None, :], 0), axis=2)
    return (segment, places[None, :] - begins)


def rope_tables(positions, head_size):
    half_size = head_size // 2
    frequency = rope_base ** (-2.0 * jnp.arange(half_size, dtype=jnp.float32) / head_size)
    angles = positions.astype(jnp.float32)[..., None] * frequency
    return (jnp.cos(angles), jnp.sin(angles))


def rotate(heads_in, cos_table, sin_table):
    half_size = heads_in.shape[-1] // 2
    first_half = heads_in[..., :half_size]
    second_half = heads_in[..., half_size:]
    cos_head = cos_table[..., None, :]
    sin_head = sin_table[..., None, :]
    return jnp.concatenate(
        [
            first_half * cos_head - second_half * sin_head,
            second_half * cos_head + first_half * sin_head,
        ],
        axis=-1,
    )


ALL = ("dp", "expert")


DEVICES = pl.DeviceIdType.MESH


def greet(device):
    pl.semaphore_signal(
        pltpu.get_barrier_semaphore(), inc=1, device_id=device, device_id_type=DEVICES
    )


def send(source, target, send_sem, arrive_sem, device):
    return pltpu.make_async_remote_copy(
        src_ref=source,
        dst_ref=target,
        send_sem=send_sem,
        recv_sem=arrive_sem,
        device_id=device,
        device_id_type=DEVICES,
    )


def contract(a, b, a_dim, b_dim):
    return lax.dot_general(
        a, b, (((a_dim,), (b_dim,)), ((), ())), preferred_element_type=jnp.float32
    )


def corners(dp):
    return dp + 1 - 2 * (dp % 2), (dp + 2) % 4


def gather_square_kernel(x_ref, out_ref, sent, arrived, own_sem):
    dp, place = lax.axis_index("dp"), lax.axis_index("expert")
    side_x, side_y = corners(dp)
    devices = ((side_x, place), (side_y, place))
    for device in devices:
        greet(device)
    pl.semaphore_wait(pltpu.get_barrier_semaphore(), 2)

    def copy(corner, p, way, source=None):
        target = out_ref.at[corner, p]
        return send(
            target if source is None else source,
            target,
            sent.at[corner, p, way],
            arrived.at[corner, p],
            devices[way],
        )

    for p in (0, 1):
        pltpu.make_async_copy(x_ref.at[p], out_ref.at[dp, p], own_sem.at[p]).start()
        for way in (0, 1):
            copy(dp, p, way, x_ref.at[p]).start()
    copy(side_x, 0, 0).wait_recv()
    copy(side_x, 0, 1).start()
    copy(side_y, 0, 0).wait_recv()
    copy(side_x, 1, 0).wait_recv()
    copy(side_y, 1, 0).wait_recv()
    copy(side_y, 1, 0).start()
    for p in (0, 1):
        copy(3 - dp, p, 0).wait_recv()
        for way in (0, 1):
            copy(dp, p, way).wait_send()
        pltpu.make_async_copy(x_ref.at[p], out_ref.at[dp, p], own_sem.at[p]).wait()
    copy(side_x, 0, 1).wait_send()
    copy(side_y, 1, 0).wait_send()


def gather_dp(rows):
    count, width = rows.shape
    gathered = pl.pallas_call(
        gather_square_kernel,
        out_shape=jax.ShapeDtypeStruct((4, 2, count // 2, width), rows.dtype),
        in_specs=[pl.BlockSpec(memory_space=pltpu.VMEM)],
        out_specs=pl.BlockSpec(memory_space=pl.ANY),
        scratch_shapes=[
            pltpu.SemaphoreType.DMA((4, 2, 2)),
            pltpu.SemaphoreType.DMA((4, 2)),
            pltpu.SemaphoreType.DMA((2,)),
        ],
        compiler_params=pltpu.CompilerParams(collective_id=10, has_side_effects=True),
        name="gather_dp",
    )(rows.reshape(2, count // 2, width))
    return gathered.reshape(4 * count, width)


def farthest(line, z, k):
    return ranked(line, z, k, lambda place, at: (-abs(place - at), place))


def reduce_kernel(
    square,
    line,
    paired,
    x_ref,
    out_ref,
    acc,
    got_pair,
    got_x,
    got_y,
    got_far_x,
    got_far_y,
    got_below,
    got_above,
    load_sem,
    pair_sem,
    x_sem,
    y_sem,
    far_x_sem,
    far_y_sem,
    below_sem,
    above_sem,
):
    dp, place = lax.axis_index("dp"), lax.axis_index("expert")
    z, c = place // 2, place % 2
    side_x, side_y = corners(dp)
    core = c if paired else 0
    own = dp if square else 0
    quarters = (3 - dp, side_x, side_y, dp) if square else (0,)
    to_x, to_y = (side_x, place), (side_y, place)
    to_pair, to_up, to_down = (dp, 2 * z + 1 - c), (dp, place + 2), (dp, place - 2)
    greeted = 0
    if square:
        greet(to_x)
        greet(to_y)
        greeted += 2
    if paired:
        greet(to_pair)
        greeted += 1
    if line > 1:
        pl.when(z > 0)(lambda: greet(to_down))
        pl.when(z < line - 1)(lambda: greet(to_up))
        greeted = greeted + (z > 0).astype(jnp.int32) + (z < line - 1).astype(jnp.int32)
    pl.semaphore_wait(pltpu.get_barrier_semaphore(), greeted)

    def load(q, height, p):
        return pltpu.make_async_copy(
            x_ref.at[q, height, core, p], acc.at[q, height, p], load_sem.at[q, height, p]
        )

    def hand(q, height, p):
        at = (q, height, p)
        source = x_ref.at[q, height, 1 - core, p]
        return send(source, got_pair.at[at], pair_sem.at[0, *at], pair_sem.at[1, *at], to_pair)

    def along_x(height, p):
        at = (height, p)
        return send(
            acc.at[side_x, height, p], got_x.at[at], x_sem.at[0, *at], x_sem.at[1, *at], to_x
        )

    def along_y(height, p):
        at = (height, p)
        return send(
            acc.at[side_y, height, p], got_y.at[at], y_sem.at[0, *at], y_sem.at[1, *at], to_y
        )

    def far_x(height):
        return send(
            acc.at[3 - dp, height, 0],
            got_far_x.at[height],
            far_x_sem.at[0, height],
            far_x_sem.at[1, height],
            to_x,
        )

    def far_y(height):
        return send(
            acc.at[3 - dp, height, 1],
            got_far_y.at[height],
            far_y_sem.at[0, height],
            far_y_sem.at[1, height],
            to_y,
        )

    def climb(height, p):
        at = (height, p)
        return send(
            acc.at[own, height, p], got_below.at[at], below_sem.at[0, *at], below_sem.at[1, *at], to_up
        )

    def descend(height, p):
        at = (height, p)
        return send(
            acc.at[own, height, p],
            got_above.at[at],
            above_sem.at[0, *at],
            above_sem.at[1, *at],
            to_down,
        )

    def height_of(k):
        return farthest(line, z, k) if line > 1 else 0

    def start(k, carry):
        for q in quarters:
            for p in (0, 1):
                load(q, height_of(k), p).start()
                if paired:
                    hand(q, height_of(k), p).start()
        return carry

    lax.fori_loop(0, line, start, 0)

    def step(k, carry):
        def cores():
            height = height_of(k)
            for q in quarters:
                for p in (0, 1):
                    load(q, height, p).wait()
                    if paired:
                        hand(q, height, p).wait_recv()
                        acc[q, height, p] = acc[q, height, p] + got_pair[q, height, p]
                if square and q is quarters[0]:
                    far_x(height).start()
                    far_y(height).start()

        def sides():
            height = height_of(k - 1)
            along_x(height, 0).start()
            along_y(height, 1).start()
            far_x(height).wait_recv()
            acc[side_y, height, 0] = acc[side_y, height, 0] + got_far_x[height]
            along_y(height, 0).start()
            far_y(height).wait_recv()
            acc[side_x, height, 1] = acc[side_x, height, 1] + got_far_y[height]
            along_x(height, 1).start()

        def column():
            height = height_of(k - 2)
            for p in (0, 1):
                if square:
                    along_x(height, p).wait_recv()
                    along_y(height, p).wait_recv()
                    total = acc[own, height, p].astype(jnp.float32)
                    total = total + got_x[height, p].astype(jnp.float32)
                    total = total + got_y[height, p].astype(jnp.float32)
                    acc[own, height, p] = total.astype(acc.dtype)
                if line > 1:
                    pl.when((z == 0) & (height > z))(lambda: climb(height, p).start())
                    pl.when((z == line - 1) & (height < z))(lambda: descend(height, p).start())

        def pass_on():
            height = height_of(k - 3)
            for p in (0, 1):

                def upwards():
                    climb(height, p).wait_recv()
                    acc[own, height, p] = acc[own, height, p] + got_below[height, p]
                    climb(height, p).start()

                def downwards():
                    descend(height, p).wait_recv()
                    acc[own, height, p] = acc[own, height, p] + got_above[height, p]
                    descend(height, p).start()

                pl.when((height > z) & (z > 0))(upwards)
                pl.when((height < z) & (z < line - 1))(downwards)

        pl.when(k < line)(cores)
        if square:
            pl.when((k >= 1) & (k < line + 1))(sides)
        pl.when((k >= 2) & (k < line + 2))(column)
        if line > 1:
            pl.when(k >= 3)(pass_on)
        return carry

    lax.fori_loop(0, line + (3 if line > 1 else 2), step, 0)
    home = z if line > 1 else 0
    for p in (0, 1):
        out_ref[p] = acc[own, home, p].astype(jnp.float32)
        if line > 1:

            def from_below():
                climb(z, p).wait_recv()
                out_ref[p] = out_ref[p] + got_below[z, p].astype(jnp.float32)

            def from_above():
                descend(z, p).wait_recv()
                out_ref[p] = out_ref[p] + got_above[z, p].astype(jnp.float32)

            pl.when(z > 0)(from_below)
            pl.when(z < line - 1)(from_above)

    def finish(height, carry):
        if square:
            far_x(height).wait_send()
            far_y(height).wait_send()
        for p in (0, 1):
            if paired:
                for q in quarters:
                    hand(q, height, p).wait_send()
            if square:
                along_x(height, p).wait_send()
                along_y(height, p).wait_send()
            if line > 1:
                pl.when(height > z)(lambda: climb(height, p).wait_send())
                pl.when(height < z)(lambda: descend(height, p).wait_send())
        return carry

    lax.fori_loop(0, line, finish, 0)


def reduce_to(parts, square, line, paired, name, number):
    _, rows, width = parts.shape
    quarters, cores, half = (4 if square else 1), (2 if paired else 1), rows // 2

    def space(used, *shape):
        return pltpu.VMEM((*shape, half, width) if used else (*shape, 16, 128), parts.dtype)

    sems = pltpu.SemaphoreType.DMA
    total = pl.pallas_call(
        functools.partial(reduce_kernel, square, line, paired),
        out_shape=jax.ShapeDtypeStruct((2, half, width), jnp.float32),
        in_specs=[pl.BlockSpec(memory_space=pl.ANY)],
        out_specs=pl.BlockSpec(memory_space=pltpu.VMEM),
        scratch_shapes=[
            space(True, quarters, line, 2),
            space(paired, quarters, line, 2),
            space(square, line, 2),
            space(square, line, 2),
            space(square, line),
            space(square, line),
            space(line > 1, line, 2),
            space(line > 1, line, 2),
            sems((quarters, line, 2)),
            sems((2, quarters, line, 2)),
            sems((2, line, 2)),
            sems((2, line, 2)),
            sems((2, line)),
            sems((2, line)),
            sems((2, line, 2)),
            sems((2, line, 2)),
        ],
        compiler_params=pltpu.CompilerParams(
            collective_id=number, has_side_effects=True, vmem_limit_bytes=60 << 20
        ),
        name=name,
    )(parts.reshape(quarters, line, cores, 2, half, width))
    return total.reshape(rows, width)


def scatter_dp(rows):
    return reduce_to(rows.reshape(4, -1, rows.shape[1]), True, 1, False, "scatter_dp", 3)


def visit_others(line, z, visit):
    def turn(k, carry):
        visit((z + k) % line)
        return carry

    lax.fori_loop(1, line, turn, 0)


def greet_line(line, dp, z, c):
    visit_others(line, z, lambda other: greet((dp, 2 * other + c)))
    greet((dp, 2 * z + 1 - c))
    pl.semaphore_wait(pltpu.get_barrier_semaphore(), line)


def columns(z):
    return pl.ds(pl.multiple_of(z * HD, HD), HD)


def to_heads_kernel(line, shared, *refs):
    count = len(shared)
    ins, outs = refs[:count], refs[count : 2 * count]
    sent, arrived, pair_sent, pair_arrived, own_sem = refs[2 * count :]
    dp, place = lax.axis_index("dp"), lax.axis_index("expert")
    z, c = place // 2, place % 2
    pair = (dp, 2 * z + 1 - c)
    greet_line(line, dp, z, c)

    def block(i, origin):
        return outs[i].at[origin, c] if shared[i] else outs[i].at[origin]

    def out(i, other):
        source = ins[i].at[:, columns(other)]
        device = (dp, 2 * other + c)
        return send(source, block(i, z), sent.at[i, other], arrived.at[i, z], device)

    def into(i, origin):
        part = block(i, origin)
        return send(part, part, sent.at[i, origin], arrived.at[i, origin], pair)

    def share(i, origin, source=None):
        part = block(i, origin)
        return send(
            part if source is None else source,
            part,
            pair_sent.at[i, origin],
            pair_arrived.at[i, origin],
            pair,
        )

    def own(i):
        return pltpu.make_async_copy(ins[i].at[:, columns(z)], block(i, z), own_sem.at[i])

    def dispatch(other):
        for i in range(count):
            out(i, other).start()

    visit_others(line, z, dispatch)
    for i in range(count):
        own(i).start()
        if shared[i]:
            share(i, z, ins[i].at[:, columns(z)]).start()

    def receive(origin):
        for i in range(count):
            into(i, origin).wait_recv()
            if shared[i]:
                share(i, origin).start()

    visit_others(line, z, receive)

    def finish(other):
        for i in range(count):
            out(i, other).wait_send()

    visit_others(line, z, finish)
    for i in range(count):
        own(i).wait()
        if shared[i]:

            def settle(origin, carry):
                share(i, origin).wait()
                return carry

            lax.fori_loop(0, line, settle, 0)


def to_heads(arrays, shared, line, name, number):
    rows = arrays[0].shape[0]
    count = len(arrays)
    sems = pltpu.SemaphoreType.DMA
    return pl.pallas_call(
        functools.partial(to_heads_kernel, line, shared),
        out_shape=[
            jax.ShapeDtypeStruct((line, 2, rows, HD) if both else (line, rows, HD), array.dtype)
            for array, both in zip(arrays, shared)
        ],
        in_specs=[pl.BlockSpec(memory_space=pltpu.VMEM)] * count,
        out_specs=[pl.BlockSpec(memory_space=pl.ANY)] * count,
        scratch_shapes=[sems((count, line))] * 4 + [sems((count,))],
        compiler_params=pltpu.CompilerParams(collective_id=number, has_side_effects=True),
        name=name,
    )(*arrays)


def to_tokens_kernel(line, summed, *refs):
    count, sums = len(summed), sum(summed)
    ins, outs = refs[:count], refs[count : 2 * count]
    mine, theirs = refs[2 * count : 2 * count + 2]
    sent, arrived, pair_sem, load_sem, own_sem = refs[2 * count + 2 :]
    dp, place = lax.axis_index("dp"), lax.axis_index("expert")
    z, c = place // 2, place % 2
    pair = (dp, 2 * z + 1 - c)
    greet_line(line, dp, z, c)
    at_sum = [sum(summed[:i]) for i in range(count)]

    def load(i, other):
        return pltpu.make_async_copy(
            ins[i].at[other, c], mine.at[at_sum[i], other], load_sem.at[at_sum[i], other]
        )

    def hand(i, other):
        s = at_sum[i]
        return send(
            ins[i].at[other, 1 - c],
            theirs.at[s, other],
            pair_sem.at[0, s, other],
            pair_sem.at[1, s, other],
            pair,
        )

    def source(i, other):
        return mine.at[at_sum[i], other] if summed[i] else ins[i].at[other]

    def out(i, other):
        target = outs[i].at[:, columns(z)]
        device = (dp, 2 * other + c)
        return send(source(i, other), target, sent.at[i, other], arrived.at[i, z], device)

    def into(i, origin):
        part = outs[i].at[:, columns(origin)]
        return send(part, part, sent.at[i, origin], arrived.at[i, origin], pair)

    def own(i):
        return pltpu.make_async_copy(source(i, z), outs[i].at[:, columns(z)], own_sem.at[i])

    def prepare(other):
        for i in range(count):
            if summed[i]:
                load(i, other).start()
                hand(i, other).start()

    def add(i, other):
        if summed[i]:
            load(i, other).wait()
            hand(i, other).wait_recv()
            s = at_sum[i]
            mine[s, other] = mine[s, other] + theirs[s, other]

    def dispatch(other):
        for i in range(count):
            add(i, other)
            out(i, other).start()

    if sums:
        visit_others(line, z, prepare)
        prepare(z)
    visit_others(line, z, dispatch)
    for i in range(count):
        add(i, z)
        own(i).start()

    def finish(other):
        for i in range(count):
            into(i, other).wait_recv()
            out(i, other).wait_send()
            if summed[i]:
                hand(i, other).wait_send()

    visit_others(line, z, finish)
    for i in range(count):
        own(i).wait()
        if summed[i]:
            hand(i, z).wait_send()


def to_tokens(arrays, summed, line, name, number):
    rows = arrays[0].shape[-2]
    count, sums = len(arrays), max(sum(summed), 1)
    sems = pltpu.SemaphoreType.DMA
    dtype = arrays[0].dtype
    held = (sums, line, rows, HD) if sum(summed) else (1, 1, 16, HD)
    return pl.pallas_call(
        functools.partial(to_tokens_kernel, line, summed),
        out_shape=[jax.ShapeDtypeStruct((rows, line * HD), dtype)] * count,
        in_specs=[pl.BlockSpec(memory_space=pl.ANY)] * count,
        out_specs=[pl.BlockSpec(memory_space=pl.ANY)] * count,
        scratch_shapes=[pltpu.VMEM(held, dtype)] * 2
        + [
            sems((count, line)),
            sems((count, line)),
            sems((2, sums, line)),
            sems((sums, line)),
            sems((count,)),
        ],
        compiler_params=pltpu.CompilerParams(collective_id=number, has_side_effects=True),
        name=name,
    )(*arrays)


KEY_TILE = 512


def masked_scores(keys, queries, tile, first, starts):
    scores = contract(keys, queries, 1, 1) * HD ** (-0.5)
    key_at = tile * KEY_TILE + lax.broadcasted_iota(jnp.int32, scores.shape, 0)
    query_at = first + lax.broadcasted_iota(jnp.int32, (1, scores.shape[1]), 1)
    return jnp.where((key_at >= starts) & (key_at <= query_at), scores, masked_score)


def attend_kernel(bounds, q_ref, k_ref, v_ref, start_ref, o_ref, total_ref):
    i = pl.program_id(0)
    queries, starts = q_ref[0], start_ref[0]
    span = queries.shape[0]

    def tile_step(tile, carry):
        largest, total, acc = carry
        rows = pl.ds(pl.multiple_of(tile * KEY_TILE, KEY_TILE), KEY_TILE)
        scores = masked_scores(k_ref[rows, :], queries, tile, bounds[2, i], starts)
        new = jnp.maximum(largest, jnp.max(scores, axis=0, keepdims=True))
        weights = jnp.exp(scores - new)
        fade = jnp.exp(largest - new)
        total = fade * total + jnp.sum(weights, axis=0, keepdims=True)
        acc = fade * acc + contract(v_ref[rows, :], weights.astype(jnp.bfloat16), 0, 0)
        return new, total, acc

    largest, total, acc = lax.fori_loop(
        bounds[0, i],
        bounds[1, i],
        tile_step,
        (
            jnp.full((1, span), masked_score, jnp.float32),
            jnp.zeros((1, span), jnp.float32),
            jnp.zeros((HD, span), jnp.float32),
        ),
    )
    o_ref[0] = (acc / total).T.astype(o_ref.dtype)
    total_ref[0] = largest + jnp.log(total)


def attend_back_kernel(
    bounds, q_ref, k_ref, v_ref, start_ref, total_ref, delta_ref, d_ref, dq_ref, dk_ref, dv_ref, dk, dv
):
    i = pl.program_id(0)
    queries, starts, grad = q_ref[0], start_ref[0], d_ref[0]
    total, delta = total_ref[0], delta_ref[0]

    @pl.when(i == 0)
    def _():
        dk[...] = jnp.zeros_like(dk)
        dv[...] = jnp.zeros_like(dv)

    def tile_step(tile, acc):
        rows = pl.ds(pl.multiple_of(tile * KEY_TILE, KEY_TILE), KEY_TILE)
        keys = k_ref[rows, :]
        scores = masked_scores(keys, queries, tile, bounds[2, i], starts)
        weights = jnp.exp(scores - total)
        grad_weights = contract(v_ref[rows, :], grad, 1, 1)
        grad_scores = (weights * (grad_weights - delta)).astype(jnp.bfloat16)
        dv[rows, :] += contract(weights.astype(jnp.bfloat16), grad, 1, 0)
        dk[rows, :] += contract(grad_scores, queries, 1, 0)
        return acc + contract(keys, grad_scores, 0, 0)

    acc = jnp.zeros((HD, queries.shape[0]), jnp.float32)
    acc = lax.fori_loop(bounds[0, i], bounds[1, i], tile_step, acc)
    dq_ref[0] = (acc * HD ** (-0.5)).T.astype(dq_ref.dtype)

    @pl.when(i == pl.num_programs(0) - 1)
    def _():
        dk_ref[...] = (dk[...] * HD ** (-0.5)).astype(dk_ref.dtype)
        dv_ref[...] = dv[...].astype(dv_ref.dtype)


def attend(bounds, queries, keys, values, starts):
    line, span, _ = queries.shape
    pack = keys.shape[0]
    block = pl.BlockSpec((1, span, HD), lambda i, _: (i, 0, 0))
    row = pl.BlockSpec((1, 1, span), lambda i, _: (i, 0, 0))
    whole = pl.BlockSpec((pack, HD), lambda i, _: (0, 0))
    return pl.pallas_call(
        attend_kernel,
        grid_spec=pltpu.PrefetchScalarGridSpec(
            num_scalar_prefetch=1,
            grid=(line,),
            in_specs=[block, whole, whole, row],
            out_specs=[block, row],
        ),
        out_shape=[
            jax.ShapeDtypeStruct(queries.shape, jnp.bfloat16),
            jax.ShapeDtypeStruct(starts.shape, jnp.float32),
        ],
        name="attend",
    )(bounds, queries, keys, values, starts)


def attend_back(bounds, queries, keys, values, starts, total, delta, grad):
    line, span, _ = queries.shape
    pack = keys.shape[0]
    block = pl.BlockSpec((1, span, HD), lambda i, _: (i, 0, 0))
    row = pl.BlockSpec((1, 1, span), lambda i, _: (i, 0, 0))
    whole = pl.BlockSpec((pack, HD), lambda i, _: (0, 0))
    return pl.pallas_call(
        attend_back_kernel,
        grid_spec=pltpu.PrefetchScalarGridSpec(
            num_scalar_prefetch=1,
            grid=(line,),
            in_specs=[block, whole, whole, row, row, row, block],
            out_specs=[block, whole, whole],
            scratch_shapes=[pltpu.VMEM((pack, HD), jnp.float32)] * 2,
        ),
        out_shape=[jax.ShapeDtypeStruct(queries.shape, jnp.bfloat16)]
        + [jax.ShapeDtypeStruct((pack, HD), jnp.bfloat16)] * 2,
        name="attend_back",
    )(bounds, queries, keys, values, starts, total, delta, grad)


def by_head(layout, line):
    positions = layout[1][0]
    pack = positions.shape[0]
    span = pack // (2 * line)
    core = lax.axis_index("expert") % 2
    starts = (jnp.arange(pack, dtype=jnp.int32) - positions).reshape(line, 2, 1, span)
    starts = lax.dynamic_index_in_dim(starts, core, 1, keepdims=False)
    first = (2 * jnp.arange(line, dtype=jnp.int32) + core) * span
    bounds = jnp.stack(
        [starts[:, 0, 0] // KEY_TILE, (first + span - 1) // KEY_TILE + 1, first]
    ).astype(jnp.int32)

    def forward(queries, keys, values):
        q, k, v = to_heads(
            [queries, keys, values], (False, True, True), line, "scatter_heads", 6
        )
        k, v = k.reshape(pack, HD), v.reshape(pack, HD)
        out, total = attend(bounds, q, k, v, starts)
        (attended,) = to_tokens([out], (False,), line, "gather_heads", 7)
        return attended, (q, k, v, out, total)

    def backward(kept, grad):
        q, k, v, out, total = kept
        (grad,) = to_heads([grad], (False,), line, "scatter_grads", 8)
        delta = jnp.sum(grad.astype(jnp.float32) * out.astype(jnp.float32), axis=-1)
        dq, dk, dv = attend_back(bounds, q, k, v, starts, total, delta[:, None, :], grad)
        shape = (line, 2, span, HD)
        return to_tokens(
            [dq, dk.reshape(shape), dv.reshape(shape)],
            (False, True, True),
            line,
            "gather_grads",
            9,
        )

    return forward, backward


def by_query(layout, offset_rows):
    segment = layout[0][0]
    pack = segment.shape[0]

    def heads(rows):
        return rows.reshape(rows.shape[0], -1, HD)

    def score_block(queries, keys):
        rows = queries.shape[0]
        scores = jnp.einsum("shd,lhd->hsl", queries, keys, preferred_element_type=jnp.float32)
        own = lax.dynamic_slice_in_dim(segment, offset_rows, rows, 0)
        query_places = offset_rows + jnp.arange(rows, dtype=jnp.int32)
        key_places = jnp.arange(pack, dtype=jnp.int32)
        allowed = (own[:, None] == segment[None, :]) & (
            key_places[None, :] <= query_places[:, None]
        )
        return jnp.where(allowed[None], scores * HD ** (-0.5), masked_score)

    def forward(queries, keys, values):
        q = heads(queries)
        k = heads(lax.all_gather(keys, "expert", axis=0, tiled=True))
        v = heads(lax.all_gather(values, "expert", axis=0, tiled=True))
        scores = score_block(q, k)
        largest = jnp.max(scores, axis=-1, keepdims=True)
        total = largest + jnp.log(jnp.sum(jnp.exp(scores - largest), axis=-1, keepdims=True))
        weights = jnp.exp(scores - total).astype(jnp.bfloat16)
        attended = jnp.einsum("hsl,lhd->shd", weights, v, preferred_element_type=jnp.float32)
        return attended.astype(jnp.bfloat16).reshape(queries.shape), (q, k, v, total)

    def backward(kept, grad):
        q, k, v, total = kept
        shape = grad.shape
        grad = heads(grad)
        weights = jnp.exp(score_block(q, k) - total)
        grad_weights = jnp.einsum("shd,lhd->hsl", grad, v, preferred_element_type=jnp.float32)
        delta = jnp.sum(weights * grad_weights, axis=-1, keepdims=True)
        grad_scores = (weights * (grad_weights - delta)).astype(jnp.bfloat16)
        dq = jnp.einsum("hsl,lhd->shd", grad_scores, k, preferred_element_type=jnp.float32)
        dk = jnp.einsum("hsl,shd->lhd", grad_scores, q, preferred_element_type=jnp.float32)
        weights = weights.astype(jnp.bfloat16)
        dv = jnp.einsum("hsl,shd->lhd", weights, grad, preferred_element_type=jnp.float32)

        def to_owner(part):
            part = part.astype(jnp.bfloat16).reshape(pack, shape[1])
            return lax.psum_scatter(part, "expert", scatter_dimension=0, tiled=True)

        scale = HD ** (-0.5)
        return (dq * scale).reshape(shape), to_owner(dk * scale), to_owner(dv)

    return forward, backward


def nearest(line, z, k):
    return ranked(line, z, k, lambda place, at: (abs(place - at), place))


def ranked(line, z, k, rank):
    total = jnp.int32(0)
    for at in range(line):
        order = sorted(range(line), key=lambda place: rank(place, at))
        place = sum([jnp.where(k == i, order[i], 0) for i in range(line)])
        total = total + jnp.where(z == at, place, 0)
    return total


def gate_act_kernel(
    line,
    x_ref,
    top_ref,
    wg_ref,
    wu_ref,
    wd_ref,
    xn_ref,
    grads_ref,
    scaled_ref,
    gates_ref,
    xbuf,
    top_buf,
    grads_buf,
    scaled_buf,
    gates_buf,
    sent,
    arrived,
    own_sem,
    top_sem,
    xn_sem,
    grads_sem,
    scaled_sem,
    gates_sem,
):
    dp, place = lax.axis_index("dp"), lax.axis_index("expert")
    z, c = place // 2, place % 2
    side_x, side_y = corners(dp)
    far = 3 - dp
    devices = (
        (dp, place + 2),
        (dp, place - 2),
        (side_x, place),
        (side_y, place),
        (dp, 2 * z + 1 - c),
    )
    up, down, along_x, along_y, pair = range(5)
    has_up, has_down = z < line - 1, z > 0
    for way in (along_x, along_y, pair):
        greet(devices[way])
    pl.when(has_up)(lambda: greet(devices[up]))
    pl.when(has_down)(lambda: greet(devices[down]))
    greeted = 3 + has_up.astype(jnp.int32) + has_down.astype(jnp.int32)
    pl.semaphore_wait(pltpu.get_barrier_semaphore(), greeted)
    local, width, units = wg_ref.shape
    rows = top_buf.shape[1]
    first = place * local

    def slot(corner, height, core):
        return corner * (2 * line) + 2 * height + core

    def copy(s, p, way, source=None):
        target = xbuf.at[s, p]
        return send(
            target if source is None else source,
            target,
            sent.at[s, p, way],
            arrived.at[s, p],
            devices[way],
        )

    def arrive(s, p):
        copy(s, p, pair).wait_recv()

    mine = slot(dp, z, c)
    for p in (0, 1):
        pltpu.make_async_copy(x_ref.at[p], xbuf.at[mine, p], own_sem.at[p]).start()
        pl.when(has_up)(lambda: copy(mine, p, up, x_ref.at[p]).start())
        pl.when(has_down)(lambda: copy(mine, p, down, x_ref.at[p]).start())
        for way in (along_x, along_y, pair):
            copy(mine, p, way, x_ref.at[p]).start()

    def decode(i):
        turn, j = i // 4, i % 4
        k = turn - (j > 0).astype(jnp.int32) - (j == 3).astype(jnp.int32)
        valid = (i >= 0) & (k >= 0) & (k < line)
        corner = jnp.where(j == 0, dp, jnp.where(j == 1, side_x, jnp.where(j == 2, side_y, far)))
        return j, k, valid, corner, nearest(line, z, k)

    def top_load(i, corner, height):
        block = corner * line + height
        return pltpu.make_async_copy(top_ref.at[block], top_buf.at[i % 2], top_sem.at[i % 2])

    def xn_out(block):
        return pltpu.make_async_copy(
            xbuf.at[pl.ds(2 * block, 2), :, :, pl.ds(0, width)],
            xn_ref.at[pl.ds(2 * block, 2)],
            xn_sem.at[block],
        )

    def grads_out(block):
        return pltpu.make_async_copy(grads_buf.at[block], grads_ref.at[block], grads_sem.at[block])

    def scaled_out(block):
        return pltpu.make_async_copy(
            scaled_buf.at[block], scaled_ref.at[block], scaled_sem.at[block]
        )

    def gates_out(block):
        return pltpu.make_async_copy(gates_buf.at[block], gates_ref.at[block], gates_sem.at[block])

    def compute(i):
        j, k, _, corner, height = decode(i)
        block = corner * line + height
        for p in (0, 1):
            arrive(slot(corner, height, 1 - c), p)
        xn_out(block).start()
        top_load(i, corner, height).wait()
        lanes = lax.broadcasted_iota(jnp.int32, (rows, 128), 1)

        def tokens():
            return xbuf[pl.ds(2 * block, 2), :, :, pl.ds(0, width)].reshape(rows, width)

        table = xbuf[pl.ds(2 * block, 2), :, :, pl.ds(width, 128)].reshape(rows, 128)
        table = table.astype(jnp.float32)
        gate_grads = jnp.zeros((rows, 128), jnp.float32)
        for e in range(local):
            at = (lanes == first + e) | (lanes == first + e + 64)
            gate = jnp.sum(jnp.where(at, table, 0.0), axis=1, keepdims=True)
            g = contract(tokens(), wg_ref[e], 1, 0)
            u = contract(tokens(), wu_ref[e], 1, 0)
            h = contract(top_buf[i % 2], wd_ref[e], 1, 1)
            sigmoid = 1.0 / (1.0 + jnp.exp(-g))
            silu = g * sigmoid
            act = silu * u
            gate_grad = jnp.sum(act * h, axis=1, keepdims=True)
            gate_grads = gate_grads + jnp.where(lanes == first + e, gate_grad, 0.0)
            grad_act = h * gate
            dg = grad_act * u * sigmoid * (1.0 + g * (1.0 - sigmoid))
            du = grad_act * silu
            scaled_buf[block, :, e * units : (e + 1) * units] = (act * gate).astype(jnp.bfloat16)
            grads_buf[block, :, e * units : (e + 1) * units] = dg.astype(jnp.bfloat16)
            at = (local + e) * units
            grads_buf[block, :, at : at + units] = du.astype(jnp.bfloat16)
        gates_buf[block] = gate_grads.astype(jnp.bfloat16)
        grads_out(block).start()
        scaled_out(block).start()
        gates_out(block).start()

    def step(i, carry):
        j, k, valid, corner, height = decode(i)
        s = slot(corner, height, c)

        def own():
            for p in (0, 1):
                pltpu.make_async_copy(x_ref.at[p], xbuf.at[mine, p], own_sem.at[p]).wait()

        def column():
            for p in (0, 1):
                arrive(s, p)
                pl.when(has_up & (height < z))(lambda: copy(s, p, up).start())
                pl.when(has_down & (height > z))(lambda: copy(s, p, down).start())
                for way in (along_x, along_y, pair):
                    copy(s, p, way).start()

        def sides():
            for p in (0, 1):
                arrive(s, p)
                copy(s, p, pair).start()
            pl.when(j == 1)(lambda: copy(s, 0, along_y).start())
            pl.when(j == 2)(lambda: copy(s, 1, along_x).start())

        def opposite():
            for p in (0, 1):
                arrive(s, p)
                copy(s, p, pair).start()

        pl.when(valid & (j == 0) & (k == 0))(own)
        pl.when(valid & (j == 0) & (k > 0))(column)
        pl.when(valid & ((j == 1) | (j == 2)))(sides)
        pl.when(valid & (j == 3))(opposite)
        pl.when(valid)(lambda: top_load(i, corner, height).start())
        pl.when(decode(i - 1)[2])(lambda: compute(i - 1))
        return carry

    lax.fori_loop(0, 4 * (line + 2) + 1, step, 0)

    def finish(height, carry):
        for p in (0, 1):
            for corner in range(4):
                copy(slot(corner, height, c), p, pair).wait_send()
            s = slot(dp, height, c)
            copy(s, p, along_x).wait_send()
            copy(s, p, along_y).wait_send()
            pl.when(has_up & (height <= z))(lambda: copy(s, p, up).wait_send())
            pl.when(has_down & (height >= z))(lambda: copy(s, p, down).wait_send())
        copy(slot(side_x, height, c), 0, along_y).wait_send()
        copy(slot(side_y, height, c), 1, along_x).wait_send()
        for corner in range(4):
            block = corner * line + height
            xn_out(block).wait()
            grads_out(block).wait()
            scaled_out(block).wait()
            gates_out(block).wait()
        return carry

    lax.fori_loop(0, line, finish, 0)


def gate_act(own, tops, w_gate, w_up, w_down, line):
    count, wide = own.shape
    local, width, units = w_gate.shape
    slots, blocks, rows, half = 8 * line, 4 * line, 2 * count, count // 2
    sems = pltpu.SemaphoreType.DMA
    dtype = own.dtype
    xn, grads, scaled, gates = pl.pallas_call(
        functools.partial(gate_act_kernel, line),
        out_shape=[
            jax.ShapeDtypeStruct((slots, 2, half, width), dtype),
            jax.ShapeDtypeStruct((blocks, rows, 2 * local * units), dtype),
            jax.ShapeDtypeStruct((blocks, rows, local * units), dtype),
            jax.ShapeDtypeStruct((blocks, rows, 128), dtype),
        ],
        in_specs=[
            pl.BlockSpec(memory_space=pltpu.VMEM),
            pl.BlockSpec(memory_space=pl.ANY),
            pl.BlockSpec(memory_space=pltpu.VMEM),
            pl.BlockSpec(memory_space=pltpu.VMEM),
            pl.BlockSpec(memory_space=pltpu.VMEM),
        ],
        out_specs=[pl.BlockSpec(memory_space=pl.ANY)] * 4,
        scratch_shapes=[
            pltpu.VMEM((slots, 2, half, wide), dtype),
            pltpu.VMEM((2, rows, width), dtype),
            pltpu.VMEM((blocks, rows, 2 * local * units), dtype),
            pltpu.VMEM((blocks, rows, local * units), dtype),
            pltpu.VMEM((blocks, rows, 128), dtype),
            sems((slots, 2, 5)),
            sems((slots, 2)),
            sems((2,)),
            sems((2,)),
            sems((blocks,)),
            sems((blocks,)),
            sems((blocks,)),
            sems((blocks,)),
        ],
        compiler_params=pltpu.CompilerParams(
            collective_id=1, has_side_effects=True, vmem_limit_bytes=60 << 20
        ),
        name="gate_act",
    )(own.reshape(2, half, wide), tops.reshape(blocks, rows, width), w_gate, w_up, w_down)
    return xn.reshape(slots * count, width), grads, scaled, gates


def product_sum_kernel(
    line,
    flipped,
    extra,
    grads,
    *refs,
):
    a_ref, w_ref = refs[0], refs[1]
    e_ref = refs[2] if extra else None
    refs = refs[3:] if extra else refs[2:]
    if grads:
        work_refs, refs = (*refs[:3], *refs[4:7], *refs[-12:]), (refs[3], *refs[7:-12])
    (
        out_ref,
        made,
        a_buf,
        e_buf,
        got_pair,
        got_x,
        got_y,
        got_far_x,
        got_far_y,
        got_below,
        got_above,
        load_sem,
        extra_sem,
        pair_sem,
        x_sem,
        y_sem,
        far_x_sem,
        far_y_sem,
        below_sem,
        above_sem,
    ) = refs
    dp, place = lax.axis_index("dp"), lax.axis_index("expert")
    z, c = place // 2, place % 2
    side_x, side_y = corners(dp)
    far = 3 - dp
    to_x, to_y, to_pair = (side_x, place), (side_y, place), (dp, 2 * z + 1 - c)
    to_up, to_down = (dp, place + 2), (dp, place - 2)
    for device in (to_x, to_y, to_pair):
        greet(device)
    pl.when(z > 0)(lambda: greet(to_down))
    pl.when(z < line - 1)(lambda: greet(to_up))
    greeted = 3 + (z > 0).astype(jnp.int32) + (z < line - 1).astype(jnp.int32)
    pl.semaphore_wait(pltpu.get_barrier_semaphore(), greeted)
    count = 4 * line
    width = w_ref.shape[0] if flipped else w_ref.shape[1]
    half = made.shape[4]
    chunk = 512

    def mine(q, height, p):
        return made.at[q, height, c, p]

    def hand(q, height, p):
        at = (q, height, p)
        source = made.at[q, height, 1 - c, p]
        return send(source, got_pair.at[at], pair_sem.at[0, *at], pair_sem.at[1, *at], to_pair)

    def along_x(height, p):
        at = (height, p)
        source = mine(side_x, height, p)
        return send(source, got_x.at[at], x_sem.at[0, *at], x_sem.at[1, *at], to_x)

    def along_y(height, p):
        at = (height, p)
        source = mine(side_y, height, p)
        return send(source, got_y.at[at], y_sem.at[0, *at], y_sem.at[1, *at], to_y)

    def far_x(height):
        source = mine(far, height, 0)
        return send(
            source, got_far_x.at[height], far_x_sem.at[0, height], far_x_sem.at[1, height], to_x
        )

    def far_y(height):
        source = mine(far, height, 1)
        return send(
            source, got_far_y.at[height], far_y_sem.at[0, height], far_y_sem.at[1, height], to_y
        )

    def climb(height, p):
        at = (height, p)
        source = mine(dp, height, p)
        return send(source, got_below.at[at], below_sem.at[0, *at], below_sem.at[1, *at], to_up)

    def descend(height, p):
        at = (height, p)
        source = mine(dp, height, p)
        return send(source, got_above.at[at], above_sem.at[0, *at], above_sem.at[1, *at], to_down)

    def decode(i):
        k, j = i // 4, i % 4
        q = jnp.where(j == 0, far, jnp.where(j == 1, side_x, jnp.where(j == 2, side_y, dp)))
        return k, j, q, farthest(line, z, k)

    def load(i):
        _, _, q, height = decode(i)
        return pltpu.make_async_copy(
            a_ref.at[q * line + height], a_buf.at[i % 2], load_sem.at[i % 2]
        )

    def load_extra(i):
        _, _, q, height = decode(i)
        return pltpu.make_async_copy(
            e_ref.at[q * line + height], e_buf.at[i % 2], extra_sem.at[i % 2]
        )

    def start_load(i):
        load(i).start()
        if extra:
            load_extra(i).start()

    def add(q, height, p, other):
        at = (q, height, c, p)
        made[at] = made[at] + other[...]

    def compute(i):
        _, _, q, height = decode(i)
        load(i).wait()
        if extra:
            load_extra(i).wait()
        pl.when(i + 1 < count)(lambda: start_load(i + 1))
        for at in range(0, width, chunk):
            if flipped:
                part = contract(a_buf[i % 2], w_ref[at : at + chunk, :], 1, 1)
            else:
                part = contract(a_buf[i % 2], w_ref[:, at : at + chunk], 1, 0)
            part = part.astype(made.dtype).reshape(2, 2, half, chunk)
            made[q, height, :, :, :, at : at + chunk] = part
        if extra:
            made[q, height, :, :, :, width : width + 128] = e_buf[i % 2].reshape(2, 2, half, 128)
        for p in (0, 1):
            hand(q, height, p).start()

    def settle(i):
        _, j, q, height = decode(i)
        for p in (0, 1):
            hand(q, height, p).wait_recv()
            add(q, height, p, got_pair.at[q, height, p])

        def opposite():
            far_x(height).start()
            far_y(height).start()

        def side_of_x():
            along_x(height, 0).start()
            far_y(height).wait_recv()
            add(side_x, height, 1, got_far_y.at[height])
            along_x(height, 1).start()

        def side_of_y():
            along_y(height, 1).start()
            far_x(height).wait_recv()
            add(side_y, height, 0, got_far_x.at[height])
            along_y(height, 0).start()

        pl.when(j == 0)(opposite)
        pl.when(j == 1)(side_of_x)
        pl.when(j == 2)(side_of_y)

    def column(height):
        for p in (0, 1):
            along_x(height, p).wait_recv()
            along_y(height, p).wait_recv()
            total = made[dp, height, c, p].astype(jnp.float32)
            total = total + got_x[height, p].astype(jnp.float32)
            total = total + got_y[height, p].astype(jnp.float32)
            made[dp, height, c, p] = total.astype(made.dtype)
            pl.when((z == 0) & (height > z))(lambda: climb(height, p).start())
            pl.when((z == line - 1) & (height < z))(lambda: descend(height, p).start())

    def pass_on(height):
        for p in (0, 1):

            def upwards():
                climb(height, p).wait_recv()
                add(dp, height, p, got_below.at[height, p])
                climb(height, p).start()

            def downwards():
                descend(height, p).wait_recv()
                add(dp, height, p, got_above.at[height, p])
                descend(height, p).start()

            pl.when((height > z) & (z > 0))(upwards)
            pl.when((height < z) & (z < line - 1))(downwards)

    start_load(0)
    work, work_end, turns = weight_grads(a_ref, *work_refs) if grads else (None, None, 1)

    def step(i, carry):
        k, j, _, _ = decode(i)
        pl.when(i < count)(lambda: compute(i))
        pl.when((i >= 1) & (i <= count))(lambda: settle(i - 1))
        if grads:
            every = count // turns
            pl.when((i < count) & (i % every == 0))(lambda: work(i // every))
        late = farthest(line, z, k - 2)
        pl.when((k >= 2) & (j == 0))(lambda: column(late))
        pl.when((k >= 2) & (j == 3))(lambda: pass_on(late))
        return carry

    lax.fori_loop(0, count + 8, step, 0)
    if grads:
        work_end()
    for p in (0, 1):
        out_ref[p] = made[dp, z, c, p].astype(jnp.float32)

        def from_below():
            climb(z, p).wait_recv()
            out_ref[p] = out_ref[p] + got_below[z, p].astype(jnp.float32)

        def from_above():
            descend(z, p).wait_recv()
            out_ref[p] = out_ref[p] + got_above[z, p].astype(jnp.float32)

        pl.when(z > 0)(from_below)
        pl.when(z < line - 1)(from_above)

    def finish(height, carry):
        far_x(height).wait_send()
        far_y(height).wait_send()
        for p in (0, 1):
            for q in range(4):
                hand(q, height, p).wait_send()
            along_x(height, p).wait_send()
            along_y(height, p).wait_send()
            pl.when(height > z)(lambda: climb(height, p).wait_send())
            pl.when(height < z)(lambda: descend(height, p).wait_send())
        return carry

    lax.fori_loop(0, line, finish, 0)


def weight_grads(
    scaled_ref,
    xn_ref,
    top_ref,
    units_ref,
    gate_ref,
    up_ref,
    down_ref,
    chunk_buf,
    units_buf,
    scaled_buf,
    total,
    both_out,
    down_out,
    chunk_sem,
    units_sem,
    scaled_sem,
    gate_sem,
    up_sem,
    down_sem,
):
    local, width, units = gate_ref.shape
    span = chunk_buf.shape[2]
    blocks, rows, _ = units_buf.shape
    step_blocks = max(1, min(blocks, 1024 // rows))
    turns = 2 * (width // span)

    def at(n):
        return pl.ds(pl.multiple_of(n // 2 * span, span), span)

    def chunk(n, source):
        return pltpu.make_async_copy(
            source.at[:, at(n)], chunk_buf.at[n % 2], chunk_sem.at[n % 2]
        )

    def start_chunk(n):
        pl.when(n % 2 == 0)(lambda: chunk(n, xn_ref).start())
        pl.when(n % 2 == 1)(lambda: chunk(n, top_ref).start())

    def both(n, e):
        gate = pltpu.make_async_copy(
            both_out.at[:, pl.ds(e * units, units)], gate_ref.at[e, at(n), :], gate_sem.at[e]
        )
        up = pltpu.make_async_copy(
            both_out.at[:, pl.ds((local + e) * units, units)],
            up_ref.at[e, at(n), :],
            up_sem.at[e],
        )
        return gate, up

    def down(n, e):
        return pltpu.make_async_copy(down_out.at[e], down_ref.at[e, :, at(n)], down_sem.at[e])

    units_load = pltpu.make_async_copy(units_ref, units_buf, units_sem.at[0])
    scaled_load = pltpu.make_async_copy(scaled_ref, scaled_buf, scaled_sem.at[0])
    start_chunk(0)
    units_load.start()
    scaled_load.start()

    def add_up(n, right, lanes):
        total[:, :lanes] = jnp.zeros((span, lanes), jnp.float32)

        def part(k, carry):
            depth = step_blocks * rows
            left = chunk_buf[n % 2, pl.ds(pl.multiple_of(k * depth, depth), depth), :]
            with_rows = right[pl.ds(k * step_blocks, step_blocks)].reshape(depth, lanes)
            total[:, :lanes] += contract(left, with_rows, 0, 0)
            return carry

        lax.fori_loop(0, blocks // step_blocks, part, 0)

    def turn(n):
        pl.when(n + 1 < turns)(lambda: start_chunk(n + 1))

        def even():
            chunk(n, xn_ref).wait()
            pl.when(n == 0)(units_load.wait)
            add_up(n, units_buf, 2 * local * units)

            @pl.when(n > 1)
            def _():
                for e in range(local):
                    for copy in both(n - 2, e):
                        copy.wait()

            both_out[...] = total[...].astype(both_out.dtype)
            for e in range(local):
                for copy in both(n, e):
                    copy.start()

        def odd():
            chunk(n, top_ref).wait()
            pl.when(n == 1)(scaled_load.wait)
            add_up(n, scaled_buf, local * units)

            @pl.when(n > 2)
            def _():
                for e in range(local):
                    down(n - 2, e).wait()

            for e in range(local):
                value = total[:, e * units : (e + 1) * units].T
                down_out[e] = value.astype(down_out.dtype)
                down(n, e).start()

        pl.when(n % 2 == 0)(even)
        pl.when(n % 2 == 1)(odd)

    def end():
        for e in range(local):
            for copy in both(turns - 2, e):
                copy.wait()
            down(turns - 1, e).wait()

    return turn, end, turns


def product_sum(blocks, weights, flipped, extra, line, name, number, grads=None):
    count, rows, depth = blocks.shape
    width = weights.shape[0] if flipped else weights.shape[1]
    wide = width + (0 if extra is None else 128)
    half = rows // 4
    sems = pltpu.SemaphoreType.DMA
    dtype = blocks.dtype

    def space(*shape):
        return pltpu.VMEM((*shape, half, wide), dtype)

    anywhere, inside = pl.BlockSpec(memory_space=pl.ANY), pl.BlockSpec(memory_space=pltpu.VMEM)
    out_shape = [jax.ShapeDtypeStruct((2, half, wide), jnp.float32)]
    work_in, work_space = [], []
    if grads is not None:
        xn, tops, both, shape = grads
        local, _, units = shape
        work_in, span = [xn, tops, both], 256
        up_down = [shape, shape, (local, units, width)]
        out_shape += [jax.ShapeDtypeStruct(each, dtype) for each in up_down]
        work_space = [
            pltpu.VMEM((2, xn.shape[0], span), dtype),
            pltpu.VMEM(both.shape, dtype),
            pltpu.VMEM(blocks.shape, dtype),
            pltpu.VMEM((span, both.shape[2]), jnp.float32),
            pltpu.VMEM((span, both.shape[2]), dtype),
            pltpu.VMEM((local, units, span), dtype),
            sems((2,)),
            sems((1,)),
            sems((1,)),
            sems((local,)),
            sems((local,)),
            sems((local,)),
        ]
    total, *work_out = pl.pallas_call(
        functools.partial(product_sum_kernel, line, flipped, extra is not None, grads is not None),
        out_shape=out_shape,
        in_specs=[anywhere, inside]
        + ([] if extra is None else [anywhere])
        + [anywhere] * len(work_in),
        out_specs=[inside] + [anywhere] * (len(out_shape) - 1),
        scratch_shapes=[
            space(4, line, 2, 2),
            pltpu.VMEM((2, rows, depth), dtype),
            pltpu.VMEM((2, rows, 128), dtype),
            space(4, line, 2),
            space(line, 2),
            space(line, 2),
            space(line),
            space(line),
            space(line, 2),
            space(line, 2),
            sems((2,)),
            sems((2,)),
            sems((2, 4, line, 2)),
            sems((2, line, 2)),
            sems((2, line, 2)),
            sems((2, line)),
            sems((2, line)),
            sems((2, line, 2)),
            sems((2, line, 2)),
            *work_space,
        ],
        compiler_params=pltpu.CompilerParams(
            collective_id=number, has_side_effects=True, vmem_limit_bytes=63 << 20
        ),
        name=name,
    )(blocks, weights, *([] if extra is None else [extra]), *work_in)
    return total.reshape(2 * half, wide), *work_out


def closing_kernel(
    line,
    shared_rows,
    parts_ref,
    first_ref,
    grad_ref,
    unit_ref,
    inverse_ref,
    gain_ref,
    output_ref,
    summed_ref,
    shared_ref,
    outputs_ref,
    grads_ref,
    acc,
    got_pair,
    got_below,
    got_above,
    part,
    got_x,
    got_y,
    got_far_x,
    got_far_y,
    grad_own,
    small,
    got_small,
    load_sem,
    pair_sem,
    below_sem,
    above_sem,
    part_sem,
    x_sem,
    y_sem,
    far_x_sem,
    far_y_sem,
    spread_sem,
    arrive_sem,
    own_sem,
    small_sem,
):
    dp, place = lax.axis_index("dp"), lax.axis_index("expert")
    z, c = place // 2, place % 2
    side_x, side_y = corners(dp)
    far = 3 - dp
    to_x, to_y, to_pair = (side_x, place), (side_y, place), (dp, 2 * z + 1 - c)
    to_up, to_down = (dp, place + 2), (dp, place - 2)
    for device in (to_x, to_y, to_pair):
        greet(device)
    pl.when(z > 0)(lambda: greet(to_down))
    pl.when(z < line - 1)(lambda: greet(to_up))
    greeted = 3 + (z > 0).astype(jnp.int32) + (z < line - 1).astype(jnp.int32)
    pl.semaphore_wait(pltpu.get_barrier_semaphore(), greeted)

    def load(height, p):
        return pltpu.make_async_copy(
            parts_ref.at[height, c, p], acc.at[height, p], load_sem.at[height, p]
        )

    def hand(height, p):
        at = (height, p)
        source = parts_ref.at[height, 1 - c, p]
        return send(source, got_pair.at[at], pair_sem.at[0, *at], pair_sem.at[1, *at], to_pair)

    def climb(height, p):
        at = (height, p)
        return send(
            acc.at[at], got_below.at[at], below_sem.at[0, *at], below_sem.at[1, *at], to_up
        )

    def descend(height, p):
        at = (height, p)
        return send(
            acc.at[at], got_above.at[at], above_sem.at[0, *at], above_sem.at[1, *at], to_down
        )

    def start(k, carry):
        height = farthest(line, z, k)
        for p in (0, 1):
            load(height, p).start()
            hand(height, p).start()
        return carry

    def pair_sum(k, carry):
        height = farthest(line, z, k)
        for p in (0, 1):
            load(height, p).wait()
            hand(height, p).wait_recv()
            acc[height, p] = acc[height, p] + got_pair[height, p]
            pl.when((z == 0) & (height > z))(lambda: climb(height, p).start())
            pl.when((z == line - 1) & (height < z))(lambda: descend(height, p).start())
        return carry

    def pass_on(k, carry):
        height = farthest(line, z, k)
        for p in (0, 1):

            def upwards():
                climb(height, p).wait_recv()
                acc[height, p] = acc[height, p] + got_below[height, p]
                climb(height, p).start()

            def downwards():
                descend(height, p).wait_recv()
                acc[height, p] = acc[height, p] + got_above[height, p]
                descend(height, p).start()

            pl.when((height > z) & (z > 0))(upwards)
            pl.when((height < z) & (z < line - 1))(downwards)
        return carry

    def first_load(q, p):
        return pltpu.make_async_copy(first_ref.at[q, p], part.at[q, p], part_sem.at[q, p])

    def along_x(p):
        return send(part.at[side_x, p], got_x.at[p], x_sem.at[0, p], x_sem.at[1, p], to_x)

    def along_y(p):
        return send(part.at[side_y, p], got_y.at[p], y_sem.at[0, p], y_sem.at[1, p], to_y)

    def far_x():
        return send(part.at[far, 0], got_far_x, far_x_sem.at[0], far_x_sem.at[1], to_x)

    def far_y():
        return send(part.at[far, 1], got_far_y, far_y_sem.at[0], far_y_sem.at[1], to_y)

    spreads = ((output_ref, outputs_ref), (grad_own, grads_ref))

    def spread(a, corner, p, way, source=None):
        target = spreads[a][1].at[corner, p]
        return send(
            target if source is None else source,
            target,
            spread_sem.at[a, corner, p, way],
            arrive_sem.at[a, corner, p],
            (to_x, to_y)[way],
        )

    def own_copy(a, p):
        return pltpu.make_async_copy(
            spreads[a][0].at[p], spreads[a][1].at[dp, p], own_sem.at[a, p]
        )

    def spread_own(a, p):
        own_copy(a, p).start()
        for way in (0, 1):
            spread(a, dp, p, way, spreads[a][0].at[p]).start()

    def spread_far(a):
        spread(a, side_x, 0, 0).wait_recv()
        spread(a, side_x, 0, 1).start()
        spread(a, side_y, 1, 0).wait_recv()
        spread(a, side_y, 1, 0).start()

    lax.fori_loop(0, 1, start, 0)
    for q in (far, side_x, side_y, dp):
        for p in (0, 1):
            first_load(q, p).start()
    lax.fori_loop(1, line, start, 0)
    for q in (far, side_x, side_y, dp):
        for p in (0, 1):
            first_load(q, p).wait()
    far_x().start()
    far_y().start()
    along_x(0).start()
    along_y(1).start()
    lax.fori_loop(0, 1, pair_sum, 0)
    far_x().wait_recv()
    part[side_y, 0] = part[side_y, 0] + got_far_x[...]
    along_y(0).start()
    far_y().wait_recv()
    part[side_x, 1] = part[side_x, 1] + got_far_y[...]
    along_x(1).start()
    for p in (0, 1):
        spread_own(0, p)
    lax.fori_loop(1, line, pair_sum, 0)
    for p in (0, 1):
        along_x(p).wait_recv()
        along_y(p).wait_recv()
        total = part[dp, p].astype(jnp.float32)
        total = total + got_x[p].astype(jnp.float32) + got_y[p].astype(jnp.float32)
        total = total * gain_ref[...]
        unit = unit_ref[p]
        mean = jnp.sum(total * unit, axis=1, keepdims=True) * (1.0 / unit.shape[1])
        rows = grad_ref[p] + inverse_ref[p] * (total - unit * mean)
        grad_own[p] = rows.astype(grad_own.dtype)
        spread_own(1, p)
    lax.fori_loop(0, 1, pass_on, 0)
    spread_far(0)
    lax.fori_loop(1, 2, pass_on, 0)
    spread_far(1)
    lax.fori_loop(2, line, pass_on, 0)
    for p in (0, 1):
        summed_ref[p] = acc[z, p].astype(jnp.float32)

        def from_below():
            climb(z, p).wait_recv()
            summed_ref[p] = summed_ref[p] + got_below[z, p].astype(jnp.float32)

        def from_above():
            descend(z, p).wait_recv()
            summed_ref[p] = summed_ref[p] + got_above[z, p].astype(jnp.float32)

        pl.when(z > 0)(from_below)
        pl.when(z < line - 1)(from_above)

    last = summed_ref.shape[1] - shared_rows
    for side, device in enumerate((to_x, to_y)):
        value = summed_ref[1, last:, :] if side == 0 else shared_ref[...]
        small[side] = value.astype(small.dtype)
        spread(side, side_x, 1, 0).wait_recv()
        spread(side, side_y, 0, 0).wait_recv()
        for p in (0, 1):
            spread(side, far, p, 0).wait_recv()
            for way in (0, 1):
                spread(side, dp, p, way).wait_send()
            own_copy(side, p).wait()
        spread(side, side_x, 0, 1).wait_send()
        spread(side, side_y, 1, 0).wait_send()
        exchange = send(
            small.at[side], got_small.at[side], small_sem.at[0, side], small_sem.at[1, side], device
        )
        exchange.start()
        exchange.wait_recv()
        shared_ref[...] = small[side].astype(jnp.float32) + got_small[side].astype(jnp.float32)
        exchange.wait_send()

    far_x().wait_send()
    far_y().wait_send()
    for p in (0, 1):
        along_x(p).wait_send()
        along_y(p).wait_send()

    def finish(height, carry):
        for p in (0, 1):
            hand(height, p).wait_send()
            pl.when(height > z)(lambda: climb(height, p).wait_send())
            pl.when(height < z)(lambda: descend(height, p).wait_send())
        return carry

    lax.fori_loop(0, line, finish, 0)


def closing(parts, first, grad, unit, inverse, gain, output, shared_rows, line):
    _, rows, wide = parts.shape
    own, width = output.shape
    high, half = rows // 2, own // 2
    sems = pltpu.SemaphoreType.DMA
    dtype = parts.dtype
    single = jnp.float32
    anywhere, inside = pl.BlockSpec(memory_space=pl.ANY), pl.BlockSpec(memory_space=pltpu.VMEM)
    everyone = jax.ShapeDtypeStruct((4, 2, half, width), dtype)
    summed, shared, outputs, grads = pl.pallas_call(
        functools.partial(closing_kernel, line, shared_rows),
        out_shape=[
            jax.ShapeDtypeStruct((2, high, wide), single),
            jax.ShapeDtypeStruct((shared_rows, wide), single),
            everyone,
            everyone,
        ],
        in_specs=[anywhere, anywhere] + [inside] * 5,
        out_specs=[inside, inside, anywhere, anywhere],
        scratch_shapes=[
            pltpu.VMEM((line, 2, high, wide), dtype),
            pltpu.VMEM((line, 2, high, wide), dtype),
            pltpu.VMEM((line, 2, high, wide), dtype),
            pltpu.VMEM((line, 2, high, wide), dtype),
            pltpu.VMEM((4, 2, half, width), dtype),
            pltpu.VMEM((2, half, width), dtype),
            pltpu.VMEM((2, half, width), dtype),
            pltpu.VMEM((half, width), dtype),
            pltpu.VMEM((half, width), dtype),
            pltpu.VMEM((2, half, width), dtype),
            pltpu.VMEM((2, shared_rows, wide), dtype),
            pltpu.VMEM((2, shared_rows, wide), dtype),
            sems((line, 2)),
            sems((2, line, 2)),
            sems((2, line, 2)),
            sems((2, line, 2)),
            sems((4, 2)),
            sems((2, 2)),
            sems((2, 2)),
            sems((2,)),
            sems((2,)),
            sems((2, 4, 2, 2)),
            sems((2, 4, 2)),
            sems((2, 2)),
            sems((2, 2)),
        ],
        compiler_params=pltpu.CompilerParams(
            collective_id=5, has_side_effects=True, vmem_limit_bytes=60 << 20
        ),
        name="closing",
    )(
        parts.reshape(line, 2, 2, high, wide),
        first.reshape(4, 2, half, width),
        grad.reshape(2, half, width),
        unit.reshape(2, half, width),
        inverse.reshape(2, half, 1),
        gain.reshape(1, width),
        output.reshape(2, half, width),
    )
    return (
        summed.reshape(rows, wide),
        shared,
        outputs.reshape(4 * own, width),
        grads.reshape(4 * own, width),
    )


def head_totals(first_sum, second_sum):
    return lax.psum((first_sum, second_sum), "dp")


def per_device(
    inputs,
    attention_norm_gain,
    w_query,
    w_key,
    w_value,
    w_out,
    q_gain,
    k_gain,
    expert_norm_gain,
    w_router,
    w_gate,
    w_up,
    w_down,
    routes,
    lengths,
    d_output,
):
    pack_count, seg_rows, model_width = inputs.shape
    local_width = w_query.shape[1]
    local_heads = local_width // HD
    experts = w_router.shape[1]
    groups = lax.axis_size("expert")
    line = groups // 2
    pack_span = seg_rows * groups
    local_experts = w_gate.shape[0]
    offset_rows = lax.axis_index("expert") * seg_rows
    segment, positions = doc_layout(lengths, pack_span)
    pos_query = lax.dynamic_slice_in_dim(positions, offset_rows, seg_rows, 1)
    cos_table, sin_table = rope_tables(pos_query, HD)
    head_shape = (pack_count, seg_rows, local_heads, HD)
    inputs_single_float = inputs.astype(jnp.float32)
    first_inverse_norm = lax.rsqrt(
        jnp.mean(inputs_single_float * inputs_single_float, axis=-1, keepdims=True) + epsilon
    )
    first_unit_input = inputs_single_float * first_inverse_norm
    first_normed_input = (first_unit_input * attention_norm_gain).astype(jnp.bfloat16)
    q_raw = jnp.dot(first_normed_input, w_query, preferred_element_type=jnp.float32)
    k_raw = jnp.dot(first_normed_input, w_key, preferred_element_type=jnp.float32)
    value_rows = jnp.dot(first_normed_input, w_value, preferred_element_type=jnp.float32).astype(
        jnp.bfloat16
    )
    q_sum, k_sum = head_totals(jnp.sum(q_raw * q_raw, axis=-1), jnp.sum(k_raw * k_raw, axis=-1))
    q_inv = lax.rsqrt(q_sum[..., None] / model_width + epsilon)
    k_inv = lax.rsqrt(k_sum[..., None] / model_width + epsilon)
    q_hat = q_raw * q_inv
    k_hat = k_raw * k_inv
    queries = rotate((q_hat * q_gain).reshape(head_shape), cos_table, sin_table).astype(
        jnp.bfloat16
    )
    key_rows = (
        rotate((k_hat * k_gain).reshape(head_shape), cos_table, sin_table)
        .astype(jnp.bfloat16)
        .reshape(pack_count, seg_rows, local_width)
    )
    layout = (segment, positions)
    if local_heads == line:
        attention = by_head(layout, line)
    else:
        attention = by_query(layout, offset_rows)
    attended, kept = attention[0](queries.reshape(seg_rows, local_width), key_rows[0], value_rows[0])
    attn_part = jnp.dot(
        attended, w_out, preferred_element_type=jnp.float32
    )
    own = lax.axis_index("dp")
    part_rows = seg_rows // lax.axis_size("dp")

    def own_rows(rows):
        return lax.dynamic_slice_in_dim(rows, own * part_rows, part_rows, 0)

    hidden_state = own_rows(inputs_single_float[0]) + scatter_dp(attn_part.astype(jnp.bfloat16))
    second_inverse_norm = lax.rsqrt(
        jnp.mean(hidden_state * hidden_state, axis=-1, keepdims=True) + epsilon
    )
    second_unit_input = hidden_state * second_inverse_norm
    second_normed_input = second_unit_input * expert_norm_gain
    router = jax.nn.softmax(
        jnp.dot(second_normed_input, w_router, precision=lax.Precision.HIGHEST), axis=-1
    )
    chosen = own_rows(routes[:, 0, :])
    expert_range = jnp.arange(experts, dtype=jnp.int32)
    named = jnp.any(chosen[:, :, None] == expert_range, axis=1)
    top_own = own_rows(d_output[0])
    top_all = lax.all_gather(top_own, ALL, axis=0, tiled=True)
    gate_table = jnp.where(named, router, 0.0)
    gate_high = gate_table.astype(jnp.bfloat16)
    gate_low = (gate_table - gate_high.astype(jnp.float32)).astype(jnp.bfloat16)
    widen = ((0, 0), (0, 64 - experts))
    own_tokens = jnp.concatenate(
        [
            second_normed_input.astype(jnp.bfloat16),
            jnp.pad(gate_high, widen),
            jnp.pad(gate_low, widen),
        ],
        axis=1,
    )
    xn_all, grad_units, scaled, gate_part = gate_act(
        own_tokens, top_all, w_gate, w_up, w_down, line
    )
    w_both = jnp.concatenate([*w_gate, *w_up], axis=1)
    (grad_tokens,) = product_sum(grad_units, w_both, True, gate_part, line, "grad_tokens", 4)
    moe_out, grad_gate, grad_up, grad_down = product_sum(
        scaled,
        w_down.reshape(-1, model_width),
        False,
        None,
        line,
        "expert_sum",
        2,
        (xn_all, top_all, grad_units, w_gate.shape),
    )
    output = (hidden_state + moe_out).astype(jnp.bfloat16)
    grad_xn_exp = grad_tokens[:, :model_width]
    gate_sums = grad_tokens[:, model_width : model_width + experts]
    grad_router_probs = jnp.where(named, gate_sums, 0.0)
    grad_logits = router * (
        grad_router_probs - jnp.sum(router * grad_router_probs, axis=-1, keepdims=True)
    )
    grad_second_normed_input = grad_xn_exp + jnp.einsum(
        "se,de->sd", grad_logits, w_router, precision=lax.Precision.HIGHEST
    )
    grad_router = jnp.einsum(
        "sd,se->de", second_normed_input, grad_logits, precision=lax.Precision.HIGHEST
    )
    grad_expert_norm_gain = jnp.sum(grad_second_normed_input * second_unit_input, axis=0)
    grad_second_unit_input = grad_second_normed_input * expert_norm_gain
    grad_hidden = top_own.astype(jnp.float32) + second_inverse_norm * (
        grad_second_unit_input
        - second_unit_input
        * jnp.mean(grad_second_unit_input * second_unit_input, axis=-1, keepdims=True)
    )
    grad_attn = gather_dp(grad_hidden.astype(jnp.bfloat16))
    grad_out = jnp.einsum("sk,sd->kd", attended, grad_attn, preferred_element_type=jnp.float32)
    grad_heads = jnp.einsum(
        "sd,kd->sk", grad_attn, w_out, preferred_element_type=jnp.float32
    ).astype(jnp.bfloat16)
    grad_queries, grad_keys, grad_values = attention[1](kept, grad_heads)
    grad_queries = grad_queries.astype(jnp.float32).reshape(head_shape)
    grad_q_normed = rotate(grad_queries, cos_table, -sin_table).reshape(
        pack_count, seg_rows, local_width
    )
    grad_k_normed = rotate(
        grad_keys.astype(jnp.float32).reshape(head_shape), cos_table, -sin_table).reshape(
        pack_count, seg_rows, local_width
    )
    grad_q_gain = jnp.sum(grad_q_normed * q_hat, axis=(0, 1))
    grad_k_gain = jnp.sum(grad_k_normed * k_hat, axis=(0, 1))
    grad_q_hat = grad_q_normed * q_gain
    grad_k_hat = grad_k_normed * k_gain
    q_dot, k_dot = head_totals(
        jnp.sum(grad_q_hat * q_hat, axis=-1), jnp.sum(grad_k_hat * k_hat, axis=-1)
    )
    grad_q_raw = (q_inv * (grad_q_hat - q_hat * q_dot[..., None] / model_width)).astype(
        jnp.bfloat16
    )
    grad_k_raw = (k_inv * (grad_k_hat - k_hat * k_dot[..., None] / model_width)).astype(
        jnp.bfloat16
    )
    grad_v_raw = grad_values.astype(jnp.bfloat16)[None]
    grad_heads_raw = jnp.concatenate([grad_q_raw[0], grad_k_raw[0], grad_v_raw[0]], axis=1)
    grad_projections = jnp.einsum(
        "sd,sk->dk", first_normed_input[0], grad_heads_raw, preferred_element_type=jnp.float32
    )
    grad_first_normed_input = jnp.einsum(
        "psk,dk->psd", grad_q_raw, w_query, preferred_element_type=jnp.float32
    )
    grad_first_normed_input = grad_first_normed_input + jnp.einsum(
        "psk,dk->psd", grad_k_raw, w_key, preferred_element_type=jnp.float32
    )
    grad_first_normed_input = grad_first_normed_input + jnp.einsum(
        "psk,dk->psd", grad_v_raw, w_value, preferred_element_type=jnp.float32
    )
    grad_attn_gain = jnp.sum(grad_first_normed_input[0] * first_unit_input[0], axis=0)
    wide = grad_projections.shape[1]
    small = jnp.concatenate(
        [
            grad_q_gain.reshape(groups, -1),
            grad_k_gain.reshape(groups, -1),
            grad_attn_gain.reshape(groups, -1),
            grad_expert_norm_gain.reshape(groups, -1),
            grad_router.reshape(groups, -1),
        ],
        axis=1,
    )
    small_rows = 32
    filled = small.shape[1]
    small = jnp.pad(small, ((0, 0), (0, small_rows * wide - filled)))
    parts = jnp.concatenate(
        [
            grad_projections.astype(jnp.bfloat16).reshape(groups, -1, wide),
            small.astype(jnp.bfloat16).reshape(groups, small_rows, wide),
        ],
        axis=1,
    )
    summed, shared, outputs, grad_input = closing(
        parts,
        grad_first_normed_input[0].astype(jnp.bfloat16),
        grad_hidden,
        own_rows(first_unit_input[0]),
        own_rows(first_inverse_norm[0]),
        attention_norm_gain,
        output,
        small_rows,
        line,
    )
    large_rows = summed.shape[0] - small_rows
    gain_size, norm_size = local_width // groups, model_width // groups
    own_gains = summed[large_rows:].reshape(-1)[: 2 * gain_size]
    shared = shared.reshape(-1)[2 * gain_size : filled]
    grad_out = lax.psum_scatter(
        grad_out.astype(jnp.bfloat16), "expert", scatter_dimension=0, tiled=True
    ).astype(jnp.float32)
    return (
        outputs[None],
        grad_input.astype(jnp.float32)[None],
        shared[:norm_size],
        summed[:large_rows, :local_width],
        summed[:large_rows, local_width : 2 * local_width],
        summed[:large_rows, 2 * local_width :],
        grad_out,
        own_gains[:gain_size],
        own_gains[gain_size:],
        shared[norm_size : 2 * norm_size],
        shared[2 * norm_size :].reshape(norm_size, experts),
        grad_gate.astype(jnp.float32),
        grad_up.astype(jnp.float32),
        grad_down.astype(jnp.float32),
    )


def solution(mesh):
    placed = (
        P(None, "expert", None),
        P(),
        P(None, "dp"),
        P(None, "dp"),
        P(None, "dp"),
        P("dp", None),
        P("dp"),
        P("dp"),
        P(),
        P(),
        P("expert", None, "dp"),
        P("expert", None, "dp"),
        P("expert", "dp", None),
        P("expert", None, None),
        P(),
        P(None, "expert", None),
    )
    return jax.shard_map(
        per_device,
        mesh=mesh,
        in_specs=placed,
        out_specs=(
            P(None, "expert", None),
            P(None, "expert", None),
            P("expert"),
            P("expert", "dp"),
            P("expert", "dp"),
            P("expert", "dp"),
            P(("dp", "expert"), None),
            P(("dp", "expert")),
            P(("dp", "expert")),
            P("expert"),
            P("expert", None),
            P("expert", None, "dp"),
            P("expert", None, "dp"),
            P("expert", "dp", None),
        ),
        check_vma=False,
    )
```

```python
import functools

import jax
import jax.numpy as jnp
from jax import lax
from jax.experimental import pallas as pl
from jax.experimental.pallas import tpu as pltpu
from jax.sharding import PartitionSpec as P

HD = 128


epsilon = 1e-05
rope_base = 10000.0
masked_score = -1e30


def doc_layout(lengths, pack_span):
    doc_ends = jnp.cumsum(lengths, axis=1)
    starts = doc_ends - lengths
    places = jnp.arange(pack_span, dtype=jnp.int32)
    segment = jnp.sum((places[None, :, None] >= doc_ends[:, None, :]).astype(jnp.int32), axis=2)
    member = segment[:, :, None] == jnp.arange(lengths.shape[1], dtype=jnp.int32)[None, None, :]
    begins = jnp.sum(jnp.where(member, starts[:, None, :], 0), axis=2)
    return (segment, places[None, :] - begins)


def rope_tables(positions, head_size):
    half_size = head_size // 2
    frequency = rope_base ** (-2.0 * jnp.arange(half_size, dtype=jnp.float32) / head_size)
    angles = positions.astype(jnp.float32)[..., None] * frequency
    return (jnp.cos(angles), jnp.sin(angles))


def rotate(heads_in, cos_table, sin_table):
    half_size = heads_in.shape[-1] // 2
    first_half = heads_in[..., :half_size]
    second_half = heads_in[..., half_size:]
    cos_head = cos_table[..., None, :]
    sin_head = sin_table[..., None, :]
    return jnp.concatenate(
        [
            first_half * cos_head - second_half * sin_head,
            second_half * cos_head + first_half * sin_head,
        ],
        axis=-1,
    )


ALL = ("dp", "expert")


DEVICES = pl.DeviceIdType.MESH


def greet(device):
    pl.semaphore_signal(
        pltpu.get_barrier_semaphore(), inc=1, device_id=device, device_id_type=DEVICES
    )


def send(source, target, send_sem, arrive_sem, device):
    return pltpu.make_async_remote_copy(
        src_ref=source,
        dst_ref=target,
        send_sem=send_sem,
        recv_sem=arrive_sem,
        device_id=device,
        device_id_type=DEVICES,
    )


def contract(a, b, a_dim, b_dim):
    return lax.dot_general(
        a, b, (((a_dim,), (b_dim,)), ((), ())), preferred_element_type=jnp.float32
    )


def corners(dp):
    return dp + 1 - 2 * (dp % 2), (dp + 2) % 4


def gather_square_kernel(x_ref, out_ref, sent, arrived, own_sem):
    dp, place = lax.axis_index("dp"), lax.axis_index("expert")
    side_x, side_y = corners(dp)
    devices = ((side_x, place), (side_y, place))
    for device in devices:
        greet(device)
    pl.semaphore_wait(pltpu.get_barrier_semaphore(), 2)

    def copy(corner, p, way, source=None):
        target = out_ref.at[corner, p]
        return send(
            target if source is None else source,
            target,
            sent.at[corner, p, way],
            arrived.at[corner, p],
            devices[way],
        )

    for p in (0, 1):
        pltpu.make_async_copy(x_ref.at[p], out_ref.at[dp, p], own_sem.at[p]).start()
        for way in (0, 1):
            copy(dp, p, way, x_ref.at[p]).start()
    copy(side_x, 0, 0).wait_recv()
    copy(side_x, 0, 1).start()
    copy(side_y, 0, 0).wait_recv()
    copy(side_x, 1, 0).wait_recv()
    copy(side_y, 1, 0).wait_recv()
    copy(side_y, 1, 0).start()
    for p in (0, 1):
        copy(3 - dp, p, 0).wait_recv()
        for way in (0, 1):
            copy(dp, p, way).wait_send()
        pltpu.make_async_copy(x_ref.at[p], out_ref.at[dp, p], own_sem.at[p]).wait()
    copy(side_x, 0, 1).wait_send()
    copy(side_y, 1, 0).wait_send()


def gather_dp(rows):
    count, width = rows.shape
    gathered = pl.pallas_call(
        gather_square_kernel,
        out_shape=jax.ShapeDtypeStruct((4, 2, count // 2, width), rows.dtype),
        in_specs=[pl.BlockSpec(memory_space=pltpu.VMEM)],
        out_specs=pl.BlockSpec(memory_space=pl.ANY),
        scratch_shapes=[
            pltpu.SemaphoreType.DMA((4, 2, 2)),
            pltpu.SemaphoreType.DMA((4, 2)),
            pltpu.SemaphoreType.DMA((2,)),
        ],
        compiler_params=pltpu.CompilerParams(collective_id=10, has_side_effects=True),
        name="gather_dp",
    )(rows.reshape(2, count // 2, width))
    return gathered.reshape(4 * count, width)


def farthest(line, z, k):
    return ranked(line, z, k, lambda place, at: (-abs(place - at), place))


def reduce_kernel(
    square,
    line,
    paired,
    x_ref,
    out_ref,
    acc,
    got_pair,
    got_x,
    got_y,
    got_far_x,
    got_far_y,
    got_below,
    got_above,
    load_sem,
    pair_sem,
    x_sem,
    y_sem,
    far_x_sem,
    far_y_sem,
    below_sem,
    above_sem,
):
    dp, place = lax.axis_index("dp"), lax.axis_index("expert")
    z, c = place // 2, place % 2
    side_x, side_y = corners(dp)
    core = c if paired else 0
    own = dp if square else 0
    quarters = (3 - dp, side_x, side_y, dp) if square else (0,)
    to_x, to_y = (side_x, place), (side_y, place)
    to_pair, to_up, to_down = (dp, 2 * z + 1 - c), (dp, place + 2), (dp, place - 2)
    greeted = 0
    if square:
        greet(to_x)
        greet(to_y)
        greeted += 2
    if paired:
        greet(to_pair)
        greeted += 1
    if line > 1:
        pl.when(z > 0)(lambda: greet(to_down))
        pl.when(z < line - 1)(lambda: greet(to_up))
        greeted = greeted + (z > 0).astype(jnp.int32) + (z < line - 1).astype(jnp.int32)
    pl.semaphore_wait(pltpu.get_barrier_semaphore(), greeted)

    def load(q, height, p):
        return pltpu.make_async_copy(
            x_ref.at[q, height, core, p], acc.at[q, height, p], load_sem.at[q, height, p]
        )

    def hand(q, height, p):
        at = (q, height, p)
        source = x_ref.at[q, height, 1 - core, p]
        return send(source, got_pair.at[at], pair_sem.at[0, *at], pair_sem.at[1, *at], to_pair)

    def along_x(height, p):
        at = (height, p)
        return send(
            acc.at[side_x, height, p], got_x.at[at], x_sem.at[0, *at], x_sem.at[1, *at], to_x
        )

    def along_y(height, p):
        at = (height, p)
        return send(
            acc.at[side_y, height, p], got_y.at[at], y_sem.at[0, *at], y_sem.at[1, *at], to_y
        )

    def far_x(height):
        return send(
            acc.at[3 - dp, height, 0],
            got_far_x.at[height],
            far_x_sem.at[0, height],
            far_x_sem.at[1, height],
            to_x,
        )

    def far_y(height):
        return send(
            acc.at[3 - dp, height, 1],
            got_far_y.at[height],
            far_y_sem.at[0, height],
            far_y_sem.at[1, height],
            to_y,
        )

    def climb(height, p):
        at = (height, p)
        return send(
            acc.at[own, height, p], got_below.at[at], below_sem.at[0, *at], below_sem.at[1, *at], to_up
        )

    def descend(height, p):
        at = (height, p)
        return send(
            acc.at[own, height, p],
            got_above.at[at],
            above_sem.at[0, *at],
            above_sem.at[1, *at],
            to_down,
        )

    def height_of(k):
        return farthest(line, z, k) if line > 1 else 0

    def start(k, carry):
        for q in quarters:
            for p in (0, 1):
                load(q, height_of(k), p).start()
                if paired:
                    hand(q, height_of(k), p).start()
        return carry

    lax.fori_loop(0, line, start, 0)

    def step(k, carry):
        def cores():
            height = height_of(k)
            for q in quarters:
                for p in (0, 1):
                    load(q, height, p).wait()
                    if paired:
                        hand(q, height, p).wait_recv()
                        acc[q, height, p] = acc[q, height, p] + got_pair[q, height, p]
                if square and q is quarters[0]:
                    far_x(height).start()
                    far_y(height).start()

        def sides():
            height = height_of(k - 1)
            along_x(height, 0).start()
            along_y(height, 1).start()
            far_x(height).wait_recv()
            acc[side_y, height, 0] = acc[side_y, height, 0] + got_far_x[height]
            along_y(height, 0).start()
            far_y(height).wait_recv()
            acc[side_x, height, 1] = acc[side_x, height, 1] + got_far_y[height]
            along_x(height, 1).start()

        def column():
            height = height_of(k - 2)
            for p in (0, 1):
                if square:
                    along_x(height, p).wait_recv()
                    along_y(height, p).wait_recv()
                    total = acc[own, height, p].astype(jnp.float32)
                    total = total + got_x[height, p].astype(jnp.float32)
                    total = total + got_y[height, p].astype(jnp.float32)
                    acc[own, height, p] = total.astype(acc.dtype)
                if line > 1:
                    pl.when((z == 0) & (height > z))(lambda: climb(height, p).start())
                    pl.when((z == line - 1) & (height < z))(lambda: descend(height, p).start())

        def pass_on():
            height = height_of(k - 3)
            for p in (0, 1):

                def upwards():
                    climb(height, p).wait_recv()
                    acc[own, height, p] = acc[own, height, p] + got_below[height, p]
                    climb(height, p).start()

                def downwards():
                    descend(height, p).wait_recv()
                    acc[own, height, p] = acc[own, height, p] + got_above[height, p]
                    descend(height, p).start()

                pl.when((height > z) & (z > 0))(upwards)
                pl.when((height < z) & (z < line - 1))(downwards)

        pl.when(k < line)(cores)
        if square:
            pl.when((k >= 1) & (k < line + 1))(sides)
        pl.when((k >= 2) & (k < line + 2))(column)
        if line > 1:
            pl.when(k >= 3)(pass_on)
        return carry

    lax.fori_loop(0, line + (3 if line > 1 else 2), step, 0)
    home = z if line > 1 else 0
    for p in (0, 1):
        out_ref[p] = acc[own, home, p].astype(jnp.float32)
        if line > 1:

            def from_below():
                climb(z, p).wait_recv()
                out_ref[p] = out_ref[p] + got_below[z, p].astype(jnp.float32)

            def from_above():
                descend(z, p).wait_recv()
                out_ref[p] = out_ref[p] + got_above[z, p].astype(jnp.float32)

            pl.when(z > 0)(from_below)
            pl.when(z < line - 1)(from_above)

    def finish(height, carry):
        if square:
            far_x(height).wait_send()
            far_y(height).wait_send()
        for p in (0, 1):
            if paired:
                for q in quarters:
                    hand(q, height, p).wait_send()
            if square:
                along_x(height, p).wait_send()
                along_y(height, p).wait_send()
            if line > 1:
                pl.when(height > z)(lambda: climb(height, p).wait_send())
                pl.when(height < z)(lambda: descend(height, p).wait_send())
        return carry

    lax.fori_loop(0, line, finish, 0)


def reduce_to(parts, square, line, paired, name, number):
    _, rows, width = parts.shape
    quarters, cores, half = (4 if square else 1), (2 if paired else 1), rows // 2

    def space(used, *shape):
        return pltpu.VMEM((*shape, half, width) if used else (*shape, 16, 128), parts.dtype)

    sems = pltpu.SemaphoreType.DMA
    total = pl.pallas_call(
        functools.partial(reduce_kernel, square, line, paired),
        out_shape=jax.ShapeDtypeStruct((2, half, width), jnp.float32),
        in_specs=[pl.BlockSpec(memory_space=pl.ANY)],
        out_specs=pl.BlockSpec(memory_space=pltpu.VMEM),
        scratch_shapes=[
            space(True, quarters, line, 2),
            space(paired, quarters, line, 2),
            space(square, line, 2),
            space(square, line, 2),
            space(square, line),
            space(square, line),
            space(line > 1, line, 2),
            space(line > 1, line, 2),
            sems((quarters, line, 2)),
            sems((2, quarters, line, 2)),
            sems((2, line, 2)),
            sems((2, line, 2)),
            sems((2, line)),
            sems((2, line)),
            sems((2, line, 2)),
            sems((2, line, 2)),
        ],
        compiler_params=pltpu.CompilerParams(
            collective_id=number, has_side_effects=True, vmem_limit_bytes=60 << 20
        ),
        name=name,
    )(parts.reshape(quarters, line, cores, 2, half, width))
    return total.reshape(rows, width)


def scatter_dp(rows):
    return reduce_to(rows.reshape(4, -1, rows.shape[1]), True, 1, False, "scatter_dp", 3)


def visit_others(line, z, visit):
    def turn(k, carry):
        visit((z + k) % line)
        return carry

    lax.fori_loop(1, line, turn, 0)


def greet_line(line, dp, z, c):
    visit_others(line, z, lambda other: greet((dp, 2 * other + c)))
    greet((dp, 2 * z + 1 - c))
    pl.semaphore_wait(pltpu.get_barrier_semaphore(), line)


def columns(z):
    return pl.ds(pl.multiple_of(z * HD, HD), HD)


def to_heads_kernel(line, shared, *refs):
    count = len(shared)
    ins, outs = refs[:count], refs[count : 2 * count]
    sent, arrived, pair_sent, pair_arrived, own_sem = refs[2 * count :]
    dp, place = lax.axis_index("dp"), lax.axis_index("expert")
    z, c = place // 2, place % 2
    pair = (dp, 2 * z + 1 - c)
    greet_line(line, dp, z, c)

    def block(i, origin):
        return outs[i].at[origin, c] if shared[i] else outs[i].at[origin]

    def out(i, other):
        source = ins[i].at[:, columns(other)]
        device = (dp, 2 * other + c)
        return send(source, block(i, z), sent.at[i, other], arrived.at[i, z], device)

    def into(i, origin):
        part = block(i, origin)
        return send(part, part, sent.at[i, origin], arrived.at[i, origin], pair)

    def share(i, origin, source=None):
        part = block(i, origin)
        return send(
            part if source is None else source,
            part,
            pair_sent.at[i, origin],
            pair_arrived.at[i, origin],
            pair,
        )

    def own(i):
        return pltpu.make_async_copy(ins[i].at[:, columns(z)], block(i, z), own_sem.at[i])

    def dispatch(other):
        for i in range(count):
            out(i, other).start()

    visit_others(line, z, dispatch)
    for i in range(count):
        own(i).start()
        if shared[i]:
            share(i, z, ins[i].at[:, columns(z)]).start()

    def receive(origin):
        for i in range(count):
            into(i, origin).wait_recv()
            if shared[i]:
                share(i, origin).start()

    visit_others(line, z, receive)

    def finish(other):
        for i in range(count):
            out(i, other).wait_send()

    visit_others(line, z, finish)
    for i in range(count):
        own(i).wait()
        if shared[i]:

            def settle(origin, carry):
                share(i, origin).wait()
                return carry

            lax.fori_loop(0, line, settle, 0)


def to_heads(arrays, shared, line, name, number):
    rows = arrays[0].shape[0]
    count = len(arrays)
    sems = pltpu.SemaphoreType.DMA
    return pl.pallas_call(
        functools.partial(to_heads_kernel, line, shared),
        out_shape=[
            jax.ShapeDtypeStruct((line, 2, rows, HD) if both else (line, rows, HD), array.dtype)
            for array, both in zip(arrays, shared)
        ],
        in_specs=[pl.BlockSpec(memory_space=pltpu.VMEM)] * count,
        out_specs=[pl.BlockSpec(memory_space=pl.ANY)] * count,
        scratch_shapes=[sems((count, line))] * 4 + [sems((count,))],
        compiler_params=pltpu.CompilerParams(collective_id=number, has_side_effects=True),
        name=name,
    )(*arrays)


def to_tokens_kernel(line, summed, *refs):
    count, sums = len(summed), sum(summed)
    ins, outs = refs[:count], refs[count : 2 * count]
    mine, theirs = refs[2 * count : 2 * count + 2]
    sent, arrived, pair_sem, load_sem, own_sem = refs[2 * count + 2 :]
    dp, place = lax.axis_index("dp"), lax.axis_index("expert")
    z, c = place // 2, place % 2
    pair = (dp, 2 * z + 1 - c)
    greet_line(line, dp, z, c)
    at_sum = [sum(summed[:i]) for i in range(count)]

    def load(i, other):
        return pltpu.make_async_copy(
            ins[i].at[other, c], mine.at[at_sum[i], other], load_sem.at[at_sum[i], other]
        )

    def hand(i, other):
        s = at_sum[i]
        return send(
            ins[i].at[other, 1 - c],
            theirs.at[s, other],
            pair_sem.at[0, s, other],
            pair_sem.at[1, s, other],
            pair,
        )

    def source(i, other):
        return mine.at[at_sum[i], other] if summed[i] else ins[i].at[other]

    def out(i, other):
        target = outs[i].at[:, columns(z)]
        device = (dp, 2 * other + c)
        return send(source(i, other), target, sent.at[i, other], arrived.at[i, z], device)

    def into(i, origin):
        part = outs[i].at[:, columns(origin)]
        return send(part, part, sent.at[i, origin], arrived.at[i, origin], pair)

    def own(i):
        return pltpu.make_async_copy(source(i, z), outs[i].at[:, columns(z)], own_sem.at[i])

    def prepare(other):
        for i in range(count):
            if summed[i]:
                load(i, other).start()
                hand(i, other).start()

    def add(i, other):
        if summed[i]:
            load(i, other).wait()
            hand(i, other).wait_recv()
            s = at_sum[i]
            mine[s, other] = mine[s, other] + theirs[s, other]

    def dispatch(other):
        for i in range(count):
            add(i, other)
            out(i, other).start()

    if sums:
        visit_others(line, z, prepare)
        prepare(z)
    visit_others(line, z, dispatch)
    for i in range(count):
        add(i, z)
        own(i).start()

    def finish(other):
        for i in range(count):
            into(i, other).wait_recv()
            out(i, other).wait_send()
            if summed[i]:
                hand(i, other).wait_send()

    visit_others(line, z, finish)
    for i in range(count):
        own(i).wait()
        if summed[i]:
            hand(i, z).wait_send()


def to_tokens(arrays, summed, line, name, number):
    rows = arrays[0].shape[-2]
    count, sums = len(arrays), max(sum(summed), 1)
    sems = pltpu.SemaphoreType.DMA
    dtype = arrays[0].dtype
    held = (sums, line, rows, HD) if sum(summed) else (1, 1, 16, HD)
    return pl.pallas_call(
        functools.partial(to_tokens_kernel, line, summed),
        out_shape=[jax.ShapeDtypeStruct((rows, line * HD), dtype)] * count,
        in_specs=[pl.BlockSpec(memory_space=pl.ANY)] * count,
        out_specs=[pl.BlockSpec(memory_space=pl.ANY)] * count,
        scratch_shapes=[pltpu.VMEM(held, dtype)] * 2
        + [
            sems((count, line)),
            sems((count, line)),
            sems((2, sums, line)),
            sems((sums, line)),
            sems((count,)),
        ],
        compiler_params=pltpu.CompilerParams(collective_id=number, has_side_effects=True),
        name=name,
    )(*arrays)


KEY_TILE = 512


def masked_scores(keys, queries, tile, first, starts):
    scores = contract(keys, queries, 1, 1) * HD ** (-0.5)
    key_at = tile * KEY_TILE + lax.broadcasted_iota(jnp.int32, scores.shape, 0)
    query_at = first + lax.broadcasted_iota(jnp.int32, (1, scores.shape[1]), 1)
    return jnp.where((key_at >= starts) & (key_at <= query_at), scores, masked_score)


def attend_kernel(bounds, q_ref, k_ref, v_ref, start_ref, o_ref, total_ref):
    i = pl.program_id(0)
    queries, starts = q_ref[0], start_ref[0]
    span = queries.shape[0]

    def tile_step(tile, carry):
        largest, total, acc = carry
        rows = pl.ds(pl.multiple_of(tile * KEY_TILE, KEY_TILE), KEY_TILE)
        scores = masked_scores(k_ref[rows, :], queries, tile, bounds[2, i], starts)
        new = jnp.maximum(largest, jnp.max(scores, axis=0, keepdims=True))
        weights = jnp.exp(scores - new)
        fade = jnp.exp(largest - new)
        total = fade * total + jnp.sum(weights, axis=0, keepdims=True)
        acc = fade * acc + contract(v_ref[rows, :], weights.astype(jnp.bfloat16), 0, 0)
        return new, total, acc

    largest, total, acc = lax.fori_loop(
        bounds[0, i],
        bounds[1, i],
        tile_step,
        (
            jnp.full((1, span), masked_score, jnp.float32),
            jnp.zeros((1, span), jnp.float32),
            jnp.zeros((HD, span), jnp.float32),
        ),
    )
    o_ref[0] = (acc / total).T.astype(o_ref.dtype)
    total_ref[0] = largest + jnp.log(total)


def attend_back_kernel(
    bounds, q_ref, k_ref, v_ref, start_ref, total_ref, delta_ref, d_ref, dq_ref, dk_ref, dv_ref, dk, dv
):
    i = pl.program_id(0)
    queries, starts, grad = q_ref[0], start_ref[0], d_ref[0]
    total, delta = total_ref[0], delta_ref[0]

    @pl.when(i == 0)
    def _():
        dk[...] = jnp.zeros_like(dk)
        dv[...] = jnp.zeros_like(dv)

    def tile_step(tile, acc):
        rows = pl.ds(pl.multiple_of(tile * KEY_TILE, KEY_TILE), KEY_TILE)
        keys = k_ref[rows, :]
        scores = masked_scores(keys, queries, tile, bounds[2, i], starts)
        weights = jnp.exp(scores - total)
        grad_weights = contract(v_ref[rows, :], grad, 1, 1)
        grad_scores = (weights * (grad_weights - delta)).astype(jnp.bfloat16)
        dv[rows, :] += contract(weights.astype(jnp.bfloat16), grad, 1, 0)
        dk[rows, :] += contract(grad_scores, queries, 1, 0)
        return acc + contract(keys, grad_scores, 0, 0)

    acc = jnp.zeros((HD, queries.shape[0]), jnp.float32)
    acc = lax.fori_loop(bounds[0, i], bounds[1, i], tile_step, acc)
    dq_ref[0] = (acc * HD ** (-0.5)).T.astype(dq_ref.dtype)

    @pl.when(i == pl.num_programs(0) - 1)
    def _():
        dk_ref[...] = (dk[...] * HD ** (-0.5)).astype(dk_ref.dtype)
        dv_ref[...] = dv[...].astype(dv_ref.dtype)


def attend(bounds, queries, keys, values, starts):
    line, span, _ = queries.shape
    pack = keys.shape[0]
    block = pl.BlockSpec((1, span, HD), lambda i, _: (i, 0, 0))
    row = pl.BlockSpec((1, 1, span), lambda i, _: (i, 0, 0))
    whole = pl.BlockSpec((pack, HD), lambda i, _: (0, 0))
    return pl.pallas_call(
        attend_kernel,
        grid_spec=pltpu.PrefetchScalarGridSpec(
            num_scalar_prefetch=1,
            grid=(line,),
            in_specs=[block, whole, whole, row],
            out_specs=[block, row],
        ),
        out_shape=[
            jax.ShapeDtypeStruct(queries.shape, jnp.bfloat16),
            jax.ShapeDtypeStruct(starts.shape, jnp.float32),
        ],
        name="attend",
    )(bounds, queries, keys, values, starts)


def attend_back(bounds, queries, keys, values, starts, total, delta, grad):
    line, span, _ = queries.shape
    pack = keys.shape[0]
    block = pl.BlockSpec((1, span, HD), lambda i, _: (i, 0, 0))
    row = pl.BlockSpec((1, 1, span), lambda i, _: (i, 0, 0))
    whole = pl.BlockSpec((pack, HD), lambda i, _: (0, 0))
    return pl.pallas_call(
        attend_back_kernel,
        grid_spec=pltpu.PrefetchScalarGridSpec(
            num_scalar_prefetch=1,
            grid=(line,),
            in_specs=[block, whole, whole, row, row, row, block],
            out_specs=[block, whole, whole],
            scratch_shapes=[pltpu.VMEM((pack, HD), jnp.float32)] * 2,
        ),
        out_shape=[jax.ShapeDtypeStruct(queries.shape, jnp.bfloat16)]
        + [jax.ShapeDtypeStruct((pack, HD), jnp.bfloat16)] * 2,
        name="attend_back",
    )(bounds, queries, keys, values, starts, total, delta, grad)


def by_head(layout, line):
    positions = layout[1][0]
    pack = positions.shape[0]
    span = pack // (2 * line)
    core = lax.axis_index("expert") % 2
    starts = (jnp.arange(pack, dtype=jnp.int32) - positions).reshape(line, 2, 1, span)
    starts = lax.dynamic_index_in_dim(starts, core, 1, keepdims=False)
    first = (2 * jnp.arange(line, dtype=jnp.int32) + core) * span
    bounds = jnp.stack(
        [starts[:, 0, 0] // KEY_TILE, (first + span - 1) // KEY_TILE + 1, first]
    ).astype(jnp.int32)

    def forward(queries, keys, values):
        q, k, v = to_heads(
            [queries, keys, values], (False, True, True), line, "scatter_heads", 6
        )
        k, v = k.reshape(pack, HD), v.reshape(pack, HD)
        out, total = attend(bounds, q, k, v, starts)
        (attended,) = to_tokens([out], (False,), line, "gather_heads", 7)
        return attended, (q, k, v, out, total)

    def backward(kept, grad):
        q, k, v, out, total = kept
        (grad,) = to_heads([grad], (False,), line, "scatter_grads", 8)
        delta = jnp.sum(grad.astype(jnp.float32) * out.astype(jnp.float32), axis=-1)
        dq, dk, dv = attend_back(bounds, q, k, v, starts, total, delta[:, None, :], grad)
        shape = (line, 2, span, HD)
        return to_tokens(
            [dq, dk.reshape(shape), dv.reshape(shape)],
            (False, True, True),
            line,
            "gather_grads",
            9,
        )

    return forward, backward


def by_query(layout, offset_rows):
    segment = layout[0][0]
    pack = segment.shape[0]

    def heads(rows):
        return rows.reshape(rows.shape[0], -1, HD)

    def score_block(queries, keys):
        rows = queries.shape[0]
        scores = jnp.einsum("shd,lhd->hsl", queries, keys, preferred_element_type=jnp.float32)
        own = lax.dynamic_slice_in_dim(segment, offset_rows, rows, 0)
        query_places = offset_rows + jnp.arange(rows, dtype=jnp.int32)
        key_places = jnp.arange(pack, dtype=jnp.int32)
        allowed = (own[:, None] == segment[None, :]) & (
            key_places[None, :] <= query_places[:, None]
        )
        return jnp.where(allowed[None], scores * HD ** (-0.5), masked_score)

    def forward(queries, keys, values):
        q = heads(queries)
        k = heads(lax.all_gather(keys, "expert", axis=0, tiled=True))
        v = heads(lax.all_gather(values, "expert", axis=0, tiled=True))
        scores = score_block(q, k)
        largest = jnp.max(scores, axis=-1, keepdims=True)
        total = largest + jnp.log(jnp.sum(jnp.exp(scores - largest), axis=-1, keepdims=True))
        weights = jnp.exp(scores - total).astype(jnp.bfloat16)
        attended = jnp.einsum("hsl,lhd->shd", weights, v, preferred_element_type=jnp.float32)
        return attended.astype(jnp.bfloat16).reshape(queries.shape), (q, k, v, total)

    def backward(kept, grad):
        q, k, v, total = kept
        shape = grad.shape
        grad = heads(grad)
        weights = jnp.exp(score_block(q, k) - total)
        grad_weights = jnp.einsum("shd,lhd->hsl", grad, v, preferred_element_type=jnp.float32)
        delta = jnp.sum(weights * grad_weights, axis=-1, keepdims=True)
        grad_scores = (weights * (grad_weights - delta)).astype(jnp.bfloat16)
        dq = jnp.einsum("hsl,lhd->shd", grad_scores, k, preferred_element_type=jnp.float32)
        dk = jnp.einsum("hsl,shd->lhd", grad_scores, q, preferred_element_type=jnp.float32)
        weights = weights.astype(jnp.bfloat16)
        dv = jnp.einsum("hsl,shd->lhd", weights, grad, preferred_element_type=jnp.float32)

        def to_owner(part):
            part = part.astype(jnp.bfloat16).reshape(pack, shape[1])
            return lax.psum_scatter(part, "expert", scatter_dimension=0, tiled=True)

        scale = HD ** (-0.5)
        return (dq * scale).reshape(shape), to_owner(dk * scale), to_owner(dv)

    return forward, backward


def nearest(line, z, k):
    return ranked(line, z, k, lambda place, at: (abs(place - at), place))


def ranked(line, z, k, rank):
    total = jnp.int32(0)
    for at in range(line):
        order = sorted(range(line), key=lambda place: rank(place, at))
        place = sum([jnp.where(k == i, order[i], 0) for i in range(line)])
        total = total + jnp.where(z == at, place, 0)
    return total


def gate_act_kernel(
    line,
    x_ref,
    top_ref,
    wg_ref,
    wu_ref,
    wd_ref,
    xn_ref,
    grads_ref,
    scaled_ref,
    gates_ref,
    xbuf,
    top_buf,
    grads_buf,
    scaled_buf,
    gates_buf,
    sent,
    arrived,
    own_sem,
    top_sem,
    xn_sem,
    grads_sem,
    scaled_sem,
    gates_sem,
):
    dp, place = lax.axis_index("dp"), lax.axis_index("expert")
    z, c = place // 2, place % 2
    side_x, side_y = corners(dp)
    far = 3 - dp
    devices = (
        (dp, place + 2),
        (dp, place - 2),
        (side_x, place),
        (side_y, place),
        (dp, 2 * z + 1 - c),
    )
    up, down, along_x, along_y, pair = range(5)
    has_up, has_down = z < line - 1, z > 0
    for way in (along_x, along_y, pair):
        greet(devices[way])
    pl.when(has_up)(lambda: greet(devices[up]))
    pl.when(has_down)(lambda: greet(devices[down]))
    greeted = 3 + has_up.astype(jnp.int32) + has_down.astype(jnp.int32)
    pl.semaphore_wait(pltpu.get_barrier_semaphore(), greeted)
    local, width, units = wg_ref.shape
    rows = top_buf.shape[1]
    first = place * local

    def slot(corner, height, core):
        return corner * (2 * line) + 2 * height + core

    def copy(s, p, way, source=None):
        target = xbuf.at[s, p]
        return send(
            target if source is None else source,
            target,
            sent.at[s, p, way],
            arrived.at[s, p],
            devices[way],
        )

    def arrive(s, p):
        copy(s, p, pair).wait_recv()

    mine = slot(dp, z, c)
    for p in (0, 1):
        pltpu.make_async_copy(x_ref.at[p], xbuf.at[mine, p], own_sem.at[p]).start()
        pl.when(has_up)(lambda: copy(mine, p, up, x_ref.at[p]).start())
        pl.when(has_down)(lambda: copy(mine, p, down, x_ref.at[p]).start())
        for way in (along_x, along_y, pair):
            copy(mine, p, way, x_ref.at[p]).start()

    def decode(i):
        turn, j = i // 4, i % 4
        k = turn - (j > 0).astype(jnp.int32) - (j == 3).astype(jnp.int32)
        valid = (i >= 0) & (k >= 0) & (k < line)
        corner = jnp.where(j == 0, dp, jnp.where(j == 1, side_x, jnp.where(j == 2, side_y, far)))
        return j, k, valid, corner, nearest(line, z, k)

    def top_load(i, corner, height):
        block = corner * line + height
        return pltpu.make_async_copy(top_ref.at[block], top_buf.at[i % 2], top_sem.at[i % 2])

    def xn_out(block):
        return pltpu.make_async_copy(
            xbuf.at[pl.ds(2 * block, 2), :, :, pl.ds(0, width)],
            xn_ref.at[pl.ds(2 * block, 2)],
            xn_sem.at[block],
        )

    def grads_out(block):
        return pltpu.make_async_copy(grads_buf.at[block], grads_ref.at[block], grads_sem.at[block])

    def scaled_out(block):
        return pltpu.make_async_copy(
            scaled_buf.at[block], scaled_ref.at[block], scaled_sem.at[block]
        )

    def gates_out(block):
        return pltpu.make_async_copy(gates_buf.at[block], gates_ref.at[block], gates_sem.at[block])

    def compute(i):
        j, k, _, corner, height = decode(i)
        block = corner * line + height
        for p in (0, 1):
            arrive(slot(corner, height, 1 - c), p)
        xn_out(block).start()
        top_load(i, corner, height).wait()
        lanes = lax.broadcasted_iota(jnp.int32, (rows, 128), 1)

        def tokens():
            return xbuf[pl.ds(2 * block, 2), :, :, pl.ds(0, width)].reshape(rows, width)

        table = xbuf[pl.ds(2 * block, 2), :, :, pl.ds(width, 128)].reshape(rows, 128)
        table = table.astype(jnp.float32)
        gate_grads = jnp.zeros((rows, 128), jnp.float32)
        for e in range(local):
            at = (lanes == first + e) | (lanes == first + e + 64)
            gate = jnp.sum(jnp.where(at, table, 0.0), axis=1, keepdims=True)
            g = contract(tokens(), wg_ref[e], 1, 0)
            u = contract(tokens(), wu_ref[e], 1, 0)
            h = contract(top_buf[i % 2], wd_ref[e], 1, 1)
            sigmoid = 1.0 / (1.0 + jnp.exp(-g))
            silu = g * sigmoid
            act = silu * u
            gate_grad = jnp.sum(act * h, axis=1, keepdims=True)
            gate_grads = gate_grads + jnp.where(lanes == first + e, gate_grad, 0.0)
            grad_act = h * gate
            dg = grad_act * u * sigmoid * (1.0 + g * (1.0 - sigmoid))
            du = grad_act * silu
            scaled_buf[block, :, e * units : (e + 1) * units] = (act * gate).astype(jnp.bfloat16)
            grads_buf[block, :, e * units : (e + 1) * units] = dg.astype(jnp.bfloat16)
            at = (local + e) * units
            grads_buf[block, :, at : at + units] = du.astype(jnp.bfloat16)
        gates_buf[block] = gate_grads.astype(jnp.bfloat16)
        grads_out(block).start()
        scaled_out(block).start()
        gates_out(block).start()

    def step(i, carry):
        j, k, valid, corner, height = decode(i)
        s = slot(corner, height, c)

        def own():
            for p in (0, 1):
                pltpu.make_async_copy(x_ref.at[p], xbuf.at[mine, p], own_sem.at[p]).wait()

        def column():
            for p in (0, 1):
                arrive(s, p)
                pl.when(has_up & (height < z))(lambda: copy(s, p, up).start())
                pl.when(has_down & (height > z))(lambda: copy(s, p, down).start())
                for way in (along_x, along_y, pair):
                    copy(s, p, way).start()

        def sides():
            for p in (0, 1):
                arrive(s, p)
                copy(s, p, pair).start()
            pl.when(j == 1)(lambda: copy(s, 0, along_y).start())
            pl.when(j == 2)(lambda: copy(s, 1, along_x).start())

        def opposite():
            for p in (0, 1):
                arrive(s, p)
                copy(s, p, pair).start()

        pl.when(valid & (j == 0) & (k == 0))(own)
        pl.when(valid & (j == 0) & (k > 0))(column)
        pl.when(valid & ((j == 1) | (j == 2)))(sides)
        pl.when(valid & (j == 3))(opposite)
        pl.when(valid)(lambda: top_load(i, corner, height).start())
        pl.when(decode(i - 1)[2])(lambda: compute(i - 1))
        return carry

    lax.fori_loop(0, 4 * (line + 2) + 1, step, 0)

    def finish(height, carry):
        for p in (0, 1):
            for corner in range(4):
                copy(slot(corner, height, c), p, pair).wait_send()
            s = slot(dp, height, c)
            copy(s, p, along_x).wait_send()
            copy(s, p, along_y).wait_send()
            pl.when(has_up & (height <= z))(lambda: copy(s, p, up).wait_send())
            pl.when(has_down & (height >= z))(lambda: copy(s, p, down).wait_send())
        copy(slot(side_x, height, c), 0, along_y).wait_send()
        copy(slot(side_y, height, c), 1, along_x).wait_send()
        for corner in range(4):
            block = corner * line + height
            xn_out(block).wait()
            grads_out(block).wait()
            scaled_out(block).wait()
            gates_out(block).wait()
        return carry

    lax.fori_loop(0, line, finish, 0)


def gate_act(own, tops, w_gate, w_up, w_down, line):
    count, wide = own.shape
    local, width, units = w_gate.shape
    slots, blocks, rows, half = 8 * line, 4 * line, 2 * count, count // 2
    sems = pltpu.SemaphoreType.DMA
    dtype = own.dtype
    xn, grads, scaled, gates = pl.pallas_call(
        functools.partial(gate_act_kernel, line),
        out_shape=[
            jax.ShapeDtypeStruct((slots, 2, half, width), dtype),
            jax.ShapeDtypeStruct((blocks, rows, 2 * local * units), dtype),
            jax.ShapeDtypeStruct((blocks, rows, local * units), dtype),
            jax.ShapeDtypeStruct((blocks, rows, 128), dtype),
        ],
        in_specs=[
            pl.BlockSpec(memory_space=pltpu.VMEM),
            pl.BlockSpec(memory_space=pl.ANY),
            pl.BlockSpec(memory_space=pltpu.VMEM),
            pl.BlockSpec(memory_space=pltpu.VMEM),
            pl.BlockSpec(memory_space=pltpu.VMEM),
        ],
        out_specs=[pl.BlockSpec(memory_space=pl.ANY)] * 4,
        scratch_shapes=[
            pltpu.VMEM((slots, 2, half, wide), dtype),
            pltpu.VMEM((2, rows, width), dtype),
            pltpu.VMEM((blocks, rows, 2 * local * units), dtype),
            pltpu.VMEM((blocks, rows, local * units), dtype),
            pltpu.VMEM((blocks, rows, 128), dtype),
            sems((slots, 2, 5)),
            sems((slots, 2)),
            sems((2,)),
            sems((2,)),
            sems((blocks,)),
            sems((blocks,)),
            sems((blocks,)),
            sems((blocks,)),
        ],
        compiler_params=pltpu.CompilerParams(
            collective_id=1, has_side_effects=True, vmem_limit_bytes=60 << 20
        ),
        name="gate_act",
    )(own.reshape(2, half, wide), tops.reshape(blocks, rows, width), w_gate, w_up, w_down)
    return xn.reshape(slots * count, width), grads, scaled, gates


def column_products(left_ref, right_ref, chunk_buf, right_buf, total, chunk_sem, right_sem, store):
    span = chunk_buf.shape[2]
    blocks, rows, _ = right_buf.shape
    joined = max(1, min(blocks, 1024 // rows))
    depth = joined * rows
    turns = left_ref.shape[1] // span

    def at(n):
        return pl.ds(pl.multiple_of(n * span, span), span)

    def chunk(n):
        return pltpu.make_async_copy(
            left_ref.at[:, at(n)], chunk_buf.at[n % 2], chunk_sem.at[n % 2]
        )

    right_load = pltpu.make_async_copy(right_ref, right_buf, right_sem.at[0])
    chunk(0).start()
    right_load.start()

    def turn(n):
        pl.when(n + 1 < turns)(lambda: chunk(n + 1).start())
        chunk(n).wait()
        pl.when(n == 0)(right_load.wait)
        total[...] = jnp.zeros_like(total)

        def part(k, carry):
            left = chunk_buf[n % 2, pl.ds(pl.multiple_of(k * depth, depth), depth), :]
            right = right_buf[pl.ds(k * joined, joined)].reshape(depth, right_buf.shape[2])
            total[...] += contract(left, right, 0, 0)
            return carry

        lax.fori_loop(0, blocks // joined, part, 0)
        store(n, at(n))

    return turn, turns


def gate_up_grads(
    xn_ref, units_ref, gate_ref, up_ref, chunk_buf, units_buf, total, both, chunk_sem, units_sem, out_sem
):
    local, _, units = gate_ref.shape
    outs = (gate_ref, up_ref)

    def copies(at):
        return [
            pltpu.make_async_copy(
                both.at[:, pl.ds((kind * local + e) * units, units)],
                outs[kind].at[e, at, :],
                out_sem.at[kind, e],
            )
            for kind in (0, 1)
            for e in range(local)
        ]

    start = pl.ds(0, chunk_buf.shape[2])

    def store(n, at):
        @pl.when(n > 0)
        def _():
            for copy in copies(start):
                copy.wait()

        both[...] = total[...].astype(both.dtype)
        for copy in copies(at):
            copy.start()

    def end():
        for copy in copies(start):
            copy.wait()

    turn, turns = column_products(
        xn_ref, units_ref, chunk_buf, units_buf, total, chunk_sem, units_sem, store
    )
    return turn, end, turns


def down_grads(
    top_ref, scaled_ref, down_ref, chunk_buf, scaled_buf, total, out, chunk_sem, scaled_sem, out_sem
):
    local, units, _ = down_ref.shape

    def copies(at):
        return [
            pltpu.make_async_copy(out.at[e], down_ref.at[e, :, at], out_sem.at[e])
            for e in range(local)
        ]

    start = pl.ds(0, chunk_buf.shape[2])

    def store(n, at):
        @pl.when(n > 0)
        def _():
            for copy in copies(start):
                copy.wait()

        for e in range(local):
            out[e] = total[:, e * units : (e + 1) * units].T.astype(out.dtype)
        for copy in copies(at):
            copy.start()

    def end():
        for copy in copies(start):
            copy.wait()

    turn, turns = column_products(
        top_ref, scaled_ref, chunk_buf, scaled_buf, total, chunk_sem, scaled_sem, store
    )
    return turn, end, turns


SPAN = 256


def product_sum_kernel(
    line,
    flipped,
    extra,
    grads,
    *refs,
):
    a_ref, w_ref = refs[0], refs[1]
    e_ref = refs[2] if extra else None
    refs = refs[3:] if extra else refs[2:]
    if grads:
        work_refs, refs = (*refs[:2], *refs[3:5], *refs[-7:]), (refs[2], *refs[5:-7])
    (
        out_ref,
        made,
        a_buf,
        e_buf,
        got_pair,
        got_x,
        got_y,
        got_far_x,
        got_far_y,
        got_below,
        got_above,
        load_sem,
        extra_sem,
        pair_sem,
        x_sem,
        y_sem,
        far_x_sem,
        far_y_sem,
        below_sem,
        above_sem,
    ) = refs
    dp, place = lax.axis_index("dp"), lax.axis_index("expert")
    z, c = place // 2, place % 2
    side_x, side_y = corners(dp)
    far = 3 - dp
    to_x, to_y, to_pair = (side_x, place), (side_y, place), (dp, 2 * z + 1 - c)
    to_up, to_down = (dp, place + 2), (dp, place - 2)
    for device in (to_x, to_y, to_pair):
        greet(device)
    pl.when(z > 0)(lambda: greet(to_down))
    pl.when(z < line - 1)(lambda: greet(to_up))
    greeted = 3 + (z > 0).astype(jnp.int32) + (z < line - 1).astype(jnp.int32)
    pl.semaphore_wait(pltpu.get_barrier_semaphore(), greeted)
    count = 4 * line
    width = w_ref.shape[0] if flipped else w_ref.shape[1]
    half = made.shape[4]
    chunk = 512

    def mine(q, height, p):
        return made.at[q, height, c, p]

    def hand(q, height, p):
        at = (q, height, p)
        source = made.at[q, height, 1 - c, p]
        return send(source, got_pair.at[at], pair_sem.at[0, *at], pair_sem.at[1, *at], to_pair)

    def along_x(height, p):
        at = (height, p)
        source = mine(side_x, height, p)
        return send(source, got_x.at[at], x_sem.at[0, *at], x_sem.at[1, *at], to_x)

    def along_y(height, p):
        at = (height, p)
        source = mine(side_y, height, p)
        return send(source, got_y.at[at], y_sem.at[0, *at], y_sem.at[1, *at], to_y)

    def far_x(height):
        source = mine(far, height, 0)
        return send(
            source, got_far_x.at[height], far_x_sem.at[0, height], far_x_sem.at[1, height], to_x
        )

    def far_y(height):
        source = mine(far, height, 1)
        return send(
            source, got_far_y.at[height], far_y_sem.at[0, height], far_y_sem.at[1, height], to_y
        )

    def climb(height, p):
        at = (height, p)
        source = mine(dp, height, p)
        return send(source, got_below.at[at], below_sem.at[0, *at], below_sem.at[1, *at], to_up)

    def descend(height, p):
        at = (height, p)
        source = mine(dp, height, p)
        return send(source, got_above.at[at], above_sem.at[0, *at], above_sem.at[1, *at], to_down)

    def decode(i):
        k, j = i // 4, i % 4
        q = jnp.where(j == 0, far, jnp.where(j == 1, side_x, jnp.where(j == 2, side_y, dp)))
        return k, j, q, farthest(line, z, k)

    def load(i):
        _, _, q, height = decode(i)
        return pltpu.make_async_copy(
            a_ref.at[q * line + height], a_buf.at[i % 2], load_sem.at[i % 2]
        )

    def load_extra(i):
        _, _, q, height = decode(i)
        return pltpu.make_async_copy(
            e_ref.at[q * line + height], e_buf.at[i % 2], extra_sem.at[i % 2]
        )

    def start_load(i):
        load(i).start()
        if extra:
            load_extra(i).start()

    def add(q, height, p, other):
        at = (q, height, c, p)
        made[at] = made[at] + other[...]

    def compute(i):
        _, _, q, height = decode(i)
        load(i).wait()
        if extra:
            load_extra(i).wait()
        pl.when(i + 1 < count)(lambda: start_load(i + 1))
        for at in range(0, width, chunk):
            if flipped:
                part = contract(a_buf[i % 2], w_ref[at : at + chunk, :], 1, 1)
            else:
                part = contract(a_buf[i % 2], w_ref[:, at : at + chunk], 1, 0)
            part = part.astype(made.dtype).reshape(2, 2, half, chunk)
            made[q, height, :, :, :, at : at + chunk] = part
        if extra:
            made[q, height, :, :, :, width : width + 128] = e_buf[i % 2].reshape(2, 2, half, 128)
        for p in (0, 1):
            hand(q, height, p).start()

    def settle(i):
        _, j, q, height = decode(i)
        for p in (0, 1):
            hand(q, height, p).wait_recv()
            add(q, height, p, got_pair.at[q, height, p])

        def opposite():
            far_x(height).start()
            far_y(height).start()

        def side_of_x():
            along_x(height, 0).start()
            far_y(height).wait_recv()
            add(side_x, height, 1, got_far_y.at[height])
            along_x(height, 1).start()

        def side_of_y():
            along_y(height, 1).start()
            far_x(height).wait_recv()
            add(side_y, height, 0, got_far_x.at[height])
            along_y(height, 0).start()

        pl.when(j == 0)(opposite)
        pl.when(j == 1)(side_of_x)
        pl.when(j == 2)(side_of_y)

    def column(height):
        for p in (0, 1):
            along_x(height, p).wait_recv()
            along_y(height, p).wait_recv()
            total = made[dp, height, c, p].astype(jnp.float32)
            total = total + got_x[height, p].astype(jnp.float32)
            total = total + got_y[height, p].astype(jnp.float32)
            made[dp, height, c, p] = total.astype(made.dtype)
            pl.when((z == 0) & (height > z))(lambda: climb(height, p).start())
            pl.when((z == line - 1) & (height < z))(lambda: descend(height, p).start())

    def pass_on(height):
        for p in (0, 1):

            def upwards():
                climb(height, p).wait_recv()
                add(dp, height, p, got_below.at[height, p])
                climb(height, p).start()

            def downwards():
                descend(height, p).wait_recv()
                add(dp, height, p, got_above.at[height, p])
                descend(height, p).start()

            pl.when((height > z) & (z > 0))(upwards)
            pl.when((height < z) & (z < line - 1))(downwards)

    start_load(0)
    work, work_end, turns = gate_up_grads(*work_refs) if grads else (None, None, 1)

    def step(i, carry):
        k, j, _, _ = decode(i)
        pl.when(i < count)(lambda: compute(i))
        pl.when((i >= 1) & (i <= count))(lambda: settle(i - 1))
        if grads:
            every = count // turns
            pl.when((i < count) & (i % every == 0))(lambda: work(i // every))
        late = farthest(line, z, k - 2)
        pl.when((k >= 2) & (j == 0))(lambda: column(late))
        pl.when((k >= 2) & (j == 3))(lambda: pass_on(late))
        return carry

    lax.fori_loop(0, count + 8, step, 0)
    if grads:
        work_end()
    for p in (0, 1):
        out_ref[p] = made[dp, z, c, p].astype(jnp.float32)

        def from_below():
            climb(z, p).wait_recv()
            out_ref[p] = out_ref[p] + got_below[z, p].astype(jnp.float32)

        def from_above():
            descend(z, p).wait_recv()
            out_ref[p] = out_ref[p] + got_above[z, p].astype(jnp.float32)

        pl.when(z > 0)(from_below)
        pl.when(z < line - 1)(from_above)

    def finish(height, carry):
        far_x(height).wait_send()
        far_y(height).wait_send()
        for p in (0, 1):
            for q in range(4):
                hand(q, height, p).wait_send()
            along_x(height, p).wait_send()
            along_y(height, p).wait_send()
            pl.when(height > z)(lambda: climb(height, p).wait_send())
            pl.when(height < z)(lambda: descend(height, p).wait_send())
        return carry

    lax.fori_loop(0, line, finish, 0)


def product_sum(blocks, weights, flipped, extra, line, name, number, grads=None):
    count, rows, depth = blocks.shape
    width = weights.shape[0] if flipped else weights.shape[1]
    wide = width + (0 if extra is None else 128)
    half = rows // 4
    sems = pltpu.SemaphoreType.DMA
    dtype = blocks.dtype

    def space(*shape):
        return pltpu.VMEM((*shape, half, wide), dtype)

    anywhere, inside = pl.BlockSpec(memory_space=pl.ANY), pl.BlockSpec(memory_space=pltpu.VMEM)
    out_shape = [jax.ShapeDtypeStruct((2, half, wide), jnp.float32)]
    work_in, work_space = [], []
    if grads is not None:
        xn, both, shape = grads
        work_in = [xn, both]
        out_shape += [jax.ShapeDtypeStruct(shape, dtype)] * 2
        work_space = [
            pltpu.VMEM((2, xn.shape[0], SPAN), dtype),
            pltpu.VMEM(both.shape, dtype),
            pltpu.VMEM((SPAN, both.shape[2]), jnp.float32),
            pltpu.VMEM((SPAN, both.shape[2]), dtype),
            sems((2,)),
            sems((1,)),
            sems((2, shape[0])),
        ]
    total, *work_out = pl.pallas_call(
        functools.partial(product_sum_kernel, line, flipped, extra is not None, grads is not None),
        out_shape=out_shape,
        in_specs=[anywhere, inside]
        + ([] if extra is None else [anywhere])
        + [anywhere] * len(work_in),
        out_specs=[inside] + [anywhere] * (len(out_shape) - 1),
        scratch_shapes=[
            space(4, line, 2, 2),
            pltpu.VMEM((2, rows, depth), dtype),
            pltpu.VMEM((2, rows, 128), dtype),
            space(4, line, 2),
            space(line, 2),
            space(line, 2),
            space(line),
            space(line),
            space(line, 2),
            space(line, 2),
            sems((2,)),
            sems((2,)),
            sems((2, 4, line, 2)),
            sems((2, line, 2)),
            sems((2, line, 2)),
            sems((2, line)),
            sems((2, line)),
            sems((2, line, 2)),
            sems((2, line, 2)),
            *work_space,
        ],
        compiler_params=pltpu.CompilerParams(
            collective_id=number, has_side_effects=True, vmem_limit_bytes=63 << 20
        ),
        name=name,
    )(blocks, weights, *([] if extra is None else [extra]), *work_in)
    return total.reshape(2 * half, wide), *work_out


def closing_kernel(
    line,
    shared_rows,
    parts_ref,
    small_ref,
    first_ref,
    grad_ref,
    unit_ref,
    inverse_ref,
    gain_ref,
    output_ref,
    top_ref,
    scaled_ref,
    summed_ref,
    shared_ref,
    outputs_ref,
    grads_ref,
    down_ref,
    acc,
    got_pair,
    got_below,
    got_above,
    part,
    got_x,
    got_y,
    got_far_x,
    got_far_y,
    grad_own,
    small,
    got_small,
    load_sem,
    pair_sem,
    load_small_sem,
    pair_small_sem,
    below_sem,
    above_sem,
    part_sem,
    x_sem,
    y_sem,
    far_x_sem,
    far_y_sem,
    spread_sem,
    arrive_sem,
    own_sem,
    small_sem,
    *work_refs,
):
    dp, place = lax.axis_index("dp"), lax.axis_index("expert")
    z, c = place // 2, place % 2
    side_x, side_y = corners(dp)
    far = 3 - dp
    to_x, to_y, to_pair = (side_x, place), (side_y, place), (dp, 2 * z + 1 - c)
    to_up, to_down = (dp, place + 2), (dp, place - 2)
    for device in (to_x, to_y, to_pair):
        greet(device)
    pl.when(z > 0)(lambda: greet(to_down))
    pl.when(z < line - 1)(lambda: greet(to_up))
    greeted = 3 + (z > 0).astype(jnp.int32) + (z < line - 1).astype(jnp.int32)
    pl.semaphore_wait(pltpu.get_barrier_semaphore(), greeted)

    large = parts_ref.shape[3]
    top_rows, low_rows = pl.ds(0, large), pl.ds(large, shared_rows // 2)

    def loads(height, p):
        return (
            pltpu.make_async_copy(
                parts_ref.at[height, c, p], acc.at[height, p, top_rows], load_sem.at[height, p]
            ),
            pltpu.make_async_copy(
                small_ref.at[height, c, p], acc.at[height, p, low_rows], load_small_sem.at[height, p]
            ),
        )

    def hands(height, p):
        at = (height, p)
        return (
            send(
                parts_ref.at[height, 1 - c, p],
                got_pair.at[height, p, top_rows],
                pair_sem.at[0, *at],
                pair_sem.at[1, *at],
                to_pair,
            ),
            send(
                small_ref.at[height, 1 - c, p],
                got_pair.at[height, p, low_rows],
                pair_small_sem.at[0, *at],
                pair_small_sem.at[1, *at],
                to_pair,
            ),
        )

    def climb(height, p):
        at = (height, p)
        return send(
            acc.at[at], got_below.at[at], below_sem.at[0, *at], below_sem.at[1, *at], to_up
        )

    def descend(height, p):
        at = (height, p)
        return send(
            acc.at[at], got_above.at[at], above_sem.at[0, *at], above_sem.at[1, *at], to_down
        )

    def start(k, carry):
        height = farthest(line, z, k)
        for p in (0, 1):
            for copy in (*loads(height, p), *hands(height, p)):
                copy.start()
        return carry

    def pair_sum(k, carry):
        height = farthest(line, z, k)
        for p in (0, 1):
            for copy in loads(height, p):
                copy.wait()
            for copy in hands(height, p):
                copy.wait_recv()
            acc[height, p] = acc[height, p] + got_pair[height, p]
            pl.when((z == 0) & (height > z))(lambda: climb(height, p).start())
            pl.when((z == line - 1) & (height < z))(lambda: descend(height, p).start())
        return carry

    def pass_on(k, carry):
        height = farthest(line, z, k)
        for p in (0, 1):

            def upwards():
                climb(height, p).wait_recv()
                acc[height, p] = acc[height, p] + got_below[height, p]
                climb(height, p).start()

            def downwards():
                descend(height, p).wait_recv()
                acc[height, p] = acc[height, p] + got_above[height, p]
                descend(height, p).start()

            pl.when((height > z) & (z > 0))(upwards)
            pl.when((height < z) & (z < line - 1))(downwards)
        return carry

    def first_load(q, p):
        return pltpu.make_async_copy(first_ref.at[q, p], part.at[q, p], part_sem.at[q, p])

    def along_x(p):
        return send(part.at[side_x, p], got_x.at[p], x_sem.at[0, p], x_sem.at[1, p], to_x)

    def along_y(p):
        return send(part.at[side_y, p], got_y.at[p], y_sem.at[0, p], y_sem.at[1, p], to_y)

    def far_x():
        return send(part.at[far, 0], got_far_x, far_x_sem.at[0], far_x_sem.at[1], to_x)

    def far_y():
        return send(part.at[far, 1], got_far_y, far_y_sem.at[0], far_y_sem.at[1], to_y)

    spreads = ((output_ref, outputs_ref), (grad_own, grads_ref))

    def spread(a, corner, p, way, source=None):
        target = spreads[a][1].at[corner, p]
        return send(
            target if source is None else source,
            target,
            spread_sem.at[a, corner, p, way],
            arrive_sem.at[a, corner, p],
            (to_x, to_y)[way],
        )

    def own_copy(a, p):
        return pltpu.make_async_copy(
            spreads[a][0].at[p], spreads[a][1].at[dp, p], own_sem.at[a, p]
        )

    def spread_own(a, p):
        own_copy(a, p).start()
        for way in (0, 1):
            spread(a, dp, p, way, spreads[a][0].at[p]).start()

    def spread_far(a):
        spread(a, side_x, 0, 0).wait_recv()
        spread(a, side_x, 0, 1).start()
        spread(a, side_y, 1, 0).wait_recv()
        spread(a, side_y, 1, 0).start()

    work, work_end, turns = down_grads(top_ref, scaled_ref, down_ref, *work_refs)
    pauses = 4

    def meanwhile(i):
        def turn(n, carry):
            work(n)
            return carry

        lax.fori_loop(turns * i // pauses, turns * (i + 1) // pauses, turn, 0)

    lax.fori_loop(0, 1, start, 0)
    for q in (far, side_x, side_y, dp):
        for p in (0, 1):
            first_load(q, p).start()
    lax.fori_loop(1, line, start, 0)
    for q in (far, side_x, side_y, dp):
        for p in (0, 1):
            first_load(q, p).wait()
    far_x().start()
    far_y().start()
    along_x(0).start()
    along_y(1).start()
    lax.fori_loop(0, 1, pair_sum, 0)
    far_x().wait_recv()
    part[side_y, 0] = part[side_y, 0] + got_far_x[...]
    along_y(0).start()
    far_y().wait_recv()
    part[side_x, 1] = part[side_x, 1] + got_far_y[...]
    along_x(1).start()
    for p in (0, 1):
        spread_own(0, p)
    lax.fori_loop(1, line, pair_sum, 0)
    meanwhile(0)
    lax.fori_loop(0, 1, pass_on, 0)
    for p in (0, 1):
        along_x(p).wait_recv()
        along_y(p).wait_recv()
        total = part[dp, p].astype(jnp.float32)
        total = total + got_x[p].astype(jnp.float32) + got_y[p].astype(jnp.float32)
        total = total * gain_ref[...]
        unit = unit_ref[p]
        mean = jnp.sum(total * unit, axis=1, keepdims=True) * (1.0 / unit.shape[1])
        rows = grad_ref[p] + inverse_ref[p] * (total - unit * mean)
        grad_own[p] = rows.astype(grad_own.dtype)
        spread_own(1, p)
    meanwhile(1)
    spread_far(0)
    lax.fori_loop(1, 2, pass_on, 0)
    spread_far(1)
    meanwhile(2)
    lax.fori_loop(2, line, pass_on, 0)
    meanwhile(3)
    for p in (0, 1):
        summed_ref[p] = acc[z, p].astype(jnp.float32)

        def from_below():
            climb(z, p).wait_recv()
            summed_ref[p] = summed_ref[p] + got_below[z, p].astype(jnp.float32)

        def from_above():
            descend(z, p).wait_recv()
            summed_ref[p] = summed_ref[p] + got_above[z, p].astype(jnp.float32)

        pl.when(z > 0)(from_below)
        pl.when(z < line - 1)(from_above)

    for side, device in enumerate((to_x, to_y)):
        value = summed_ref[:, large:, :] if side == 0 else shared_ref[...]
        small[side] = value.astype(small.dtype)
        spread(side, side_x, 1, 0).wait_recv()
        spread(side, side_y, 0, 0).wait_recv()
        for p in (0, 1):
            spread(side, far, p, 0).wait_recv()
            for way in (0, 1):
                spread(side, dp, p, way).wait_send()
            own_copy(side, p).wait()
        spread(side, side_x, 0, 1).wait_send()
        spread(side, side_y, 1, 0).wait_send()
        exchange = send(
            small.at[side], got_small.at[side], small_sem.at[0, side], small_sem.at[1, side], device
        )
        exchange.start()
        exchange.wait_recv()
        shared_ref[...] = small[side].astype(jnp.float32) + got_small[side].astype(jnp.float32)
        exchange.wait_send()

    far_x().wait_send()
    far_y().wait_send()
    for p in (0, 1):
        along_x(p).wait_send()
        along_y(p).wait_send()

    def finish(height, carry):
        for p in (0, 1):
            for copy in hands(height, p):
                copy.wait_send()
            pl.when(height > z)(lambda: climb(height, p).wait_send())
            pl.when(height < z)(lambda: descend(height, p).wait_send())
        return carry

    lax.fori_loop(0, line, finish, 0)
    work_end()


def closing(parts, small, first, grad, unit, inverse, gain, output, tops, scaled, shape, line):
    _, rows, wide = parts.shape
    shared_rows = small.shape[1]
    own, width = output.shape
    high, half = (rows + shared_rows) // 2, own // 2
    local, units, _ = shape
    sems = pltpu.SemaphoreType.DMA
    dtype = parts.dtype
    single = jnp.float32
    anywhere, inside = pl.BlockSpec(memory_space=pl.ANY), pl.BlockSpec(memory_space=pltpu.VMEM)
    everyone = jax.ShapeDtypeStruct((4, 2, half, width), dtype)
    summed, shared, outputs, grads, down = pl.pallas_call(
        functools.partial(closing_kernel, line, shared_rows),
        out_shape=[
            jax.ShapeDtypeStruct((2, high, wide), single),
            jax.ShapeDtypeStruct((2, shared_rows // 2, wide), single),
            everyone,
            everyone,
            jax.ShapeDtypeStruct(shape, dtype),
        ],
        in_specs=[anywhere] * 3 + [inside] * 5 + [anywhere] * 2,
        out_specs=[inside, inside, anywhere, anywhere, anywhere],
        scratch_shapes=[
            pltpu.VMEM((line, 2, high, wide), dtype),
            pltpu.VMEM((line, 2, high, wide), dtype),
            pltpu.VMEM((line, 2, high, wide), dtype),
            pltpu.VMEM((line, 2, high, wide), dtype),
            pltpu.VMEM((4, 2, half, width), dtype),
            pltpu.VMEM((2, half, width), dtype),
            pltpu.VMEM((2, half, width), dtype),
            pltpu.VMEM((half, width), dtype),
            pltpu.VMEM((half, width), dtype),
            pltpu.VMEM((2, half, width), dtype),
            pltpu.VMEM((2, 2, shared_rows // 2, wide), dtype),
            pltpu.VMEM((2, 2, shared_rows // 2, wide), dtype),
            sems((line, 2)),
            sems((2, line, 2)),
            sems((line, 2)),
            sems((2, line, 2)),
            sems((2, line, 2)),
            sems((2, line, 2)),
            sems((4, 2)),
            sems((2, 2)),
            sems((2, 2)),
            sems((2,)),
            sems((2,)),
            sems((2, 4, 2, 2)),
            sems((2, 4, 2)),
            sems((2, 2)),
            sems((2, 2)),
            pltpu.VMEM((2, tops.shape[0], SPAN), dtype),
            pltpu.VMEM(scaled.shape, dtype),
            pltpu.VMEM((SPAN, local * units), single),
            pltpu.VMEM((local, units, SPAN), dtype),
            sems((2,)),
            sems((1,)),
            sems((local,)),
        ],
        compiler_params=pltpu.CompilerParams(
            collective_id=5, has_side_effects=True, vmem_limit_bytes=60 << 20
        ),
        name="closing",
    )(
        parts.reshape(line, 2, 2, rows // 2, wide),
        small.reshape(line, 2, 2, shared_rows // 2, wide),
        first.reshape(4, 2, half, width),
        grad.reshape(2, half, width),
        unit.reshape(2, half, width),
        inverse.reshape(2, half, 1),
        gain.reshape(1, width),
        output.reshape(2, half, width),
        tops,
        scaled,
    )
    return (
        summed[:, : rows // 2].reshape(rows, wide),
        summed[:, rows // 2 :],
        shared,
        outputs.reshape(4 * own, width),
        grads.reshape(4 * own, width),
        down,
    )


def head_totals(first_sum, second_sum):
    return lax.psum((first_sum, second_sum), "dp")


def per_device(
    inputs,
    attention_norm_gain,
    w_query,
    w_key,
    w_value,
    w_out,
    q_gain,
    k_gain,
    expert_norm_gain,
    w_router,
    w_gate,
    w_up,
    w_down,
    routes,
    lengths,
    d_output,
):
    pack_count, seg_rows, model_width = inputs.shape
    local_width = w_query.shape[1]
    local_heads = local_width // HD
    experts = w_router.shape[1]
    groups = lax.axis_size("expert")
    line = groups // 2
    pack_span = seg_rows * groups
    local_experts = w_gate.shape[0]
    offset_rows = lax.axis_index("expert") * seg_rows
    segment, positions = doc_layout(lengths, pack_span)
    pos_query = lax.dynamic_slice_in_dim(positions, offset_rows, seg_rows, 1)
    cos_table, sin_table = rope_tables(pos_query, HD)
    head_shape = (pack_count, seg_rows, local_heads, HD)
    inputs_single_float = inputs.astype(jnp.float32)
    first_inverse_norm = lax.rsqrt(
        jnp.mean(inputs_single_float * inputs_single_float, axis=-1, keepdims=True) + epsilon
    )
    first_unit_input = inputs_single_float * first_inverse_norm
    first_normed_input = (first_unit_input * attention_norm_gain).astype(jnp.bfloat16)
    q_raw = jnp.dot(first_normed_input, w_query, preferred_element_type=jnp.float32)
    k_raw = jnp.dot(first_normed_input, w_key, preferred_element_type=jnp.float32)
    value_rows = jnp.dot(first_normed_input, w_value, preferred_element_type=jnp.float32).astype(
        jnp.bfloat16
    )
    q_sum, k_sum = head_totals(jnp.sum(q_raw * q_raw, axis=-1), jnp.sum(k_raw * k_raw, axis=-1))
    q_inv = lax.rsqrt(q_sum[..., None] / model_width + epsilon)
    k_inv = lax.rsqrt(k_sum[..., None] / model_width + epsilon)
    q_hat = q_raw * q_inv
    k_hat = k_raw * k_inv
    queries = rotate((q_hat * q_gain).reshape(head_shape), cos_table, sin_table).astype(
        jnp.bfloat16
    )
    key_rows = (
        rotate((k_hat * k_gain).reshape(head_shape), cos_table, sin_table)
        .astype(jnp.bfloat16)
        .reshape(pack_count, seg_rows, local_width)
    )
    layout = (segment, positions)
    if local_heads == line:
        attention = by_head(layout, line)
    else:
        attention = by_query(layout, offset_rows)
    attended, kept = attention[0](queries.reshape(seg_rows, local_width), key_rows[0], value_rows[0])
    attn_part = jnp.dot(
        attended, w_out, preferred_element_type=jnp.float32
    )
    own = lax.axis_index("dp")
    part_rows = seg_rows // lax.axis_size("dp")

    def own_rows(rows):
        return lax.dynamic_slice_in_dim(rows, own * part_rows, part_rows, 0)

    hidden_state = own_rows(inputs_single_float[0]) + scatter_dp(attn_part.astype(jnp.bfloat16))
    second_inverse_norm = lax.rsqrt(
        jnp.mean(hidden_state * hidden_state, axis=-1, keepdims=True) + epsilon
    )
    second_unit_input = hidden_state * second_inverse_norm
    second_normed_input = second_unit_input * expert_norm_gain
    router = jax.nn.softmax(
        jnp.dot(second_normed_input, w_router, precision=lax.Precision.HIGHEST), axis=-1
    )
    chosen = own_rows(routes[:, 0, :])
    expert_range = jnp.arange(experts, dtype=jnp.int32)
    named = jnp.any(chosen[:, :, None] == expert_range, axis=1)
    top_own = own_rows(d_output[0])
    top_all = lax.all_gather(top_own, "expert", axis=0, tiled=True)
    top_all = lax.all_gather(top_all, "dp", axis=0, tiled=True)
    gate_table = jnp.where(named, router, 0.0)
    gate_high = gate_table.astype(jnp.bfloat16)
    gate_low = (gate_table - gate_high.astype(jnp.float32)).astype(jnp.bfloat16)
    widen = ((0, 0), (0, 64 - experts))
    own_tokens = jnp.concatenate(
        [
            second_normed_input.astype(jnp.bfloat16),
            jnp.pad(gate_high, widen),
            jnp.pad(gate_low, widen),
        ],
        axis=1,
    )
    xn_all, grad_units, scaled, gate_part = gate_act(
        own_tokens, top_all, w_gate, w_up, w_down, line
    )
    w_both = jnp.concatenate([*w_gate, *w_up], axis=1)
    (grad_tokens,) = product_sum(grad_units, w_both, True, gate_part, line, "grad_tokens", 4)
    moe_out, grad_gate, grad_up = product_sum(
        scaled,
        w_down.reshape(-1, model_width),
        False,
        None,
        line,
        "expert_sum",
        2,
        (xn_all, grad_units, w_gate.shape),
    )
    output = (hidden_state + moe_out).astype(jnp.bfloat16)
    grad_xn_exp = grad_tokens[:, :model_width]
    gate_sums = grad_tokens[:, model_width : model_width + experts]
    grad_router_probs = jnp.where(named, gate_sums, 0.0)
    grad_logits = router * (
        grad_router_probs - jnp.sum(router * grad_router_probs, axis=-1, keepdims=True)
    )
    grad_second_normed_input = grad_xn_exp + jnp.einsum(
        "se,de->sd", grad_logits, w_router, precision=lax.Precision.HIGHEST
    )
    grad_router = jnp.einsum(
        "sd,se->de", second_normed_input, grad_logits, precision=lax.Precision.HIGHEST
    )
    grad_expert_norm_gain = jnp.sum(grad_second_normed_input * second_unit_input, axis=0)
    grad_second_unit_input = grad_second_normed_input * expert_norm_gain
    grad_hidden = top_own.astype(jnp.float32) + second_inverse_norm * (
        grad_second_unit_input
        - second_unit_input
        * jnp.mean(grad_second_unit_input * second_unit_input, axis=-1, keepdims=True)
    )
    grad_attn = gather_dp(grad_hidden.astype(jnp.bfloat16))
    grad_out = jnp.einsum("sk,sd->kd", attended, grad_attn, preferred_element_type=jnp.float32)
    grad_heads = jnp.einsum(
        "sd,kd->sk", grad_attn, w_out, preferred_element_type=jnp.float32
    ).astype(jnp.bfloat16)
    grad_queries, grad_keys, grad_values = attention[1](kept, grad_heads)
    grad_queries = grad_queries.astype(jnp.float32).reshape(head_shape)
    grad_q_normed = rotate(grad_queries, cos_table, -sin_table).reshape(
        pack_count, seg_rows, local_width
    )
    grad_k_normed = rotate(
        grad_keys.astype(jnp.float32).reshape(head_shape), cos_table, -sin_table).reshape(
        pack_count, seg_rows, local_width
    )
    grad_q_gain = jnp.sum(grad_q_normed * q_hat, axis=(0, 1))
    grad_k_gain = jnp.sum(grad_k_normed * k_hat, axis=(0, 1))
    grad_q_hat = grad_q_normed * q_gain
    grad_k_hat = grad_k_normed * k_gain
    q_dot, k_dot = head_totals(
        jnp.sum(grad_q_hat * q_hat, axis=-1), jnp.sum(grad_k_hat * k_hat, axis=-1)
    )
    grad_q_raw = (q_inv * (grad_q_hat - q_hat * q_dot[..., None] / model_width)).astype(
        jnp.bfloat16
    )
    grad_k_raw = (k_inv * (grad_k_hat - k_hat * k_dot[..., None] / model_width)).astype(
        jnp.bfloat16
    )
    grad_v_raw = grad_values.astype(jnp.bfloat16)[None]
    grad_heads_raw = jnp.concatenate([grad_q_raw[0], grad_k_raw[0], grad_v_raw[0]], axis=1)
    grad_projections = jnp.einsum(
        "sd,sk->dk", first_normed_input[0], grad_heads_raw, preferred_element_type=jnp.float32
    )
    grad_first_normed_input = jnp.einsum(
        "psk,dk->psd", grad_q_raw, w_query, preferred_element_type=jnp.float32
    )
    grad_first_normed_input = grad_first_normed_input + jnp.einsum(
        "psk,dk->psd", grad_k_raw, w_key, preferred_element_type=jnp.float32
    )
    grad_first_normed_input = grad_first_normed_input + jnp.einsum(
        "psk,dk->psd", grad_v_raw, w_value, preferred_element_type=jnp.float32
    )
    grad_attn_gain = jnp.sum(grad_first_normed_input[0] * first_unit_input[0], axis=0)
    wide = grad_projections.shape[1]
    small = jnp.concatenate(
        [
            grad_q_gain.reshape(groups, -1),
            grad_k_gain.reshape(groups, -1),
            grad_attn_gain.reshape(groups, -1),
            grad_expert_norm_gain.reshape(groups, -1),
            grad_router.reshape(groups, -1),
        ],
        axis=1,
    )
    small_rows = 32
    filled = small.shape[1]
    small = jnp.pad(small, ((0, 0), (0, small_rows * wide - filled)))
    summed, own_small, shared, outputs, grad_input, grad_down = closing(
        grad_projections.astype(jnp.bfloat16).reshape(groups, -1, wide),
        small.astype(jnp.bfloat16).reshape(groups, small_rows, wide),
        grad_first_normed_input[0].astype(jnp.bfloat16),
        grad_hidden,
        own_rows(first_unit_input[0]),
        own_rows(first_inverse_norm[0]),
        attention_norm_gain,
        output,
        top_all,
        scaled,
        w_down.shape,
        line,
    )
    gain_size, norm_size = local_width // groups, model_width // groups
    own_gains = own_small.reshape(-1)[: 2 * gain_size]
    shared = shared.reshape(-1)[2 * gain_size : filled]
    grad_out = lax.psum_scatter(
        grad_out.astype(jnp.bfloat16), "expert", scatter_dimension=0, tiled=True
    ).astype(jnp.float32)
    return (
        outputs[None],
        grad_input.astype(jnp.float32)[None],
        shared[:norm_size],
        summed[:, :local_width],
        summed[:, local_width : 2 * local_width],
        summed[:, 2 * local_width :],
        grad_out,
        own_gains[:gain_size],
        own_gains[gain_size:],
        shared[norm_size : 2 * norm_size],
        shared[2 * norm_size :].reshape(norm_size, experts),
        grad_gate.astype(jnp.float32),
        grad_up.astype(jnp.float32),
        grad_down.astype(jnp.float32),
    )


def solution(mesh):
    placed = (
        P(None, "expert", None),
        P(),
        P(None, "dp"),
        P(None, "dp"),
        P(None, "dp"),
        P("dp", None),
        P("dp"),
        P("dp"),
        P(),
        P(),
        P("expert", None, "dp"),
        P("expert", None, "dp"),
        P("expert", "dp", None),
        P("expert", None, None),
        P(),
        P(None, "expert", None),
    )
    return jax.shard_map(
        per_device,
        mesh=mesh,
        in_specs=placed,
        out_specs=(
            P(None, "expert", None),
            P(None, "expert", None),
            P("expert"),
            P("expert", "dp"),
            P("expert", "dp"),
            P("expert", "dp"),
            P(("dp", "expert"), None),
            P(("dp", "expert")),
            P(("dp", "expert")),
            P("expert"),
            P("expert", None),
            P("expert", None, "dp"),
            P("expert", None, "dp"),
            P("expert", "dp", None),
        ),
        check_vma=False,
    )
```

```python
import functools

import jax
import jax.numpy as jnp
from jax import lax
from jax.experimental import pallas as pl
from jax.experimental.pallas import tpu as pltpu
from jax.sharding import PartitionSpec as P

HD = 128


epsilon = 1e-05
rope_base = 10000.0
masked_score = -1e30


def doc_layout(lengths, pack_span):
    doc_ends = jnp.cumsum(lengths, axis=1)
    starts = doc_ends - lengths
    places = jnp.arange(pack_span, dtype=jnp.int32)
    segment = jnp.sum((places[None, :, None] >= doc_ends[:, None, :]).astype(jnp.int32), axis=2)
    member = segment[:, :, None] == jnp.arange(lengths.shape[1], dtype=jnp.int32)[None, None, :]
    begins = jnp.sum(jnp.where(member, starts[:, None, :], 0), axis=2)
    return (segment, places[None, :] - begins)


def rope_tables(positions, head_size):
    half_size = head_size // 2
    frequency = rope_base ** (-2.0 * jnp.arange(half_size, dtype=jnp.float32) / head_size)
    angles = positions.astype(jnp.float32)[..., None] * frequency
    cos, sin = jnp.cos(angles), jnp.sin(angles)
    return jnp.concatenate([cos, cos], axis=-1), jnp.concatenate([-sin, sin], axis=-1)


ALL = ("dp", "expert")


DEVICES = pl.DeviceIdType.MESH


def greet(device):
    pl.semaphore_signal(
        pltpu.get_barrier_semaphore(), inc=1, device_id=device, device_id_type=DEVICES
    )


def send(source, target, send_sem, arrive_sem, device):
    return pltpu.make_async_remote_copy(
        src_ref=source,
        dst_ref=target,
        send_sem=send_sem,
        recv_sem=arrive_sem,
        device_id=device,
        device_id_type=DEVICES,
    )


def contract(a, b, a_dim, b_dim):
    return lax.dot_general(
        a, b, (((a_dim,), (b_dim,)), ((), ())), preferred_element_type=jnp.float32
    )


def corners(dp):
    return dp + 1 - 2 * (dp % 2), (dp + 2) % 4


def gather_square_kernel(x_ref, out_ref, sent, arrived, own_sem):
    dp, place = lax.axis_index("dp"), lax.axis_index("expert")
    side_x, side_y = corners(dp)
    devices = ((side_x, place), (side_y, place))
    for device in devices:
        greet(device)
    pl.semaphore_wait(pltpu.get_barrier_semaphore(), 2)

    def copy(corner, p, way, source=None):
        target = out_ref.at[corner, p]
        return send(
            target if source is None else source,
            target,
            sent.at[corner, p, way],
            arrived.at[corner, p],
            devices[way],
        )

    for p in (0, 1):
        pltpu.make_async_copy(x_ref.at[p], out_ref.at[dp, p], own_sem.at[p]).start()
        for way in (0, 1):
            copy(dp, p, way, x_ref.at[p]).start()
    copy(side_x, 0, 0).wait_recv()
    copy(side_x, 0, 1).start()
    copy(side_y, 0, 0).wait_recv()
    copy(side_x, 1, 0).wait_recv()
    copy(side_y, 1, 0).wait_recv()
    copy(side_y, 1, 0).start()
    for p in (0, 1):
        copy(3 - dp, p, 0).wait_recv()
        for way in (0, 1):
            copy(dp, p, way).wait_send()
        pltpu.make_async_copy(x_ref.at[p], out_ref.at[dp, p], own_sem.at[p]).wait()
    copy(side_x, 0, 1).wait_send()
    copy(side_y, 1, 0).wait_send()


def gather_dp(rows):
    count, width = rows.shape
    gathered = pl.pallas_call(
        gather_square_kernel,
        out_shape=jax.ShapeDtypeStruct((4, 2, count // 2, width), rows.dtype),
        in_specs=[pl.BlockSpec(memory_space=pltpu.VMEM)],
        out_specs=pl.BlockSpec(memory_space=pl.ANY),
        scratch_shapes=[
            pltpu.SemaphoreType.DMA((4, 2, 2)),
            pltpu.SemaphoreType.DMA((4, 2)),
            pltpu.SemaphoreType.DMA((2,)),
        ],
        compiler_params=pltpu.CompilerParams(collective_id=10, has_side_effects=True),
        name="gather_dp",
    )(rows.reshape(2, count // 2, width))
    return gathered.reshape(4 * count, width)


def farthest(line, z, k):
    return ranked(line, z, k, lambda place, at: (-abs(place - at), place))


def reduce_kernel(
    square,
    line,
    paired,
    x_ref,
    out_ref,
    acc,
    got_pair,
    got_x,
    got_y,
    got_far_x,
    got_far_y,
    got_below,
    got_above,
    load_sem,
    pair_sem,
    x_sem,
    y_sem,
    far_x_sem,
    far_y_sem,
    below_sem,
    above_sem,
):
    dp, place = lax.axis_index("dp"), lax.axis_index("expert")
    z, c = place // 2, place % 2
    side_x, side_y = corners(dp)
    core = c if paired else 0
    own = dp if square else 0
    quarters = (3 - dp, side_x, side_y, dp) if square else (0,)
    to_x, to_y = (side_x, place), (side_y, place)
    to_pair, to_up, to_down = (dp, 2 * z + 1 - c), (dp, place + 2), (dp, place - 2)
    greeted = 0
    if square:
        greet(to_x)
        greet(to_y)
        greeted += 2
    if paired:
        greet(to_pair)
        greeted += 1
    if line > 1:
        pl.when(z > 0)(lambda: greet(to_down))
        pl.when(z < line - 1)(lambda: greet(to_up))
        greeted = greeted + (z > 0).astype(jnp.int32) + (z < line - 1).astype(jnp.int32)
    pl.semaphore_wait(pltpu.get_barrier_semaphore(), greeted)

    def load(q, height, p):
        return pltpu.make_async_copy(
            x_ref.at[q, height, core, p], acc.at[q, height, p], load_sem.at[q, height, p]
        )

    def hand(q, height, p):
        at = (q, height, p)
        source = x_ref.at[q, height, 1 - core, p]
        return send(source, got_pair.at[at], pair_sem.at[0, *at], pair_sem.at[1, *at], to_pair)

    def along_x(height, p):
        at = (height, p)
        return send(
            acc.at[side_x, height, p], got_x.at[at], x_sem.at[0, *at], x_sem.at[1, *at], to_x
        )

    def along_y(height, p):
        at = (height, p)
        return send(
            acc.at[side_y, height, p], got_y.at[at], y_sem.at[0, *at], y_sem.at[1, *at], to_y
        )

    def far_x(height):
        return send(
            acc.at[3 - dp, height, 0],
            got_far_x.at[height],
            far_x_sem.at[0, height],
            far_x_sem.at[1, height],
            to_x,
        )

    def far_y(height):
        return send(
            acc.at[3 - dp, height, 1],
            got_far_y.at[height],
            far_y_sem.at[0, height],
            far_y_sem.at[1, height],
            to_y,
        )

    def climb(height, p):
        at = (height, p)
        return send(
            acc.at[own, height, p], got_below.at[at], below_sem.at[0, *at], below_sem.at[1, *at], to_up
        )

    def descend(height, p):
        at = (height, p)
        return send(
            acc.at[own, height, p],
            got_above.at[at],
            above_sem.at[0, *at],
            above_sem.at[1, *at],
            to_down,
        )

    def height_of(k):
        return farthest(line, z, k) if line > 1 else 0

    def start(k, carry):
        for q in quarters:
            for p in (0, 1):
                load(q, height_of(k), p).start()
                if paired:
                    hand(q, height_of(k), p).start()
        return carry

    lax.fori_loop(0, line, start, 0)

    def step(k, carry):
        def cores():
            height = height_of(k)
            for q in quarters:
                for p in (0, 1):
                    load(q, height, p).wait()
                    if paired:
                        hand(q, height, p).wait_recv()
                        acc[q, height, p] = acc[q, height, p] + got_pair[q, height, p]
                if square and q is quarters[0]:
                    far_x(height).start()
                    far_y(height).start()

        def sides():
            height = height_of(k - 1)
            along_x(height, 0).start()
            along_y(height, 1).start()
            far_x(height).wait_recv()
            acc[side_y, height, 0] = acc[side_y, height, 0] + got_far_x[height]
            along_y(height, 0).start()
            far_y(height).wait_recv()
            acc[side_x, height, 1] = acc[side_x, height, 1] + got_far_y[height]
            along_x(height, 1).start()

        def column():
            height = height_of(k - 2)
            for p in (0, 1):
                if square:
                    along_x(height, p).wait_recv()
                    along_y(height, p).wait_recv()
                    total = acc[own, height, p].astype(jnp.float32)
                    total = total + got_x[height, p].astype(jnp.float32)
                    total = total + got_y[height, p].astype(jnp.float32)
                    acc[own, height, p] = total.astype(acc.dtype)
                if line > 1:
                    pl.when((z == 0) & (height > z))(lambda: climb(height, p).start())
                    pl.when((z == line - 1) & (height < z))(lambda: descend(height, p).start())

        def pass_on():
            height = height_of(k - 3)
            for p in (0, 1):

                def upwards():
                    climb(height, p).wait_recv()
                    acc[own, height, p] = acc[own, height, p] + got_below[height, p]
                    climb(height, p).start()

                def downwards():
                    descend(height, p).wait_recv()
                    acc[own, height, p] = acc[own, height, p] + got_above[height, p]
                    descend(height, p).start()

                pl.when((height > z) & (z > 0))(upwards)
                pl.when((height < z) & (z < line - 1))(downwards)

        pl.when(k < line)(cores)
        if square:
            pl.when((k >= 1) & (k < line + 1))(sides)
        pl.when((k >= 2) & (k < line + 2))(column)
        if line > 1:
            pl.when(k >= 3)(pass_on)
        return carry

    lax.fori_loop(0, line + (3 if line > 1 else 2), step, 0)
    home = z if line > 1 else 0
    for p in (0, 1):
        out_ref[p] = acc[own, home, p].astype(jnp.float32)
        if line > 1:

            def from_below():
                climb(z, p).wait_recv()
                out_ref[p] = out_ref[p] + got_below[z, p].astype(jnp.float32)

            def from_above():
                descend(z, p).wait_recv()
                out_ref[p] = out_ref[p] + got_above[z, p].astype(jnp.float32)

            pl.when(z > 0)(from_below)
            pl.when(z < line - 1)(from_above)

    def finish(height, carry):
        if square:
            far_x(height).wait_send()
            far_y(height).wait_send()
        for p in (0, 1):
            if paired:
                for q in quarters:
                    hand(q, height, p).wait_send()
            if square:
                along_x(height, p).wait_send()
                along_y(height, p).wait_send()
            if line > 1:
                pl.when(height > z)(lambda: climb(height, p).wait_send())
                pl.when(height < z)(lambda: descend(height, p).wait_send())
        return carry

    lax.fori_loop(0, line, finish, 0)


def reduce_to(parts, square, line, paired, name, number):
    _, rows, width = parts.shape
    quarters, cores, half = (4 if square else 1), (2 if paired else 1), rows // 2

    def space(used, *shape):
        return pltpu.VMEM((*shape, half, width) if used else (*shape, 16, 128), parts.dtype)

    sems = pltpu.SemaphoreType.DMA
    total = pl.pallas_call(
        functools.partial(reduce_kernel, square, line, paired),
        out_shape=jax.ShapeDtypeStruct((2, half, width), jnp.float32),
        in_specs=[pl.BlockSpec(memory_space=pl.ANY)],
        out_specs=pl.BlockSpec(memory_space=pltpu.VMEM),
        scratch_shapes=[
            space(True, quarters, line, 2),
            space(paired, quarters, line, 2),
            space(square, line, 2),
            space(square, line, 2),
            space(square, line),
            space(square, line),
            space(line > 1, line, 2),
            space(line > 1, line, 2),
            sems((quarters, line, 2)),
            sems((2, quarters, line, 2)),
            sems((2, line, 2)),
            sems((2, line, 2)),
            sems((2, line)),
            sems((2, line)),
            sems((2, line, 2)),
            sems((2, line, 2)),
        ],
        compiler_params=pltpu.CompilerParams(
            collective_id=number, has_side_effects=True, vmem_limit_bytes=60 << 20
        ),
        name=name,
    )(parts.reshape(quarters, line, cores, 2, half, width))
    return total.reshape(rows, width)


def scatter_dp(rows):
    return reduce_to(rows.reshape(4, -1, rows.shape[1]), True, 1, False, "scatter_dp", 3)


def visit_others(line, z, visit):
    def turn(k, carry):
        visit((z + k) % line)
        return carry

    lax.fori_loop(1, line, turn, 0)


def greet_line(line, dp, z, c):
    visit_others(line, z, lambda other: greet((dp, 2 * other + c)))
    greet((dp, 2 * z + 1 - c))
    pl.semaphore_wait(pltpu.get_barrier_semaphore(), line)


def columns(z):
    return pl.ds(pl.multiple_of(z * HD, HD), HD)


def to_heads_kernel(line, shared, *refs):
    count = len(shared)
    ins, outs = refs[:count], refs[count : 2 * count]
    sent, arrived, pair_sent, pair_arrived, own_sem = refs[2 * count :]
    dp, place = lax.axis_index("dp"), lax.axis_index("expert")
    z, c = place // 2, place % 2
    pair = (dp, 2 * z + 1 - c)
    greet_line(line, dp, z, c)

    def block(i, origin):
        return outs[i].at[origin, c] if shared[i] else outs[i].at[origin]

    def out(i, other):
        source = ins[i].at[:, columns(other)]
        device = (dp, 2 * other + c)
        return send(source, block(i, z), sent.at[i, other], arrived.at[i, z], device)

    def into(i, origin):
        part = block(i, origin)
        return send(part, part, sent.at[i, origin], arrived.at[i, origin], pair)

    def share(i, origin, source=None):
        part = block(i, origin)
        return send(
            part if source is None else source,
            part,
            pair_sent.at[i, origin],
            pair_arrived.at[i, origin],
            pair,
        )

    def own(i):
        return pltpu.make_async_copy(ins[i].at[:, columns(z)], block(i, z), own_sem.at[i])

    def dispatch(other):
        for i in range(count):
            out(i, other).start()

    visit_others(line, z, dispatch)
    for i in range(count):
        own(i).start()
        if shared[i]:
            share(i, z, ins[i].at[:, columns(z)]).start()

    def receive(origin):
        for i in range(count):
            into(i, origin).wait_recv()
            if shared[i]:
                share(i, origin).start()

    visit_others(line, z, receive)

    def finish(other):
        for i in range(count):
            out(i, other).wait_send()

    visit_others(line, z, finish)
    for i in range(count):
        own(i).wait()
        if shared[i]:

            def settle(origin, carry):
                share(i, origin).wait()
                return carry

            lax.fori_loop(0, line, settle, 0)


def to_heads(arrays, shared, line, name, number):
    rows = arrays[0].shape[0]
    count = len(arrays)
    sems = pltpu.SemaphoreType.DMA
    return pl.pallas_call(
        functools.partial(to_heads_kernel, line, shared),
        out_shape=[
            jax.ShapeDtypeStruct((line, 2, rows, HD) if both else (line, rows, HD), array.dtype)
            for array, both in zip(arrays, shared)
        ],
        in_specs=[pl.BlockSpec(memory_space=pltpu.VMEM)] * count,
        out_specs=[pl.BlockSpec(memory_space=pl.ANY)] * count,
        scratch_shapes=[sems((count, line))] * 4 + [sems((count,))],
        compiler_params=pltpu.CompilerParams(collective_id=number, has_side_effects=True),
        name=name,
    )(*arrays)


def to_tokens_kernel(line, summed, *refs):
    count, sums = len(summed), sum(summed)
    ins, outs = refs[:count], refs[count : 2 * count]
    mine, theirs = refs[2 * count : 2 * count + 2]
    sent, arrived, pair_sem, load_sem, own_sem = refs[2 * count + 2 :]
    dp, place = lax.axis_index("dp"), lax.axis_index("expert")
    z, c = place // 2, place % 2
    pair = (dp, 2 * z + 1 - c)
    greet_line(line, dp, z, c)
    at_sum = [sum(summed[:i]) for i in range(count)]

    def load(i, other):
        return pltpu.make_async_copy(
            ins[i].at[other, c], mine.at[at_sum[i], other], load_sem.at[at_sum[i], other]
        )

    def hand(i, other):
        s = at_sum[i]
        return send(
            ins[i].at[other, 1 - c],
            theirs.at[s, other],
            pair_sem.at[0, s, other],
            pair_sem.at[1, s, other],
            pair,
        )

    def source(i, other):
        return mine.at[at_sum[i], other] if summed[i] else ins[i].at[other]

    def out(i, other):
        target = outs[i].at[:, columns(z)]
        device = (dp, 2 * other + c)
        return send(source(i, other), target, sent.at[i, other], arrived.at[i, z], device)

    def into(i, origin):
        part = outs[i].at[:, columns(origin)]
        return send(part, part, sent.at[i, origin], arrived.at[i, origin], pair)

    def own(i):
        return pltpu.make_async_copy(source(i, z), outs[i].at[:, columns(z)], own_sem.at[i])

    def prepare(other):
        for i in range(count):
            if summed[i]:
                load(i, other).start()
                hand(i, other).start()

    def add(i, other):
        if summed[i]:
            load(i, other).wait()
            hand(i, other).wait_recv()
            s = at_sum[i]
            mine[s, other] = mine[s, other] + theirs[s, other]

    def dispatch(other):
        for i in range(count):
            add(i, other)
            out(i, other).start()

    if sums:
        visit_others(line, z, prepare)
        prepare(z)
    visit_others(line, z, dispatch)
    for i in range(count):
        add(i, z)
        own(i).start()

    def finish(other):
        for i in range(count):
            into(i, other).wait_recv()
            out(i, other).wait_send()
            if summed[i]:
                hand(i, other).wait_send()

    visit_others(line, z, finish)
    for i in range(count):
        own(i).wait()
        if summed[i]:
            hand(i, z).wait_send()


def to_tokens(arrays, summed, line, name, number):
    rows = arrays[0].shape[-2]
    count, sums = len(arrays), max(sum(summed), 1)
    sems = pltpu.SemaphoreType.DMA
    dtype = arrays[0].dtype
    held = (sums, line, rows, HD) if sum(summed) else (1, 1, 16, HD)
    return pl.pallas_call(
        functools.partial(to_tokens_kernel, line, summed),
        out_shape=[jax.ShapeDtypeStruct((rows, line * HD), dtype)] * count,
        in_specs=[pl.BlockSpec(memory_space=pl.ANY)] * count,
        out_specs=[pl.BlockSpec(memory_space=pl.ANY)] * count,
        scratch_shapes=[pltpu.VMEM(held, dtype)] * 2
        + [
            sems((count, line)),
            sems((count, line)),
            sems((2, sums, line)),
            sems((sums, line)),
            sems((count,)),
        ],
        compiler_params=pltpu.CompilerParams(collective_id=number, has_side_effects=True),
        name=name,
    )(*arrays)


KEY_TILE = 512


def masked_scores(keys, queries, tile, first, starts):
    scores = contract(keys, queries, 1, 1) * HD ** (-0.5)
    key_at = tile * KEY_TILE + lax.broadcasted_iota(jnp.int32, scores.shape, 0)
    query_at = first + lax.broadcasted_iota(jnp.int32, (1, scores.shape[1]), 1)
    return jnp.where((key_at >= starts) & (key_at <= query_at), scores, masked_score)


def attend_kernel(bounds, q_ref, k_ref, v_ref, start_ref, o_ref, total_ref):
    i = pl.program_id(0)
    queries, starts = q_ref[0], start_ref[0]
    span = queries.shape[0]

    def tile_step(tile, carry):
        largest, total, acc = carry
        rows = pl.ds(pl.multiple_of(tile * KEY_TILE, KEY_TILE), KEY_TILE)
        scores = masked_scores(k_ref[rows, :], queries, tile, bounds[2, i], starts)
        new = jnp.maximum(largest, jnp.max(scores, axis=0, keepdims=True))
        weights = jnp.exp(scores - new)
        fade = jnp.exp(largest - new)
        total = fade * total + jnp.sum(weights, axis=0, keepdims=True)
        acc = fade * acc + contract(v_ref[rows, :], weights.astype(jnp.bfloat16), 0, 0)
        return new, total, acc

    largest, total, acc = lax.fori_loop(
        bounds[0, i],
        bounds[1, i],
        tile_step,
        (
            jnp.full((1, span), masked_score, jnp.float32),
            jnp.zeros((1, span), jnp.float32),
            jnp.zeros((HD, span), jnp.float32),
        ),
    )
    o_ref[0] = (acc / total).T.astype(o_ref.dtype)
    total_ref[0] = largest + jnp.log(total)


def attend_back_kernel(
    bounds, q_ref, k_ref, v_ref, start_ref, total_ref, delta_ref, d_ref, dq_ref, dk_ref, dv_ref, dk, dv
):
    i = pl.program_id(0)
    queries, starts, grad = q_ref[0], start_ref[0], d_ref[0]
    total, delta = total_ref[0], delta_ref[0]

    @pl.when(i == 0)
    def _():
        dk[...] = jnp.zeros_like(dk)
        dv[...] = jnp.zeros_like(dv)

    def tile_step(tile, acc):
        rows = pl.ds(pl.multiple_of(tile * KEY_TILE, KEY_TILE), KEY_TILE)
        keys = k_ref[rows, :]
        scores = masked_scores(keys, queries, tile, bounds[2, i], starts)
        weights = jnp.exp(scores - total)
        grad_weights = contract(v_ref[rows, :], grad, 1, 1)
        grad_scores = (weights * (grad_weights - delta)).astype(jnp.bfloat16)
        dv[rows, :] += contract(weights.astype(jnp.bfloat16), grad, 1, 0)
        dk[rows, :] += contract(grad_scores, queries, 1, 0)
        return acc + contract(keys, grad_scores, 0, 0)

    acc = jnp.zeros((HD, queries.shape[0]), jnp.float32)
    acc = lax.fori_loop(bounds[0, i], bounds[1, i], tile_step, acc)
    dq_ref[0] = (acc * HD ** (-0.5)).T.astype(dq_ref.dtype)

    @pl.when(i == pl.num_programs(0) - 1)
    def _():
        dk_ref[...] = (dk[...] * HD ** (-0.5)).astype(dk_ref.dtype)
        dv_ref[...] = dv[...].astype(dv_ref.dtype)


def attend(bounds, queries, keys, values, starts):
    line, span, _ = queries.shape
    pack = keys.shape[0]
    block = pl.BlockSpec((1, span, HD), lambda i, _: (i, 0, 0))
    row = pl.BlockSpec((1, 1, span), lambda i, _: (i, 0, 0))
    whole = pl.BlockSpec((pack, HD), lambda i, _: (0, 0))
    return pl.pallas_call(
        attend_kernel,
        grid_spec=pltpu.PrefetchScalarGridSpec(
            num_scalar_prefetch=1,
            grid=(line,),
            in_specs=[block, whole, whole, row],
            out_specs=[block, row],
        ),
        out_shape=[
            jax.ShapeDtypeStruct(queries.shape, jnp.bfloat16),
            jax.ShapeDtypeStruct(starts.shape, jnp.float32),
        ],
        name="attend",
    )(bounds, queries, keys, values, starts)


def attend_back(bounds, queries, keys, values, starts, total, delta, grad):
    line, span, _ = queries.shape
    pack = keys.shape[0]
    block = pl.BlockSpec((1, span, HD), lambda i, _: (i, 0, 0))
    row = pl.BlockSpec((1, 1, span), lambda i, _: (i, 0, 0))
    whole = pl.BlockSpec((pack, HD), lambda i, _: (0, 0))
    return pl.pallas_call(
        attend_back_kernel,
        grid_spec=pltpu.PrefetchScalarGridSpec(
            num_scalar_prefetch=1,
            grid=(line,),
            in_specs=[block, whole, whole, row, row, row, block],
            out_specs=[block, whole, whole],
            scratch_shapes=[pltpu.VMEM((pack, HD), jnp.float32)] * 2,
        ),
        out_shape=[jax.ShapeDtypeStruct(queries.shape, jnp.bfloat16)]
        + [jax.ShapeDtypeStruct((pack, HD), jnp.bfloat16)] * 2,
        name="attend_back",
    )(bounds, queries, keys, values, starts, total, delta, grad)


def by_head(layout, line):
    positions = layout[1][0]
    pack = positions.shape[0]
    span = pack // (2 * line)
    core = lax.axis_index("expert") % 2
    starts = (jnp.arange(pack, dtype=jnp.int32) - positions).reshape(line, 2, 1, span)
    starts = lax.dynamic_index_in_dim(starts, core, 1, keepdims=False)
    first = (2 * jnp.arange(line, dtype=jnp.int32) + core) * span
    bounds = jnp.stack(
        [starts[:, 0, 0] // KEY_TILE, (first + span - 1) // KEY_TILE + 1, first]
    ).astype(jnp.int32)

    def forward(queries, keys, values):
        q, k, v = to_heads(
            [queries, keys, values], (False, True, True), line, "scatter_heads", 6
        )
        k, v = k.reshape(pack, HD), v.reshape(pack, HD)
        out, total = attend(bounds, q, k, v, starts)
        (attended,) = to_tokens([out], (False,), line, "gather_heads", 7)
        return attended, (q, k, v, out, total)

    def backward(kept, grad):
        q, k, v, out, total = kept
        (grad,) = to_heads([grad], (False,), line, "scatter_grads", 8)
        delta = jnp.sum(grad.astype(jnp.float32) * out.astype(jnp.float32), axis=-1)
        dq, dk, dv = attend_back(bounds, q, k, v, starts, total, delta[:, None, :], grad)
        shape = (line, 2, span, HD)
        return to_tokens(
            [dq, dk.reshape(shape), dv.reshape(shape)],
            (False, True, True),
            line,
            "gather_grads",
            9,
        )

    return forward, backward


def by_query(layout, offset_rows):
    segment = layout[0][0]
    pack = segment.shape[0]

    def heads(rows):
        return rows.reshape(rows.shape[0], -1, HD)

    def score_block(queries, keys):
        rows = queries.shape[0]
        scores = jnp.einsum("shd,lhd->hsl", queries, keys, preferred_element_type=jnp.float32)
        own = lax.dynamic_slice_in_dim(segment, offset_rows, rows, 0)
        query_places = offset_rows + jnp.arange(rows, dtype=jnp.int32)
        key_places = jnp.arange(pack, dtype=jnp.int32)
        allowed = (own[:, None] == segment[None, :]) & (
            key_places[None, :] <= query_places[:, None]
        )
        return jnp.where(allowed[None], scores * HD ** (-0.5), masked_score)

    def forward(queries, keys, values):
        q = heads(queries)
        k = heads(lax.all_gather(keys, "expert", axis=0, tiled=True))
        v = heads(lax.all_gather(values, "expert", axis=0, tiled=True))
        scores = score_block(q, k)
        largest = jnp.max(scores, axis=-1, keepdims=True)
        total = largest + jnp.log(jnp.sum(jnp.exp(scores - largest), axis=-1, keepdims=True))
        weights = jnp.exp(scores - total).astype(jnp.bfloat16)
        attended = jnp.einsum("hsl,lhd->shd", weights, v, preferred_element_type=jnp.float32)
        return attended.astype(jnp.bfloat16).reshape(queries.shape), (q, k, v, total)

    def backward(kept, grad):
        q, k, v, total = kept
        shape = grad.shape
        grad = heads(grad)
        weights = jnp.exp(score_block(q, k) - total)
        grad_weights = jnp.einsum("shd,lhd->hsl", grad, v, preferred_element_type=jnp.float32)
        delta = jnp.sum(weights * grad_weights, axis=-1, keepdims=True)
        grad_scores = (weights * (grad_weights - delta)).astype(jnp.bfloat16)
        dq = jnp.einsum("hsl,lhd->shd", grad_scores, k, preferred_element_type=jnp.float32)
        dk = jnp.einsum("hsl,shd->lhd", grad_scores, q, preferred_element_type=jnp.float32)
        weights = weights.astype(jnp.bfloat16)
        dv = jnp.einsum("hsl,shd->lhd", weights, grad, preferred_element_type=jnp.float32)

        def to_owner(part):
            part = part.astype(jnp.bfloat16).reshape(pack, shape[1])
            return lax.psum_scatter(part, "expert", scatter_dimension=0, tiled=True)

        scale = HD ** (-0.5)
        return (dq * scale).reshape(shape), to_owner(dk * scale), to_owner(dv)

    return forward, backward


def nearest(line, z, k):
    return ranked(line, z, k, lambda place, at: (abs(place - at), place))


def ranked(line, z, k, rank):
    total = jnp.int32(0)
    for at in range(line):
        order = sorted(range(line), key=lambda place: rank(place, at))
        place = sum([jnp.where(k == i, order[i], 0) for i in range(line)])
        total = total + jnp.where(z == at, place, 0)
    return total


def gate_act_kernel(
    line,
    x_ref,
    top_ref,
    wg_ref,
    wu_ref,
    wd_ref,
    xn_ref,
    grads_ref,
    scaled_ref,
    gates_ref,
    xbuf,
    top_buf,
    grads_buf,
    scaled_buf,
    gates_buf,
    sent,
    arrived,
    own_sem,
    top_sem,
    xn_sem,
    grads_sem,
    scaled_sem,
    gates_sem,
):
    dp, place = lax.axis_index("dp"), lax.axis_index("expert")
    z, c = place // 2, place % 2
    side_x, side_y = corners(dp)
    far = 3 - dp
    devices = (
        (dp, place + 2),
        (dp, place - 2),
        (side_x, place),
        (side_y, place),
        (dp, 2 * z + 1 - c),
    )
    up, down, along_x, along_y, pair = range(5)
    has_up, has_down = z < line - 1, z > 0
    for way in (along_x, along_y, pair):
        greet(devices[way])
    pl.when(has_up)(lambda: greet(devices[up]))
    pl.when(has_down)(lambda: greet(devices[down]))
    greeted = 3 + has_up.astype(jnp.int32) + has_down.astype(jnp.int32)
    pl.semaphore_wait(pltpu.get_barrier_semaphore(), greeted)
    local, width, units = wg_ref.shape
    rows = top_buf.shape[1]
    first = place * local

    def slot(corner, height, core):
        return corner * (2 * line) + 2 * height + core

    def copy(s, p, way, source=None):
        target = xbuf.at[s, p]
        return send(
            target if source is None else source,
            target,
            sent.at[s, p, way],
            arrived.at[s, p],
            devices[way],
        )

    def arrive(s, p):
        copy(s, p, pair).wait_recv()

    mine = slot(dp, z, c)
    for p in (0, 1):
        pltpu.make_async_copy(x_ref.at[p], xbuf.at[mine, p], own_sem.at[p]).start()
        pl.when(has_up)(lambda: copy(mine, p, up, x_ref.at[p]).start())
        pl.when(has_down)(lambda: copy(mine, p, down, x_ref.at[p]).start())
        for way in (along_x, along_y, pair):
            copy(mine, p, way, x_ref.at[p]).start()

    def decode(i):
        turn, j = i // 4, i % 4
        k = turn - (j > 0).astype(jnp.int32) - (j == 3).astype(jnp.int32)
        valid = (i >= 0) & (k >= 0) & (k < line)
        corner = jnp.where(j == 0, dp, jnp.where(j == 1, side_x, jnp.where(j == 2, side_y, far)))
        return j, k, valid, corner, nearest(line, z, k)

    def top_load(i, corner, height):
        block = corner * line + height
        return pltpu.make_async_copy(top_ref.at[block], top_buf.at[i % 2], top_sem.at[i % 2])

    def xn_out(block):
        return pltpu.make_async_copy(
            xbuf.at[pl.ds(2 * block, 2), :, :, pl.ds(0, width)],
            xn_ref.at[pl.ds(2 * block, 2)],
            xn_sem.at[block],
        )

    def grads_out(block):
        return pltpu.make_async_copy(grads_buf.at[block], grads_ref.at[block], grads_sem.at[block])

    def scaled_out(block):
        return pltpu.make_async_copy(
            scaled_buf.at[block], scaled_ref.at[block], scaled_sem.at[block]
        )

    def gates_out(block):
        return pltpu.make_async_copy(gates_buf.at[block], gates_ref.at[block], gates_sem.at[block])

    def compute(i):
        j, k, _, corner, height = decode(i)
        block = corner * line + height
        for p in (0, 1):
            arrive(slot(corner, height, 1 - c), p)
        xn_out(block).start()
        top_load(i, corner, height).wait()
        lanes = lax.broadcasted_iota(jnp.int32, (rows, 128), 1)

        def tokens():
            return xbuf[pl.ds(2 * block, 2), :, :, pl.ds(0, width)].reshape(rows, width)

        table = xbuf[pl.ds(2 * block, 2), :, :, pl.ds(width, 128)].reshape(rows, 128)
        table = table.astype(jnp.float32)
        gate_grads = jnp.zeros((rows, 128), jnp.float32)
        for e in range(local):
            at = (lanes == first + e) | (lanes == first + e + 64)
            gate = jnp.sum(jnp.where(at, table, 0.0), axis=1, keepdims=True)
            g = contract(tokens(), wg_ref[e], 1, 0)
            u = contract(tokens(), wu_ref[e], 1, 0)
            h = contract(top_buf[i % 2], wd_ref[e], 1, 1)
            sigmoid = 1.0 / (1.0 + jnp.exp(-g))
            silu = g * sigmoid
            act = silu * u
            gate_grad = jnp.sum(act * h, axis=1, keepdims=True)
            gate_grads = gate_grads + jnp.where(lanes == first + e, gate_grad, 0.0)
            grad_act = h * gate
            dg = grad_act * u * sigmoid * (1.0 + g * (1.0 - sigmoid))
            du = grad_act * silu
            scaled_buf[block, :, e * units : (e + 1) * units] = (act * gate).astype(jnp.bfloat16)
            grads_buf[block, :, e * units : (e + 1) * units] = dg.astype(jnp.bfloat16)
            at = (local + e) * units
            grads_buf[block, :, at : at + units] = du.astype(jnp.bfloat16)
        gates_buf[block] = gate_grads.astype(jnp.bfloat16)
        grads_out(block).start()
        scaled_out(block).start()
        gates_out(block).start()

    def step(i, carry):
        j, k, valid, corner, height = decode(i)
        s = slot(corner, height, c)

        def own():
            for p in (0, 1):
                pltpu.make_async_copy(x_ref.at[p], xbuf.at[mine, p], own_sem.at[p]).wait()

        def column():
            for p in (0, 1):
                arrive(s, p)
                pl.when(has_up & (height < z))(lambda: copy(s, p, up).start())
                pl.when(has_down & (height > z))(lambda: copy(s, p, down).start())
                for way in (along_x, along_y, pair):
                    copy(s, p, way).start()

        def sides():
            for p in (0, 1):
                arrive(s, p)
                copy(s, p, pair).start()
            pl.when(j == 1)(lambda: copy(s, 0, along_y).start())
            pl.when(j == 2)(lambda: copy(s, 1, along_x).start())

        def opposite():
            for p in (0, 1):
                arrive(s, p)
                copy(s, p, pair).start()

        pl.when(valid & (j == 0) & (k == 0))(own)
        pl.when(valid & (j == 0) & (k > 0))(column)
        pl.when(valid & ((j == 1) | (j == 2)))(sides)
        pl.when(valid & (j == 3))(opposite)
        pl.when(valid)(lambda: top_load(i, corner, height).start())
        pl.when(decode(i - 1)[2])(lambda: compute(i - 1))
        return carry

    lax.fori_loop(0, 4 * (line + 2) + 1, step, 0)

    def finish(height, carry):
        for p in (0, 1):
            for corner in range(4):
                copy(slot(corner, height, c), p, pair).wait_send()
            s = slot(dp, height, c)
            copy(s, p, along_x).wait_send()
            copy(s, p, along_y).wait_send()
            pl.when(has_up & (height <= z))(lambda: copy(s, p, up).wait_send())
            pl.when(has_down & (height >= z))(lambda: copy(s, p, down).wait_send())
        copy(slot(side_x, height, c), 0, along_y).wait_send()
        copy(slot(side_y, height, c), 1, along_x).wait_send()
        for corner in range(4):
            block = corner * line + height
            xn_out(block).wait()
            grads_out(block).wait()
            scaled_out(block).wait()
            gates_out(block).wait()
        return carry

    lax.fori_loop(0, line, finish, 0)


def gate_act(own, tops, w_gate, w_up, w_down, line):
    count, wide = own.shape
    local, width, units = w_gate.shape
    slots, blocks, rows, half = 8 * line, 4 * line, 2 * count, count // 2
    sems = pltpu.SemaphoreType.DMA
    dtype = own.dtype
    xn, grads, scaled, gates = pl.pallas_call(
        functools.partial(gate_act_kernel, line),
        out_shape=[
            jax.ShapeDtypeStruct((slots, 2, half, width), dtype),
            jax.ShapeDtypeStruct((blocks, rows, 2 * local * units), dtype),
            jax.ShapeDtypeStruct((blocks, rows, local * units), dtype),
            jax.ShapeDtypeStruct((blocks, rows, 128), dtype),
        ],
        in_specs=[
            pl.BlockSpec(memory_space=pltpu.VMEM),
            pl.BlockSpec(memory_space=pl.ANY),
            pl.BlockSpec(memory_space=pltpu.VMEM),
            pl.BlockSpec(memory_space=pltpu.VMEM),
            pl.BlockSpec(memory_space=pltpu.VMEM),
        ],
        out_specs=[pl.BlockSpec(memory_space=pl.ANY)] * 4,
        scratch_shapes=[
            pltpu.VMEM((slots, 2, half, wide), dtype),
            pltpu.VMEM((2, rows, width), dtype),
            pltpu.VMEM((blocks, rows, 2 * local * units), dtype),
            pltpu.VMEM((blocks, rows, local * units), dtype),
            pltpu.VMEM((blocks, rows, 128), dtype),
            sems((slots, 2, 5)),
            sems((slots, 2)),
            sems((2,)),
            sems((2,)),
            sems((blocks,)),
            sems((blocks,)),
            sems((blocks,)),
            sems((blocks,)),
        ],
        compiler_params=pltpu.CompilerParams(
            collective_id=1, has_side_effects=True, vmem_limit_bytes=60 << 20
        ),
        name="gate_act",
    )(own.reshape(2, half, wide), tops.reshape(blocks, rows, width), w_gate, w_up, w_down)
    return xn.reshape(slots * count, width), grads, scaled, gates


def column_products(left_ref, right_ref, chunk_buf, right_buf, total, chunk_sem, right_sem, store):
    span = chunk_buf.shape[2]
    blocks, rows, _ = right_buf.shape
    joined = max(1, min(blocks, 1024 // rows))
    depth = joined * rows
    turns = left_ref.shape[1] // span

    def at(n):
        return pl.ds(pl.multiple_of(n * span, span), span)

    def chunk(n):
        return pltpu.make_async_copy(
            left_ref.at[:, at(n)], chunk_buf.at[n % 2], chunk_sem.at[n % 2]
        )

    right_load = pltpu.make_async_copy(right_ref, right_buf, right_sem.at[0])
    chunk(0).start()
    right_load.start()

    def turn(n):
        pl.when(n + 1 < turns)(lambda: chunk(n + 1).start())
        chunk(n).wait()
        pl.when(n == 0)(right_load.wait)
        total[...] = jnp.zeros_like(total)

        def part(k, carry):
            left = chunk_buf[n % 2, pl.ds(pl.multiple_of(k * depth, depth), depth), :]
            right = right_buf[pl.ds(k * joined, joined)].reshape(depth, right_buf.shape[2])
            total[...] += contract(left, right, 0, 0)
            return carry

        lax.fori_loop(0, blocks // joined, part, 0)
        store(n, at(n))

    return turn, turns


def gate_up_grads(
    xn_ref, units_ref, gate_ref, up_ref, chunk_buf, units_buf, total, both, chunk_sem, units_sem, out_sem
):
    local, _, units = gate_ref.shape
    outs = (gate_ref, up_ref)

    def copies(at):
        return [
            pltpu.make_async_copy(
                both.at[:, pl.ds((kind * local + e) * units, units)],
                outs[kind].at[e, at, :],
                out_sem.at[kind, e],
            )
            for kind in (0, 1)
            for e in range(local)
        ]

    start = pl.ds(0, chunk_buf.shape[2])

    def store(n, at):
        @pl.when(n > 0)
        def _():
            for copy in copies(start):
                copy.wait()

        both[...] = total[...].astype(both.dtype)
        for copy in copies(at):
            copy.start()

    def end():
        for copy in copies(start):
            copy.wait()

    turn, turns = column_products(
        xn_ref, units_ref, chunk_buf, units_buf, total, chunk_sem, units_sem, store
    )
    return turn, end, turns


def down_grads(
    top_ref, scaled_ref, down_ref, chunk_buf, scaled_buf, total, out, chunk_sem, scaled_sem, out_sem
):
    local, units, _ = down_ref.shape

    def copies(at):
        return [
            pltpu.make_async_copy(out.at[e], down_ref.at[e, :, at], out_sem.at[e])
            for e in range(local)
        ]

    start = pl.ds(0, chunk_buf.shape[2])

    def store(n, at):
        @pl.when(n > 0)
        def _():
            for copy in copies(start):
                copy.wait()

        for e in range(local):
            out[e] = total[:, e * units : (e + 1) * units].T.astype(out.dtype)
        for copy in copies(at):
            copy.start()

    def end():
        for copy in copies(start):
            copy.wait()

    turn, turns = column_products(
        top_ref, scaled_ref, chunk_buf, scaled_buf, total, chunk_sem, scaled_sem, store
    )
    return turn, end, turns


SPAN = 256


def product_sum_kernel(
    line,
    flipped,
    extra,
    grads,
    *refs,
):
    a_ref, w_ref = refs[0], refs[1]
    e_ref = refs[2] if extra else None
    refs = refs[3:] if extra else refs[2:]
    if grads:
        work_refs, refs = (*refs[:2], *refs[3:5], *refs[-7:]), (refs[2], *refs[5:-7])
    (
        out_ref,
        made,
        a_buf,
        e_buf,
        got_pair,
        got_x,
        got_y,
        got_far_x,
        got_far_y,
        got_below,
        got_above,
        load_sem,
        extra_sem,
        pair_sem,
        x_sem,
        y_sem,
        far_x_sem,
        far_y_sem,
        below_sem,
        above_sem,
    ) = refs
    dp, place = lax.axis_index("dp"), lax.axis_index("expert")
    z, c = place // 2, place % 2
    side_x, side_y = corners(dp)
    far = 3 - dp
    to_x, to_y, to_pair = (side_x, place), (side_y, place), (dp, 2 * z + 1 - c)
    to_up, to_down = (dp, place + 2), (dp, place - 2)
    for device in (to_x, to_y, to_pair):
        greet(device)
    pl.when(z > 0)(lambda: greet(to_down))
    pl.when(z < line - 1)(lambda: greet(to_up))
    greeted = 3 + (z > 0).astype(jnp.int32) + (z < line - 1).astype(jnp.int32)
    pl.semaphore_wait(pltpu.get_barrier_semaphore(), greeted)
    count = 4 * line
    width = w_ref.shape[0] if flipped else w_ref.shape[1]
    half = made.shape[4]
    chunk = 512

    def mine(q, height, p):
        return made.at[q, height, c, p]

    def hand(q, height, p):
        at = (q, height, p)
        source = made.at[q, height, 1 - c, p]
        return send(source, got_pair.at[at], pair_sem.at[0, *at], pair_sem.at[1, *at], to_pair)

    def along_x(height, p):
        at = (height, p)
        source = mine(side_x, height, p)
        return send(source, got_x.at[at], x_sem.at[0, *at], x_sem.at[1, *at], to_x)

    def along_y(height, p):
        at = (height, p)
        source = mine(side_y, height, p)
        return send(source, got_y.at[at], y_sem.at[0, *at], y_sem.at[1, *at], to_y)

    def far_x(height):
        source = mine(far, height, 0)
        return send(
            source, got_far_x.at[height], far_x_sem.at[0, height], far_x_sem.at[1, height], to_x
        )

    def far_y(height):
        source = mine(far, height, 1)
        return send(
            source, got_far_y.at[height], far_y_sem.at[0, height], far_y_sem.at[1, height], to_y
        )

    def climb(height, p):
        at = (height, p)
        source = mine(dp, height, p)
        return send(source, got_below.at[at], below_sem.at[0, *at], below_sem.at[1, *at], to_up)

    def descend(height, p):
        at = (height, p)
        source = mine(dp, height, p)
        return send(source, got_above.at[at], above_sem.at[0, *at], above_sem.at[1, *at], to_down)

    def decode(i):
        k, j = i // 4, i % 4
        q = jnp.where(j == 0, far, jnp.where(j == 1, side_x, jnp.where(j == 2, side_y, dp)))
        return k, j, q, farthest(line, z, k)

    def load(i):
        _, _, q, height = decode(i)
        return pltpu.make_async_copy(
            a_ref.at[q * line + height], a_buf.at[i % 2], load_sem.at[i % 2]
        )

    def load_extra(i):
        _, _, q, height = decode(i)
        return pltpu.make_async_copy(
            e_ref.at[q * line + height], e_buf.at[i % 2], extra_sem.at[i % 2]
        )

    def start_load(i):
        load(i).start()
        if extra:
            load_extra(i).start()

    def add(q, height, p, other):
        at = (q, height, c, p)
        made[at] = made[at] + other[...]

    def compute(i):
        _, _, q, height = decode(i)
        load(i).wait()
        if extra:
            load_extra(i).wait()
        pl.when(i + 1 < count)(lambda: start_load(i + 1))
        for at in range(0, width, chunk):
            if flipped:
                part = contract(a_buf[i % 2], w_ref[at : at + chunk, :], 1, 1)
            else:
                part = contract(a_buf[i % 2], w_ref[:, at : at + chunk], 1, 0)
            part = part.astype(made.dtype).reshape(2, 2, half, chunk)
            made[q, height, :, :, :, at : at + chunk] = part
        if extra:
            made[q, height, :, :, :, width : width + 128] = e_buf[i % 2].reshape(2, 2, half, 128)
        for p in (0, 1):
            hand(q, height, p).start()

    def settle(i):
        _, j, q, height = decode(i)
        for p in (0, 1):
            hand(q, height, p).wait_recv()
            add(q, height, p, got_pair.at[q, height, p])

        def opposite():
            far_x(height).start()
            far_y(height).start()

        pl.when(j == 0)(opposite)
        pl.when(j == 1)(lambda: along_x(height, 0).start())
        pl.when(j == 2)(lambda: along_y(height, 1).start())

    def settle_far(i):
        _, j, _, height = decode(i)

        def side_of_x():
            far_y(height).wait_recv()
            add(side_x, height, 1, got_far_y.at[height])
            along_x(height, 1).start()

        def side_of_y():
            far_x(height).wait_recv()
            add(side_y, height, 0, got_far_x.at[height])
            along_y(height, 0).start()

        pl.when(j == 1)(side_of_x)
        pl.when(j == 2)(side_of_y)

    def column(height):
        for p in (0, 1):
            along_x(height, p).wait_recv()
            along_y(height, p).wait_recv()
            total = made[dp, height, c, p].astype(jnp.float32)
            total = total + got_x[height, p].astype(jnp.float32)
            total = total + got_y[height, p].astype(jnp.float32)
            made[dp, height, c, p] = total.astype(made.dtype)
            pl.when((z == 0) & (height > z))(lambda: climb(height, p).start())
            pl.when((z == line - 1) & (height < z))(lambda: descend(height, p).start())

    def pass_on(height):
        for p in (0, 1):

            def upwards():
                climb(height, p).wait_recv()
                add(dp, height, p, got_below.at[height, p])
                climb(height, p).start()

            def downwards():
                descend(height, p).wait_recv()
                add(dp, height, p, got_above.at[height, p])
                descend(height, p).start()

            pl.when((height > z) & (z > 0))(upwards)
            pl.when((height < z) & (z < line - 1))(downwards)

    start_load(0)
    work, work_end, turns = gate_up_grads(*work_refs) if grads else (None, None, 1)

    def step(i, carry):
        k, j, _, _ = decode(i)
        pl.when(i < count)(lambda: compute(i))
        pl.when((i >= 1) & (i <= count))(lambda: settle(i - 1))
        if grads:
            every = count // turns
            pl.when((i < count) & (i % every == 0))(lambda: work(i // every))
        pl.when((i >= 4) & (i < count + 4))(lambda: settle_far(i - 4))
        pl.when((k >= 3) & (j == 2))(lambda: pass_on(farthest(line, z, k - 3)))
        pl.when((k >= 2) & (j == 3))(lambda: column(farthest(line, z, k - 2)))
        return carry

    lax.fori_loop(0, count + 8, step, 0)
    if grads:
        work_end()
    for p in (0, 1):
        out_ref[p] = made[dp, z, c, p].astype(jnp.float32)

        def from_below():
            climb(z, p).wait_recv()
            out_ref[p] = out_ref[p] + got_below[z, p].astype(jnp.float32)

        def from_above():
            descend(z, p).wait_recv()
            out_ref[p] = out_ref[p] + got_above[z, p].astype(jnp.float32)

        pl.when(z > 0)(from_below)
        pl.when(z < line - 1)(from_above)

    def finish(height, carry):
        far_x(height).wait_send()
        far_y(height).wait_send()
        for p in (0, 1):
            for q in range(4):
                hand(q, height, p).wait_send()
            along_x(height, p).wait_send()
            along_y(height, p).wait_send()
            pl.when(height > z)(lambda: climb(height, p).wait_send())
            pl.when(height < z)(lambda: descend(height, p).wait_send())
        return carry

    lax.fori_loop(0, line, finish, 0)


def product_sum(blocks, weights, flipped, extra, line, name, number, grads=None):
    count, rows, depth = blocks.shape
    width = weights.shape[0] if flipped else weights.shape[1]
    wide = width + (0 if extra is None else 128)
    half = rows // 4
    sems = pltpu.SemaphoreType.DMA
    dtype = blocks.dtype

    def space(*shape):
        return pltpu.VMEM((*shape, half, wide), dtype)

    anywhere, inside = pl.BlockSpec(memory_space=pl.ANY), pl.BlockSpec(memory_space=pltpu.VMEM)
    out_shape = [jax.ShapeDtypeStruct((2, half, wide), jnp.float32)]
    work_in, work_space = [], []
    if grads is not None:
        xn, both, shape = grads
        work_in = [xn, both]
        out_shape += [jax.ShapeDtypeStruct(shape, dtype)] * 2
        work_space = [
            pltpu.VMEM((2, xn.shape[0], SPAN), dtype),
            pltpu.VMEM(both.shape, dtype),
            pltpu.VMEM((SPAN, both.shape[2]), jnp.float32),
            pltpu.VMEM((SPAN, both.shape[2]), dtype),
            sems((2,)),
            sems((1,)),
            sems((2, shape[0])),
        ]
    total, *work_out = pl.pallas_call(
        functools.partial(product_sum_kernel, line, flipped, extra is not None, grads is not None),
        out_shape=out_shape,
        in_specs=[anywhere, inside]
        + ([] if extra is None else [anywhere])
        + [anywhere] * len(work_in),
        out_specs=[inside] + [anywhere] * (len(out_shape) - 1),
        scratch_shapes=[
            space(4, line, 2, 2),
            pltpu.VMEM((2, rows, depth), dtype),
            pltpu.VMEM((2, rows, 128), dtype),
            space(4, line, 2),
            space(line, 2),
            space(line, 2),
            space(line),
            space(line),
            space(line, 2),
            space(line, 2),
            sems((2,)),
            sems((2,)),
            sems((2, 4, line, 2)),
            sems((2, line, 2)),
            sems((2, line, 2)),
            sems((2, line)),
            sems((2, line)),
            sems((2, line, 2)),
            sems((2, line, 2)),
            *work_space,
        ],
        compiler_params=pltpu.CompilerParams(
            collective_id=number, has_side_effects=True, vmem_limit_bytes=63 << 20
        ),
        name=name,
    )(blocks, weights, *([] if extra is None else [extra]), *work_in)
    return total.reshape(2 * half, wide), *work_out


def closing_kernel(
    line,
    shared_rows,
    parts_ref,
    small_ref,
    first_ref,
    grad_ref,
    unit_ref,
    inverse_ref,
    gain_ref,
    output_ref,
    top_ref,
    scaled_ref,
    summed_ref,
    shared_ref,
    outputs_ref,
    grads_ref,
    down_ref,
    acc,
    got_pair,
    got_below,
    got_above,
    part,
    got_x,
    got_y,
    got_far_x,
    got_far_y,
    grad_own,
    small,
    got_small,
    load_sem,
    pair_sem,
    load_small_sem,
    pair_small_sem,
    below_sem,
    above_sem,
    part_sem,
    x_sem,
    y_sem,
    far_x_sem,
    far_y_sem,
    spread_sem,
    arrive_sem,
    own_sem,
    small_sem,
    *work_refs,
):
    dp, place = lax.axis_index("dp"), lax.axis_index("expert")
    z, c = place // 2, place % 2
    side_x, side_y = corners(dp)
    far = 3 - dp
    to_x, to_y, to_pair = (side_x, place), (side_y, place), (dp, 2 * z + 1 - c)
    to_up, to_down = (dp, place + 2), (dp, place - 2)
    for device in (to_x, to_y, to_pair):
        greet(device)
    pl.when(z > 0)(lambda: greet(to_down))
    pl.when(z < line - 1)(lambda: greet(to_up))
    greeted = 3 + (z > 0).astype(jnp.int32) + (z < line - 1).astype(jnp.int32)
    pl.semaphore_wait(pltpu.get_barrier_semaphore(), greeted)

    large = parts_ref.shape[3]
    top_rows, low_rows = pl.ds(0, large), pl.ds(large, shared_rows // 2)

    def loads(height, p):
        return (
            pltpu.make_async_copy(
                parts_ref.at[height, c, p], acc.at[height, p, top_rows], load_sem.at[height, p]
            ),
            pltpu.make_async_copy(
                small_ref.at[height, c, p], acc.at[height, p, low_rows], load_small_sem.at[height, p]
            ),
        )

    def hands(height, p):
        at = (height, p)
        return (
            send(
                parts_ref.at[height, 1 - c, p],
                got_pair.at[height, p, top_rows],
                pair_sem.at[0, *at],
                pair_sem.at[1, *at],
                to_pair,
            ),
            send(
                small_ref.at[height, 1 - c, p],
                got_pair.at[height, p, low_rows],
                pair_small_sem.at[0, *at],
                pair_small_sem.at[1, *at],
                to_pair,
            ),
        )

    def climb(height, p):
        at = (height, p)
        return send(
            acc.at[at], got_below.at[at], below_sem.at[0, *at], below_sem.at[1, *at], to_up
        )

    def descend(height, p):
        at = (height, p)
        return send(
            acc.at[at], got_above.at[at], above_sem.at[0, *at], above_sem.at[1, *at], to_down
        )

    def start(k, carry):
        height = farthest(line, z, k)
        for p in (0, 1):
            for copy in (*loads(height, p), *hands(height, p)):
                copy.start()
        return carry

    def pair_sum(k, carry):
        height = farthest(line, z, k)
        for p in (0, 1):
            for copy in loads(height, p):
                copy.wait()
            for copy in hands(height, p):
                copy.wait_recv()
            acc[height, p] = acc[height, p] + got_pair[height, p]
            pl.when((z == 0) & (height > z))(lambda: climb(height, p).start())
            pl.when((z == line - 1) & (height < z))(lambda: descend(height, p).start())
        return carry

    def pass_on(k, carry):
        height = farthest(line, z, k)
        for p in (0, 1):

            def upwards():
                climb(height, p).wait_recv()
                acc[height, p] = acc[height, p] + got_below[height, p]
                climb(height, p).start()

            def downwards():
                descend(height, p).wait_recv()
                acc[height, p] = acc[height, p] + got_above[height, p]
                descend(height, p).start()

            pl.when((height > z) & (z > 0))(upwards)
            pl.when((height < z) & (z < line - 1))(downwards)
        return carry

    def first_load(q, p):
        return pltpu.make_async_copy(first_ref.at[q, p], part.at[q, p], part_sem.at[q, p])

    def along_x(p):
        return send(part.at[side_x, p], got_x.at[p], x_sem.at[0, p], x_sem.at[1, p], to_x)

    def along_y(p):
        return send(part.at[side_y, p], got_y.at[p], y_sem.at[0, p], y_sem.at[1, p], to_y)

    def far_x():
        return send(part.at[far, 0], got_far_x, far_x_sem.at[0], far_x_sem.at[1], to_x)

    def far_y():
        return send(part.at[far, 1], got_far_y, far_y_sem.at[0], far_y_sem.at[1], to_y)

    spreads = ((output_ref, outputs_ref), (grad_own, grads_ref))

    def spread(a, corner, p, way, source=None):
        target = spreads[a][1].at[corner, p]
        return send(
            target if source is None else source,
            target,
            spread_sem.at[a, corner, p, way],
            arrive_sem.at[a, corner, p],
            (to_x, to_y)[way],
        )

    def own_copy(a, p):
        return pltpu.make_async_copy(
            spreads[a][0].at[p], spreads[a][1].at[dp, p], own_sem.at[a, p]
        )

    def spread_own(a, p):
        own_copy(a, p).start()
        for way in (0, 1):
            spread(a, dp, p, way, spreads[a][0].at[p]).start()

    def spread_far(a):
        spread(a, side_x, 0, 0).wait_recv()
        spread(a, side_x, 0, 1).start()
        spread(a, side_y, 1, 0).wait_recv()
        spread(a, side_y, 1, 0).start()

    work, work_end, turns = down_grads(top_ref, scaled_ref, down_ref, *work_refs)
    pauses = 4

    def meanwhile(i):
        def turn(n, carry):
            work(n)
            return carry

        lax.fori_loop(turns * i // pauses, turns * (i + 1) // pauses, turn, 0)

    lax.fori_loop(0, 1, start, 0)
    for q in (far, side_x, side_y, dp):
        for p in (0, 1):
            first_load(q, p).start()
    lax.fori_loop(1, line, start, 0)
    for q in (far, side_x, side_y, dp):
        for p in (0, 1):
            first_load(q, p).wait()
    far_x().start()
    far_y().start()
    along_x(0).start()
    along_y(1).start()
    lax.fori_loop(0, 1, pair_sum, 0)
    far_x().wait_recv()
    part[side_y, 0] = part[side_y, 0] + got_far_x[...]
    along_y(0).start()
    far_y().wait_recv()
    part[side_x, 1] = part[side_x, 1] + got_far_y[...]
    along_x(1).start()
    for p in (0, 1):
        spread_own(0, p)
    lax.fori_loop(1, line, pair_sum, 0)
    meanwhile(0)
    lax.fori_loop(0, 1, pass_on, 0)
    for p in (0, 1):
        along_x(p).wait_recv()
        along_y(p).wait_recv()
        total = part[dp, p].astype(jnp.float32)
        total = total + got_x[p].astype(jnp.float32) + got_y[p].astype(jnp.float32)
        total = total * gain_ref[...]
        unit = unit_ref[p]
        mean = jnp.sum(total * unit, axis=1, keepdims=True) * (1.0 / unit.shape[1])
        rows = grad_ref[p] + inverse_ref[p] * (total - unit * mean)
        grad_own[p] = rows.astype(grad_own.dtype)
        spread_own(1, p)
    meanwhile(1)
    spread_far(0)
    lax.fori_loop(1, 2, pass_on, 0)
    spread_far(1)
    meanwhile(2)
    lax.fori_loop(2, line, pass_on, 0)
    meanwhile(3)
    for p in (0, 1):
        summed_ref[p] = acc[z, p].astype(jnp.float32)

        def from_below():
            climb(z, p).wait_recv()
            summed_ref[p] = summed_ref[p] + got_below[z, p].astype(jnp.float32)

        def from_above():
            descend(z, p).wait_recv()
            summed_ref[p] = summed_ref[p] + got_above[z, p].astype(jnp.float32)

        pl.when(z > 0)(from_below)
        pl.when(z < line - 1)(from_above)

    for side, device in enumerate((to_x, to_y)):
        value = summed_ref[:, large:, :] if side == 0 else shared_ref[...]
        small[side] = value.astype(small.dtype)
        spread(side, side_x, 1, 0).wait_recv()
        spread(side, side_y, 0, 0).wait_recv()
        for p in (0, 1):
            spread(side, far, p, 0).wait_recv()
            for way in (0, 1):
                spread(side, dp, p, way).wait_send()
            own_copy(side, p).wait()
        spread(side, side_x, 0, 1).wait_send()
        spread(side, side_y, 1, 0).wait_send()
        exchange = send(
            small.at[side], got_small.at[side], small_sem.at[0, side], small_sem.at[1, side], device
        )
        exchange.start()
        exchange.wait_recv()
        shared_ref[...] = small[side].astype(jnp.float32) + got_small[side].astype(jnp.float32)
        exchange.wait_send()

    far_x().wait_send()
    far_y().wait_send()
    for p in (0, 1):
        along_x(p).wait_send()
        along_y(p).wait_send()

    def finish(height, carry):
        for p in (0, 1):
            for copy in hands(height, p):
                copy.wait_send()
            pl.when(height > z)(lambda: climb(height, p).wait_send())
            pl.when(height < z)(lambda: descend(height, p).wait_send())
        return carry

    lax.fori_loop(0, line, finish, 0)
    work_end()


def closing(parts, small, first, grad, unit, inverse, gain, output, tops, scaled, shape, line):
    _, rows, wide = parts.shape
    shared_rows = small.shape[1]
    own, width = output.shape
    high, half = (rows + shared_rows) // 2, own // 2
    local, units, _ = shape
    sems = pltpu.SemaphoreType.DMA
    dtype = parts.dtype
    single = jnp.float32
    anywhere, inside = pl.BlockSpec(memory_space=pl.ANY), pl.BlockSpec(memory_space=pltpu.VMEM)
    everyone = jax.ShapeDtypeStruct((4, 2, half, width), dtype)
    summed, shared, outputs, grads, down = pl.pallas_call(
        functools.partial(closing_kernel, line, shared_rows),
        out_shape=[
            jax.ShapeDtypeStruct((2, high, wide), single),
            jax.ShapeDtypeStruct((2, shared_rows // 2, wide), single),
            everyone,
            everyone,
            jax.ShapeDtypeStruct(shape, dtype),
        ],
        in_specs=[anywhere] * 3 + [inside] * 5 + [anywhere] * 2,
        out_specs=[inside, inside, anywhere, anywhere, anywhere],
        scratch_shapes=[
            pltpu.VMEM((line, 2, high, wide), dtype),
            pltpu.VMEM((line, 2, high, wide), dtype),
            pltpu.VMEM((line, 2, high, wide), dtype),
            pltpu.VMEM((line, 2, high, wide), dtype),
            pltpu.VMEM((4, 2, half, width), dtype),
            pltpu.VMEM((2, half, width), dtype),
            pltpu.VMEM((2, half, width), dtype),
            pltpu.VMEM((half, width), dtype),
            pltpu.VMEM((half, width), dtype),
            pltpu.VMEM((2, half, width), dtype),
            pltpu.VMEM((2, 2, shared_rows // 2, wide), dtype),
            pltpu.VMEM((2, 2, shared_rows // 2, wide), dtype),
            sems((line, 2)),
            sems((2, line, 2)),
            sems((line, 2)),
            sems((2, line, 2)),
            sems((2, line, 2)),
            sems((2, line, 2)),
            sems((4, 2)),
            sems((2, 2)),
            sems((2, 2)),
            sems((2,)),
            sems((2,)),
            sems((2, 4, 2, 2)),
            sems((2, 4, 2)),
            sems((2, 2)),
            sems((2, 2)),
            pltpu.VMEM((2, tops.shape[0], SPAN), dtype),
            pltpu.VMEM(scaled.shape, dtype),
            pltpu.VMEM((SPAN, local * units), single),
            pltpu.VMEM((local, units, SPAN), dtype),
            sems((2,)),
            sems((1,)),
            sems((local,)),
        ],
        compiler_params=pltpu.CompilerParams(
            collective_id=5, has_side_effects=True, vmem_limit_bytes=60 << 20
        ),
        name="closing",
    )(
        parts.reshape(line, 2, 2, rows // 2, wide),
        small.reshape(line, 2, 2, shared_rows // 2, wide),
        first.reshape(4, 2, half, width),
        grad.reshape(2, half, width),
        unit.reshape(2, half, width),
        inverse.reshape(2, half, 1),
        gain.reshape(1, width),
        output.reshape(2, half, width),
        tops,
        scaled,
    )
    return (
        summed[:, : rows // 2].reshape(rows, wide),
        summed[:, rows // 2 :],
        shared,
        outputs.reshape(4 * own, width),
        grads.reshape(4 * own, width),
        down,
    )


def square_sum(values, got, sem, side, device):
    copy = send(values.at[side], got.at[side], sem.at[0, side], sem.at[1, side], device)
    copy.start()
    copy.wait()
    return values[side] + got[side]


def as_rows(column):
    return jnp.broadcast_to(column, (column.shape[0], 128)).T[:8]


def as_column(rows):
    return jnp.broadcast_to(rows[:1], (128, rows.shape[1])).T[:, :1]


def meet_square(dp, place):
    side_x, side_y = corners(dp)
    devices = ((side_x, place), (side_y, place))
    for device in devices:
        greet(device)
    pl.semaphore_wait(pltpu.get_barrier_semaphore(), 2)
    return devices


def normed_heads_kernel(
    model_width, q_ref, k_ref, q_gain, k_gain, cos_ref, sin_ref, queries, keys, inverse, sums, got, sem
):
    devices = meet_square(lax.axis_index("dp"), lax.axis_index("expert"))
    raws, gains, outs = (q_ref, k_ref), (q_gain, k_gain), (queries, keys)
    for i, raw in enumerate(raws):
        total = jnp.sum(raw[...] * raw[...], axis=1, keepdims=True)
        sums[0, 8 * i : 8 * i + 8] = as_rows(total)
    sums[1] = square_sum(sums, got, sem, 0, devices[0])
    total = square_sum(sums, got, sem, 1, devices[1])
    inverse[...] = lax.rsqrt(total * (1.0 / model_width) + epsilon)
    for i, raw in enumerate(raws):
        scale = as_column(inverse[8 * i : 8 * i + 8])
        for at in range(0, raw.shape[1], HD):
            head = raw[:, at : at + HD] * scale * gains[i][:, at : at + HD]
            turned = head * cos_ref[...] + pltpu.roll(head, HD // 2, 1) * sin_ref[...]
            outs[i][:, at : at + HD] = turned.astype(outs[i].dtype)


def normed_heads(q_raw, k_raw, q_gain, k_gain, cos, sin, model_width):
    rows, width = q_raw.shape
    head = jax.ShapeDtypeStruct((rows, width), jnp.bfloat16)
    return pl.pallas_call(
        functools.partial(normed_heads_kernel, model_width),
        out_shape=[head, head, jax.ShapeDtypeStruct((16, rows), jnp.float32)],
        in_specs=[pl.BlockSpec(memory_space=pltpu.VMEM)] * 6,
        out_specs=[pl.BlockSpec(memory_space=pltpu.VMEM)] * 3,
        scratch_shapes=[
            pltpu.VMEM((2, 16, rows), jnp.float32),
            pltpu.VMEM((2, 16, rows), jnp.float32),
            pltpu.SemaphoreType.DMA((2, 2)),
        ],
        compiler_params=pltpu.CompilerParams(
            collective_id=11, has_side_effects=True, vmem_limit_bytes=40 << 20
        ),
        name="normed_heads",
    )(q_raw, k_raw, q_gain.reshape(1, width), k_gain.reshape(1, width), cos, sin)


def normed_heads_back_kernel(
    model_width,
    dq_ref,
    dk_ref,
    dv_ref,
    q_ref,
    k_ref,
    q_gain,
    k_gain,
    cos_ref,
    sin_ref,
    inverse,
    grads,
    gain_grads,
    sums,
    got,
    sem,
):
    devices = meet_square(lax.axis_index("dp"), lax.axis_index("expert"))
    raws, gains, news = (q_ref, k_ref), (q_gain, k_gain), (dq_ref, dk_ref)
    rows, width = q_ref.shape

    def parts(i, at):
        cut = slice(at, at + HD)
        new = news[i][:, cut].astype(jnp.float32)
        back = new * cos_ref[...] - pltpu.roll(new, HD // 2, 1) * sin_ref[...]
        unit = raws[i][:, cut] * as_column(inverse[8 * i : 8 * i + 8])
        return back, unit, back * gains[i][:, cut]

    for i in (0, 1):
        total = jnp.zeros((rows, 1), jnp.float32)
        for at in range(0, width, HD):
            back, unit, scaled = parts(i, at)
            gain_grad = jnp.sum(back * unit, axis=0, keepdims=True)
            gain_grads[8 * i : 8 * i + 8, at : at + HD] = jnp.broadcast_to(gain_grad, (8, HD))
            total = total + jnp.sum(scaled * unit, axis=1, keepdims=True)
        sums[0, 8 * i : 8 * i + 8] = as_rows(total)
    sums[1] = square_sum(sums, got, sem, 0, devices[0])
    dots = square_sum(sums, got, sem, 1, devices[1]) * (1.0 / model_width)
    for i in (0, 1):
        dot = as_column(dots[8 * i : 8 * i + 8])
        scale = as_column(inverse[8 * i : 8 * i + 8])
        for at in range(0, width, HD):
            _, unit, scaled = parts(i, at)
            value = scale * (scaled - unit * dot)
            grads[:, i * width + at : i * width + at + HD] = value.astype(grads.dtype)
    grads[:, 2 * width :] = dv_ref[...]


def normed_heads_back(dq, dk, dv, q_raw, k_raw, q_gain, k_gain, cos, sin, inverse, model_width):
    rows, width = q_raw.shape
    return pl.pallas_call(
        functools.partial(normed_heads_back_kernel, model_width),
        out_shape=[
            jax.ShapeDtypeStruct((rows, 3 * width), jnp.bfloat16),
            jax.ShapeDtypeStruct((16, width), jnp.float32),
        ],
        in_specs=[pl.BlockSpec(memory_space=pltpu.VMEM)] * 10,
        out_specs=[pl.BlockSpec(memory_space=pltpu.VMEM)] * 2,
        scratch_shapes=[
            pltpu.VMEM((2, 16, rows), jnp.float32),
            pltpu.VMEM((2, 16, rows), jnp.float32),
            pltpu.SemaphoreType.DMA((2, 2)),
        ],
        compiler_params=pltpu.CompilerParams(
            collective_id=12, has_side_effects=True, vmem_limit_bytes=40 << 20
        ),
        name="normed_heads_back",
    )(
        dq,
        dk,
        dv,
        q_raw,
        k_raw,
        q_gain.reshape(1, width),
        k_gain.reshape(1, width),
        cos,
        sin,
        inverse,
    )


def per_device(
    inputs,
    attention_norm_gain,
    w_query,
    w_key,
    w_value,
    w_out,
    q_gain,
    k_gain,
    expert_norm_gain,
    w_router,
    w_gate,
    w_up,
    w_down,
    routes,
    lengths,
    d_output,
):
    pack_count, seg_rows, model_width = inputs.shape
    local_width = w_query.shape[1]
    local_heads = local_width // HD
    experts = w_router.shape[1]
    groups = lax.axis_size("expert")
    line = groups // 2
    pack_span = seg_rows * groups
    local_experts = w_gate.shape[0]
    offset_rows = lax.axis_index("expert") * seg_rows
    segment, positions = doc_layout(lengths, pack_span)
    pos_query = lax.dynamic_slice_in_dim(positions, offset_rows, seg_rows, 1)
    cos_table, sin_table = rope_tables(pos_query[0], HD)
    inputs_single_float = inputs.astype(jnp.float32)
    first_inverse_norm = lax.rsqrt(
        jnp.mean(inputs_single_float * inputs_single_float, axis=-1, keepdims=True) + epsilon
    )
    first_unit_input = inputs_single_float * first_inverse_norm
    first_normed_input = (first_unit_input * attention_norm_gain).astype(jnp.bfloat16)
    q_raw = jnp.dot(first_normed_input[0], w_query, preferred_element_type=jnp.float32)
    k_raw = jnp.dot(first_normed_input[0], w_key, preferred_element_type=jnp.float32)
    value_rows = jnp.dot(first_normed_input[0], w_value, preferred_element_type=jnp.float32).astype(
        jnp.bfloat16
    )
    queries, keys, head_inverse = normed_heads(
        q_raw, k_raw, q_gain, k_gain, cos_table, sin_table, model_width
    )
    layout = (segment, positions)
    if local_heads == line:
        attention = by_head(layout, line)
    else:
        attention = by_query(layout, offset_rows)
    attended, kept = attention[0](queries, keys, value_rows)
    attn_part = jnp.dot(
        attended, w_out, preferred_element_type=jnp.float32
    )
    own = lax.axis_index("dp")
    part_rows = seg_rows // lax.axis_size("dp")

    def own_rows(rows):
        return lax.dynamic_slice_in_dim(rows, own * part_rows, part_rows, 0)

    hidden_state = own_rows(inputs_single_float[0]) + scatter_dp(attn_part.astype(jnp.bfloat16))
    second_inverse_norm = lax.rsqrt(
        jnp.mean(hidden_state * hidden_state, axis=-1, keepdims=True) + epsilon
    )
    second_unit_input = hidden_state * second_inverse_norm
    second_normed_input = second_unit_input * expert_norm_gain
    router = jax.nn.softmax(
        jnp.dot(second_normed_input, w_router, precision=lax.Precision.HIGHEST), axis=-1
    )
    chosen = own_rows(routes[:, 0, :])
    expert_range = jnp.arange(experts, dtype=jnp.int32)
    named = jnp.any(chosen[:, :, None] == expert_range, axis=1)
    top_own = own_rows(d_output[0])
    top_all = lax.all_gather(top_own, ALL, axis=0, tiled=True)
    gate_table = jnp.where(named, router, 0.0)
    gate_high = gate_table.astype(jnp.bfloat16)
    gate_low = (gate_table - gate_high.astype(jnp.float32)).astype(jnp.bfloat16)
    widen = ((0, 0), (0, 64 - experts))
    own_tokens = jnp.concatenate(
        [
            second_normed_input.astype(jnp.bfloat16),
            jnp.pad(gate_high, widen),
            jnp.pad(gate_low, widen),
        ],
        axis=1,
    )
    xn_all, grad_units, scaled, gate_part = gate_act(
        own_tokens, top_all, w_gate, w_up, w_down, line
    )
    w_both = jnp.concatenate([*w_gate, *w_up], axis=1)
    (grad_tokens,) = product_sum(grad_units, w_both, True, gate_part, line, "grad_tokens", 4)
    moe_out, grad_gate, grad_up = product_sum(
        scaled,
        w_down.reshape(-1, model_width),
        False,
        None,
        line,
        "expert_sum",
        2,
        (xn_all, grad_units, w_gate.shape),
    )
    output = (hidden_state + moe_out).astype(jnp.bfloat16)
    grad_xn_exp = grad_tokens[:, :model_width]
    gate_sums = grad_tokens[:, model_width : model_width + experts]
    grad_router_probs = jnp.where(named, gate_sums, 0.0)
    grad_logits = router * (
        grad_router_probs - jnp.sum(router * grad_router_probs, axis=-1, keepdims=True)
    )
    grad_second_normed_input = grad_xn_exp + jnp.einsum(
        "se,de->sd", grad_logits, w_router, precision=lax.Precision.HIGHEST
    )
    grad_router = jnp.einsum(
        "sd,se->de", second_normed_input, grad_logits, precision=lax.Precision.HIGHEST
    )
    grad_expert_norm_gain = jnp.sum(grad_second_normed_input * second_unit_input, axis=0)
    grad_second_unit_input = grad_second_normed_input * expert_norm_gain
    grad_hidden = top_own.astype(jnp.float32) + second_inverse_norm * (
        grad_second_unit_input
        - second_unit_input
        * jnp.mean(grad_second_unit_input * second_unit_input, axis=-1, keepdims=True)
    )
    grad_attn = gather_dp(grad_hidden.astype(jnp.bfloat16))
    grad_out = jnp.einsum("sk,sd->kd", attended, grad_attn, preferred_element_type=jnp.float32)
    grad_heads = jnp.einsum(
        "sd,kd->sk", grad_attn, w_out, preferred_element_type=jnp.float32
    ).astype(jnp.bfloat16)
    grad_queries, grad_keys, grad_values = attention[1](kept, grad_heads)
    grad_heads_raw, gain_grads = normed_heads_back(
        grad_queries.astype(jnp.bfloat16),
        grad_keys,
        grad_values,
        q_raw,
        k_raw,
        q_gain,
        k_gain,
        cos_table,
        sin_table,
        head_inverse,
        model_width,
    )
    grad_q_gain, grad_k_gain = gain_grads[0], gain_grads[8]
    grad_projections = jnp.einsum(
        "sd,sk->dk", first_normed_input[0], grad_heads_raw, preferred_element_type=jnp.float32
    )
    grad_first_normed_input = sum(
        contract(grad_heads_raw[:, i * local_width : (i + 1) * local_width], weight, 1, 1)
        for i, weight in enumerate((w_query, w_key, w_value))
    )
    grad_attn_gain = jnp.sum(grad_first_normed_input * first_unit_input[0], axis=0)
    wide = grad_projections.shape[1]
    small = jnp.concatenate(
        [
            grad_q_gain.reshape(groups, -1),
            grad_k_gain.reshape(groups, -1),
            grad_attn_gain.reshape(groups, -1),
            grad_expert_norm_gain.reshape(groups, -1),
            grad_router.reshape(groups, -1),
        ],
        axis=1,
    )
    small_rows = 32
    filled = small.shape[1]
    small = jnp.pad(small, ((0, 0), (0, small_rows * wide - filled)))
    summed, own_small, shared, outputs, grad_input, grad_down = closing(
        grad_projections.astype(jnp.bfloat16).reshape(groups, -1, wide),
        small.astype(jnp.bfloat16).reshape(groups, small_rows, wide),
        grad_first_normed_input.astype(jnp.bfloat16),
        grad_hidden,
        own_rows(first_unit_input[0]),
        own_rows(first_inverse_norm[0]),
        attention_norm_gain,
        output,
        top_all,
        scaled,
        w_down.shape,
        line,
    )
    gain_size, norm_size = local_width // groups, model_width // groups
    own_gains = own_small.reshape(-1)[: 2 * gain_size]
    shared = shared.reshape(-1)[2 * gain_size : filled]
    grad_out = lax.psum_scatter(
        grad_out.astype(jnp.bfloat16), "expert", scatter_dimension=0, tiled=True
    ).astype(jnp.float32)
    return (
        outputs[None],
        grad_input.astype(jnp.float32)[None],
        shared[:norm_size],
        summed[:, :local_width],
        summed[:, local_width : 2 * local_width],
        summed[:, 2 * local_width :],
        grad_out,
        own_gains[:gain_size],
        own_gains[gain_size:],
        shared[norm_size : 2 * norm_size],
        shared[2 * norm_size :].reshape(norm_size, experts),
        grad_gate.astype(jnp.float32),
        grad_up.astype(jnp.float32),
        grad_down.astype(jnp.float32),
    )


def solution(mesh):
    placed = (
        P(None, "expert", None),
        P(),
        P(None, "dp"),
        P(None, "dp"),
        P(None, "dp"),
        P("dp", None),
        P("dp"),
        P("dp"),
        P(),
        P(),
        P("expert", None, "dp"),
        P("expert", None, "dp"),
        P("expert", "dp", None),
        P("expert", None, None),
        P(),
        P(None, "expert", None),
    )
    return jax.shard_map(
        per_device,
        mesh=mesh,
        in_specs=placed,
        out_specs=(
            P(None, "expert", None),
            P(None, "expert", None),
            P("expert"),
            P("expert", "dp"),
            P("expert", "dp"),
            P("expert", "dp"),
            P(("dp", "expert"), None),
            P(("dp", "expert")),
            P(("dp", "expert")),
            P("expert"),
            P("expert", None),
            P("expert", None, "dp"),
            P("expert", None, "dp"),
            P("expert", "dp", None),
        ),
        check_vma=False,
    )
```

```python
import functools

import jax
import jax.numpy as jnp
from jax import lax
from jax.experimental import pallas as pl
from jax.experimental.pallas import tpu as pltpu
from jax.sharding import PartitionSpec as P

HD = 128


epsilon = 1e-05
rope_base = 10000.0
masked_score = -1e30


def doc_layout(lengths, pack_span):
    doc_ends = jnp.cumsum(lengths, axis=1)
    starts = doc_ends - lengths
    places = jnp.arange(pack_span, dtype=jnp.int32)
    segment = jnp.sum((places[None, :, None] >= doc_ends[:, None, :]).astype(jnp.int32), axis=2)
    member = segment[:, :, None] == jnp.arange(lengths.shape[1], dtype=jnp.int32)[None, None, :]
    begins = jnp.sum(jnp.where(member, starts[:, None, :], 0), axis=2)
    return (segment, places[None, :] - begins)


def rope_tables(positions, head_size):
    half_size = head_size // 2
    frequency = rope_base ** (-2.0 * jnp.arange(half_size, dtype=jnp.float32) / head_size)
    angles = positions.astype(jnp.float32)[..., None] * frequency
    cos, sin = jnp.cos(angles), jnp.sin(angles)
    return jnp.concatenate([cos, cos], axis=-1), jnp.concatenate([-sin, sin], axis=-1)


ALL = ("dp", "expert")


DEVICES = pl.DeviceIdType.MESH


def greet(device):
    pl.semaphore_signal(
        pltpu.get_barrier_semaphore(), inc=1, device_id=device, device_id_type=DEVICES
    )


def send(source, target, send_sem, arrive_sem, device):
    return pltpu.make_async_remote_copy(
        src_ref=source,
        dst_ref=target,
        send_sem=send_sem,
        recv_sem=arrive_sem,
        device_id=device,
        device_id_type=DEVICES,
    )


def contract(a, b, a_dim, b_dim):
    return lax.dot_general(
        a, b, (((a_dim,), (b_dim,)), ((), ())), preferred_element_type=jnp.float32
    )


def corners(dp):
    return dp + 1 - 2 * (dp % 2), (dp + 2) % 4


def gather_square_kernel(x_ref, out_ref, sent, arrived, own_sem):
    dp, place = lax.axis_index("dp"), lax.axis_index("expert")
    side_x, side_y = corners(dp)
    devices = ((side_x, place), (side_y, place))
    for device in devices:
        greet(device)
    pl.semaphore_wait(pltpu.get_barrier_semaphore(), 2)

    def copy(corner, p, way, source=None):
        target = out_ref.at[corner, p]
        return send(
            target if source is None else source,
            target,
            sent.at[corner, p, way],
            arrived.at[corner, p],
            devices[way],
        )

    for p in (0, 1):
        pltpu.make_async_copy(x_ref.at[p], out_ref.at[dp, p], own_sem.at[p]).start()
        for way in (0, 1):
            copy(dp, p, way, x_ref.at[p]).start()
    copy(side_x, 0, 0).wait_recv()
    copy(side_x, 0, 1).start()
    copy(side_y, 0, 0).wait_recv()
    copy(side_x, 1, 0).wait_recv()
    copy(side_y, 1, 0).wait_recv()
    copy(side_y, 1, 0).start()
    for p in (0, 1):
        copy(3 - dp, p, 0).wait_recv()
        for way in (0, 1):
            copy(dp, p, way).wait_send()
        pltpu.make_async_copy(x_ref.at[p], out_ref.at[dp, p], own_sem.at[p]).wait()
    copy(side_x, 0, 1).wait_send()
    copy(side_y, 1, 0).wait_send()


def gather_dp(rows):
    count, width = rows.shape
    gathered = pl.pallas_call(
        gather_square_kernel,
        out_shape=jax.ShapeDtypeStruct((4, 2, count // 2, width), rows.dtype),
        in_specs=[pl.BlockSpec(memory_space=pltpu.VMEM)],
        out_specs=pl.BlockSpec(memory_space=pl.ANY),
        scratch_shapes=[
            pltpu.SemaphoreType.DMA((4, 2, 2)),
            pltpu.SemaphoreType.DMA((4, 2)),
            pltpu.SemaphoreType.DMA((2,)),
        ],
        compiler_params=pltpu.CompilerParams(collective_id=10, has_side_effects=True),
        name="gather_dp",
    )(rows.reshape(2, count // 2, width))
    return gathered.reshape(4 * count, width)


def farthest(line, z, k):
    return ranked(line, z, k, lambda place, at: (-abs(place - at), place))


def reduce_kernel(
    square,
    line,
    paired,
    x_ref,
    out_ref,
    acc,
    got_pair,
    got_x,
    got_y,
    got_far_x,
    got_far_y,
    got_below,
    got_above,
    load_sem,
    pair_sem,
    x_sem,
    y_sem,
    far_x_sem,
    far_y_sem,
    below_sem,
    above_sem,
):
    dp, place = lax.axis_index("dp"), lax.axis_index("expert")
    z, c = place // 2, place % 2
    side_x, side_y = corners(dp)
    core = c if paired else 0
    own = dp if square else 0
    quarters = (3 - dp, side_x, side_y, dp) if square else (0,)
    to_x, to_y = (side_x, place), (side_y, place)
    to_pair, to_up, to_down = (dp, 2 * z + 1 - c), (dp, place + 2), (dp, place - 2)
    greeted = 0
    if square:
        greet(to_x)
        greet(to_y)
        greeted += 2
    if paired:
        greet(to_pair)
        greeted += 1
    if line > 1:
        pl.when(z > 0)(lambda: greet(to_down))
        pl.when(z < line - 1)(lambda: greet(to_up))
        greeted = greeted + (z > 0).astype(jnp.int32) + (z < line - 1).astype(jnp.int32)
    pl.semaphore_wait(pltpu.get_barrier_semaphore(), greeted)

    def load(q, height, p):
        return pltpu.make_async_copy(
            x_ref.at[q, height, core, p], acc.at[q, height, p], load_sem.at[q, height, p]
        )

    def hand(q, height, p):
        at = (q, height, p)
        source = x_ref.at[q, height, 1 - core, p]
        return send(source, got_pair.at[at], pair_sem.at[0, *at], pair_sem.at[1, *at], to_pair)

    def along_x(height, p):
        at = (height, p)
        return send(
            acc.at[side_x, height, p], got_x.at[at], x_sem.at[0, *at], x_sem.at[1, *at], to_x
        )

    def along_y(height, p):
        at = (height, p)
        return send(
            acc.at[side_y, height, p], got_y.at[at], y_sem.at[0, *at], y_sem.at[1, *at], to_y
        )

    def far_x(height):
        return send(
            acc.at[3 - dp, height, 0],
            got_far_x.at[height],
            far_x_sem.at[0, height],
            far_x_sem.at[1, height],
            to_x,
        )

    def far_y(height):
        return send(
            acc.at[3 - dp, height, 1],
            got_far_y.at[height],
            far_y_sem.at[0, height],
            far_y_sem.at[1, height],
            to_y,
        )

    def climb(height, p):
        at = (height, p)
        return send(
            acc.at[own, height, p], got_below.at[at], below_sem.at[0, *at], below_sem.at[1, *at], to_up
        )

    def descend(height, p):
        at = (height, p)
        return send(
            acc.at[own, height, p],
            got_above.at[at],
            above_sem.at[0, *at],
            above_sem.at[1, *at],
            to_down,
        )

    def height_of(k):
        return farthest(line, z, k) if line > 1 else 0

    def start(k, carry):
        for q in quarters:
            for p in (0, 1):
                load(q, height_of(k), p).start()
                if paired:
                    hand(q, height_of(k), p).start()
        return carry

    lax.fori_loop(0, line, start, 0)

    def step(k, carry):
        def cores():
            height = height_of(k)
            for q in quarters:
                for p in (0, 1):
                    load(q, height, p).wait()
                    if paired:
                        hand(q, height, p).wait_recv()
                        acc[q, height, p] = acc[q, height, p] + got_pair[q, height, p]
                if square and q is quarters[0]:
                    far_x(height).start()
                    far_y(height).start()

        def sides():
            height = height_of(k - 1)
            along_x(height, 0).start()
            along_y(height, 1).start()
            far_x(height).wait_recv()
            acc[side_y, height, 0] = acc[side_y, height, 0] + got_far_x[height]
            along_y(height, 0).start()
            far_y(height).wait_recv()
            acc[side_x, height, 1] = acc[side_x, height, 1] + got_far_y[height]
            along_x(height, 1).start()

        def column():
            height = height_of(k - 2)
            for p in (0, 1):
                if square:
                    along_x(height, p).wait_recv()
                    along_y(height, p).wait_recv()
                    total = acc[own, height, p].astype(jnp.float32)
                    total = total + got_x[height, p].astype(jnp.float32)
                    total = total + got_y[height, p].astype(jnp.float32)
                    acc[own, height, p] = total.astype(acc.dtype)
                if line > 1:
                    pl.when((z == 0) & (height > z))(lambda: climb(height, p).start())
                    pl.when((z == line - 1) & (height < z))(lambda: descend(height, p).start())

        def pass_on():
            height = height_of(k - 3)
            for p in (0, 1):

                def upwards():
                    climb(height, p).wait_recv()
                    acc[own, height, p] = acc[own, height, p] + got_below[height, p]
                    climb(height, p).start()

                def downwards():
                    descend(height, p).wait_recv()
                    acc[own, height, p] = acc[own, height, p] + got_above[height, p]
                    descend(height, p).start()

                pl.when((height > z) & (z > 0))(upwards)
                pl.when((height < z) & (z < line - 1))(downwards)

        pl.when(k < line)(cores)
        if square:
            pl.when((k >= 1) & (k < line + 1))(sides)
        pl.when((k >= 2) & (k < line + 2))(column)
        if line > 1:
            pl.when(k >= 3)(pass_on)
        return carry

    lax.fori_loop(0, line + (3 if line > 1 else 2), step, 0)
    home = z if line > 1 else 0
    for p in (0, 1):
        out_ref[p] = acc[own, home, p].astype(jnp.float32)
        if line > 1:

            def from_below():
                climb(z, p).wait_recv()
                out_ref[p] = out_ref[p] + got_below[z, p].astype(jnp.float32)

            def from_above():
                descend(z, p).wait_recv()
                out_ref[p] = out_ref[p] + got_above[z, p].astype(jnp.float32)

            pl.when(z > 0)(from_below)
            pl.when(z < line - 1)(from_above)

    def finish(height, carry):
        if square:
            far_x(height).wait_send()
            far_y(height).wait_send()
        for p in (0, 1):
            if paired:
                for q in quarters:
                    hand(q, height, p).wait_send()
            if square:
                along_x(height, p).wait_send()
                along_y(height, p).wait_send()
            if line > 1:
                pl.when(height > z)(lambda: climb(height, p).wait_send())
                pl.when(height < z)(lambda: descend(height, p).wait_send())
        return carry

    lax.fori_loop(0, line, finish, 0)


def reduce_to(parts, square, line, paired, name, number):
    _, rows, width = parts.shape
    quarters, cores, half = (4 if square else 1), (2 if paired else 1), rows // 2

    def space(used, *shape):
        return pltpu.VMEM((*shape, half, width) if used else (*shape, 16, 128), parts.dtype)

    sems = pltpu.SemaphoreType.DMA
    total = pl.pallas_call(
        functools.partial(reduce_kernel, square, line, paired),
        out_shape=jax.ShapeDtypeStruct((2, half, width), jnp.float32),
        in_specs=[pl.BlockSpec(memory_space=pl.ANY)],
        out_specs=pl.BlockSpec(memory_space=pltpu.VMEM),
        scratch_shapes=[
            space(True, quarters, line, 2),
            space(paired, quarters, line, 2),
            space(square, line, 2),
            space(square, line, 2),
            space(square, line),
            space(square, line),
            space(line > 1, line, 2),
            space(line > 1, line, 2),
            sems((quarters, line, 2)),
            sems((2, quarters, line, 2)),
            sems((2, line, 2)),
            sems((2, line, 2)),
            sems((2, line)),
            sems((2, line)),
            sems((2, line, 2)),
            sems((2, line, 2)),
        ],
        compiler_params=pltpu.CompilerParams(
            collective_id=number, has_side_effects=True, vmem_limit_bytes=60 << 20
        ),
        name=name,
    )(parts.reshape(quarters, line, cores, 2, half, width))
    return total.reshape(rows, width)


def scatter_dp(rows):
    return reduce_to(rows.reshape(4, -1, rows.shape[1]), True, 1, False, "scatter_dp", 3)


def visit_others(line, z, visit):
    def turn(k, carry):
        visit((z + k) % line)
        return carry

    lax.fori_loop(1, line, turn, 0)


def greet_line(line, dp, z, c):
    visit_others(line, z, lambda other: greet((dp, 2 * other + c)))
    greet((dp, 2 * z + 1 - c))
    pl.semaphore_wait(pltpu.get_barrier_semaphore(), line)


def columns(z):
    return pl.ds(pl.multiple_of(z * HD, HD), HD)


def to_heads_kernel(line, shared, *refs):
    count = len(shared)
    ins, outs = refs[:count], refs[count : 2 * count]
    sent, arrived, pair_sent, pair_arrived, own_sem = refs[2 * count :]
    dp, place = lax.axis_index("dp"), lax.axis_index("expert")
    z, c = place // 2, place % 2
    pair = (dp, 2 * z + 1 - c)
    greet_line(line, dp, z, c)

    def block(i, origin):
        return outs[i].at[origin, c] if shared[i] else outs[i].at[origin]

    def out(i, other):
        source = ins[i].at[:, columns(other)]
        device = (dp, 2 * other + c)
        return send(source, block(i, z), sent.at[i, other], arrived.at[i, z], device)

    def into(i, origin):
        part = block(i, origin)
        return send(part, part, sent.at[i, origin], arrived.at[i, origin], pair)

    def share(i, origin, source=None):
        part = block(i, origin)
        return send(
            part if source is None else source,
            part,
            pair_sent.at[i, origin],
            pair_arrived.at[i, origin],
            pair,
        )

    def own(i):
        return pltpu.make_async_copy(ins[i].at[:, columns(z)], block(i, z), own_sem.at[i])

    def dispatch(other):
        for i in range(count):
            out(i, other).start()

    visit_others(line, z, dispatch)
    for i in range(count):
        own(i).start()
        if shared[i]:
            share(i, z, ins[i].at[:, columns(z)]).start()

    def receive(origin):
        for i in range(count):
            into(i, origin).wait_recv()
            if shared[i]:
                share(i, origin).start()

    visit_others(line, z, receive)

    def finish(other):
        for i in range(count):
            out(i, other).wait_send()

    visit_others(line, z, finish)
    for i in range(count):
        own(i).wait()
        if shared[i]:

            def settle(origin, carry):
                share(i, origin).wait()
                return carry

            lax.fori_loop(0, line, settle, 0)


def to_heads(arrays, shared, line, name, number):
    rows = arrays[0].shape[0]
    count = len(arrays)
    sems = pltpu.SemaphoreType.DMA
    return pl.pallas_call(
        functools.partial(to_heads_kernel, line, shared),
        out_shape=[
            jax.ShapeDtypeStruct((line, 2, rows, HD) if both else (line, rows, HD), array.dtype)
            for array, both in zip(arrays, shared)
        ],
        in_specs=[pl.BlockSpec(memory_space=pltpu.VMEM)] * count,
        out_specs=[pl.BlockSpec(memory_space=pl.ANY)] * count,
        scratch_shapes=[sems((count, line))] * 4 + [sems((count,))],
        compiler_params=pltpu.CompilerParams(collective_id=number, has_side_effects=True),
        name=name,
    )(*arrays)


def to_tokens_kernel(line, summed, *refs):
    count, sums = len(summed), sum(summed)
    ins, outs = refs[:count], refs[count : 2 * count]
    mine, theirs = refs[2 * count : 2 * count + 2]
    sent, arrived, pair_sem, load_sem, own_sem = refs[2 * count + 2 :]
    dp, place = lax.axis_index("dp"), lax.axis_index("expert")
    z, c = place // 2, place % 2
    pair = (dp, 2 * z + 1 - c)
    greet_line(line, dp, z, c)
    at_sum = [sum(summed[:i]) for i in range(count)]

    def load(i, other):
        return pltpu.make_async_copy(
            ins[i].at[other, c], mine.at[at_sum[i], other], load_sem.at[at_sum[i], other]
        )

    def hand(i, other):
        s = at_sum[i]
        return send(
            ins[i].at[other, 1 - c],
            theirs.at[s, other],
            pair_sem.at[0, s, other],
            pair_sem.at[1, s, other],
            pair,
        )

    def source(i, other):
        return mine.at[at_sum[i], other] if summed[i] else ins[i].at[other]

    def out(i, other):
        target = outs[i].at[:, columns(z)]
        device = (dp, 2 * other + c)
        return send(source(i, other), target, sent.at[i, other], arrived.at[i, z], device)

    def into(i, origin):
        part = outs[i].at[:, columns(origin)]
        return send(part, part, sent.at[i, origin], arrived.at[i, origin], pair)

    def own(i):
        return pltpu.make_async_copy(source(i, z), outs[i].at[:, columns(z)], own_sem.at[i])

    def prepare(other):
        for i in range(count):
            if summed[i]:
                load(i, other).start()
                hand(i, other).start()

    def add(i, other):
        if summed[i]:
            load(i, other).wait()
            hand(i, other).wait_recv()
            s = at_sum[i]
            mine[s, other] = mine[s, other] + theirs[s, other]

    def dispatch(other):
        for i in range(count):
            add(i, other)
            out(i, other).start()

    if sums:
        visit_others(line, z, prepare)
        prepare(z)
    visit_others(line, z, dispatch)
    for i in range(count):
        add(i, z)
        own(i).start()

    def finish(other):
        for i in range(count):
            into(i, other).wait_recv()
            out(i, other).wait_send()
            if summed[i]:
                hand(i, other).wait_send()

    visit_others(line, z, finish)
    for i in range(count):
        own(i).wait()
        if summed[i]:
            hand(i, z).wait_send()


def to_tokens(arrays, summed, line, name, number):
    rows = arrays[0].shape[-2]
    count, sums = len(arrays), max(sum(summed), 1)
    sems = pltpu.SemaphoreType.DMA
    dtype = arrays[0].dtype
    held = (sums, line, rows, HD) if sum(summed) else (1, 1, 16, HD)
    return pl.pallas_call(
        functools.partial(to_tokens_kernel, line, summed),
        out_shape=[jax.ShapeDtypeStruct((rows, line * HD), dtype)] * count,
        in_specs=[pl.BlockSpec(memory_space=pl.ANY)] * count,
        out_specs=[pl.BlockSpec(memory_space=pl.ANY)] * count,
        scratch_shapes=[pltpu.VMEM(held, dtype)] * 2
        + [
            sems((count, line)),
            sems((count, line)),
            sems((2, sums, line)),
            sems((sums, line)),
            sems((count,)),
        ],
        compiler_params=pltpu.CompilerParams(collective_id=number, has_side_effects=True),
        name=name,
    )(*arrays)


KEY_TILE = 512


def masked_scores(keys, queries, tile, first, starts):
    scores = contract(keys, queries, 1, 1) * HD ** (-0.5)
    key_at = tile * KEY_TILE + lax.broadcasted_iota(jnp.int32, scores.shape, 0)
    query_at = first + lax.broadcasted_iota(jnp.int32, (1, scores.shape[1]), 1)
    return jnp.where((key_at >= starts) & (key_at <= query_at), scores, masked_score)


def attend_kernel(bounds, q_ref, k_ref, v_ref, start_ref, o_ref, total_ref):
    i = pl.program_id(0)
    queries, starts = q_ref[0], start_ref[0]
    span = queries.shape[0]

    def tile_step(tile, carry):
        largest, total, acc = carry
        rows = pl.ds(pl.multiple_of(tile * KEY_TILE, KEY_TILE), KEY_TILE)
        scores = masked_scores(k_ref[rows, :], queries, tile, bounds[2, i], starts)
        new = jnp.maximum(largest, jnp.max(scores, axis=0, keepdims=True))
        weights = jnp.exp(scores - new)
        fade = jnp.exp(largest - new)
        total = fade * total + jnp.sum(weights, axis=0, keepdims=True)
        acc = fade * acc + contract(v_ref[rows, :], weights.astype(jnp.bfloat16), 0, 0)
        return new, total, acc

    largest, total, acc = lax.fori_loop(
        bounds[0, i],
        bounds[1, i],
        tile_step,
        (
            jnp.full((1, span), masked_score, jnp.float32),
            jnp.zeros((1, span), jnp.float32),
            jnp.zeros((HD, span), jnp.float32),
        ),
    )
    o_ref[0] = (acc / total).T.astype(o_ref.dtype)
    total_ref[0] = largest + jnp.log(total)


def attend_back_kernel(
    bounds, q_ref, k_ref, v_ref, start_ref, total_ref, delta_ref, d_ref, dq_ref, dk_ref, dv_ref, dk, dv
):
    i = pl.program_id(0)
    queries, starts, grad = q_ref[0], start_ref[0], d_ref[0]
    total, delta = total_ref[0], delta_ref[0]

    @pl.when(i == 0)
    def _():
        dk[...] = jnp.zeros_like(dk)
        dv[...] = jnp.zeros_like(dv)

    def tile_step(tile, acc):
        rows = pl.ds(pl.multiple_of(tile * KEY_TILE, KEY_TILE), KEY_TILE)
        keys = k_ref[rows, :]
        scores = masked_scores(keys, queries, tile, bounds[2, i], starts)
        weights = jnp.exp(scores - total)
        grad_weights = contract(v_ref[rows, :], grad, 1, 1)
        grad_scores = (weights * (grad_weights - delta)).astype(jnp.bfloat16)
        dv[rows, :] += contract(weights.astype(jnp.bfloat16), grad, 1, 0)
        dk[rows, :] += contract(grad_scores, queries, 1, 0)
        return acc + contract(keys, grad_scores, 0, 0)

    acc = jnp.zeros((HD, queries.shape[0]), jnp.float32)
    acc = lax.fori_loop(bounds[0, i], bounds[1, i], tile_step, acc)
    dq_ref[0] = (acc * HD ** (-0.5)).T.astype(dq_ref.dtype)

    @pl.when(i == pl.num_programs(0) - 1)
    def _():
        dk_ref[...] = (dk[...] * HD ** (-0.5)).astype(dk_ref.dtype)
        dv_ref[...] = dv[...].astype(dv_ref.dtype)


def attend(bounds, queries, keys, values, starts):
    line, span, _ = queries.shape
    pack = keys.shape[0]
    block = pl.BlockSpec((1, span, HD), lambda i, _: (i, 0, 0))
    row = pl.BlockSpec((1, 1, span), lambda i, _: (i, 0, 0))
    whole = pl.BlockSpec((pack, HD), lambda i, _: (0, 0))
    return pl.pallas_call(
        attend_kernel,
        grid_spec=pltpu.PrefetchScalarGridSpec(
            num_scalar_prefetch=1,
            grid=(line,),
            in_specs=[block, whole, whole, row],
            out_specs=[block, row],
        ),
        out_shape=[
            jax.ShapeDtypeStruct(queries.shape, jnp.bfloat16),
            jax.ShapeDtypeStruct(starts.shape, jnp.float32),
        ],
        name="attend",
    )(bounds, queries, keys, values, starts)


def attend_back(bounds, queries, keys, values, starts, total, delta, grad):
    line, span, _ = queries.shape
    pack = keys.shape[0]
    block = pl.BlockSpec((1, span, HD), lambda i, _: (i, 0, 0))
    row = pl.BlockSpec((1, 1, span), lambda i, _: (i, 0, 0))
    whole = pl.BlockSpec((pack, HD), lambda i, _: (0, 0))
    return pl.pallas_call(
        attend_back_kernel,
        grid_spec=pltpu.PrefetchScalarGridSpec(
            num_scalar_prefetch=1,
            grid=(line,),
            in_specs=[block, whole, whole, row, row, row, block],
            out_specs=[block, whole, whole],
            scratch_shapes=[pltpu.VMEM((pack, HD), jnp.float32)] * 2,
        ),
        out_shape=[jax.ShapeDtypeStruct(queries.shape, jnp.bfloat16)]
        + [jax.ShapeDtypeStruct((pack, HD), jnp.bfloat16)] * 2,
        name="attend_back",
    )(bounds, queries, keys, values, starts, total, delta, grad)


def out_sum_kernel(
    line,
    o_ref,
    w_ref,
    attended_ref,
    out_ref,
    att,
    made,
    got_x,
    got_y,
    got_far_x,
    got_far_y,
    sent,
    arrived,
    own_sem,
    att_sem,
    x_sem,
    y_sem,
    far_x_sem,
    far_y_sem,
):
    dp, place = lax.axis_index("dp"), lax.axis_index("expert")
    z, c = place // 2, place % 2
    side_x, side_y = corners(dp)
    far = 3 - dp
    to_x, to_y = (side_x, place), (side_y, place)
    visit_others(line, z, lambda other: greet((dp, 2 * other + c)))
    greet(to_x)
    greet(to_y)
    pl.semaphore_wait(pltpu.get_barrier_semaphore(), line + 1)
    rows, half, width = att.shape[1], made.shape[2], made.shape[3]
    chunk = 512
    order = (far, side_x, side_y, dp)

    def block(q):
        return pl.ds(pl.multiple_of(q * rows, rows), rows)

    def out(q, other):
        device = (dp, 2 * other + c)
        source, target = o_ref.at[other, block(q)], att.at[q, :, columns(z)]
        return send(source, target, sent.at[q, other], arrived.at[q, z], device)

    def into(q, origin):
        part = att.at[q, :, columns(origin)]
        return send(part, part, sent.at[q, origin], arrived.at[q, origin], to_x)

    def own(q):
        return pltpu.make_async_copy(
            o_ref.at[z, block(q)], att.at[q, :, columns(z)], own_sem.at[q]
        )

    def att_out(q):
        return pltpu.make_async_copy(att.at[q], attended_ref.at[block(q)], att_sem.at[q])

    def along_x(p):
        return send(made.at[side_x, p], got_x.at[p], x_sem.at[0, p], x_sem.at[1, p], to_x)

    def along_y(p):
        return send(made.at[side_y, p], got_y.at[p], y_sem.at[0, p], y_sem.at[1, p], to_y)

    def far_x():
        return send(made.at[far, 0], got_far_x, far_x_sem.at[0], far_x_sem.at[1], to_x)

    def far_y():
        return send(made.at[far, 1], got_far_y, far_y_sem.at[0], far_y_sem.at[1], to_y)

    for q in order:
        visit_others(line, z, lambda other: out(q, other).start())
        own(q).start()
    for i, q in enumerate(order):
        visit_others(line, z, lambda origin: into(q, origin).wait_recv())
        own(q).wait()
        att_out(q).start()
        for at in range(0, width, chunk):
            part = contract(att[q], w_ref[:, at : at + chunk], 1, 0).astype(made.dtype)
            made[q, :, :, at : at + chunk] = part.reshape(2, half, chunk)
        if i == 0:
            far_x().start()
            far_y().start()
        if i == 1:
            along_x(0).start()
        if i == 2:
            along_y(1).start()
    far_y().wait_recv()
    made[side_x, 1] = made[side_x, 1] + got_far_y[...]
    along_x(1).start()
    far_x().wait_recv()
    made[side_y, 0] = made[side_y, 0] + got_far_x[...]
    along_y(0).start()
    for p in (0, 1):
        along_x(p).wait_recv()
        along_y(p).wait_recv()
        total = made[dp, p].astype(jnp.float32)
        out_ref[p] = total + got_x[p].astype(jnp.float32) + got_y[p].astype(jnp.float32)
    far_x().wait_send()
    far_y().wait_send()
    for p in (0, 1):
        along_x(p).wait_send()
        along_y(p).wait_send()
    for q in order:
        visit_others(line, z, lambda other: out(q, other).wait_send())
        att_out(q).wait()


def out_sum(heads, w_out, line):
    rows = heads.shape[1]
    depth, width = w_out.shape
    quarter, half = rows // 4, rows // 8
    sems = pltpu.SemaphoreType.DMA
    dtype = heads.dtype
    anywhere, inside = pl.BlockSpec(memory_space=pl.ANY), pl.BlockSpec(memory_space=pltpu.VMEM)
    attended, total = pl.pallas_call(
        functools.partial(out_sum_kernel, line),
        out_shape=[
            jax.ShapeDtypeStruct((rows, depth), dtype),
            jax.ShapeDtypeStruct((2, half, width), jnp.float32),
        ],
        in_specs=[anywhere, inside],
        out_specs=[anywhere, inside],
        scratch_shapes=[
            pltpu.VMEM((4, quarter, depth), dtype),
            pltpu.VMEM((4, 2, half, width), dtype),
            pltpu.VMEM((2, half, width), dtype),
            pltpu.VMEM((2, half, width), dtype),
            pltpu.VMEM((half, width), dtype),
            pltpu.VMEM((half, width), dtype),
            sems((4, line)),
            sems((4, line)),
            sems((4,)),
            sems((4,)),
            sems((2, 2)),
            sems((2, 2)),
            sems((2,)),
            sems((2,)),
        ],
        compiler_params=pltpu.CompilerParams(
            collective_id=7, has_side_effects=True, vmem_limit_bytes=40 << 20
        ),
        name="out_sum",
    )(heads, w_out)
    return attended, total.reshape(quarter, width)


def out_back_kernel(
    line, x_ref, w_ref, all_ref, grad_ref, buf, grads, spread_sem, arrive_sem, own_sem, all_sem, sent, arrived, mine_sem
):
    dp, place = lax.axis_index("dp"), lax.axis_index("expert")
    z, c = place // 2, place % 2
    side_x, side_y = corners(dp)
    far = 3 - dp
    devices = ((side_x, place), (side_y, place))
    visit_others(line, z, lambda other: greet((dp, 2 * other + c)))
    for device in devices:
        greet(device)
    pl.semaphore_wait(pltpu.get_barrier_semaphore(), line + 1)
    rows = grads.shape[1]

    def spread(corner, p, way, source=None):
        target = buf.at[corner, p]
        return send(
            target if source is None else source,
            target,
            spread_sem.at[corner, p, way],
            arrive_sem.at[corner, p],
            devices[way],
        )

    def own(p):
        return pltpu.make_async_copy(x_ref.at[p], buf.at[dp, p], own_sem.at[p])

    def all_out(q):
        return pltpu.make_async_copy(buf.at[q], all_ref.at[q], all_sem.at[q])

    def block(q):
        return pl.ds(pl.multiple_of(q * rows, rows), rows)

    def out(q, other):
        device = (dp, 2 * other + c)
        source, target = grads.at[q, :, columns(other)], grad_ref.at[z, block(q)]
        return send(source, target, sent.at[q, other], arrived.at[q, z], device)

    def into(q, origin):
        part = grad_ref.at[origin, block(q)]
        return send(part, part, sent.at[q, origin], arrived.at[q, origin], devices[0])

    def mine(q):
        return pltpu.make_async_copy(
            grads.at[q, :, columns(z)], grad_ref.at[z, block(q)], mine_sem.at[q]
        )

    def product(q):
        all_out(q).start()
        value = contract(buf[q].reshape(rows, buf.shape[3]), w_ref[...], 1, 1)
        grads[q] = value.astype(grads.dtype)
        visit_others(line, z, lambda other: out(q, other).start())
        mine(q).start()

    for p in (0, 1):
        spread(dp, p, 0, x_ref.at[p]).start()
        spread(dp, 1 - p, 1, x_ref.at[1 - p]).start()
        own(p).start()
    for p in (0, 1):
        own(p).wait()
    product(dp)
    spread(side_x, 0, 0).wait_recv()
    spread(side_x, 0, 1).start()
    spread(side_y, 1, 0).wait_recv()
    spread(side_y, 1, 0).start()
    spread(side_x, 1, 0).wait_recv()
    product(side_x)
    spread(side_y, 0, 0).wait_recv()
    product(side_y)
    for p in (0, 1):
        spread(far, p, 0).wait_recv()
    product(far)
    for q in (dp, side_x, side_y, far):
        visit_others(line, z, lambda origin: into(q, origin).wait_recv())
        visit_others(line, z, lambda other: out(q, other).wait_send())
        mine(q).wait()
        all_out(q).wait()
    for p in (0, 1):
        for way in (0, 1):
            spread(dp, p, way).wait_send()
    spread(side_x, 0, 1).wait_send()
    spread(side_y, 1, 0).wait_send()


def out_back(own, w_out, line):
    quarter, width = own.shape
    depth = w_out.shape[0]
    half = quarter // 2
    sems = pltpu.SemaphoreType.DMA
    dtype = own.dtype
    anywhere, inside = pl.BlockSpec(memory_space=pl.ANY), pl.BlockSpec(memory_space=pltpu.VMEM)
    everyone, grad = pl.pallas_call(
        functools.partial(out_back_kernel, line),
        out_shape=[
            jax.ShapeDtypeStruct((4, 2, half, width), dtype),
            jax.ShapeDtypeStruct((line, 4 * quarter, HD), dtype),
        ],
        in_specs=[inside, inside],
        out_specs=[anywhere, anywhere],
        scratch_shapes=[
            pltpu.VMEM((4, 2, half, width), dtype),
            pltpu.VMEM((4, quarter, depth), dtype),
            sems((4, 2, 2)),
            sems((4, 2)),
            sems((2,)),
            sems((4,)),
            sems((4, line)),
            sems((4, line)),
            sems((4,)),
        ],
        compiler_params=pltpu.CompilerParams(
            collective_id=8, has_side_effects=True, vmem_limit_bytes=40 << 20
        ),
        name="out_back",
    )(own.reshape(2, half, width), w_out)
    return everyone.reshape(4 * quarter, width), grad


def by_head(layout, w_out, line):
    positions = layout[1][0]
    pack = positions.shape[0]
    span = pack // (2 * line)
    core = lax.axis_index("expert") % 2
    starts = (jnp.arange(pack, dtype=jnp.int32) - positions).reshape(line, 2, 1, span)
    starts = lax.dynamic_index_in_dim(starts, core, 1, keepdims=False)
    first = (2 * jnp.arange(line, dtype=jnp.int32) + core) * span
    bounds = jnp.stack(
        [starts[:, 0, 0] // KEY_TILE, (first + span - 1) // KEY_TILE + 1, first]
    ).astype(jnp.int32)

    def forward(queries, keys, values):
        q, k, v = to_heads(
            [queries, keys, values], (False, True, True), line, "scatter_heads", 6
        )
        k, v = k.reshape(pack, HD), v.reshape(pack, HD)
        out, total = attend(bounds, q, k, v, starts)
        return *out_sum(out, w_out, line), (q, k, v, out, total)

    def backward(kept, grad_own):
        q, k, v, out, total = kept
        grad_all, grad = out_back(grad_own, w_out, line)
        delta = jnp.sum(grad.astype(jnp.float32) * out.astype(jnp.float32), axis=-1)
        dq, dk, dv = attend_back(bounds, q, k, v, starts, total, delta[:, None, :], grad)
        shape = (line, 2, span, HD)
        grads = to_tokens(
            [dq, dk.reshape(shape), dv.reshape(shape)],
            (False, True, True),
            line,
            "gather_grads",
            9,
        )
        return grad_all, *grads

    return forward, backward


def by_query(layout, w_out, offset_rows):
    segment = layout[0][0]
    pack = segment.shape[0]

    def heads(rows):
        return rows.reshape(rows.shape[0], -1, HD)

    def score_block(queries, keys):
        rows = queries.shape[0]
        scores = jnp.einsum("shd,lhd->hsl", queries, keys, preferred_element_type=jnp.float32)
        own = lax.dynamic_slice_in_dim(segment, offset_rows, rows, 0)
        query_places = offset_rows + jnp.arange(rows, dtype=jnp.int32)
        key_places = jnp.arange(pack, dtype=jnp.int32)
        allowed = (own[:, None] == segment[None, :]) & (
            key_places[None, :] <= query_places[:, None]
        )
        return jnp.where(allowed[None], scores * HD ** (-0.5), masked_score)

    def forward(queries, keys, values):
        q = heads(queries)
        k = heads(lax.all_gather(keys, "expert", axis=0, tiled=True))
        v = heads(lax.all_gather(values, "expert", axis=0, tiled=True))
        scores = score_block(q, k)
        largest = jnp.max(scores, axis=-1, keepdims=True)
        total = largest + jnp.log(jnp.sum(jnp.exp(scores - largest), axis=-1, keepdims=True))
        weights = jnp.exp(scores - total).astype(jnp.bfloat16)
        attended = jnp.einsum("hsl,lhd->shd", weights, v, preferred_element_type=jnp.float32)
        attended = attended.astype(jnp.bfloat16).reshape(queries.shape)
        projected = scatter_dp(contract(attended, w_out, 1, 0).astype(jnp.bfloat16))
        return attended, projected, (q, k, v, total)

    def backward(kept, grad_own):
        q, k, v, total = kept
        grad_all = gather_dp(grad_own)
        grad = contract(grad_all, w_out, 1, 1).astype(jnp.bfloat16)
        shape = grad.shape
        grad = heads(grad)
        weights = jnp.exp(score_block(q, k) - total)
        grad_weights = jnp.einsum("shd,lhd->hsl", grad, v, preferred_element_type=jnp.float32)
        delta = jnp.sum(weights * grad_weights, axis=-1, keepdims=True)
        grad_scores = (weights * (grad_weights - delta)).astype(jnp.bfloat16)
        dq = jnp.einsum("hsl,lhd->shd", grad_scores, k, preferred_element_type=jnp.float32)
        dk = jnp.einsum("hsl,shd->lhd", grad_scores, q, preferred_element_type=jnp.float32)
        weights = weights.astype(jnp.bfloat16)
        dv = jnp.einsum("hsl,shd->lhd", weights, grad, preferred_element_type=jnp.float32)

        def to_owner(part):
            part = part.astype(jnp.bfloat16).reshape(pack, shape[1])
            return lax.psum_scatter(part, "expert", scatter_dimension=0, tiled=True)

        scale = HD ** (-0.5)
        dq = (dq * scale).reshape(shape)
        return grad_all, dq, to_owner(dk * scale), to_owner(dv)

    return forward, backward


def nearest(line, z, k):
    return ranked(line, z, k, lambda place, at: (abs(place - at), place))


def ranked(line, z, k, rank):
    total = jnp.int32(0)
    for at in range(line):
        order = sorted(range(line), key=lambda place: rank(place, at))
        place = sum([jnp.where(k == i, order[i], 0) for i in range(line)])
        total = total + jnp.where(z == at, place, 0)
    return total


def gate_act_kernel(
    line,
    x_ref,
    top_ref,
    wg_ref,
    wu_ref,
    wd_ref,
    xn_ref,
    grads_ref,
    scaled_ref,
    gates_ref,
    xbuf,
    top_buf,
    grads_buf,
    scaled_buf,
    gates_buf,
    sent,
    arrived,
    own_sem,
    top_sem,
    xn_sem,
    grads_sem,
    scaled_sem,
    gates_sem,
):
    dp, place = lax.axis_index("dp"), lax.axis_index("expert")
    z, c = place // 2, place % 2
    side_x, side_y = corners(dp)
    far = 3 - dp
    devices = (
        (dp, place + 2),
        (dp, place - 2),
        (side_x, place),
        (side_y, place),
        (dp, 2 * z + 1 - c),
    )
    up, down, along_x, along_y, pair = range(5)
    has_up, has_down = z < line - 1, z > 0
    for way in (along_x, along_y, pair):
        greet(devices[way])
    pl.when(has_up)(lambda: greet(devices[up]))
    pl.when(has_down)(lambda: greet(devices[down]))
    greeted = 3 + has_up.astype(jnp.int32) + has_down.astype(jnp.int32)
    pl.semaphore_wait(pltpu.get_barrier_semaphore(), greeted)
    local, width, units = wg_ref.shape
    rows = top_buf.shape[1]
    first = place * local

    def slot(corner, height, core):
        return corner * (2 * line) + 2 * height + core

    def copy(s, p, way, source=None):
        target = xbuf.at[s, p]
        return send(
            target if source is None else source,
            target,
            sent.at[s, p, way],
            arrived.at[s, p],
            devices[way],
        )

    def arrive(s, p):
        copy(s, p, pair).wait_recv()

    mine = slot(dp, z, c)
    for p in (0, 1):
        pltpu.make_async_copy(x_ref.at[p], xbuf.at[mine, p], own_sem.at[p]).start()
        pl.when(has_up)(lambda: copy(mine, p, up, x_ref.at[p]).start())
        pl.when(has_down)(lambda: copy(mine, p, down, x_ref.at[p]).start())
        for way in (along_x, along_y, pair):
            copy(mine, p, way, x_ref.at[p]).start()

    def decode(i):
        turn, j = i // 4, i % 4
        k = turn - (j > 0).astype(jnp.int32) - (j == 3).astype(jnp.int32)
        valid = (i >= 0) & (k >= 0) & (k < line)
        corner = jnp.where(j == 0, dp, jnp.where(j == 1, side_x, jnp.where(j == 2, side_y, far)))
        return j, k, valid, corner, nearest(line, z, k)

    def top_load(i, corner, height):
        block = corner * line + height
        return pltpu.make_async_copy(top_ref.at[block], top_buf.at[i % 2], top_sem.at[i % 2])

    def xn_out(block):
        return pltpu.make_async_copy(
            xbuf.at[pl.ds(2 * block, 2), :, :, pl.ds(0, width)],
            xn_ref.at[pl.ds(2 * block, 2)],
            xn_sem.at[block],
        )

    def grads_out(block):
        return pltpu.make_async_copy(grads_buf.at[block], grads_ref.at[block], grads_sem.at[block])

    def scaled_out(block):
        return pltpu.make_async_copy(
            scaled_buf.at[block], scaled_ref.at[block], scaled_sem.at[block]
        )

    def gates_out(block):
        return pltpu.make_async_copy(gates_buf.at[block], gates_ref.at[block], gates_sem.at[block])

    def compute(i):
        j, k, _, corner, height = decode(i)
        block = corner * line + height
        for p in (0, 1):
            arrive(slot(corner, height, 1 - c), p)
        xn_out(block).start()
        top_load(i, corner, height).wait()
        lanes = lax.broadcasted_iota(jnp.int32, (rows, 128), 1)

        def tokens():
            return xbuf[pl.ds(2 * block, 2), :, :, pl.ds(0, width)].reshape(rows, width)

        table = xbuf[pl.ds(2 * block, 2), :, :, pl.ds(width, 128)].reshape(rows, 128)
        table = table.astype(jnp.float32)
        gate_grads = jnp.zeros((rows, 128), jnp.float32)
        for e in range(local):
            at = (lanes == first + e) | (lanes == first + e + 64)
            gate = jnp.sum(jnp.where(at, table, 0.0), axis=1, keepdims=True)
            g = contract(tokens(), wg_ref[e], 1, 0)
            u = contract(tokens(), wu_ref[e], 1, 0)
            h = contract(top_buf[i % 2], wd_ref[e], 1, 1)
            sigmoid = 1.0 / (1.0 + jnp.exp(-g))
            silu = g * sigmoid
            act = silu * u
            gate_grad = jnp.sum(act * h, axis=1, keepdims=True)
            gate_grads = gate_grads + jnp.where(lanes == first + e, gate_grad, 0.0)
            grad_act = h * gate
            dg = grad_act * u * sigmoid * (1.0 + g * (1.0 - sigmoid))
            du = grad_act * silu
            scaled_buf[block, :, e * units : (e + 1) * units] = (act * gate).astype(jnp.bfloat16)
            grads_buf[block, :, e * units : (e + 1) * units] = dg.astype(jnp.bfloat16)
            at = (local + e) * units
            grads_buf[block, :, at : at + units] = du.astype(jnp.bfloat16)
        gates_buf[block] = gate_grads.astype(jnp.bfloat16)
        grads_out(block).start()
        scaled_out(block).start()
        gates_out(block).start()

    def step(i, carry):
        j, k, valid, corner, height = decode(i)
        s = slot(corner, height, c)

        def own():
            for p in (0, 1):
                pltpu.make_async_copy(x_ref.at[p], xbuf.at[mine, p], own_sem.at[p]).wait()

        def column():
            for p in (0, 1):
                arrive(s, p)
                pl.when(has_up & (height < z))(lambda: copy(s, p, up).start())
                pl.when(has_down & (height > z))(lambda: copy(s, p, down).start())
                for way in (along_x, along_y, pair):
                    copy(s, p, way).start()

        def sides():
            for p in (0, 1):
                arrive(s, p)
                copy(s, p, pair).start()
            pl.when(j == 1)(lambda: copy(s, 0, along_y).start())
            pl.when(j == 2)(lambda: copy(s, 1, along_x).start())

        def opposite():
            for p in (0, 1):
                arrive(s, p)
                copy(s, p, pair).start()

        pl.when(valid & (j == 0) & (k == 0))(own)
        pl.when(valid & (j == 0) & (k > 0))(column)
        pl.when(valid & ((j == 1) | (j == 2)))(sides)
        pl.when(valid & (j == 3))(opposite)
        pl.when(valid)(lambda: top_load(i, corner, height).start())
        pl.when(decode(i - 1)[2])(lambda: compute(i - 1))
        return carry

    lax.fori_loop(0, 4 * (line + 2) + 1, step, 0)

    def finish(height, carry):
        for p in (0, 1):
            for corner in range(4):
                copy(slot(corner, height, c), p, pair).wait_send()
            s = slot(dp, height, c)
            copy(s, p, along_x).wait_send()
            copy(s, p, along_y).wait_send()
            pl.when(has_up & (height <= z))(lambda: copy(s, p, up).wait_send())
            pl.when(has_down & (height >= z))(lambda: copy(s, p, down).wait_send())
        copy(slot(side_x, height, c), 0, along_y).wait_send()
        copy(slot(side_y, height, c), 1, along_x).wait_send()
        for corner in range(4):
            block = corner * line + height
            xn_out(block).wait()
            grads_out(block).wait()
            scaled_out(block).wait()
            gates_out(block).wait()
        return carry

    lax.fori_loop(0, line, finish, 0)


def gate_act(own, tops, w_gate, w_up, w_down, line):
    count, wide = own.shape
    local, width, units = w_gate.shape
    slots, blocks, rows, half = 8 * line, 4 * line, 2 * count, count // 2
    sems = pltpu.SemaphoreType.DMA
    dtype = own.dtype
    xn, grads, scaled, gates = pl.pallas_call(
        functools.partial(gate_act_kernel, line),
        out_shape=[
            jax.ShapeDtypeStruct((slots, 2, half, width), dtype),
            jax.ShapeDtypeStruct((blocks, rows, 2 * local * units), dtype),
            jax.ShapeDtypeStruct((blocks, rows, local * units), dtype),
            jax.ShapeDtypeStruct((blocks, rows, 128), dtype),
        ],
        in_specs=[
            pl.BlockSpec(memory_space=pltpu.VMEM),
            pl.BlockSpec(memory_space=pl.ANY),
            pl.BlockSpec(memory_space=pltpu.VMEM),
            pl.BlockSpec(memory_space=pltpu.VMEM),
            pl.BlockSpec(memory_space=pltpu.VMEM),
        ],
        out_specs=[pl.BlockSpec(memory_space=pl.ANY)] * 4,
        scratch_shapes=[
            pltpu.VMEM((slots, 2, half, wide), dtype),
            pltpu.VMEM((2, rows, width), dtype),
            pltpu.VMEM((blocks, rows, 2 * local * units), dtype),
            pltpu.VMEM((blocks, rows, local * units), dtype),
            pltpu.VMEM((blocks, rows, 128), dtype),
            sems((slots, 2, 5)),
            sems((slots, 2)),
            sems((2,)),
            sems((2,)),
            sems((blocks,)),
            sems((blocks,)),
            sems((blocks,)),
            sems((blocks,)),
        ],
        compiler_params=pltpu.CompilerParams(
            collective_id=1, has_side_effects=True, vmem_limit_bytes=60 << 20
        ),
        name="gate_act",
    )(own.reshape(2, half, wide), tops.reshape(blocks, rows, width), w_gate, w_up, w_down)
    return xn.reshape(slots * count, width), grads, scaled, gates


def column_products(left_ref, right_ref, chunk_buf, right_buf, total, chunk_sem, right_sem, store):
    span = chunk_buf.shape[2]
    blocks, rows, _ = right_buf.shape
    joined = max(1, min(blocks, 1024 // rows))
    depth = joined * rows
    turns = left_ref.shape[1] // span

    def at(n):
        return pl.ds(pl.multiple_of(n * span, span), span)

    def chunk(n):
        return pltpu.make_async_copy(
            left_ref.at[:, at(n)], chunk_buf.at[n % 2], chunk_sem.at[n % 2]
        )

    right_load = pltpu.make_async_copy(right_ref, right_buf, right_sem.at[0])
    chunk(0).start()
    right_load.start()

    def turn(n):
        pl.when(n + 1 < turns)(lambda: chunk(n + 1).start())
        chunk(n).wait()
        pl.when(n == 0)(right_load.wait)
        total[...] = jnp.zeros_like(total)

        def part(k, carry):
            left = chunk_buf[n % 2, pl.ds(pl.multiple_of(k * depth, depth), depth), :]
            right = right_buf[pl.ds(k * joined, joined)].reshape(depth, right_buf.shape[2])
            total[...] += contract(left, right, 0, 0)
            return carry

        lax.fori_loop(0, blocks // joined, part, 0)
        store(n, at(n))

    return turn, turns


def gate_up_grads(
    xn_ref, units_ref, gate_ref, up_ref, chunk_buf, units_buf, total, both, chunk_sem, units_sem, out_sem
):
    local, _, units = gate_ref.shape
    outs = (gate_ref, up_ref)

    def copies(at):
        return [
            pltpu.make_async_copy(
                both.at[:, pl.ds((kind * local + e) * units, units)],
                outs[kind].at[e, at, :],
                out_sem.at[kind, e],
            )
            for kind in (0, 1)
            for e in range(local)
        ]

    start = pl.ds(0, chunk_buf.shape[2])

    def store(n, at):
        @pl.when(n > 0)
        def _():
            for copy in copies(start):
                copy.wait()

        both[...] = total[...].astype(both.dtype)
        for copy in copies(at):
            copy.start()

    def end():
        for copy in copies(start):
            copy.wait()

    turn, turns = column_products(
        xn_ref, units_ref, chunk_buf, units_buf, total, chunk_sem, units_sem, store
    )
    return turn, end, turns


def down_grads(
    top_ref, scaled_ref, down_ref, chunk_buf, scaled_buf, total, out, chunk_sem, scaled_sem, out_sem
):
    local, units, _ = down_ref.shape

    def copies(at):
        return [
            pltpu.make_async_copy(out.at[e], down_ref.at[e, :, at], out_sem.at[e])
            for e in range(local)
        ]

    start = pl.ds(0, chunk_buf.shape[2])

    def store(n, at):
        @pl.when(n > 0)
        def _():
            for copy in copies(start):
                copy.wait()

        for e in range(local):
            out[e] = total[:, e * units : (e + 1) * units].T.astype(out.dtype)
        for copy in copies(at):
            copy.start()

    def end():
        for copy in copies(start):
            copy.wait()

    turn, turns = column_products(
        top_ref, scaled_ref, chunk_buf, scaled_buf, total, chunk_sem, scaled_sem, store
    )
    return turn, end, turns


SPAN = 256


def product_sum_kernel(
    line,
    flipped,
    extra,
    grads,
    *refs,
):
    a_ref, w_ref = refs[0], refs[1]
    e_ref = refs[2] if extra else None
    refs = refs[3:] if extra else refs[2:]
    if grads:
        work_refs, refs = (*refs[:2], *refs[3:5], *refs[-7:]), (refs[2], *refs[5:-7])
    (
        out_ref,
        made,
        a_buf,
        e_buf,
        got_pair,
        got_x,
        got_y,
        got_far_x,
        got_far_y,
        got_below,
        got_above,
        load_sem,
        extra_sem,
        pair_sem,
        x_sem,
        y_sem,
        far_x_sem,
        far_y_sem,
        below_sem,
        above_sem,
    ) = refs
    dp, place = lax.axis_index("dp"), lax.axis_index("expert")
    z, c = place // 2, place % 2
    side_x, side_y = corners(dp)
    far = 3 - dp
    to_x, to_y, to_pair = (side_x, place), (side_y, place), (dp, 2 * z + 1 - c)
    to_up, to_down = (dp, place + 2), (dp, place - 2)
    for device in (to_x, to_y, to_pair):
        greet(device)
    pl.when(z > 0)(lambda: greet(to_down))
    pl.when(z < line - 1)(lambda: greet(to_up))
    greeted = 3 + (z > 0).astype(jnp.int32) + (z < line - 1).astype(jnp.int32)
    pl.semaphore_wait(pltpu.get_barrier_semaphore(), greeted)
    count = 4 * line
    width = w_ref.shape[0] if flipped else w_ref.shape[1]
    half = made.shape[4]
    chunk = 512

    def mine(q, height, p):
        return made.at[q, height, c, p]

    def hand(q, height, p):
        at = (q, height, p)
        source = made.at[q, height, 1 - c, p]
        return send(source, got_pair.at[at], pair_sem.at[0, *at], pair_sem.at[1, *at], to_pair)

    def along_x(height, p):
        at = (height, p)
        source = mine(side_x, height, p)
        return send(source, got_x.at[at], x_sem.at[0, *at], x_sem.at[1, *at], to_x)

    def along_y(height, p):
        at = (height, p)
        source = mine(side_y, height, p)
        return send(source, got_y.at[at], y_sem.at[0, *at], y_sem.at[1, *at], to_y)

    def far_x(height):
        source = mine(far, height, 0)
        return send(
            source, got_far_x.at[height], far_x_sem.at[0, height], far_x_sem.at[1, height], to_x
        )

    def far_y(height):
        source = mine(far, height, 1)
        return send(
            source, got_far_y.at[height], far_y_sem.at[0, height], far_y_sem.at[1, height], to_y
        )

    def climb(height, p):
        at = (height, p)
        source = mine(dp, height, p)
        return send(source, got_below.at[at], below_sem.at[0, *at], below_sem.at[1, *at], to_up)

    def descend(height, p):
        at = (height, p)
        source = mine(dp, height, p)
        return send(source, got_above.at[at], above_sem.at[0, *at], above_sem.at[1, *at], to_down)

    def decode(i):
        k, j = i // 4, i % 4
        q = jnp.where(j == 0, far, jnp.where(j == 1, side_x, jnp.where(j == 2, side_y, dp)))
        return k, j, q, farthest(line, z, k)

    def load(i):
        _, _, q, height = decode(i)
        return pltpu.make_async_copy(
            a_ref.at[q * line + height], a_buf.at[i % 2], load_sem.at[i % 2]
        )

    def load_extra(i):
        _, _, q, height = decode(i)
        return pltpu.make_async_copy(
            e_ref.at[q * line + height], e_buf.at[i % 2], extra_sem.at[i % 2]
        )

    def start_load(i):
        load(i).start()
        if extra:
            load_extra(i).start()

    def add(q, height, p, other):
        at = (q, height, c, p)
        made[at] = made[at] + other[...]

    def compute(i):
        _, _, q, height = decode(i)
        load(i).wait()
        if extra:
            load_extra(i).wait()
        pl.when(i + 1 < count)(lambda: start_load(i + 1))
        for at in range(0, width, chunk):
            if flipped:
                part = contract(a_buf[i % 2], w_ref[at : at + chunk, :], 1, 1)
            else:
                part = contract(a_buf[i % 2], w_ref[:, at : at + chunk], 1, 0)
            part = part.astype(made.dtype).reshape(2, 2, half, chunk)
            made[q, height, :, :, :, at : at + chunk] = part
        if extra:
            made[q, height, :, :, :, width : width + 128] = e_buf[i % 2].reshape(2, 2, half, 128)
        for p in (0, 1):
            hand(q, height, p).start()

    def settle(i):
        _, j, q, height = decode(i)
        for p in (0, 1):
            hand(q, height, p).wait_recv()
            add(q, height, p, got_pair.at[q, height, p])

        def opposite():
            far_x(height).start()
            far_y(height).start()

        pl.when(j == 0)(opposite)
        pl.when(j == 1)(lambda: along_x(height, 0).start())
        pl.when(j == 2)(lambda: along_y(height, 1).start())

    def settle_far(i):
        _, j, _, height = decode(i)

        def side_of_x():
            far_y(height).wait_recv()
            add(side_x, height, 1, got_far_y.at[height])
            along_x(height, 1).start()

        def side_of_y():
            far_x(height).wait_recv()
            add(side_y, height, 0, got_far_x.at[height])
            along_y(height, 0).start()

        pl.when(j == 1)(side_of_x)
        pl.when(j == 2)(side_of_y)

    def column(height):
        for p in (0, 1):
            along_x(height, p).wait_recv()
            along_y(height, p).wait_recv()
            total = made[dp, height, c, p].astype(jnp.float32)
            total = total + got_x[height, p].astype(jnp.float32)
            total = total + got_y[height, p].astype(jnp.float32)
            made[dp, height, c, p] = total.astype(made.dtype)
            pl.when((z == 0) & (height > z))(lambda: climb(height, p).start())
            pl.when((z == line - 1) & (height < z))(lambda: descend(height, p).start())

    def pass_on(height):
        for p in (0, 1):

            def upwards():
                climb(height, p).wait_recv()
                add(dp, height, p, got_below.at[height, p])
                climb(height, p).start()

            def downwards():
                descend(height, p).wait_recv()
                add(dp, height, p, got_above.at[height, p])
                descend(height, p).start()

            pl.when((height > z) & (z > 0))(upwards)
            pl.when((height < z) & (z < line - 1))(downwards)

    start_load(0)
    work, work_end, turns = gate_up_grads(*work_refs) if grads else (None, None, 1)

    def step(i, carry):
        k, j, _, _ = decode(i)
        pl.when(i < count)(lambda: compute(i))
        pl.when((i >= 1) & (i <= count))(lambda: settle(i - 1))
        if grads:
            every = count // turns
            pl.when((i < count) & (i % every == 0))(lambda: work(i // every))
        pl.when((i >= 4) & (i < count + 4))(lambda: settle_far(i - 4))
        pl.when((k >= 3) & (j == 2))(lambda: pass_on(farthest(line, z, k - 3)))
        pl.when((k >= 2) & (j == 3))(lambda: column(farthest(line, z, k - 2)))
        return carry

    lax.fori_loop(0, count + 8, step, 0)
    if grads:
        work_end()
    for p in (0, 1):
        out_ref[p] = made[dp, z, c, p].astype(jnp.float32)

        def from_below():
            climb(z, p).wait_recv()
            out_ref[p] = out_ref[p] + got_below[z, p].astype(jnp.float32)

        def from_above():
            descend(z, p).wait_recv()
            out_ref[p] = out_ref[p] + got_above[z, p].astype(jnp.float32)

        pl.when(z > 0)(from_below)
        pl.when(z < line - 1)(from_above)

    def finish(height, carry):
        far_x(height).wait_send()
        far_y(height).wait_send()
        for p in (0, 1):
            for q in range(4):
                hand(q, height, p).wait_send()
            along_x(height, p).wait_send()
            along_y(height, p).wait_send()
            pl.when(height > z)(lambda: climb(height, p).wait_send())
            pl.when(height < z)(lambda: descend(height, p).wait_send())
        return carry

    lax.fori_loop(0, line, finish, 0)


def product_sum(blocks, weights, flipped, extra, line, name, number, grads=None):
    count, rows, depth = blocks.shape
    width = weights.shape[0] if flipped else weights.shape[1]
    wide = width + (0 if extra is None else 128)
    half = rows // 4
    sems = pltpu.SemaphoreType.DMA
    dtype = blocks.dtype

    def space(*shape):
        return pltpu.VMEM((*shape, half, wide), dtype)

    anywhere, inside = pl.BlockSpec(memory_space=pl.ANY), pl.BlockSpec(memory_space=pltpu.VMEM)
    out_shape = [jax.ShapeDtypeStruct((2, half, wide), jnp.float32)]
    work_in, work_space = [], []
    if grads is not None:
        xn, both, shape = grads
        work_in = [xn, both]
        out_shape += [jax.ShapeDtypeStruct(shape, dtype)] * 2
        work_space = [
            pltpu.VMEM((2, xn.shape[0], SPAN), dtype),
            pltpu.VMEM(both.shape, dtype),
            pltpu.VMEM((SPAN, both.shape[2]), jnp.float32),
            pltpu.VMEM((SPAN, both.shape[2]), dtype),
            sems((2,)),
            sems((1,)),
            sems((2, shape[0])),
        ]
    total, *work_out = pl.pallas_call(
        functools.partial(product_sum_kernel, line, flipped, extra is not None, grads is not None),
        out_shape=out_shape,
        in_specs=[anywhere, inside]
        + ([] if extra is None else [anywhere])
        + [anywhere] * len(work_in),
        out_specs=[inside] + [anywhere] * (len(out_shape) - 1),
        scratch_shapes=[
            space(4, line, 2, 2),
            pltpu.VMEM((2, rows, depth), dtype),
            pltpu.VMEM((2, rows, 128), dtype),
            space(4, line, 2),
            space(line, 2),
            space(line, 2),
            space(line),
            space(line),
            space(line, 2),
            space(line, 2),
            sems((2,)),
            sems((2,)),
            sems((2, 4, line, 2)),
            sems((2, line, 2)),
            sems((2, line, 2)),
            sems((2, line)),
            sems((2, line)),
            sems((2, line, 2)),
            sems((2, line, 2)),
            *work_space,
        ],
        compiler_params=pltpu.CompilerParams(
            collective_id=number, has_side_effects=True, vmem_limit_bytes=63 << 20
        ),
        name=name,
    )(blocks, weights, *([] if extra is None else [extra]), *work_in)
    return total.reshape(2 * half, wide), *work_out


def closing_kernel(
    line,
    shared_rows,
    parts_ref,
    small_ref,
    first_ref,
    grad_ref,
    unit_ref,
    inverse_ref,
    gain_ref,
    output_ref,
    top_ref,
    scaled_ref,
    summed_ref,
    shared_ref,
    outputs_ref,
    grads_ref,
    down_ref,
    acc,
    got_pair,
    got_below,
    got_above,
    part,
    got_x,
    got_y,
    got_far_x,
    got_far_y,
    grad_own,
    small,
    got_small,
    load_sem,
    pair_sem,
    load_small_sem,
    pair_small_sem,
    below_sem,
    above_sem,
    part_sem,
    x_sem,
    y_sem,
    far_x_sem,
    far_y_sem,
    spread_sem,
    arrive_sem,
    own_sem,
    small_sem,
    *work_refs,
):
    dp, place = lax.axis_index("dp"), lax.axis_index("expert")
    z, c = place // 2, place % 2
    side_x, side_y = corners(dp)
    far = 3 - dp
    to_x, to_y, to_pair = (side_x, place), (side_y, place), (dp, 2 * z + 1 - c)
    to_up, to_down = (dp, place + 2), (dp, place - 2)
    for device in (to_x, to_y, to_pair):
        greet(device)
    pl.when(z > 0)(lambda: greet(to_down))
    pl.when(z < line - 1)(lambda: greet(to_up))
    greeted = 3 + (z > 0).astype(jnp.int32) + (z < line - 1).astype(jnp.int32)
    pl.semaphore_wait(pltpu.get_barrier_semaphore(), greeted)

    large = parts_ref.shape[3]
    top_rows, low_rows = pl.ds(0, large), pl.ds(large, shared_rows // 2)

    def loads(height, p):
        return (
            pltpu.make_async_copy(
                parts_ref.at[height, c, p], acc.at[height, p, top_rows], load_sem.at[height, p]
            ),
            pltpu.make_async_copy(
                small_ref.at[height, c, p], acc.at[height, p, low_rows], load_small_sem.at[height, p]
            ),
        )

    def hands(height, p):
        at = (height, p)
        return (
            send(
                parts_ref.at[height, 1 - c, p],
                got_pair.at[height, p, top_rows],
                pair_sem.at[0, *at],
                pair_sem.at[1, *at],
                to_pair,
            ),
            send(
                small_ref.at[height, 1 - c, p],
                got_pair.at[height, p, low_rows],
                pair_small_sem.at[0, *at],
                pair_small_sem.at[1, *at],
                to_pair,
            ),
        )

    def climb(height, p):
        at = (height, p)
        return send(
            acc.at[at], got_below.at[at], below_sem.at[0, *at], below_sem.at[1, *at], to_up
        )

    def descend(height, p):
        at = (height, p)
        return send(
            acc.at[at], got_above.at[at], above_sem.at[0, *at], above_sem.at[1, *at], to_down
        )

    def start(k, carry):
        height = farthest(line, z, k)
        for p in (0, 1):
            for copy in (*loads(height, p), *hands(height, p)):
                copy.start()
        return carry

    def pair_sum(k, carry):
        height = farthest(line, z, k)
        for p in (0, 1):
            for copy in loads(height, p):
                copy.wait()
            for copy in hands(height, p):
                copy.wait_recv()
            acc[height, p] = acc[height, p] + got_pair[height, p]
            pl.when((z == 0) & (height > z))(lambda: climb(height, p).start())
            pl.when((z == line - 1) & (height < z))(lambda: descend(height, p).start())
        return carry

    def pass_on(k, carry):
        height = farthest(line, z, k)
        for p in (0, 1):

            def upwards():
                climb(height, p).wait_recv()
                acc[height, p] = acc[height, p] + got_below[height, p]
                climb(height, p).start()

            def downwards():
                descend(height, p).wait_recv()
                acc[height, p] = acc[height, p] + got_above[height, p]
                descend(height, p).start()

            pl.when((height > z) & (z > 0))(upwards)
            pl.when((height < z) & (z < line - 1))(downwards)
        return carry

    def first_load(q, p):
        return pltpu.make_async_copy(first_ref.at[q, p], part.at[q, p], part_sem.at[q, p])

    def along_x(p):
        return send(part.at[side_x, p], got_x.at[p], x_sem.at[0, p], x_sem.at[1, p], to_x)

    def along_y(p):
        return send(part.at[side_y, p], got_y.at[p], y_sem.at[0, p], y_sem.at[1, p], to_y)

    def far_x():
        return send(part.at[far, 0], got_far_x, far_x_sem.at[0], far_x_sem.at[1], to_x)

    def far_y():
        return send(part.at[far, 1], got_far_y, far_y_sem.at[0], far_y_sem.at[1], to_y)

    spreads = ((output_ref, outputs_ref), (grad_own, grads_ref))

    def spread(a, corner, p, way, source=None):
        target = spreads[a][1].at[corner, p]
        return send(
            target if source is None else source,
            target,
            spread_sem.at[a, corner, p, way],
            arrive_sem.at[a, corner, p],
            (to_x, to_y)[way],
        )

    def own_copy(a, p):
        return pltpu.make_async_copy(
            spreads[a][0].at[p], spreads[a][1].at[dp, p], own_sem.at[a, p]
        )

    def spread_own(a, p):
        own_copy(a, p).start()
        for way in (0, 1):
            spread(a, dp, p, way, spreads[a][0].at[p]).start()

    def spread_far(a):
        spread(a, side_x, 0, 0).wait_recv()
        spread(a, side_x, 0, 1).start()
        spread(a, side_y, 1, 0).wait_recv()
        spread(a, side_y, 1, 0).start()

    work, work_end, turns = down_grads(top_ref, scaled_ref, down_ref, *work_refs)
    pauses = 4

    def meanwhile(i):
        def turn(n, carry):
            work(n)
            return carry

        lax.fori_loop(turns * i // pauses, turns * (i + 1) // pauses, turn, 0)

    lax.fori_loop(0, 1, start, 0)
    for q in (far, side_x, side_y, dp):
        for p in (0, 1):
            first_load(q, p).start()
    lax.fori_loop(1, line, start, 0)
    for q in (far, side_x, side_y, dp):
        for p in (0, 1):
            first_load(q, p).wait()
    far_x().start()
    far_y().start()
    along_x(0).start()
    along_y(1).start()
    lax.fori_loop(0, 1, pair_sum, 0)
    far_x().wait_recv()
    part[side_y, 0] = part[side_y, 0] + got_far_x[...]
    along_y(0).start()
    far_y().wait_recv()
    part[side_x, 1] = part[side_x, 1] + got_far_y[...]
    along_x(1).start()
    for p in (0, 1):
        spread_own(0, p)
    lax.fori_loop(1, line, pair_sum, 0)
    meanwhile(0)
    lax.fori_loop(0, 1, pass_on, 0)
    for p in (0, 1):
        along_x(p).wait_recv()
        along_y(p).wait_recv()
        total = part[dp, p].astype(jnp.float32)
        total = total + got_x[p].astype(jnp.float32) + got_y[p].astype(jnp.float32)
        total = total * gain_ref[...]
        unit = unit_ref[p]
        mean = jnp.sum(total * unit, axis=1, keepdims=True) * (1.0 / unit.shape[1])
        rows = grad_ref[p] + inverse_ref[p] * (total - unit * mean)
        grad_own[p] = rows.astype(grad_own.dtype)
        spread_own(1, p)
    meanwhile(1)
    spread_far(0)
    lax.fori_loop(1, 2, pass_on, 0)
    spread_far(1)
    meanwhile(2)
    lax.fori_loop(2, line, pass_on, 0)
    meanwhile(3)
    for p in (0, 1):
        summed_ref[p] = acc[z, p].astype(jnp.float32)

        def from_below():
            climb(z, p).wait_recv()
            summed_ref[p] = summed_ref[p] + got_below[z, p].astype(jnp.float32)

        def from_above():
            descend(z, p).wait_recv()
            summed_ref[p] = summed_ref[p] + got_above[z, p].astype(jnp.float32)

        pl.when(z > 0)(from_below)
        pl.when(z < line - 1)(from_above)

    for side, device in enumerate((to_x, to_y)):
        value = summed_ref[:, large:, :] if side == 0 else shared_ref[...]
        small[side] = value.astype(small.dtype)
        spread(side, side_x, 1, 0).wait_recv()
        spread(side, side_y, 0, 0).wait_recv()
        for p in (0, 1):
            spread(side, far, p, 0).wait_recv()
            for way in (0, 1):
                spread(side, dp, p, way).wait_send()
            own_copy(side, p).wait()
        spread(side, side_x, 0, 1).wait_send()
        spread(side, side_y, 1, 0).wait_send()
        exchange = send(
            small.at[side], got_small.at[side], small_sem.at[0, side], small_sem.at[1, side], device
        )
        exchange.start()
        exchange.wait_recv()
        shared_ref[...] = small[side].astype(jnp.float32) + got_small[side].astype(jnp.float32)
        exchange.wait_send()

    far_x().wait_send()
    far_y().wait_send()
    for p in (0, 1):
        along_x(p).wait_send()
        along_y(p).wait_send()

    def finish(height, carry):
        for p in (0, 1):
            for copy in hands(height, p):
                copy.wait_send()
            pl.when(height > z)(lambda: climb(height, p).wait_send())
            pl.when(height < z)(lambda: descend(height, p).wait_send())
        return carry

    lax.fori_loop(0, line, finish, 0)
    work_end()


def closing(parts, small, first, grad, unit, inverse, gain, output, tops, scaled, shape, line):
    _, rows, wide = parts.shape
    shared_rows = small.shape[1]
    own, width = output.shape
    high, half = (rows + shared_rows) // 2, own // 2
    local, units, _ = shape
    sems = pltpu.SemaphoreType.DMA
    dtype = parts.dtype
    single = jnp.float32
    anywhere, inside = pl.BlockSpec(memory_space=pl.ANY), pl.BlockSpec(memory_space=pltpu.VMEM)
    everyone = jax.ShapeDtypeStruct((4, 2, half, width), dtype)
    summed, shared, outputs, grads, down = pl.pallas_call(
        functools.partial(closing_kernel, line, shared_rows),
        out_shape=[
            jax.ShapeDtypeStruct((2, high, wide), single),
            jax.ShapeDtypeStruct((2, shared_rows // 2, wide), single),
            everyone,
            everyone,
            jax.ShapeDtypeStruct(shape, dtype),
        ],
        in_specs=[anywhere] * 3 + [inside] * 5 + [anywhere] * 2,
        out_specs=[inside, inside, anywhere, anywhere, anywhere],
        scratch_shapes=[
            pltpu.VMEM((line, 2, high, wide), dtype),
            pltpu.VMEM((line, 2, high, wide), dtype),
            pltpu.VMEM((line, 2, high, wide), dtype),
            pltpu.VMEM((line, 2, high, wide), dtype),
            pltpu.VMEM((4, 2, half, width), dtype),
            pltpu.VMEM((2, half, width), dtype),
            pltpu.VMEM((2, half, width), dtype),
            pltpu.VMEM((half, width), dtype),
            pltpu.VMEM((half, width), dtype),
            pltpu.VMEM((2, half, width), dtype),
            pltpu.VMEM((2, 2, shared_rows // 2, wide), dtype),
            pltpu.VMEM((2, 2, shared_rows // 2, wide), dtype),
            sems((line, 2)),
            sems((2, line, 2)),
            sems((line, 2)),
            sems((2, line, 2)),
            sems((2, line, 2)),
            sems((2, line, 2)),
            sems((4, 2)),
            sems((2, 2)),
            sems((2, 2)),
            sems((2,)),
            sems((2,)),
            sems((2, 4, 2, 2)),
            sems((2, 4, 2)),
            sems((2, 2)),
            sems((2, 2)),
            pltpu.VMEM((2, tops.shape[0], SPAN), dtype),
            pltpu.VMEM(scaled.shape, dtype),
            pltpu.VMEM((SPAN, local * units), single),
            pltpu.VMEM((local, units, SPAN), dtype),
            sems((2,)),
            sems((1,)),
            sems((local,)),
        ],
        compiler_params=pltpu.CompilerParams(
            collective_id=5, has_side_effects=True, vmem_limit_bytes=60 << 20
        ),
        name="closing",
    )(
        parts.reshape(line, 2, 2, rows // 2, wide),
        small.reshape(line, 2, 2, shared_rows // 2, wide),
        first.reshape(4, 2, half, width),
        grad.reshape(2, half, width),
        unit.reshape(2, half, width),
        inverse.reshape(2, half, 1),
        gain.reshape(1, width),
        output.reshape(2, half, width),
        tops,
        scaled,
    )
    return (
        summed[:, : rows // 2].reshape(rows, wide),
        summed[:, rows // 2 :],
        shared,
        outputs.reshape(4 * own, width),
        grads.reshape(4 * own, width),
        down,
    )


def square_sum(values, got, sem, side, device):
    copy = send(values.at[side], got.at[side], sem.at[0, side], sem.at[1, side], device)
    copy.start()
    copy.wait()
    return values[side] + got[side]


def as_rows(column):
    return jnp.broadcast_to(column, (column.shape[0], 128)).T[:8]


def as_column(rows):
    return jnp.broadcast_to(rows[:1], (128, rows.shape[1])).T[:, :1]


def meet_square(dp, place):
    side_x, side_y = corners(dp)
    devices = ((side_x, place), (side_y, place))
    for device in devices:
        greet(device)
    pl.semaphore_wait(pltpu.get_barrier_semaphore(), 2)
    return devices


def normed_heads_kernel(
    model_width, q_ref, k_ref, q_gain, k_gain, cos_ref, sin_ref, queries, keys, inverse, sums, got, sem
):
    devices = meet_square(lax.axis_index("dp"), lax.axis_index("expert"))
    raws, gains, outs = (q_ref, k_ref), (q_gain, k_gain), (queries, keys)
    for i, raw in enumerate(raws):
        total = jnp.sum(raw[...] * raw[...], axis=1, keepdims=True)
        sums[0, 8 * i : 8 * i + 8] = as_rows(total)
    sums[1] = square_sum(sums, got, sem, 0, devices[0])
    total = square_sum(sums, got, sem, 1, devices[1])
    inverse[...] = lax.rsqrt(total * (1.0 / model_width) + epsilon)
    for i, raw in enumerate(raws):
        scale = as_column(inverse[8 * i : 8 * i + 8])
        for at in range(0, raw.shape[1], HD):
            head = raw[:, at : at + HD] * scale * gains[i][:, at : at + HD]
            turned = head * cos_ref[...] + pltpu.roll(head, HD // 2, 1) * sin_ref[...]
            outs[i][:, at : at + HD] = turned.astype(outs[i].dtype)


def normed_heads(q_raw, k_raw, q_gain, k_gain, cos, sin, model_width):
    rows, width = q_raw.shape
    head = jax.ShapeDtypeStruct((rows, width), jnp.bfloat16)
    return pl.pallas_call(
        functools.partial(normed_heads_kernel, model_width),
        out_shape=[head, head, jax.ShapeDtypeStruct((16, rows), jnp.float32)],
        in_specs=[pl.BlockSpec(memory_space=pltpu.VMEM)] * 6,
        out_specs=[pl.BlockSpec(memory_space=pltpu.VMEM)] * 3,
        scratch_shapes=[
            pltpu.VMEM((2, 16, rows), jnp.float32),
            pltpu.VMEM((2, 16, rows), jnp.float32),
            pltpu.SemaphoreType.DMA((2, 2)),
        ],
        compiler_params=pltpu.CompilerParams(
            collective_id=11, has_side_effects=True, vmem_limit_bytes=40 << 20
        ),
        name="normed_heads",
    )(q_raw, k_raw, q_gain.reshape(1, width), k_gain.reshape(1, width), cos, sin)


def normed_heads_back_kernel(
    model_width,
    dq_ref,
    dk_ref,
    dv_ref,
    q_ref,
    k_ref,
    q_gain,
    k_gain,
    cos_ref,
    sin_ref,
    inverse,
    grads,
    gain_grads,
    sums,
    got,
    sem,
):
    devices = meet_square(lax.axis_index("dp"), lax.axis_index("expert"))
    raws, gains, news = (q_ref, k_ref), (q_gain, k_gain), (dq_ref, dk_ref)
    rows, width = q_ref.shape

    def parts(i, at):
        cut = slice(at, at + HD)
        new = news[i][:, cut].astype(jnp.float32)
        back = new * cos_ref[...] - pltpu.roll(new, HD // 2, 1) * sin_ref[...]
        unit = raws[i][:, cut] * as_column(inverse[8 * i : 8 * i + 8])
        return back, unit, back * gains[i][:, cut]

    for i in (0, 1):
        total = jnp.zeros((rows, 1), jnp.float32)
        for at in range(0, width, HD):
            back, unit, scaled = parts(i, at)
            gain_grad = jnp.sum(back * unit, axis=0, keepdims=True)
            gain_grads[8 * i : 8 * i + 8, at : at + HD] = jnp.broadcast_to(gain_grad, (8, HD))
            total = total + jnp.sum(scaled * unit, axis=1, keepdims=True)
        sums[0, 8 * i : 8 * i + 8] = as_rows(total)
    sums[1] = square_sum(sums, got, sem, 0, devices[0])
    dots = square_sum(sums, got, sem, 1, devices[1]) * (1.0 / model_width)
    for i in (0, 1):
        dot = as_column(dots[8 * i : 8 * i + 8])
        scale = as_column(inverse[8 * i : 8 * i + 8])
        for at in range(0, width, HD):
            _, unit, scaled = parts(i, at)
            value = scale * (scaled - unit * dot)
            grads[:, i * width + at : i * width + at + HD] = value.astype(grads.dtype)
    grads[:, 2 * width :] = dv_ref[...]


def normed_heads_back(dq, dk, dv, q_raw, k_raw, q_gain, k_gain, cos, sin, inverse, model_width):
    rows, width = q_raw.shape
    return pl.pallas_call(
        functools.partial(normed_heads_back_kernel, model_width),
        out_shape=[
            jax.ShapeDtypeStruct((rows, 3 * width), jnp.bfloat16),
            jax.ShapeDtypeStruct((16, width), jnp.float32),
        ],
        in_specs=[pl.BlockSpec(memory_space=pltpu.VMEM)] * 10,
        out_specs=[pl.BlockSpec(memory_space=pltpu.VMEM)] * 2,
        scratch_shapes=[
            pltpu.VMEM((2, 16, rows), jnp.float32),
            pltpu.VMEM((2, 16, rows), jnp.float32),
            pltpu.SemaphoreType.DMA((2, 2)),
        ],
        compiler_params=pltpu.CompilerParams(
            collective_id=12, has_side_effects=True, vmem_limit_bytes=40 << 20
        ),
        name="normed_heads_back",
    )(
        dq,
        dk,
        dv,
        q_raw,
        k_raw,
        q_gain.reshape(1, width),
        k_gain.reshape(1, width),
        cos,
        sin,
        inverse,
    )


def per_device(
    inputs,
    attention_norm_gain,
    w_query,
    w_key,
    w_value,
    w_out,
    q_gain,
    k_gain,
    expert_norm_gain,
    w_router,
    w_gate,
    w_up,
    w_down,
    routes,
    lengths,
    d_output,
):
    pack_count, seg_rows, model_width = inputs.shape
    local_width = w_query.shape[1]
    local_heads = local_width // HD
    experts = w_router.shape[1]
    groups = lax.axis_size("expert")
    line = groups // 2
    pack_span = seg_rows * groups
    local_experts = w_gate.shape[0]
    offset_rows = lax.axis_index("expert") * seg_rows
    segment, positions = doc_layout(lengths, pack_span)
    pos_query = lax.dynamic_slice_in_dim(positions, offset_rows, seg_rows, 1)
    cos_table, sin_table = rope_tables(pos_query[0], HD)
    inputs_single_float = inputs.astype(jnp.float32)
    first_inverse_norm = lax.rsqrt(
        jnp.mean(inputs_single_float * inputs_single_float, axis=-1, keepdims=True) + epsilon
    )
    first_unit_input = inputs_single_float * first_inverse_norm
    first_normed_input = (first_unit_input * attention_norm_gain).astype(jnp.bfloat16)
    q_raw = jnp.dot(first_normed_input[0], w_query, preferred_element_type=jnp.float32)
    k_raw = jnp.dot(first_normed_input[0], w_key, preferred_element_type=jnp.float32)
    value_rows = jnp.dot(first_normed_input[0], w_value, preferred_element_type=jnp.float32).astype(
        jnp.bfloat16
    )
    queries, keys, head_inverse = normed_heads(
        q_raw, k_raw, q_gain, k_gain, cos_table, sin_table, model_width
    )
    layout = (segment, positions)
    if local_heads == line:
        attention = by_head(layout, w_out, line)
    else:
        attention = by_query(layout, w_out, offset_rows)
    attended, projected, kept = attention[0](queries, keys, value_rows)
    own = lax.axis_index("dp")
    part_rows = seg_rows // lax.axis_size("dp")

    def own_rows(rows):
        return lax.dynamic_slice_in_dim(rows, own * part_rows, part_rows, 0)

    hidden_state = own_rows(inputs_single_float[0]) + projected
    second_inverse_norm = lax.rsqrt(
        jnp.mean(hidden_state * hidden_state, axis=-1, keepdims=True) + epsilon
    )
    second_unit_input = hidden_state * second_inverse_norm
    second_normed_input = second_unit_input * expert_norm_gain
    router = jax.nn.softmax(
        jnp.dot(second_normed_input, w_router, precision=lax.Precision.HIGHEST), axis=-1
    )
    chosen = own_rows(routes[:, 0, :])
    expert_range = jnp.arange(experts, dtype=jnp.int32)
    named = jnp.any(chosen[:, :, None] == expert_range, axis=1)
    top_own = own_rows(d_output[0])
    top_all = lax.all_gather(top_own, ALL, axis=0, tiled=True)
    gate_table = jnp.where(named, router, 0.0)
    gate_high = gate_table.astype(jnp.bfloat16)
    gate_low = (gate_table - gate_high.astype(jnp.float32)).astype(jnp.bfloat16)
    widen = ((0, 0), (0, 64 - experts))
    own_tokens = jnp.concatenate(
        [
            second_normed_input.astype(jnp.bfloat16),
            jnp.pad(gate_high, widen),
            jnp.pad(gate_low, widen),
        ],
        axis=1,
    )
    xn_all, grad_units, scaled, gate_part = gate_act(
        own_tokens, top_all, w_gate, w_up, w_down, line
    )
    w_both = jnp.concatenate([*w_gate, *w_up], axis=1)
    (grad_tokens,) = product_sum(grad_units, w_both, True, gate_part, line, "grad_tokens", 4)
    moe_out, grad_gate, grad_up = product_sum(
        scaled,
        w_down.reshape(-1, model_width),
        False,
        None,
        line,
        "expert_sum",
        2,
        (xn_all, grad_units, w_gate.shape),
    )
    output = (hidden_state + moe_out).astype(jnp.bfloat16)
    grad_xn_exp = grad_tokens[:, :model_width]
    gate_sums = grad_tokens[:, model_width : model_width + experts]
    grad_router_probs = jnp.where(named, gate_sums, 0.0)
    grad_logits = router * (
        grad_router_probs - jnp.sum(router * grad_router_probs, axis=-1, keepdims=True)
    )
    grad_second_normed_input = grad_xn_exp + jnp.einsum(
        "se,de->sd", grad_logits, w_router, precision=lax.Precision.HIGHEST
    )
    grad_router = jnp.einsum(
        "sd,se->de", second_normed_input, grad_logits, precision=lax.Precision.HIGHEST
    )
    grad_expert_norm_gain = jnp.sum(grad_second_normed_input * second_unit_input, axis=0)
    grad_second_unit_input = grad_second_normed_input * expert_norm_gain
    grad_hidden = top_own.astype(jnp.float32) + second_inverse_norm * (
        grad_second_unit_input
        - second_unit_input
        * jnp.mean(grad_second_unit_input * second_unit_input, axis=-1, keepdims=True)
    )
    grad_attn, grad_queries, grad_keys, grad_values = attention[1](
        kept, grad_hidden.astype(jnp.bfloat16)
    )
    grad_out = jnp.einsum("sk,sd->kd", attended, grad_attn, preferred_element_type=jnp.float32)
    grad_heads_raw, gain_grads = normed_heads_back(
        grad_queries.astype(jnp.bfloat16),
        grad_keys,
        grad_values,
        q_raw,
        k_raw,
        q_gain,
        k_gain,
        cos_table,
        sin_table,
        head_inverse,
        model_width,
    )
    grad_q_gain, grad_k_gain = gain_grads[0], gain_grads[8]
    grad_projections = jnp.einsum(
        "sd,sk->dk", first_normed_input[0], grad_heads_raw, preferred_element_type=jnp.float32
    )
    grad_first_normed_input = sum(
        contract(grad_heads_raw[:, i * local_width : (i + 1) * local_width], weight, 1, 1)
        for i, weight in enumerate((w_query, w_key, w_value))
    )
    grad_attn_gain = jnp.sum(grad_first_normed_input * first_unit_input[0], axis=0)
    wide = grad_projections.shape[1]
    small = jnp.concatenate(
        [
            grad_q_gain.reshape(groups, -1),
            grad_k_gain.reshape(groups, -1),
            grad_attn_gain.reshape(groups, -1),
            grad_expert_norm_gain.reshape(groups, -1),
            grad_router.reshape(groups, -1),
        ],
        axis=1,
    )
    small_rows = 32
    filled = small.shape[1]
    small = jnp.pad(small, ((0, 0), (0, small_rows * wide - filled)))
    summed, own_small, shared, outputs, grad_input, grad_down = closing(
        grad_projections.astype(jnp.bfloat16).reshape(groups, -1, wide),
        small.astype(jnp.bfloat16).reshape(groups, small_rows, wide),
        grad_first_normed_input.astype(jnp.bfloat16),
        grad_hidden,
        own_rows(first_unit_input[0]),
        own_rows(first_inverse_norm[0]),
        attention_norm_gain,
        output,
        top_all,
        scaled,
        w_down.shape,
        line,
    )
    gain_size, norm_size = local_width // groups, model_width // groups
    own_gains = own_small.reshape(-1)[: 2 * gain_size]
    shared = shared.reshape(-1)[2 * gain_size : filled]
    grad_out = lax.psum_scatter(
        grad_out.astype(jnp.bfloat16), "expert", scatter_dimension=0, tiled=True
    ).astype(jnp.float32)
    return (
        outputs[None],
        grad_input.astype(jnp.float32)[None],
        shared[:norm_size],
        summed[:, :local_width],
        summed[:, local_width : 2 * local_width],
        summed[:, 2 * local_width :],
        grad_out,
        own_gains[:gain_size],
        own_gains[gain_size:],
        shared[norm_size : 2 * norm_size],
        shared[2 * norm_size :].reshape(norm_size, experts),
        grad_gate.astype(jnp.float32),
        grad_up.astype(jnp.float32),
        grad_down.astype(jnp.float32),
    )


def solution(mesh):
    placed = (
        P(None, "expert", None),
        P(),
        P(None, "dp"),
        P(None, "dp"),
        P(None, "dp"),
        P("dp", None),
        P("dp"),
        P("dp"),
        P(),
        P(),
        P("expert", None, "dp"),
        P("expert", None, "dp"),
        P("expert", "dp", None),
        P("expert", None, None),
        P(),
        P(None, "expert", None),
    )
    return jax.shard_map(
        per_device,
        mesh=mesh,
        in_specs=placed,
        out_specs=(
            P(None, "expert", None),
            P(None, "expert", None),
            P("expert"),
            P("expert", "dp"),
            P("expert", "dp"),
            P("expert", "dp"),
            P(("dp", "expert"), None),
            P(("dp", "expert")),
            P(("dp", "expert")),
            P("expert"),
            P("expert", None),
            P("expert", None, "dp"),
            P("expert", None, "dp"),
            P("expert", "dp", None),
        ),
        check_vma=False,
    )
```

```python
import functools

import jax
import jax.numpy as jnp
from jax import lax
from jax.experimental import pallas as pl
from jax.experimental.pallas import tpu as pltpu
from jax.sharding import PartitionSpec as P

HD = 128


epsilon = 1e-05
rope_base = 10000.0
masked_score = -1e30


def doc_layout(lengths, pack_span):
    doc_ends = jnp.cumsum(lengths, axis=1)
    starts = doc_ends - lengths
    places = jnp.arange(pack_span, dtype=jnp.int32)
    segment = jnp.sum((places[None, :, None] >= doc_ends[:, None, :]).astype(jnp.int32), axis=2)
    member = segment[:, :, None] == jnp.arange(lengths.shape[1], dtype=jnp.int32)[None, None, :]
    begins = jnp.sum(jnp.where(member, starts[:, None, :], 0), axis=2)
    return (segment, places[None, :] - begins)


def rope_tables(positions, head_size):
    half_size = head_size // 2
    frequency = rope_base ** (-2.0 * jnp.arange(half_size, dtype=jnp.float32) / head_size)
    angles = positions.astype(jnp.float32)[..., None] * frequency
    cos, sin = jnp.cos(angles), jnp.sin(angles)
    return jnp.concatenate([cos, cos], axis=-1), jnp.concatenate([-sin, sin], axis=-1)


ALL = ("dp", "expert")


DEVICES = pl.DeviceIdType.MESH


def greet(device):
    pl.semaphore_signal(
        pltpu.get_barrier_semaphore(), inc=1, device_id=device, device_id_type=DEVICES
    )


def send(source, target, send_sem, arrive_sem, device):
    return pltpu.make_async_remote_copy(
        src_ref=source,
        dst_ref=target,
        send_sem=send_sem,
        recv_sem=arrive_sem,
        device_id=device,
        device_id_type=DEVICES,
    )


def contract(a, b, a_dim, b_dim):
    return lax.dot_general(
        a, b, (((a_dim,), (b_dim,)), ((), ())), preferred_element_type=jnp.float32
    )


def corners(dp):
    return dp + 1 - 2 * (dp % 2), (dp + 2) % 4


def gather_square_kernel(x_ref, out_ref, sent, arrived, own_sem):
    dp, place = lax.axis_index("dp"), lax.axis_index("expert")
    side_x, side_y = corners(dp)
    devices = ((side_x, place), (side_y, place))
    for device in devices:
        greet(device)
    pl.semaphore_wait(pltpu.get_barrier_semaphore(), 2)

    def copy(corner, p, way, source=None):
        target = out_ref.at[corner, p]
        return send(
            target if source is None else source,
            target,
            sent.at[corner, p, way],
            arrived.at[corner, p],
            devices[way],
        )

    for p in (0, 1):
        pltpu.make_async_copy(x_ref.at[p], out_ref.at[dp, p], own_sem.at[p]).start()
        for way in (0, 1):
            copy(dp, p, way, x_ref.at[p]).start()
    copy(side_x, 0, 0).wait_recv()
    copy(side_x, 0, 1).start()
    copy(side_y, 0, 0).wait_recv()
    copy(side_x, 1, 0).wait_recv()
    copy(side_y, 1, 0).wait_recv()
    copy(side_y, 1, 0).start()
    for p in (0, 1):
        copy(3 - dp, p, 0).wait_recv()
        for way in (0, 1):
            copy(dp, p, way).wait_send()
        pltpu.make_async_copy(x_ref.at[p], out_ref.at[dp, p], own_sem.at[p]).wait()
    copy(side_x, 0, 1).wait_send()
    copy(side_y, 1, 0).wait_send()


def gather_dp(rows):
    count, width = rows.shape
    gathered = pl.pallas_call(
        gather_square_kernel,
        out_shape=jax.ShapeDtypeStruct((4, 2, count // 2, width), rows.dtype),
        in_specs=[pl.BlockSpec(memory_space=pltpu.VMEM)],
        out_specs=pl.BlockSpec(memory_space=pl.ANY),
        scratch_shapes=[
            pltpu.SemaphoreType.DMA((4, 2, 2)),
            pltpu.SemaphoreType.DMA((4, 2)),
            pltpu.SemaphoreType.DMA((2,)),
        ],
        compiler_params=pltpu.CompilerParams(collective_id=10, has_side_effects=True),
        name="gather_dp",
    )(rows.reshape(2, count // 2, width))
    return gathered.reshape(4 * count, width)


def farthest(line, z, k):
    return ranked(line, z, k, lambda place, at: (-abs(place - at), place))


def reduce_kernel(
    square,
    line,
    paired,
    x_ref,
    out_ref,
    acc,
    got_pair,
    got_x,
    got_y,
    got_far_x,
    got_far_y,
    got_below,
    got_above,
    load_sem,
    pair_sem,
    x_sem,
    y_sem,
    far_x_sem,
    far_y_sem,
    below_sem,
    above_sem,
):
    dp, place = lax.axis_index("dp"), lax.axis_index("expert")
    z, c = place // 2, place % 2
    side_x, side_y = corners(dp)
    core = c if paired else 0
    own = dp if square else 0
    quarters = (3 - dp, side_x, side_y, dp) if square else (0,)
    to_x, to_y = (side_x, place), (side_y, place)
    to_pair, to_up, to_down = (dp, 2 * z + 1 - c), (dp, place + 2), (dp, place - 2)
    greeted = 0
    if square:
        greet(to_x)
        greet(to_y)
        greeted += 2
    if paired:
        greet(to_pair)
        greeted += 1
    if line > 1:
        pl.when(z > 0)(lambda: greet(to_down))
        pl.when(z < line - 1)(lambda: greet(to_up))
        greeted = greeted + (z > 0).astype(jnp.int32) + (z < line - 1).astype(jnp.int32)
    pl.semaphore_wait(pltpu.get_barrier_semaphore(), greeted)

    def load(q, height, p):
        return pltpu.make_async_copy(
            x_ref.at[q, height, core, p], acc.at[q, height, p], load_sem.at[q, height, p]
        )

    def hand(q, height, p):
        at = (q, height, p)
        source = x_ref.at[q, height, 1 - core, p]
        return send(source, got_pair.at[at], pair_sem.at[0, *at], pair_sem.at[1, *at], to_pair)

    def along_x(height, p):
        at = (height, p)
        return send(
            acc.at[side_x, height, p], got_x.at[at], x_sem.at[0, *at], x_sem.at[1, *at], to_x
        )

    def along_y(height, p):
        at = (height, p)
        return send(
            acc.at[side_y, height, p], got_y.at[at], y_sem.at[0, *at], y_sem.at[1, *at], to_y
        )

    def far_x(height):
        return send(
            acc.at[3 - dp, height, 0],
            got_far_x.at[height],
            far_x_sem.at[0, height],
            far_x_sem.at[1, height],
            to_x,
        )

    def far_y(height):
        return send(
            acc.at[3 - dp, height, 1],
            got_far_y.at[height],
            far_y_sem.at[0, height],
            far_y_sem.at[1, height],
            to_y,
        )

    def climb(height, p):
        at = (height, p)
        return send(
            acc.at[own, height, p], got_below.at[at], below_sem.at[0, *at], below_sem.at[1, *at], to_up
        )

    def descend(height, p):
        at = (height, p)
        return send(
            acc.at[own, height, p],
            got_above.at[at],
            above_sem.at[0, *at],
            above_sem.at[1, *at],
            to_down,
        )

    def height_of(k):
        return farthest(line, z, k) if line > 1 else 0

    def start(k, carry):
        for q in quarters:
            for p in (0, 1):
                load(q, height_of(k), p).start()
                if paired:
                    hand(q, height_of(k), p).start()
        return carry

    lax.fori_loop(0, line, start, 0)

    def step(k, carry):
        def cores():
            height = height_of(k)
            for q in quarters:
                for p in (0, 1):
                    load(q, height, p).wait()
                    if paired:
                        hand(q, height, p).wait_recv()
                        acc[q, height, p] = acc[q, height, p] + got_pair[q, height, p]
                if square and q is quarters[0]:
                    far_x(height).start()
                    far_y(height).start()

        def sides():
            height = height_of(k - 1)
            along_x(height, 0).start()
            along_y(height, 1).start()
            far_x(height).wait_recv()
            acc[side_y, height, 0] = acc[side_y, height, 0] + got_far_x[height]
            along_y(height, 0).start()
            far_y(height).wait_recv()
            acc[side_x, height, 1] = acc[side_x, height, 1] + got_far_y[height]
            along_x(height, 1).start()

        def column():
            height = height_of(k - 2)
            for p in (0, 1):
                if square:
                    along_x(height, p).wait_recv()
                    along_y(height, p).wait_recv()
                    total = acc[own, height, p].astype(jnp.float32)
                    total = total + got_x[height, p].astype(jnp.float32)
                    total = total + got_y[height, p].astype(jnp.float32)
                    acc[own, height, p] = total.astype(acc.dtype)
                if line > 1:
                    pl.when((z == 0) & (height > z))(lambda: climb(height, p).start())
                    pl.when((z == line - 1) & (height < z))(lambda: descend(height, p).start())

        def pass_on():
            height = height_of(k - 3)
            for p in (0, 1):

                def upwards():
                    climb(height, p).wait_recv()
                    acc[own, height, p] = acc[own, height, p] + got_below[height, p]
                    climb(height, p).start()

                def downwards():
                    descend(height, p).wait_recv()
                    acc[own, height, p] = acc[own, height, p] + got_above[height, p]
                    descend(height, p).start()

                pl.when((height > z) & (z > 0))(upwards)
                pl.when((height < z) & (z < line - 1))(downwards)

        pl.when(k < line)(cores)
        if square:
            pl.when((k >= 1) & (k < line + 1))(sides)
        pl.when((k >= 2) & (k < line + 2))(column)
        if line > 1:
            pl.when(k >= 3)(pass_on)
        return carry

    lax.fori_loop(0, line + (3 if line > 1 else 2), step, 0)
    home = z if line > 1 else 0
    for p in (0, 1):
        out_ref[p] = acc[own, home, p].astype(jnp.float32)
        if line > 1:

            def from_below():
                climb(z, p).wait_recv()
                out_ref[p] = out_ref[p] + got_below[z, p].astype(jnp.float32)

            def from_above():
                descend(z, p).wait_recv()
                out_ref[p] = out_ref[p] + got_above[z, p].astype(jnp.float32)

            pl.when(z > 0)(from_below)
            pl.when(z < line - 1)(from_above)

    def finish(height, carry):
        if square:
            far_x(height).wait_send()
            far_y(height).wait_send()
        for p in (0, 1):
            if paired:
                for q in quarters:
                    hand(q, height, p).wait_send()
            if square:
                along_x(height, p).wait_send()
                along_y(height, p).wait_send()
            if line > 1:
                pl.when(height > z)(lambda: climb(height, p).wait_send())
                pl.when(height < z)(lambda: descend(height, p).wait_send())
        return carry

    lax.fori_loop(0, line, finish, 0)


def reduce_to(parts, square, line, paired, name, number):
    _, rows, width = parts.shape
    quarters, cores, half = (4 if square else 1), (2 if paired else 1), rows // 2

    def space(used, *shape):
        return pltpu.VMEM((*shape, half, width) if used else (*shape, 16, 128), parts.dtype)

    sems = pltpu.SemaphoreType.DMA
    total = pl.pallas_call(
        functools.partial(reduce_kernel, square, line, paired),
        out_shape=jax.ShapeDtypeStruct((2, half, width), jnp.float32),
        in_specs=[pl.BlockSpec(memory_space=pl.ANY)],
        out_specs=pl.BlockSpec(memory_space=pltpu.VMEM),
        scratch_shapes=[
            space(True, quarters, line, 2),
            space(paired, quarters, line, 2),
            space(square, line, 2),
            space(square, line, 2),
            space(square, line),
            space(square, line),
            space(line > 1, line, 2),
            space(line > 1, line, 2),
            sems((quarters, line, 2)),
            sems((2, quarters, line, 2)),
            sems((2, line, 2)),
            sems((2, line, 2)),
            sems((2, line)),
            sems((2, line)),
            sems((2, line, 2)),
            sems((2, line, 2)),
        ],
        compiler_params=pltpu.CompilerParams(
            collective_id=number, has_side_effects=True, vmem_limit_bytes=60 << 20
        ),
        name=name,
    )(parts.reshape(quarters, line, cores, 2, half, width))
    return total.reshape(rows, width)


def scatter_dp(rows):
    return reduce_to(rows.reshape(4, -1, rows.shape[1]), True, 1, False, "scatter_dp", 3)


def visit_others(line, z, visit):
    def turn(k, carry):
        visit((z + k) % line)
        return carry

    lax.fori_loop(1, line, turn, 0)


def greet_line(line, dp, z, c):
    visit_others(line, z, lambda other: greet((dp, 2 * other + c)))
    greet((dp, 2 * z + 1 - c))
    pl.semaphore_wait(pltpu.get_barrier_semaphore(), line)


def columns(z):
    return pl.ds(pl.multiple_of(z * HD, HD), HD)


def to_heads_kernel(line, shared, *refs):
    count = len(shared)
    ins, outs = refs[:count], refs[count : 2 * count]
    sent, arrived, pair_sent, pair_arrived, own_sem = refs[2 * count :]
    dp, place = lax.axis_index("dp"), lax.axis_index("expert")
    z, c = place // 2, place % 2
    pair = (dp, 2 * z + 1 - c)
    greet_line(line, dp, z, c)

    def block(i, origin):
        return outs[i].at[origin, c] if shared[i] else outs[i].at[origin]

    def out(i, other):
        source = ins[i].at[:, columns(other)]
        device = (dp, 2 * other + c)
        return send(source, block(i, z), sent.at[i, other], arrived.at[i, z], device)

    def into(i, origin):
        part = block(i, origin)
        return send(part, part, sent.at[i, origin], arrived.at[i, origin], pair)

    def share(i, origin, source=None):
        part = block(i, origin)
        return send(
            part if source is None else source,
            part,
            pair_sent.at[i, origin],
            pair_arrived.at[i, origin],
            pair,
        )

    def own(i):
        return pltpu.make_async_copy(ins[i].at[:, columns(z)], block(i, z), own_sem.at[i])

    def dispatch(other):
        for i in range(count):
            out(i, other).start()

    visit_others(line, z, dispatch)
    for i in range(count):
        own(i).start()
        if shared[i]:
            share(i, z, ins[i].at[:, columns(z)]).start()

    def receive(origin):
        for i in range(count):
            into(i, origin).wait_recv()
            if shared[i]:
                share(i, origin).start()

    visit_others(line, z, receive)

    def finish(other):
        for i in range(count):
            out(i, other).wait_send()

    visit_others(line, z, finish)
    for i in range(count):
        own(i).wait()
        if shared[i]:

            def settle(origin, carry):
                share(i, origin).wait()
                return carry

            lax.fori_loop(0, line, settle, 0)


def to_heads(arrays, shared, line, name, number):
    rows = arrays[0].shape[0]
    count = len(arrays)
    sems = pltpu.SemaphoreType.DMA
    return pl.pallas_call(
        functools.partial(to_heads_kernel, line, shared),
        out_shape=[
            jax.ShapeDtypeStruct((line, 2, rows, HD) if both else (line, rows, HD), array.dtype)
            for array, both in zip(arrays, shared)
        ],
        in_specs=[pl.BlockSpec(memory_space=pltpu.VMEM)] * count,
        out_specs=[pl.BlockSpec(memory_space=pl.ANY)] * count,
        scratch_shapes=[sems((count, line))] * 4 + [sems((count,))],
        compiler_params=pltpu.CompilerParams(collective_id=number, has_side_effects=True),
        name=name,
    )(*arrays)


def to_tokens_kernel(line, summed, *refs):
    count, sums = len(summed), sum(summed)
    ins, outs = refs[:count], refs[count : 2 * count]
    mine, theirs = refs[2 * count : 2 * count + 2]
    sent, arrived, pair_sem, load_sem, own_sem = refs[2 * count + 2 :]
    dp, place = lax.axis_index("dp"), lax.axis_index("expert")
    z, c = place // 2, place % 2
    pair = (dp, 2 * z + 1 - c)
    greet_line(line, dp, z, c)
    at_sum = [sum(summed[:i]) for i in range(count)]

    def load(i, other):
        return pltpu.make_async_copy(
            ins[i].at[other, c], mine.at[at_sum[i], other], load_sem.at[at_sum[i], other]
        )

    def hand(i, other):
        s = at_sum[i]
        return send(
            ins[i].at[other, 1 - c],
            theirs.at[s, other],
            pair_sem.at[0, s, other],
            pair_sem.at[1, s, other],
            pair,
        )

    def source(i, other):
        return mine.at[at_sum[i], other] if summed[i] else ins[i].at[other]

    def out(i, other):
        target = outs[i].at[:, columns(z)]
        device = (dp, 2 * other + c)
        return send(source(i, other), target, sent.at[i, other], arrived.at[i, z], device)

    def into(i, origin):
        part = outs[i].at[:, columns(origin)]
        return send(part, part, sent.at[i, origin], arrived.at[i, origin], pair)

    def own(i):
        return pltpu.make_async_copy(source(i, z), outs[i].at[:, columns(z)], own_sem.at[i])

    def prepare(other):
        for i in range(count):
            if summed[i]:
                load(i, other).start()
                hand(i, other).start()

    def add(i, other):
        if summed[i]:
            load(i, other).wait()
            hand(i, other).wait_recv()
            s = at_sum[i]
            mine[s, other] = mine[s, other] + theirs[s, other]

    def dispatch(other):
        for i in range(count):
            add(i, other)
            out(i, other).start()

    if sums:
        visit_others(line, z, prepare)
        prepare(z)
    visit_others(line, z, dispatch)
    for i in range(count):
        add(i, z)
        own(i).start()

    def finish(other):
        for i in range(count):
            into(i, other).wait_recv()
            out(i, other).wait_send()
            if summed[i]:
                hand(i, other).wait_send()

    visit_others(line, z, finish)
    for i in range(count):
        own(i).wait()
        if summed[i]:
            hand(i, z).wait_send()


def to_tokens(arrays, summed, line, name, number):
    rows = arrays[0].shape[-2]
    count, sums = len(arrays), max(sum(summed), 1)
    sems = pltpu.SemaphoreType.DMA
    dtype = arrays[0].dtype
    held = (sums, line, rows, HD) if sum(summed) else (1, 1, 16, HD)
    return pl.pallas_call(
        functools.partial(to_tokens_kernel, line, summed),
        out_shape=[jax.ShapeDtypeStruct((rows, line * HD), dtype)] * count,
        in_specs=[pl.BlockSpec(memory_space=pl.ANY)] * count,
        out_specs=[pl.BlockSpec(memory_space=pl.ANY)] * count,
        scratch_shapes=[pltpu.VMEM(held, dtype)] * 2
        + [
            sems((count, line)),
            sems((count, line)),
            sems((2, sums, line)),
            sems((sums, line)),
            sems((count,)),
        ],
        compiler_params=pltpu.CompilerParams(collective_id=number, has_side_effects=True),
        name=name,
    )(*arrays)


KEY_TILE = 512


def masked_scores(keys, queries, tile, first, starts):
    scores = contract(keys, queries, 1, 1) * HD ** (-0.5)
    key_at = tile * KEY_TILE + lax.broadcasted_iota(jnp.int32, scores.shape, 0)
    query_at = first + lax.broadcasted_iota(jnp.int32, (1, scores.shape[1]), 1)
    return jnp.where((key_at >= starts) & (key_at <= query_at), scores, masked_score)


def attend_kernel(bounds, q_ref, k_ref, v_ref, start_ref, o_ref, total_ref):
    i = pl.program_id(0)
    queries, starts = q_ref[0], start_ref[0]
    span = queries.shape[0]

    def tile_step(tile, carry):
        largest, total, acc = carry
        rows = pl.ds(pl.multiple_of(tile * KEY_TILE, KEY_TILE), KEY_TILE)
        scores = masked_scores(k_ref[rows, :], queries, tile, bounds[2, i], starts)
        new = jnp.maximum(largest, jnp.max(scores, axis=0, keepdims=True))
        weights = jnp.exp(scores - new)
        fade = jnp.exp(largest - new)
        total = fade * total + jnp.sum(weights, axis=0, keepdims=True)
        acc = fade * acc + contract(v_ref[rows, :], weights.astype(jnp.bfloat16), 0, 0)
        return new, total, acc

    largest, total, acc = lax.fori_loop(
        bounds[0, i],
        bounds[1, i],
        tile_step,
        (
            jnp.full((1, span), masked_score, jnp.float32),
            jnp.zeros((1, span), jnp.float32),
            jnp.zeros((HD, span), jnp.float32),
        ),
    )
    o_ref[0] = (acc / total).T.astype(o_ref.dtype)
    total_ref[0] = largest + jnp.log(total)


def attend_back_kernel(
    bounds, q_ref, k_ref, v_ref, start_ref, total_ref, delta_ref, d_ref, dq_ref, dk_ref, dv_ref, dk, dv
):
    i = pl.program_id(0)
    queries, starts, grad = q_ref[0], start_ref[0], d_ref[0]
    total, delta = total_ref[0], delta_ref[0]

    @pl.when(i == 0)
    def _():
        dk[...] = jnp.zeros_like(dk)
        dv[...] = jnp.zeros_like(dv)

    def tile_step(tile, acc):
        rows = pl.ds(pl.multiple_of(tile * KEY_TILE, KEY_TILE), KEY_TILE)
        keys = k_ref[rows, :]
        scores = masked_scores(keys, queries, tile, bounds[2, i], starts)
        weights = jnp.exp(scores - total)
        grad_weights = contract(v_ref[rows, :], grad, 1, 1)
        grad_scores = (weights * (grad_weights - delta)).astype(jnp.bfloat16)
        dv[rows, :] += contract(weights.astype(jnp.bfloat16), grad, 1, 0)
        dk[rows, :] += contract(grad_scores, queries, 1, 0)
        return acc + contract(keys, grad_scores, 0, 0)

    acc = jnp.zeros((HD, queries.shape[0]), jnp.float32)
    acc = lax.fori_loop(bounds[0, i], bounds[1, i], tile_step, acc)
    dq_ref[0] = (acc * HD ** (-0.5)).T.astype(dq_ref.dtype)

    @pl.when(i == pl.num_programs(0) - 1)
    def _():
        dk_ref[...] = (dk[...] * HD ** (-0.5)).astype(dk_ref.dtype)
        dv_ref[...] = dv[...].astype(dv_ref.dtype)


def attend(bounds, queries, keys, values, starts):
    line, span, _ = queries.shape
    pack = keys.shape[0]
    block = pl.BlockSpec((1, span, HD), lambda i, _: (i, 0, 0))
    row = pl.BlockSpec((1, 1, span), lambda i, _: (i, 0, 0))
    whole = pl.BlockSpec((pack, HD), lambda i, _: (0, 0))
    return pl.pallas_call(
        attend_kernel,
        grid_spec=pltpu.PrefetchScalarGridSpec(
            num_scalar_prefetch=1,
            grid=(line,),
            in_specs=[block, whole, whole, row],
            out_specs=[block, row],
        ),
        out_shape=[
            jax.ShapeDtypeStruct(queries.shape, jnp.bfloat16),
            jax.ShapeDtypeStruct(starts.shape, jnp.float32),
        ],
        name="attend",
    )(bounds, queries, keys, values, starts)


def attend_back(bounds, queries, keys, values, starts, total, delta, grad):
    line, span, _ = queries.shape
    pack = keys.shape[0]
    block = pl.BlockSpec((1, span, HD), lambda i, _: (i, 0, 0))
    row = pl.BlockSpec((1, 1, span), lambda i, _: (i, 0, 0))
    whole = pl.BlockSpec((pack, HD), lambda i, _: (0, 0))
    return pl.pallas_call(
        attend_back_kernel,
        grid_spec=pltpu.PrefetchScalarGridSpec(
            num_scalar_prefetch=1,
            grid=(line,),
            in_specs=[block, whole, whole, row, row, row, block],
            out_specs=[block, whole, whole],
            scratch_shapes=[pltpu.VMEM((pack, HD), jnp.float32)] * 2,
        ),
        out_shape=[jax.ShapeDtypeStruct(queries.shape, jnp.bfloat16)]
        + [jax.ShapeDtypeStruct((pack, HD), jnp.bfloat16)] * 2,
        name="attend_back",
    )(bounds, queries, keys, values, starts, total, delta, grad)


def out_sum_kernel(
    line,
    o_ref,
    w_ref,
    attended_ref,
    out_ref,
    att,
    made,
    got_x,
    got_y,
    got_far_x,
    got_far_y,
    sent,
    arrived,
    own_sem,
    att_sem,
    x_sem,
    y_sem,
    far_x_sem,
    far_y_sem,
):
    dp, place = lax.axis_index("dp"), lax.axis_index("expert")
    z, c = place // 2, place % 2
    side_x, side_y = corners(dp)
    far = 3 - dp
    to_x, to_y = (side_x, place), (side_y, place)
    visit_others(line, z, lambda other: greet((dp, 2 * other + c)))
    greet(to_x)
    greet(to_y)
    pl.semaphore_wait(pltpu.get_barrier_semaphore(), line + 1)
    rows, half, width = att.shape[1], made.shape[2], made.shape[3]
    chunk = 512
    order = (far, side_x, side_y, dp)

    def block(q):
        return pl.ds(pl.multiple_of(q * rows, rows), rows)

    def out(q, other):
        device = (dp, 2 * other + c)
        source, target = o_ref.at[other, block(q)], att.at[q, :, columns(z)]
        return send(source, target, sent.at[q, other], arrived.at[q, z], device)

    def into(q, origin):
        part = att.at[q, :, columns(origin)]
        return send(part, part, sent.at[q, origin], arrived.at[q, origin], to_x)

    def own(q):
        return pltpu.make_async_copy(
            o_ref.at[z, block(q)], att.at[q, :, columns(z)], own_sem.at[q]
        )

    def att_out(q):
        return pltpu.make_async_copy(att.at[q], attended_ref.at[block(q)], att_sem.at[q])

    def along_x(p):
        return send(made.at[side_x, p], got_x.at[p], x_sem.at[0, p], x_sem.at[1, p], to_x)

    def along_y(p):
        return send(made.at[side_y, p], got_y.at[p], y_sem.at[0, p], y_sem.at[1, p], to_y)

    def far_x():
        return send(made.at[far, 0], got_far_x, far_x_sem.at[0], far_x_sem.at[1], to_x)

    def far_y():
        return send(made.at[far, 1], got_far_y, far_y_sem.at[0], far_y_sem.at[1], to_y)

    for q in order:
        visit_others(line, z, lambda other: out(q, other).start())
        own(q).start()
    for i, q in enumerate(order):
        visit_others(line, z, lambda origin: into(q, origin).wait_recv())
        own(q).wait()
        att_out(q).start()
        for at in range(0, width, chunk):
            part = contract(att[q], w_ref[:, at : at + chunk], 1, 0).astype(made.dtype)
            made[q, :, :, at : at + chunk] = part.reshape(2, half, chunk)
        if i == 0:
            far_x().start()
            far_y().start()
        if i == 1:
            along_x(0).start()
        if i == 2:
            along_y(1).start()
    far_y().wait_recv()
    made[side_x, 1] = made[side_x, 1] + got_far_y[...]
    along_x(1).start()
    far_x().wait_recv()
    made[side_y, 0] = made[side_y, 0] + got_far_x[...]
    along_y(0).start()
    for p in (0, 1):
        along_x(p).wait_recv()
        along_y(p).wait_recv()
        total = made[dp, p].astype(jnp.float32)
        out_ref[p] = total + got_x[p].astype(jnp.float32) + got_y[p].astype(jnp.float32)
    far_x().wait_send()
    far_y().wait_send()
    for p in (0, 1):
        along_x(p).wait_send()
        along_y(p).wait_send()
    for q in order:
        visit_others(line, z, lambda other: out(q, other).wait_send())
        att_out(q).wait()


def out_sum(heads, w_out, line):
    rows = heads.shape[1]
    depth, width = w_out.shape
    quarter, half = rows // 4, rows // 8
    sems = pltpu.SemaphoreType.DMA
    dtype = heads.dtype
    anywhere, inside = pl.BlockSpec(memory_space=pl.ANY), pl.BlockSpec(memory_space=pltpu.VMEM)
    attended, total = pl.pallas_call(
        functools.partial(out_sum_kernel, line),
        out_shape=[
            jax.ShapeDtypeStruct((rows, depth), dtype),
            jax.ShapeDtypeStruct((2, half, width), jnp.float32),
        ],
        in_specs=[anywhere, inside],
        out_specs=[anywhere, inside],
        scratch_shapes=[
            pltpu.VMEM((4, quarter, depth), dtype),
            pltpu.VMEM((4, 2, half, width), dtype),
            pltpu.VMEM((2, half, width), dtype),
            pltpu.VMEM((2, half, width), dtype),
            pltpu.VMEM((half, width), dtype),
            pltpu.VMEM((half, width), dtype),
            sems((4, line)),
            sems((4, line)),
            sems((4,)),
            sems((4,)),
            sems((2, 2)),
            sems((2, 2)),
            sems((2,)),
            sems((2,)),
        ],
        compiler_params=pltpu.CompilerParams(
            collective_id=7, has_side_effects=True, vmem_limit_bytes=40 << 20
        ),
        name="out_sum",
    )(heads, w_out)
    return attended, total.reshape(quarter, width)


def out_back_kernel(
    line, x_ref, w_ref, all_ref, grad_ref, buf, grads, spread_sem, arrive_sem, own_sem, all_sem, sent, arrived, mine_sem
):
    dp, place = lax.axis_index("dp"), lax.axis_index("expert")
    z, c = place // 2, place % 2
    side_x, side_y = corners(dp)
    far = 3 - dp
    devices = ((side_x, place), (side_y, place))
    visit_others(line, z, lambda other: greet((dp, 2 * other + c)))
    for device in devices:
        greet(device)
    pl.semaphore_wait(pltpu.get_barrier_semaphore(), line + 1)
    rows = grads.shape[1]

    def spread(corner, p, way, source=None):
        target = buf.at[corner, p]
        return send(
            target if source is None else source,
            target,
            spread_sem.at[corner, p, way],
            arrive_sem.at[corner, p],
            devices[way],
        )

    def own(p):
        return pltpu.make_async_copy(x_ref.at[p], buf.at[dp, p], own_sem.at[p])

    def all_out(q):
        return pltpu.make_async_copy(buf.at[q], all_ref.at[q], all_sem.at[q])

    def block(q):
        return pl.ds(pl.multiple_of(q * rows, rows), rows)

    def out(q, other):
        device = (dp, 2 * other + c)
        source, target = grads.at[q, :, columns(other)], grad_ref.at[z, block(q)]
        return send(source, target, sent.at[q, other], arrived.at[q, z], device)

    def into(q, origin):
        part = grad_ref.at[origin, block(q)]
        return send(part, part, sent.at[q, origin], arrived.at[q, origin], devices[0])

    def mine(q):
        return pltpu.make_async_copy(
            grads.at[q, :, columns(z)], grad_ref.at[z, block(q)], mine_sem.at[q]
        )

    def product(q):
        all_out(q).start()
        value = contract(buf[q].reshape(rows, buf.shape[3]), w_ref[...], 1, 1)
        grads[q] = value.astype(grads.dtype)
        visit_others(line, z, lambda other: out(q, other).start())
        mine(q).start()

    for p in (0, 1):
        spread(dp, p, 0, x_ref.at[p]).start()
        spread(dp, 1 - p, 1, x_ref.at[1 - p]).start()
        own(p).start()
    for p in (0, 1):
        own(p).wait()
    product(dp)
    spread(side_x, 0, 0).wait_recv()
    spread(side_x, 0, 1).start()
    spread(side_y, 1, 0).wait_recv()
    spread(side_y, 1, 0).start()
    spread(side_x, 1, 0).wait_recv()
    product(side_x)
    spread(side_y, 0, 0).wait_recv()
    product(side_y)
    for p in (0, 1):
        spread(far, p, 0).wait_recv()
    product(far)
    for q in (dp, side_x, side_y, far):
        visit_others(line, z, lambda origin: into(q, origin).wait_recv())
        visit_others(line, z, lambda other: out(q, other).wait_send())
        mine(q).wait()
        all_out(q).wait()
    for p in (0, 1):
        for way in (0, 1):
            spread(dp, p, way).wait_send()
    spread(side_x, 0, 1).wait_send()
    spread(side_y, 1, 0).wait_send()


def out_back(own, w_out, line):
    quarter, width = own.shape
    depth = w_out.shape[0]
    half = quarter // 2
    sems = pltpu.SemaphoreType.DMA
    dtype = own.dtype
    anywhere, inside = pl.BlockSpec(memory_space=pl.ANY), pl.BlockSpec(memory_space=pltpu.VMEM)
    everyone, grad = pl.pallas_call(
        functools.partial(out_back_kernel, line),
        out_shape=[
            jax.ShapeDtypeStruct((4, 2, half, width), dtype),
            jax.ShapeDtypeStruct((line, 4 * quarter, HD), dtype),
        ],
        in_specs=[inside, inside],
        out_specs=[anywhere, anywhere],
        scratch_shapes=[
            pltpu.VMEM((4, 2, half, width), dtype),
            pltpu.VMEM((4, quarter, depth), dtype),
            sems((4, 2, 2)),
            sems((4, 2)),
            sems((2,)),
            sems((4,)),
            sems((4, line)),
            sems((4, line)),
            sems((4,)),
        ],
        compiler_params=pltpu.CompilerParams(
            collective_id=8, has_side_effects=True, vmem_limit_bytes=40 << 20
        ),
        name="out_back",
    )(own.reshape(2, half, width), w_out)
    return everyone.reshape(4 * quarter, width), grad


def by_head(layout, w_out, line):
    positions = layout[1][0]
    pack = positions.shape[0]
    span = pack // (2 * line)
    core = lax.axis_index("expert") % 2
    starts = (jnp.arange(pack, dtype=jnp.int32) - positions).reshape(line, 2, 1, span)
    starts = lax.dynamic_index_in_dim(starts, core, 1, keepdims=False)
    first = (2 * jnp.arange(line, dtype=jnp.int32) + core) * span
    bounds = jnp.stack(
        [starts[:, 0, 0] // KEY_TILE, (first + span - 1) // KEY_TILE + 1, first]
    ).astype(jnp.int32)

    def forward(queries, keys, values):
        q, k, v = to_heads(
            [queries, keys, values], (False, True, True), line, "scatter_heads", 6
        )
        k, v = k.reshape(pack, HD), v.reshape(pack, HD)
        out, total = attend(bounds, q, k, v, starts)
        return *out_sum(out, w_out, line), (q, k, v, out, total)

    def backward(kept, grad_own):
        q, k, v, out, total = kept
        grad_all, grad = out_back(grad_own, w_out, line)
        delta = jnp.sum(grad.astype(jnp.float32) * out.astype(jnp.float32), axis=-1)
        dq, dk, dv = attend_back(bounds, q, k, v, starts, total, delta[:, None, :], grad)
        shape = (line, 2, span, HD)
        grads = to_tokens(
            [dq, dk.reshape(shape), dv.reshape(shape)],
            (False, True, True),
            line,
            "gather_grads",
            9,
        )
        return grad_all, *grads

    return forward, backward


def by_query(layout, w_out, offset_rows):
    segment = layout[0][0]
    pack = segment.shape[0]

    def heads(rows):
        return rows.reshape(rows.shape[0], -1, HD)

    def score_block(queries, keys):
        rows = queries.shape[0]
        scores = jnp.einsum("shd,lhd->hsl", queries, keys, preferred_element_type=jnp.float32)
        own = lax.dynamic_slice_in_dim(segment, offset_rows, rows, 0)
        query_places = offset_rows + jnp.arange(rows, dtype=jnp.int32)
        key_places = jnp.arange(pack, dtype=jnp.int32)
        allowed = (own[:, None] == segment[None, :]) & (
            key_places[None, :] <= query_places[:, None]
        )
        return jnp.where(allowed[None], scores * HD ** (-0.5), masked_score)

    def forward(queries, keys, values):
        q = heads(queries)
        k = heads(lax.all_gather(keys, "expert", axis=0, tiled=True))
        v = heads(lax.all_gather(values, "expert", axis=0, tiled=True))
        scores = score_block(q, k)
        largest = jnp.max(scores, axis=-1, keepdims=True)
        total = largest + jnp.log(jnp.sum(jnp.exp(scores - largest), axis=-1, keepdims=True))
        weights = jnp.exp(scores - total).astype(jnp.bfloat16)
        attended = jnp.einsum("hsl,lhd->shd", weights, v, preferred_element_type=jnp.float32)
        attended = attended.astype(jnp.bfloat16).reshape(queries.shape)
        projected = scatter_dp(contract(attended, w_out, 1, 0).astype(jnp.bfloat16))
        return attended, projected, (q, k, v, total)

    def backward(kept, grad_own):
        q, k, v, total = kept
        grad_all = gather_dp(grad_own)
        grad = contract(grad_all, w_out, 1, 1).astype(jnp.bfloat16)
        shape = grad.shape
        grad = heads(grad)
        weights = jnp.exp(score_block(q, k) - total)
        grad_weights = jnp.einsum("shd,lhd->hsl", grad, v, preferred_element_type=jnp.float32)
        delta = jnp.sum(weights * grad_weights, axis=-1, keepdims=True)
        grad_scores = (weights * (grad_weights - delta)).astype(jnp.bfloat16)
        dq = jnp.einsum("hsl,lhd->shd", grad_scores, k, preferred_element_type=jnp.float32)
        dk = jnp.einsum("hsl,shd->lhd", grad_scores, q, preferred_element_type=jnp.float32)
        weights = weights.astype(jnp.bfloat16)
        dv = jnp.einsum("hsl,shd->lhd", weights, grad, preferred_element_type=jnp.float32)

        def to_owner(part):
            part = part.astype(jnp.bfloat16).reshape(pack, shape[1])
            return lax.psum_scatter(part, "expert", scatter_dimension=0, tiled=True)

        scale = HD ** (-0.5)
        dq = (dq * scale).reshape(shape)
        return grad_all, dq, to_owner(dk * scale), to_owner(dv)

    return forward, backward


def nearest(line, z, k):
    return ranked(line, z, k, lambda place, at: (abs(place - at), place))


def ranked(line, z, k, rank):
    total = jnp.int32(0)
    for at in range(line):
        order = sorted(range(line), key=lambda place: rank(place, at))
        place = sum([jnp.where(k == i, order[i], 0) for i in range(line)])
        total = total + jnp.where(z == at, place, 0)
    return total


def gate_act_kernel(
    line,
    x_ref,
    top_ref,
    wg_ref,
    wu_ref,
    wd_ref,
    xn_ref,
    grads_ref,
    scaled_ref,
    gates_ref,
    xbuf,
    top_buf,
    grads_buf,
    scaled_buf,
    gates_buf,
    sent,
    arrived,
    own_sem,
    top_sem,
    xn_sem,
    grads_sem,
    scaled_sem,
    gates_sem,
):
    dp, place = lax.axis_index("dp"), lax.axis_index("expert")
    z, c = place // 2, place % 2
    side_x, side_y = corners(dp)
    far = 3 - dp
    devices = (
        (dp, place + 2),
        (dp, place - 2),
        (side_x, place),
        (side_y, place),
        (dp, 2 * z + 1 - c),
    )
    up, down, along_x, along_y, pair = range(5)
    has_up, has_down = z < line - 1, z > 0
    for way in (along_x, along_y, pair):
        greet(devices[way])
    pl.when(has_up)(lambda: greet(devices[up]))
    pl.when(has_down)(lambda: greet(devices[down]))
    greeted = 3 + has_up.astype(jnp.int32) + has_down.astype(jnp.int32)
    pl.semaphore_wait(pltpu.get_barrier_semaphore(), greeted)
    local, width, units = wg_ref.shape
    rows = top_buf.shape[1]
    first = place * local

    def slot(corner, height, core):
        return corner * (2 * line) + 2 * height + core

    def copy(s, p, way, source=None):
        target = xbuf.at[s, p]
        return send(
            target if source is None else source,
            target,
            sent.at[s, p, way],
            arrived.at[s, p],
            devices[way],
        )

    def arrive(s, p):
        copy(s, p, pair).wait_recv()

    mine = slot(dp, z, c)
    for p in (0, 1):
        pltpu.make_async_copy(x_ref.at[p], xbuf.at[mine, p], own_sem.at[p]).start()
        pl.when(has_up)(lambda: copy(mine, p, up, x_ref.at[p]).start())
        pl.when(has_down)(lambda: copy(mine, p, down, x_ref.at[p]).start())
        for way in (along_x, along_y, pair):
            copy(mine, p, way, x_ref.at[p]).start()

    def decode(i):
        turn, j = i // 4, i % 4
        k = turn - (j > 0).astype(jnp.int32) - (j == 3).astype(jnp.int32)
        valid = (i >= 0) & (k >= 0) & (k < line)
        corner = jnp.where(j == 0, dp, jnp.where(j == 1, side_x, jnp.where(j == 2, side_y, far)))
        return j, k, valid, corner, nearest(line, z, k)

    def top_load(i, corner, height):
        block = corner * line + height
        return pltpu.make_async_copy(top_ref.at[block], top_buf.at[i % 2], top_sem.at[i % 2])

    def xn_out(block):
        return pltpu.make_async_copy(
            xbuf.at[pl.ds(2 * block, 2), :, :, pl.ds(0, width)],
            xn_ref.at[pl.ds(2 * block, 2)],
            xn_sem.at[block],
        )

    def grads_out(block):
        return pltpu.make_async_copy(grads_buf.at[block], grads_ref.at[block], grads_sem.at[block])

    def scaled_out(block):
        return pltpu.make_async_copy(
            scaled_buf.at[block], scaled_ref.at[block], scaled_sem.at[block]
        )

    def gates_out(block):
        return pltpu.make_async_copy(gates_buf.at[block], gates_ref.at[block], gates_sem.at[block])

    def compute(i):
        j, k, _, corner, height = decode(i)
        block = corner * line + height
        for p in (0, 1):
            arrive(slot(corner, height, 1 - c), p)
        xn_out(block).start()
        top_load(i, corner, height).wait()
        lanes = lax.broadcasted_iota(jnp.int32, (rows, 128), 1)

        def tokens():
            return xbuf[pl.ds(2 * block, 2), :, :, pl.ds(0, width)].reshape(rows, width)

        table = xbuf[pl.ds(2 * block, 2), :, :, pl.ds(width, 128)].reshape(rows, 128)
        table = table.astype(jnp.float32)
        gate_grads = jnp.zeros((rows, 128), jnp.float32)
        for e in range(local):
            at = (lanes == first + e) | (lanes == first + e + 64)
            gate = jnp.sum(jnp.where(at, table, 0.0), axis=1, keepdims=True)
            g = contract(tokens(), wg_ref[e], 1, 0)
            u = contract(tokens(), wu_ref[e], 1, 0)
            h = contract(top_buf[i % 2], wd_ref[e], 1, 1)
            sigmoid = 1.0 / (1.0 + jnp.exp(-g))
            silu = g * sigmoid
            act = silu * u
            gate_grad = jnp.sum(act * h, axis=1, keepdims=True)
            gate_grads = gate_grads + jnp.where(lanes == first + e, gate_grad, 0.0)
            grad_act = h * gate
            dg = grad_act * u * sigmoid * (1.0 + g * (1.0 - sigmoid))
            du = grad_act * silu
            scaled_buf[block, :, e * units : (e + 1) * units] = (act * gate).astype(jnp.bfloat16)
            grads_buf[block, :, e * units : (e + 1) * units] = dg.astype(jnp.bfloat16)
            at = (local + e) * units
            grads_buf[block, :, at : at + units] = du.astype(jnp.bfloat16)
        gates_buf[block] = gate_grads.astype(jnp.bfloat16)
        grads_out(block).start()
        scaled_out(block).start()
        gates_out(block).start()

    def step(i, carry):
        j, k, valid, corner, height = decode(i)
        s = slot(corner, height, c)

        def own():
            for p in (0, 1):
                pltpu.make_async_copy(x_ref.at[p], xbuf.at[mine, p], own_sem.at[p]).wait()

        def column():
            for p in (0, 1):
                arrive(s, p)
                pl.when(has_up & (height < z))(lambda: copy(s, p, up).start())
                pl.when(has_down & (height > z))(lambda: copy(s, p, down).start())
                for way in (along_x, along_y, pair):
                    copy(s, p, way).start()

        def sides():
            for p in (0, 1):
                arrive(s, p)
                copy(s, p, pair).start()
            pl.when(j == 1)(lambda: copy(s, 0, along_y).start())
            pl.when(j == 2)(lambda: copy(s, 1, along_x).start())

        def opposite():
            for p in (0, 1):
                arrive(s, p)
                copy(s, p, pair).start()

        pl.when(valid & (j == 0) & (k == 0))(own)
        pl.when(valid & (j == 0) & (k > 0))(column)
        pl.when(valid & ((j == 1) | (j == 2)))(sides)
        pl.when(valid & (j == 3))(opposite)
        pl.when(valid)(lambda: top_load(i, corner, height).start())
        pl.when(decode(i - 1)[2])(lambda: compute(i - 1))
        return carry

    lax.fori_loop(0, 4 * (line + 2) + 1, step, 0)

    def finish(height, carry):
        for p in (0, 1):
            for corner in range(4):
                copy(slot(corner, height, c), p, pair).wait_send()
            s = slot(dp, height, c)
            copy(s, p, along_x).wait_send()
            copy(s, p, along_y).wait_send()
            pl.when(has_up & (height <= z))(lambda: copy(s, p, up).wait_send())
            pl.when(has_down & (height >= z))(lambda: copy(s, p, down).wait_send())
        copy(slot(side_x, height, c), 0, along_y).wait_send()
        copy(slot(side_y, height, c), 1, along_x).wait_send()
        for corner in range(4):
            block = corner * line + height
            xn_out(block).wait()
            grads_out(block).wait()
            scaled_out(block).wait()
            gates_out(block).wait()
        return carry

    lax.fori_loop(0, line, finish, 0)


def gate_act(own, tops, w_gate, w_up, w_down, line):
    count, wide = own.shape
    local, width, units = w_gate.shape
    slots, blocks, rows, half = 8 * line, 4 * line, 2 * count, count // 2
    sems = pltpu.SemaphoreType.DMA
    dtype = own.dtype
    xn, grads, scaled, gates = pl.pallas_call(
        functools.partial(gate_act_kernel, line),
        out_shape=[
            jax.ShapeDtypeStruct((slots, 2, half, width), dtype),
            jax.ShapeDtypeStruct((blocks, rows, 2 * local * units), dtype),
            jax.ShapeDtypeStruct((blocks, rows, local * units), dtype),
            jax.ShapeDtypeStruct((blocks, rows, 128), dtype),
        ],
        in_specs=[
            pl.BlockSpec(memory_space=pltpu.VMEM),
            pl.BlockSpec(memory_space=pl.ANY),
            pl.BlockSpec(memory_space=pltpu.VMEM),
            pl.BlockSpec(memory_space=pltpu.VMEM),
            pl.BlockSpec(memory_space=pltpu.VMEM),
        ],
        out_specs=[pl.BlockSpec(memory_space=pl.ANY)] * 4,
        scratch_shapes=[
            pltpu.VMEM((slots, 2, half, wide), dtype),
            pltpu.VMEM((2, rows, width), dtype),
            pltpu.VMEM((blocks, rows, 2 * local * units), dtype),
            pltpu.VMEM((blocks, rows, local * units), dtype),
            pltpu.VMEM((blocks, rows, 128), dtype),
            sems((slots, 2, 5)),
            sems((slots, 2)),
            sems((2,)),
            sems((2,)),
            sems((blocks,)),
            sems((blocks,)),
            sems((blocks,)),
            sems((blocks,)),
        ],
        compiler_params=pltpu.CompilerParams(
            collective_id=1, has_side_effects=True, vmem_limit_bytes=60 << 20
        ),
        name="gate_act",
    )(own.reshape(2, half, wide), tops.reshape(blocks, rows, width), w_gate, w_up, w_down)
    return xn.reshape(slots * count, width), grads, scaled, gates


def column_products(left_ref, right_ref, chunk_buf, right_buf, total, chunk_sem, right_sem, store):
    span = chunk_buf.shape[2]
    blocks, rows, _ = right_buf.shape
    joined = max(1, min(blocks, 1024 // rows))
    depth = joined * rows
    turns = left_ref.shape[1] // span

    def at(n):
        return pl.ds(pl.multiple_of(n * span, span), span)

    def chunk(n):
        return pltpu.make_async_copy(
            left_ref.at[:, at(n)], chunk_buf.at[n % 2], chunk_sem.at[n % 2]
        )

    right_load = pltpu.make_async_copy(right_ref, right_buf, right_sem.at[0])
    chunk(0).start()
    right_load.start()

    def turn(n):
        pl.when(n + 1 < turns)(lambda: chunk(n + 1).start())
        chunk(n).wait()
        pl.when(n == 0)(right_load.wait)
        total[...] = jnp.zeros_like(total)

        def part(k, carry):
            left = chunk_buf[n % 2, pl.ds(pl.multiple_of(k * depth, depth), depth), :]
            right = right_buf[pl.ds(k * joined, joined)].reshape(depth, right_buf.shape[2])
            total[...] += contract(left, right, 0, 0)
            return carry

        lax.fori_loop(0, blocks // joined, part, 0)
        store(n, at(n))

    return turn, turns


def gate_up_grads(
    xn_ref, units_ref, gate_ref, up_ref, chunk_buf, units_buf, total, both, chunk_sem, units_sem, out_sem
):
    local, _, units = gate_ref.shape
    outs = (gate_ref, up_ref)

    def copies(at):
        return [
            pltpu.make_async_copy(
                both.at[:, pl.ds((kind * local + e) * units, units)],
                outs[kind].at[e, at, :],
                out_sem.at[kind, e],
            )
            for kind in (0, 1)
            for e in range(local)
        ]

    start = pl.ds(0, chunk_buf.shape[2])

    def store(n, at):
        @pl.when(n > 0)
        def _():
            for copy in copies(start):
                copy.wait()

        both[...] = total[...].astype(both.dtype)
        for copy in copies(at):
            copy.start()

    def end():
        for copy in copies(start):
            copy.wait()

    turn, turns = column_products(
        xn_ref, units_ref, chunk_buf, units_buf, total, chunk_sem, units_sem, store
    )
    return turn, end, turns


def down_grads(
    top_ref, scaled_ref, down_ref, chunk_buf, scaled_buf, total, out, chunk_sem, scaled_sem, out_sem
):
    local, units, _ = down_ref.shape

    def copies(at):
        return [
            pltpu.make_async_copy(out.at[e], down_ref.at[e, :, at], out_sem.at[e])
            for e in range(local)
        ]

    start = pl.ds(0, chunk_buf.shape[2])

    def store(n, at):
        @pl.when(n > 0)
        def _():
            for copy in copies(start):
                copy.wait()

        for e in range(local):
            out[e] = total[:, e * units : (e + 1) * units].T.astype(out.dtype)
        for copy in copies(at):
            copy.start()

    def end():
        for copy in copies(start):
            copy.wait()

    turn, turns = column_products(
        top_ref, scaled_ref, chunk_buf, scaled_buf, total, chunk_sem, scaled_sem, store
    )
    return turn, end, turns


SPAN = 256


def line_sum(
    line,
    parts_ref,
    small_ref,
    summed_ref,
    shared_ref,
    acc,
    got_pair,
    got_below,
    got_above,
    small,
    got_small,
    load_sem,
    pair_sem,
    load_small_sem,
    pair_small_sem,
    below_sem,
    above_sem,
    small_sem,
    summed_sem,
):
    dp, place = lax.axis_index("dp"), lax.axis_index("expert")
    z, c = place // 2, place % 2
    side_x, side_y = corners(dp)
    to_pair, to_up, to_down = (dp, 2 * z + 1 - c), (dp, place + 2), (dp, place - 2)
    large = parts_ref.shape[3]
    top_rows, low_rows = pl.ds(0, large), pl.ds(large, small_ref.shape[3])

    def loads(height, p):
        return (
            pltpu.make_async_copy(
                parts_ref.at[height, c, p], acc.at[height, p, top_rows], load_sem.at[height, p]
            ),
            pltpu.make_async_copy(
                small_ref.at[height, c, p], acc.at[height, p, low_rows], load_small_sem.at[height, p]
            ),
        )

    def hands(height, p):
        at = (height, p)
        return (
            send(
                parts_ref.at[height, 1 - c, p],
                got_pair.at[height, p, top_rows],
                pair_sem.at[0, *at],
                pair_sem.at[1, *at],
                to_pair,
            ),
            send(
                small_ref.at[height, 1 - c, p],
                got_pair.at[height, p, low_rows],
                pair_small_sem.at[0, *at],
                pair_small_sem.at[1, *at],
                to_pair,
            ),
        )

    def climb(height, p):
        at = (height, p)
        return send(
            acc.at[at], got_below.at[at], below_sem.at[0, *at], below_sem.at[1, *at], to_up
        )

    def descend(height, p):
        at = (height, p)
        return send(
            acc.at[at], got_above.at[at], above_sem.at[0, *at], above_sem.at[1, *at], to_down
        )

    def start(k, carry):
        height = farthest(line, z, k)
        for p in (0, 1):
            for copy in (*loads(height, p), *hands(height, p)):
                copy.start()
        return carry

    def pair_sum(k, carry):
        height = farthest(line, z, k)
        for p in (0, 1):
            for copy in loads(height, p):
                copy.wait()
            for copy in hands(height, p):
                copy.wait_recv()
            acc[height, p] = acc[height, p] + got_pair[height, p]
            pl.when((z == 0) & (height > z))(lambda: climb(height, p).start())
            pl.when((z == line - 1) & (height < z))(lambda: descend(height, p).start())
        return carry

    def pass_on(k, carry):
        height = farthest(line, z, k)
        for p in (0, 1):

            def upwards():
                climb(height, p).wait_recv()
                acc[height, p] = acc[height, p] + got_below[height, p]
                climb(height, p).start()

            def downwards():
                descend(height, p).wait_recv()
                acc[height, p] = acc[height, p] + got_above[height, p]
                descend(height, p).start()

            pl.when((height > z) & (z > 0))(upwards)
            pl.when((height < z) & (z < line - 1))(downwards)
        return carry

    def summed_out(p):
        return pltpu.make_async_copy(acc.at[z, p], summed_ref.at[p], summed_sem.at[p])

    def end():
        for p in (0, 1):

            def from_below():
                climb(z, p).wait_recv()
                acc[z, p] = acc[z, p] + got_below[z, p]

            def from_above():
                descend(z, p).wait_recv()
                acc[z, p] = acc[z, p] + got_above[z, p]

            pl.when(z > 0)(from_below)
            pl.when(z < line - 1)(from_above)
        small[0] = acc[z, :, large:, :]

        def finish(height, carry):
            for p in (0, 1):
                for copy in hands(height, p):
                    copy.wait_send()
                pl.when(height > z)(lambda: climb(height, p).wait_send())
                pl.when(height < z)(lambda: descend(height, p).wait_send())
            return carry

        lax.fori_loop(0, line, finish, 0)
        for side, device in enumerate(((side_x, place), (side_y, place))):
            exchange = send(
                small.at[side],
                got_small.at[side],
                small_sem.at[0, side],
                small_sem.at[1, side],
                device,
            )
            exchange.start()
            exchange.wait_recv()
            total = small[side].astype(jnp.float32) + got_small[side].astype(jnp.float32)
            if side == 0:
                small[1] = total.astype(small.dtype)
                for p in (0, 1):
                    summed_out(p).start()
            else:
                shared_ref[...] = total
            exchange.wait_send()
        for p in (0, 1):
            summed_out(p).wait()

    return start, pair_sum, pass_on, end


def line_sum_space(line, rows, small_rows, wide, dtype):
    high = (rows + small_rows) // 2
    sems = pltpu.SemaphoreType.DMA
    return (
        [pltpu.VMEM((line, 2, high, wide), dtype)] * 4
        + [pltpu.VMEM((2, 2, small_rows // 2, wide), dtype)] * 2
        + [sems((line, 2)), sems((2, line, 2))] * 2
        + [sems((2, line, 2))] * 2
        + [sems((2, 2)), sems((2,))]
    )


def product_sum_kernel(
    line,
    flipped,
    extra,
    grads,
    *refs,
):
    a_ref, w_ref = refs[0], refs[1]
    e_ref = refs[2] if extra else None
    refs = refs[3:] if extra else refs[2:]
    if grads:
        top_ref, parts_ref, small_ref, out_ref, down_ref, summed_ref, shared_ref = refs[:7]
        refs, work_refs, sum_refs = (out_ref, *refs[7:-21]), refs[-21:-14], refs[-14:]
    (
        out_ref,
        made,
        a_buf,
        e_buf,
        got_pair,
        got_x,
        got_y,
        got_far_x,
        got_far_y,
        got_below,
        got_above,
        load_sem,
        extra_sem,
        pair_sem,
        x_sem,
        y_sem,
        far_x_sem,
        far_y_sem,
        below_sem,
        above_sem,
    ) = refs
    dp, place = lax.axis_index("dp"), lax.axis_index("expert")
    z, c = place // 2, place % 2
    side_x, side_y = corners(dp)
    far = 3 - dp
    to_x, to_y, to_pair = (side_x, place), (side_y, place), (dp, 2 * z + 1 - c)
    to_up, to_down = (dp, place + 2), (dp, place - 2)
    for device in (to_x, to_y, to_pair):
        greet(device)
    pl.when(z > 0)(lambda: greet(to_down))
    pl.when(z < line - 1)(lambda: greet(to_up))
    greeted = 3 + (z > 0).astype(jnp.int32) + (z < line - 1).astype(jnp.int32)
    pl.semaphore_wait(pltpu.get_barrier_semaphore(), greeted)
    count = 4 * line
    width = w_ref.shape[0] if flipped else w_ref.shape[1]
    half = made.shape[4]
    chunk = 512

    def mine(q, height, p):
        return made.at[q, height, c, p]

    def hand(q, height, p):
        at = (q, height, p)
        source = made.at[q, height, 1 - c, p]
        return send(source, got_pair.at[at], pair_sem.at[0, *at], pair_sem.at[1, *at], to_pair)

    def along_x(height, p):
        at = (height, p)
        source = mine(side_x, height, p)
        return send(source, got_x.at[at], x_sem.at[0, *at], x_sem.at[1, *at], to_x)

    def along_y(height, p):
        at = (height, p)
        source = mine(side_y, height, p)
        return send(source, got_y.at[at], y_sem.at[0, *at], y_sem.at[1, *at], to_y)

    def far_x(height):
        source = mine(far, height, 0)
        return send(
            source, got_far_x.at[height], far_x_sem.at[0, height], far_x_sem.at[1, height], to_x
        )

    def far_y(height):
        source = mine(far, height, 1)
        return send(
            source, got_far_y.at[height], far_y_sem.at[0, height], far_y_sem.at[1, height], to_y
        )

    def climb(height, p):
        at = (height, p)
        source = mine(dp, height, p)
        return send(source, got_below.at[at], below_sem.at[0, *at], below_sem.at[1, *at], to_up)

    def descend(height, p):
        at = (height, p)
        source = mine(dp, height, p)
        return send(source, got_above.at[at], above_sem.at[0, *at], above_sem.at[1, *at], to_down)

    def decode(i):
        k, j = i // 4, i % 4
        q = jnp.where(j == 0, far, jnp.where(j == 1, side_x, jnp.where(j == 2, side_y, dp)))
        return k, j, q, farthest(line, z, k)

    def load(i):
        _, _, q, height = decode(i)
        return pltpu.make_async_copy(
            a_ref.at[q * line + height], a_buf.at[i % 2], load_sem.at[i % 2]
        )

    def load_extra(i):
        _, _, q, height = decode(i)
        return pltpu.make_async_copy(
            e_ref.at[q * line + height], e_buf.at[i % 2], extra_sem.at[i % 2]
        )

    def start_load(i):
        load(i).start()
        if extra:
            load_extra(i).start()

    def add(q, height, p, other):
        at = (q, height, c, p)
        made[at] = made[at] + other[...]

    def compute(i):
        _, _, q, height = decode(i)
        load(i).wait()
        if extra:
            load_extra(i).wait()
        pl.when(i + 1 < count)(lambda: start_load(i + 1))
        for at in range(0, width, chunk):
            if flipped:
                part = contract(a_buf[i % 2], w_ref[at : at + chunk, :], 1, 1)
            else:
                part = contract(a_buf[i % 2], w_ref[:, at : at + chunk], 1, 0)
            part = part.astype(made.dtype).reshape(2, 2, half, chunk)
            made[q, height, :, :, :, at : at + chunk] = part
        if extra:
            made[q, height, :, :, :, width : width + 128] = e_buf[i % 2].reshape(2, 2, half, 128)
        for p in (0, 1):
            hand(q, height, p).start()

    def settle(i):
        _, j, q, height = decode(i)
        for p in (0, 1):
            hand(q, height, p).wait_recv()
            add(q, height, p, got_pair.at[q, height, p])

        def opposite():
            far_x(height).start()
            far_y(height).start()

        pl.when(j == 0)(opposite)
        pl.when(j == 1)(lambda: along_x(height, 0).start())
        pl.when(j == 2)(lambda: along_y(height, 1).start())

    def settle_far(i):
        _, j, _, height = decode(i)

        def side_of_x():
            far_y(height).wait_recv()
            add(side_x, height, 1, got_far_y.at[height])
            along_x(height, 1).start()

        def side_of_y():
            far_x(height).wait_recv()
            add(side_y, height, 0, got_far_x.at[height])
            along_y(height, 0).start()

        pl.when(j == 1)(side_of_x)
        pl.when(j == 2)(side_of_y)

    def column(height):
        for p in (0, 1):
            along_x(height, p).wait_recv()
            along_y(height, p).wait_recv()
            total = made[dp, height, c, p].astype(jnp.float32)
            total = total + got_x[height, p].astype(jnp.float32)
            total = total + got_y[height, p].astype(jnp.float32)
            made[dp, height, c, p] = total.astype(made.dtype)
            pl.when((z == 0) & (height > z))(lambda: climb(height, p).start())
            pl.when((z == line - 1) & (height < z))(lambda: descend(height, p).start())

    def pass_on(height):
        for p in (0, 1):

            def upwards():
                climb(height, p).wait_recv()
                add(dp, height, p, got_below.at[height, p])
                climb(height, p).start()

            def downwards():
                descend(height, p).wait_recv()
                add(dp, height, p, got_above.at[height, p])
                descend(height, p).start()

            pl.when((height > z) & (z > 0))(upwards)
            pl.when((height < z) & (z < line - 1))(downwards)

    start_load(0)
    if grads:
        work, work_end, turns = down_grads(top_ref, a_ref, down_ref, *work_refs)
        line_start, line_pair, line_pass, line_end = line_sum(
            line, parts_ref, small_ref, summed_ref, shared_ref, *sum_refs
        )
        lax.fori_loop(0, line, line_start, 0)

    def step(i, carry):
        k, j, _, _ = decode(i)
        pl.when(i < count)(lambda: compute(i))
        pl.when((i >= 1) & (i <= count))(lambda: settle(i - 1))
        if grads:
            every = count // turns
            pl.when((i < count) & (i % every == 0))(lambda: work(i // every))

            @pl.when(i < line)
            def _():
                line_pair(i, 0)

            @pl.when((i >= 6) & (i % 4 == 2) & (i < 6 + 4 * line))
            def _():
                line_pass((i - 6) // 4, 0)

        pl.when((i >= 4) & (i < count + 4))(lambda: settle_far(i - 4))
        pl.when((k >= 3) & (j == 2))(lambda: pass_on(farthest(line, z, k - 3)))
        pl.when((k >= 2) & (j == 3))(lambda: column(farthest(line, z, k - 2)))
        return carry

    lax.fori_loop(0, count + 8, step, 0)
    if grads:
        line_end()
        work_end()
    for p in (0, 1):
        out_ref[p] = made[dp, z, c, p].astype(jnp.float32)

        def from_below():
            climb(z, p).wait_recv()
            out_ref[p] = out_ref[p] + got_below[z, p].astype(jnp.float32)

        def from_above():
            descend(z, p).wait_recv()
            out_ref[p] = out_ref[p] + got_above[z, p].astype(jnp.float32)

        pl.when(z > 0)(from_below)
        pl.when(z < line - 1)(from_above)

    def finish(height, carry):
        far_x(height).wait_send()
        far_y(height).wait_send()
        for p in (0, 1):
            for q in range(4):
                hand(q, height, p).wait_send()
            along_x(height, p).wait_send()
            along_y(height, p).wait_send()
            pl.when(height > z)(lambda: climb(height, p).wait_send())
            pl.when(height < z)(lambda: descend(height, p).wait_send())
        return carry

    lax.fori_loop(0, line, finish, 0)


def product_sum(blocks, weights, flipped, extra, line, name, number, grads=None):
    count, rows, depth = blocks.shape
    width = weights.shape[0] if flipped else weights.shape[1]
    wide = width + (0 if extra is None else 128)
    half = rows // 4
    sems = pltpu.SemaphoreType.DMA
    dtype = blocks.dtype

    def space(*shape):
        return pltpu.VMEM((*shape, half, wide), dtype)

    anywhere, inside = pl.BlockSpec(memory_space=pl.ANY), pl.BlockSpec(memory_space=pltpu.VMEM)
    out_shape = [jax.ShapeDtypeStruct((2, half, wide), jnp.float32)]
    work_in, work_space = [], []
    if grads is not None:
        tops, parts, small, shape = grads
        local, units, _ = shape
        _, large, wider = parts.shape
        small_rows = small.shape[1]
        span = SPAN if large >= 8 * small_rows else SPAN // 2
        work_in = [
            tops,
            parts.reshape(line, 2, 2, large // 2, wider),
            small.reshape(line, 2, 2, small_rows // 2, wider),
        ]
        out_shape += [
            jax.ShapeDtypeStruct(shape, dtype),
            jax.ShapeDtypeStruct((2, (large + small_rows) // 2, wider), dtype),
            jax.ShapeDtypeStruct((2, small_rows // 2, wider), jnp.float32),
        ]
        work_space = [
            pltpu.VMEM((2, tops.shape[0], span), dtype),
            pltpu.VMEM(blocks.shape, dtype),
            pltpu.VMEM((span, local * units), jnp.float32),
            pltpu.VMEM((local, units, span), dtype),
            sems((2,)),
            sems((1,)),
            sems((local,)),
            *line_sum_space(line, large, small_rows, wider, dtype),
        ]
    total, *work_out = pl.pallas_call(
        functools.partial(product_sum_kernel, line, flipped, extra is not None, grads is not None),
        out_shape=out_shape,
        in_specs=[anywhere, inside]
        + ([] if extra is None else [anywhere])
        + [anywhere] * len(work_in),
        out_specs=[inside] + ([] if grads is None else [anywhere, anywhere, inside]),
        scratch_shapes=[
            space(4, line, 2, 2),
            pltpu.VMEM((2, rows, depth), dtype),
            pltpu.VMEM((2, rows, 128), dtype),
            space(4, line, 2),
            space(line, 2),
            space(line, 2),
            space(line),
            space(line),
            space(line, 2),
            space(line, 2),
            sems((2,)),
            sems((2,)),
            sems((2, 4, line, 2)),
            sems((2, line, 2)),
            sems((2, line, 2)),
            sems((2, line)),
            sems((2, line)),
            sems((2, line, 2)),
            sems((2, line, 2)),
            *work_space,
        ],
        compiler_params=pltpu.CompilerParams(
            collective_id=number, has_side_effects=True, vmem_limit_bytes=63 << 20
        ),
        name=name,
    )(blocks, weights, *([] if extra is None else [extra]), *work_in)
    return total.reshape(2 * half, wide), *work_out


def closing_kernel(
    first_ref,
    grad_ref,
    unit_ref,
    inverse_ref,
    gain_ref,
    output_ref,
    xn_ref,
    units_ref,
    outputs_ref,
    grads_ref,
    gate_ref,
    up_ref,
    part,
    got_x,
    got_y,
    got_far_x,
    got_far_y,
    grad_own,
    part_sem,
    x_sem,
    y_sem,
    far_x_sem,
    far_y_sem,
    spread_sem,
    arrive_sem,
    own_sem,
    *work_refs,
):
    dp, place = lax.axis_index("dp"), lax.axis_index("expert")
    side_x, side_y = corners(dp)
    far = 3 - dp
    to_x, to_y = meet_square(dp, place)

    def first_load(q, p):
        return pltpu.make_async_copy(first_ref.at[q, p], part.at[q, p], part_sem.at[q, p])

    def along_x(p):
        return send(part.at[side_x, p], got_x.at[p], x_sem.at[0, p], x_sem.at[1, p], to_x)

    def along_y(p):
        return send(part.at[side_y, p], got_y.at[p], y_sem.at[0, p], y_sem.at[1, p], to_y)

    def far_x():
        return send(part.at[far, 0], got_far_x, far_x_sem.at[0], far_x_sem.at[1], to_x)

    def far_y():
        return send(part.at[far, 1], got_far_y, far_y_sem.at[0], far_y_sem.at[1], to_y)

    spreads = ((output_ref, outputs_ref), (grad_own, grads_ref))

    def spread(a, corner, p, way, source=None):
        target = spreads[a][1].at[corner, p]
        return send(
            target if source is None else source,
            target,
            spread_sem.at[a, corner, p, way],
            arrive_sem.at[a, corner, p],
            (to_x, to_y)[way],
        )

    def own_copy(a, p):
        return pltpu.make_async_copy(
            spreads[a][0].at[p], spreads[a][1].at[dp, p], own_sem.at[a, p]
        )

    def spread_own(a, p):
        own_copy(a, p).start()
        for way in (0, 1):
            spread(a, dp, p, way, spreads[a][0].at[p]).start()

    def spread_far(a):
        spread(a, side_x, 0, 0).wait_recv()
        spread(a, side_x, 0, 1).start()
        spread(a, side_y, 1, 0).wait_recv()
        spread(a, side_y, 1, 0).start()

    work, work_end, turns = gate_up_grads(xn_ref, units_ref, gate_ref, up_ref, *work_refs)
    pauses = 4

    def meanwhile(i):
        def turn(n, carry):
            work(n)
            return carry

        lax.fori_loop(turns * i // pauses, turns * (i + 1) // pauses, turn, 0)

    for q in (far, side_x, side_y, dp):
        for p in (0, 1):
            first_load(q, p).start()
    for q in (far, side_x, side_y, dp):
        for p in (0, 1):
            first_load(q, p).wait()
    far_x().start()
    far_y().start()
    along_x(0).start()
    along_y(1).start()
    for p in (0, 1):
        spread_own(0, p)
    far_x().wait_recv()
    part[side_y, 0] = part[side_y, 0] + got_far_x[...]
    along_y(0).start()
    far_y().wait_recv()
    part[side_x, 1] = part[side_x, 1] + got_far_y[...]
    along_x(1).start()
    meanwhile(0)
    spread_far(0)
    for p in (0, 1):
        along_x(p).wait_recv()
        along_y(p).wait_recv()
        total = part[dp, p].astype(jnp.float32)
        total = total + got_x[p].astype(jnp.float32) + got_y[p].astype(jnp.float32)
        total = total * gain_ref[...]
        unit = unit_ref[p]
        mean = jnp.sum(total * unit, axis=1, keepdims=True) * (1.0 / unit.shape[1])
        rows = grad_ref[p] + inverse_ref[p] * (total - unit * mean)
        grad_own[p] = rows.astype(grad_own.dtype)
        spread_own(1, p)
    meanwhile(1)
    meanwhile(2)
    spread_far(1)
    meanwhile(3)
    for a in (0, 1):
        spread(a, side_x, 1, 0).wait_recv()
        spread(a, side_y, 0, 0).wait_recv()
        for p in (0, 1):
            spread(a, far, p, 0).wait_recv()
            for way in (0, 1):
                spread(a, dp, p, way).wait_send()
            own_copy(a, p).wait()
        spread(a, side_x, 0, 1).wait_send()
        spread(a, side_y, 1, 0).wait_send()
    far_x().wait_send()
    far_y().wait_send()
    for p in (0, 1):
        along_x(p).wait_send()
        along_y(p).wait_send()
    work_end()


def closing(first, grad, unit, inverse, gain, output, xn, units, shape):
    own, width = output.shape
    half = own // 2
    sems = pltpu.SemaphoreType.DMA
    dtype = output.dtype
    anywhere, inside = pl.BlockSpec(memory_space=pl.ANY), pl.BlockSpec(memory_space=pltpu.VMEM)
    everyone = jax.ShapeDtypeStruct((4, 2, half, width), dtype)
    weight = jax.ShapeDtypeStruct(shape, dtype)
    outputs, grads, gate, up = pl.pallas_call(
        closing_kernel,
        out_shape=[everyone, everyone, weight, weight],
        in_specs=[anywhere] + [inside] * 5 + [anywhere] * 2,
        out_specs=[anywhere] * 4,
        scratch_shapes=[
            pltpu.VMEM((4, 2, half, width), dtype),
            pltpu.VMEM((2, half, width), dtype),
            pltpu.VMEM((2, half, width), dtype),
            pltpu.VMEM((half, width), dtype),
            pltpu.VMEM((half, width), dtype),
            pltpu.VMEM((2, half, width), dtype),
            sems((4, 2)),
            sems((2, 2)),
            sems((2, 2)),
            sems((2,)),
            sems((2,)),
            sems((2, 4, 2, 2)),
            sems((2, 4, 2)),
            sems((2, 2)),
            pltpu.VMEM((2, xn.shape[0], SPAN), dtype),
            pltpu.VMEM(units.shape, dtype),
            pltpu.VMEM((SPAN, units.shape[2]), jnp.float32),
            pltpu.VMEM((SPAN, units.shape[2]), dtype),
            sems((2,)),
            sems((1,)),
            sems((2, shape[0])),
        ],
        compiler_params=pltpu.CompilerParams(
            collective_id=5, has_side_effects=True, vmem_limit_bytes=60 << 20
        ),
        name="closing",
    )(
        first.reshape(4, 2, half, width),
        grad.reshape(2, half, width),
        unit.reshape(2, half, width),
        inverse.reshape(2, half, 1),
        gain.reshape(1, width),
        output.reshape(2, half, width),
        xn,
        units,
    )
    return outputs.reshape(4 * own, width), grads.reshape(4 * own, width), gate, up


def square_sum(values, got, sem, side, device):
    copy = send(values.at[side], got.at[side], sem.at[0, side], sem.at[1, side], device)
    copy.start()
    copy.wait()
    return values[side] + got[side]


def as_rows(column):
    return jnp.broadcast_to(column, (column.shape[0], 128)).T[:8]


def as_column(rows):
    return jnp.broadcast_to(rows[:1], (128, rows.shape[1])).T[:, :1]


def meet_square(dp, place):
    side_x, side_y = corners(dp)
    devices = ((side_x, place), (side_y, place))
    for device in devices:
        greet(device)
    pl.semaphore_wait(pltpu.get_barrier_semaphore(), 2)
    return devices


def normed_heads_kernel(
    model_width, q_ref, k_ref, q_gain, k_gain, cos_ref, sin_ref, queries, keys, inverse, sums, got, sem
):
    devices = meet_square(lax.axis_index("dp"), lax.axis_index("expert"))
    raws, gains, outs = (q_ref, k_ref), (q_gain, k_gain), (queries, keys)
    for i, raw in enumerate(raws):
        total = jnp.sum(raw[...] * raw[...], axis=1, keepdims=True)
        sums[0, 8 * i : 8 * i + 8] = as_rows(total)
    sums[1] = square_sum(sums, got, sem, 0, devices[0])
    total = square_sum(sums, got, sem, 1, devices[1])
    inverse[...] = lax.rsqrt(total * (1.0 / model_width) + epsilon)
    for i, raw in enumerate(raws):
        scale = as_column(inverse[8 * i : 8 * i + 8])
        for at in range(0, raw.shape[1], HD):
            head = raw[:, at : at + HD] * scale * gains[i][:, at : at + HD]
            turned = head * cos_ref[...] + pltpu.roll(head, HD // 2, 1) * sin_ref[...]
            outs[i][:, at : at + HD] = turned.astype(outs[i].dtype)


def normed_heads(q_raw, k_raw, q_gain, k_gain, cos, sin, model_width):
    rows, width = q_raw.shape
    head = jax.ShapeDtypeStruct((rows, width), jnp.bfloat16)
    return pl.pallas_call(
        functools.partial(normed_heads_kernel, model_width),
        out_shape=[head, head, jax.ShapeDtypeStruct((16, rows), jnp.float32)],
        in_specs=[pl.BlockSpec(memory_space=pltpu.VMEM)] * 6,
        out_specs=[pl.BlockSpec(memory_space=pltpu.VMEM)] * 3,
        scratch_shapes=[
            pltpu.VMEM((2, 16, rows), jnp.float32),
            pltpu.VMEM((2, 16, rows), jnp.float32),
            pltpu.SemaphoreType.DMA((2, 2)),
        ],
        compiler_params=pltpu.CompilerParams(
            collective_id=11, has_side_effects=True, vmem_limit_bytes=40 << 20
        ),
        name="normed_heads",
    )(q_raw, k_raw, q_gain.reshape(1, width), k_gain.reshape(1, width), cos, sin)


def normed_heads_back_kernel(
    model_width,
    dq_ref,
    dk_ref,
    dv_ref,
    q_ref,
    k_ref,
    q_gain,
    k_gain,
    cos_ref,
    sin_ref,
    inverse,
    grads,
    gain_grads,
    sums,
    got,
    sem,
):
    devices = meet_square(lax.axis_index("dp"), lax.axis_index("expert"))
    raws, gains, news = (q_ref, k_ref), (q_gain, k_gain), (dq_ref, dk_ref)
    rows, width = q_ref.shape

    def parts(i, at):
        cut = slice(at, at + HD)
        new = news[i][:, cut].astype(jnp.float32)
        back = new * cos_ref[...] - pltpu.roll(new, HD // 2, 1) * sin_ref[...]
        unit = raws[i][:, cut] * as_column(inverse[8 * i : 8 * i + 8])
        return back, unit, back * gains[i][:, cut]

    for i in (0, 1):
        total = jnp.zeros((rows, 1), jnp.float32)
        for at in range(0, width, HD):
            back, unit, scaled = parts(i, at)
            gain_grad = jnp.sum(back * unit, axis=0, keepdims=True)
            gain_grads[8 * i : 8 * i + 8, at : at + HD] = jnp.broadcast_to(gain_grad, (8, HD))
            total = total + jnp.sum(scaled * unit, axis=1, keepdims=True)
        sums[0, 8 * i : 8 * i + 8] = as_rows(total)
    sums[1] = square_sum(sums, got, sem, 0, devices[0])
    dots = square_sum(sums, got, sem, 1, devices[1]) * (1.0 / model_width)
    for i in (0, 1):
        dot = as_column(dots[8 * i : 8 * i + 8])
        scale = as_column(inverse[8 * i : 8 * i + 8])
        for at in range(0, width, HD):
            _, unit, scaled = parts(i, at)
            value = scale * (scaled - unit * dot)
            grads[:, i * width + at : i * width + at + HD] = value.astype(grads.dtype)
    grads[:, 2 * width :] = dv_ref[...]


def normed_heads_back(dq, dk, dv, q_raw, k_raw, q_gain, k_gain, cos, sin, inverse, model_width):
    rows, width = q_raw.shape
    return pl.pallas_call(
        functools.partial(normed_heads_back_kernel, model_width),
        out_shape=[
            jax.ShapeDtypeStruct((rows, 3 * width), jnp.bfloat16),
            jax.ShapeDtypeStruct((16, width), jnp.float32),
        ],
        in_specs=[pl.BlockSpec(memory_space=pltpu.VMEM)] * 10,
        out_specs=[pl.BlockSpec(memory_space=pltpu.VMEM)] * 2,
        scratch_shapes=[
            pltpu.VMEM((2, 16, rows), jnp.float32),
            pltpu.VMEM((2, 16, rows), jnp.float32),
            pltpu.SemaphoreType.DMA((2, 2)),
        ],
        compiler_params=pltpu.CompilerParams(
            collective_id=12, has_side_effects=True, vmem_limit_bytes=40 << 20
        ),
        name="normed_heads_back",
    )(
        dq,
        dk,
        dv,
        q_raw,
        k_raw,
        q_gain.reshape(1, width),
        k_gain.reshape(1, width),
        cos,
        sin,
        inverse,
    )


def per_device(
    inputs,
    attention_norm_gain,
    w_query,
    w_key,
    w_value,
    w_out,
    q_gain,
    k_gain,
    expert_norm_gain,
    w_router,
    w_gate,
    w_up,
    w_down,
    routes,
    lengths,
    d_output,
):
    pack_count, seg_rows, model_width = inputs.shape
    local_width = w_query.shape[1]
    local_heads = local_width // HD
    experts = w_router.shape[1]
    groups = lax.axis_size("expert")
    line = groups // 2
    pack_span = seg_rows * groups
    local_experts = w_gate.shape[0]
    offset_rows = lax.axis_index("expert") * seg_rows
    segment, positions = doc_layout(lengths, pack_span)
    pos_query = lax.dynamic_slice_in_dim(positions, offset_rows, seg_rows, 1)
    cos_table, sin_table = rope_tables(pos_query[0], HD)
    inputs_single_float = inputs.astype(jnp.float32)
    first_inverse_norm = lax.rsqrt(
        jnp.mean(inputs_single_float * inputs_single_float, axis=-1, keepdims=True) + epsilon
    )
    first_unit_input = inputs_single_float * first_inverse_norm
    first_normed_input = (first_unit_input * attention_norm_gain).astype(jnp.bfloat16)
    q_raw = jnp.dot(first_normed_input[0], w_query, preferred_element_type=jnp.float32)
    k_raw = jnp.dot(first_normed_input[0], w_key, preferred_element_type=jnp.float32)
    value_rows = jnp.dot(first_normed_input[0], w_value, preferred_element_type=jnp.float32).astype(
        jnp.bfloat16
    )
    queries, keys, head_inverse = normed_heads(
        q_raw, k_raw, q_gain, k_gain, cos_table, sin_table, model_width
    )
    layout = (segment, positions)
    if local_heads == line:
        attention = by_head(layout, w_out, line)
    else:
        attention = by_query(layout, w_out, offset_rows)
    attended, projected, kept = attention[0](queries, keys, value_rows)
    own = lax.axis_index("dp")
    part_rows = seg_rows // lax.axis_size("dp")

    def own_rows(rows):
        return lax.dynamic_slice_in_dim(rows, own * part_rows, part_rows, 0)

    hidden_state = own_rows(inputs_single_float[0]) + projected
    second_inverse_norm = lax.rsqrt(
        jnp.mean(hidden_state * hidden_state, axis=-1, keepdims=True) + epsilon
    )
    second_unit_input = hidden_state * second_inverse_norm
    second_normed_input = second_unit_input * expert_norm_gain
    router = jax.nn.softmax(
        jnp.dot(second_normed_input, w_router, precision=lax.Precision.HIGHEST), axis=-1
    )
    chosen = own_rows(routes[:, 0, :])
    expert_range = jnp.arange(experts, dtype=jnp.int32)
    named = jnp.any(chosen[:, :, None] == expert_range, axis=1)
    top_own = own_rows(d_output[0])
    top_all = lax.all_gather(top_own, ALL, axis=0, tiled=True)
    gate_table = jnp.where(named, router, 0.0)
    gate_high = gate_table.astype(jnp.bfloat16)
    gate_low = (gate_table - gate_high.astype(jnp.float32)).astype(jnp.bfloat16)
    widen = ((0, 0), (0, 64 - experts))
    own_tokens = jnp.concatenate(
        [
            second_normed_input.astype(jnp.bfloat16),
            jnp.pad(gate_high, widen),
            jnp.pad(gate_low, widen),
        ],
        axis=1,
    )
    xn_all, grad_units, scaled, gate_part = gate_act(
        own_tokens, top_all, w_gate, w_up, w_down, line
    )
    w_both = jnp.concatenate([*w_gate, *w_up], axis=1)
    (grad_tokens,) = product_sum(grad_units, w_both, True, gate_part, line, "grad_tokens", 4)
    grad_xn_exp = grad_tokens[:, :model_width]
    gate_sums = grad_tokens[:, model_width : model_width + experts]
    grad_router_probs = jnp.where(named, gate_sums, 0.0)
    grad_logits = router * (
        grad_router_probs - jnp.sum(router * grad_router_probs, axis=-1, keepdims=True)
    )
    grad_second_normed_input = grad_xn_exp + jnp.einsum(
        "se,de->sd", grad_logits, w_router, precision=lax.Precision.HIGHEST
    )
    grad_router = jnp.einsum(
        "sd,se->de", second_normed_input, grad_logits, precision=lax.Precision.HIGHEST
    )
    grad_expert_norm_gain = jnp.sum(grad_second_normed_input * second_unit_input, axis=0)
    grad_second_unit_input = grad_second_normed_input * expert_norm_gain
    grad_hidden = top_own.astype(jnp.float32) + second_inverse_norm * (
        grad_second_unit_input
        - second_unit_input
        * jnp.mean(grad_second_unit_input * second_unit_input, axis=-1, keepdims=True)
    )
    grad_attn, grad_queries, grad_keys, grad_values = attention[1](
        kept, grad_hidden.astype(jnp.bfloat16)
    )
    grad_out = jnp.einsum("sk,sd->kd", attended, grad_attn, preferred_element_type=jnp.float32)
    grad_heads_raw, gain_grads = normed_heads_back(
        grad_queries.astype(jnp.bfloat16),
        grad_keys,
        grad_values,
        q_raw,
        k_raw,
        q_gain,
        k_gain,
        cos_table,
        sin_table,
        head_inverse,
        model_width,
    )
    grad_q_gain, grad_k_gain = gain_grads[0], gain_grads[8]
    grad_projections = jnp.einsum(
        "sd,sk->dk", first_normed_input[0], grad_heads_raw, preferred_element_type=jnp.float32
    )
    grad_first_normed_input = sum(
        contract(grad_heads_raw[:, i * local_width : (i + 1) * local_width], weight, 1, 1)
        for i, weight in enumerate((w_query, w_key, w_value))
    )
    grad_attn_gain = jnp.sum(grad_first_normed_input * first_unit_input[0], axis=0)
    wide = grad_projections.shape[1]
    small = jnp.concatenate(
        [
            grad_q_gain.reshape(groups, -1),
            grad_k_gain.reshape(groups, -1),
            grad_attn_gain.reshape(groups, -1),
            grad_expert_norm_gain.reshape(groups, -1),
            grad_router.reshape(groups, -1),
        ],
        axis=1,
    )
    small_rows = 32
    filled = small.shape[1]
    small = jnp.pad(small, ((0, 0), (0, small_rows * wide - filled)))
    moe_out, grad_down, summed, shared = product_sum(
        scaled,
        w_down.reshape(-1, model_width),
        False,
        None,
        line,
        "expert_sum",
        2,
        (
            top_all,
            grad_projections.astype(jnp.bfloat16).reshape(groups, -1, wide),
            small.astype(jnp.bfloat16).reshape(groups, small_rows, wide),
            w_down.shape,
        ),
    )
    large = summed.shape[1] - small_rows // 2
    own_small = summed[:, large:].astype(jnp.float32)
    summed = summed[:, :large].reshape(2 * large, wide).astype(jnp.float32)
    output = (hidden_state + moe_out).astype(jnp.bfloat16)
    outputs, grad_input, grad_gate, grad_up = closing(
        grad_first_normed_input.astype(jnp.bfloat16),
        grad_hidden,
        own_rows(first_unit_input[0]),
        own_rows(first_inverse_norm[0]),
        attention_norm_gain,
        output,
        xn_all,
        grad_units,
        w_gate.shape,
    )
    gain_size, norm_size = local_width // groups, model_width // groups
    own_gains = own_small.reshape(-1)[: 2 * gain_size]
    shared = shared.reshape(-1)[2 * gain_size : filled]
    grad_out = lax.psum_scatter(
        grad_out.astype(jnp.bfloat16), "expert", scatter_dimension=0, tiled=True
    ).astype(jnp.float32)
    return (
        outputs[None],
        grad_input.astype(jnp.float32)[None],
        shared[:norm_size],
        summed[:, :local_width],
        summed[:, local_width : 2 * local_width],
        summed[:, 2 * local_width :],
        grad_out,
        own_gains[:gain_size],
        own_gains[gain_size:],
        shared[norm_size : 2 * norm_size],
        shared[2 * norm_size :].reshape(norm_size, experts),
        grad_gate.astype(jnp.float32),
        grad_up.astype(jnp.float32),
        grad_down.astype(jnp.float32),
    )


def solution(mesh):
    placed = (
        P(None, "expert", None),
        P(),
        P(None, "dp"),
        P(None, "dp"),
        P(None, "dp"),
        P("dp", None),
        P("dp"),
        P("dp"),
        P(),
        P(),
        P("expert", None, "dp"),
        P("expert", None, "dp"),
        P("expert", "dp", None),
        P("expert", None, None),
        P(),
        P(None, "expert", None),
    )
    return jax.shard_map(
        per_device,
        mesh=mesh,
        in_specs=placed,
        out_specs=(
            P(None, "expert", None),
            P(None, "expert", None),
            P("expert"),
            P("expert", "dp"),
            P("expert", "dp"),
            P("expert", "dp"),
            P(("dp", "expert"), None),
            P(("dp", "expert")),
            P(("dp", "expert")),
            P("expert"),
            P("expert", None),
            P("expert", None, "dp"),
            P("expert", None, "dp"),
            P("expert", "dp", None),
        ),
        check_vma=False,
    )
```

```python
import functools

import jax
import jax.numpy as jnp
from jax import lax
from jax.experimental import pallas as pl
from jax.experimental.pallas import tpu as pltpu
from jax.sharding import PartitionSpec as P

HD = 128


epsilon = 1e-05
rope_base = 10000.0
masked_score = -1e30


def doc_layout(lengths, pack_span):
    doc_ends = jnp.cumsum(lengths, axis=1)
    starts = doc_ends - lengths
    places = jnp.arange(pack_span, dtype=jnp.int32)
    segment = jnp.sum((places[None, :, None] >= doc_ends[:, None, :]).astype(jnp.int32), axis=2)
    member = segment[:, :, None] == jnp.arange(lengths.shape[1], dtype=jnp.int32)[None, None, :]
    begins = jnp.sum(jnp.where(member, starts[:, None, :], 0), axis=2)
    return (segment, places[None, :] - begins)


def rope_tables(positions, head_size):
    half_size = head_size // 2
    frequency = rope_base ** (-2.0 * jnp.arange(half_size, dtype=jnp.float32) / head_size)
    angles = positions.astype(jnp.float32)[..., None] * frequency
    cos, sin = jnp.cos(angles), jnp.sin(angles)
    return jnp.concatenate([cos, cos], axis=-1), jnp.concatenate([-sin, sin], axis=-1)


ALL = ("dp", "expert")


DEVICES = pl.DeviceIdType.MESH


def greet(device):
    pl.semaphore_signal(
        pltpu.get_barrier_semaphore(), inc=1, device_id=device, device_id_type=DEVICES
    )


def send(source, target, send_sem, arrive_sem, device):
    return pltpu.make_async_remote_copy(
        src_ref=source,
        dst_ref=target,
        send_sem=send_sem,
        recv_sem=arrive_sem,
        device_id=device,
        device_id_type=DEVICES,
    )


def contract(a, b, a_dim, b_dim):
    return lax.dot_general(
        a, b, (((a_dim,), (b_dim,)), ((), ())), preferred_element_type=jnp.float32
    )


def corners(dp):
    return dp + 1 - 2 * (dp % 2), (dp + 2) % 4


def gather_square_kernel(x_ref, out_ref, sent, arrived, own_sem):
    dp, place = lax.axis_index("dp"), lax.axis_index("expert")
    side_x, side_y = corners(dp)
    devices = ((side_x, place), (side_y, place))
    for device in devices:
        greet(device)
    pl.semaphore_wait(pltpu.get_barrier_semaphore(), 2)

    def copy(corner, p, way, source=None):
        target = out_ref.at[corner, p]
        return send(
            target if source is None else source,
            target,
            sent.at[corner, p, way],
            arrived.at[corner, p],
            devices[way],
        )

    for p in (0, 1):
        pltpu.make_async_copy(x_ref.at[p], out_ref.at[dp, p], own_sem.at[p]).start()
        for way in (0, 1):
            copy(dp, p, way, x_ref.at[p]).start()
    copy(side_x, 0, 0).wait_recv()
    copy(side_x, 0, 1).start()
    copy(side_y, 0, 0).wait_recv()
    copy(side_x, 1, 0).wait_recv()
    copy(side_y, 1, 0).wait_recv()
    copy(side_y, 1, 0).start()
    for p in (0, 1):
        copy(3 - dp, p, 0).wait_recv()
        for way in (0, 1):
            copy(dp, p, way).wait_send()
        pltpu.make_async_copy(x_ref.at[p], out_ref.at[dp, p], own_sem.at[p]).wait()
    copy(side_x, 0, 1).wait_send()
    copy(side_y, 1, 0).wait_send()


def gather_dp(rows):
    count, width = rows.shape
    gathered = pl.pallas_call(
        gather_square_kernel,
        out_shape=jax.ShapeDtypeStruct((4, 2, count // 2, width), rows.dtype),
        in_specs=[pl.BlockSpec(memory_space=pltpu.VMEM)],
        out_specs=pl.BlockSpec(memory_space=pl.ANY),
        scratch_shapes=[
            pltpu.SemaphoreType.DMA((4, 2, 2)),
            pltpu.SemaphoreType.DMA((4, 2)),
            pltpu.SemaphoreType.DMA((2,)),
        ],
        compiler_params=pltpu.CompilerParams(collective_id=10, has_side_effects=True),
        name="gather_dp",
    )(rows.reshape(2, count // 2, width))
    return gathered.reshape(4 * count, width)


def farthest(line, z, k):
    return ranked(line, z, k, lambda place, at: (-abs(place - at), place))


def reduce_kernel(
    square,
    line,
    paired,
    x_ref,
    out_ref,
    acc,
    got_pair,
    got_x,
    got_y,
    got_far_x,
    got_far_y,
    got_below,
    got_above,
    load_sem,
    pair_sem,
    x_sem,
    y_sem,
    far_x_sem,
    far_y_sem,
    below_sem,
    above_sem,
):
    dp, place = lax.axis_index("dp"), lax.axis_index("expert")
    z, c = place // 2, place % 2
    side_x, side_y = corners(dp)
    core = c if paired else 0
    own = dp if square else 0
    quarters = (3 - dp, side_x, side_y, dp) if square else (0,)
    to_x, to_y = (side_x, place), (side_y, place)
    to_pair, to_up, to_down = (dp, 2 * z + 1 - c), (dp, place + 2), (dp, place - 2)
    greeted = 0
    if square:
        greet(to_x)
        greet(to_y)
        greeted += 2
    if paired:
        greet(to_pair)
        greeted += 1
    if line > 1:
        pl.when(z > 0)(lambda: greet(to_down))
        pl.when(z < line - 1)(lambda: greet(to_up))
        greeted = greeted + (z > 0).astype(jnp.int32) + (z < line - 1).astype(jnp.int32)
    pl.semaphore_wait(pltpu.get_barrier_semaphore(), greeted)

    def load(q, height, p):
        return pltpu.make_async_copy(
            x_ref.at[q, height, core, p], acc.at[q, height, p], load_sem.at[q, height, p]
        )

    def hand(q, height, p):
        at = (q, height, p)
        source = x_ref.at[q, height, 1 - core, p]
        return send(source, got_pair.at[at], pair_sem.at[0, *at], pair_sem.at[1, *at], to_pair)

    def along_x(height, p):
        at = (height, p)
        return send(
            acc.at[side_x, height, p], got_x.at[at], x_sem.at[0, *at], x_sem.at[1, *at], to_x
        )

    def along_y(height, p):
        at = (height, p)
        return send(
            acc.at[side_y, height, p], got_y.at[at], y_sem.at[0, *at], y_sem.at[1, *at], to_y
        )

    def far_x(height):
        return send(
            acc.at[3 - dp, height, 0],
            got_far_x.at[height],
            far_x_sem.at[0, height],
            far_x_sem.at[1, height],
            to_x,
        )

    def far_y(height):
        return send(
            acc.at[3 - dp, height, 1],
            got_far_y.at[height],
            far_y_sem.at[0, height],
            far_y_sem.at[1, height],
            to_y,
        )

    def climb(height, p):
        at = (height, p)
        return send(
            acc.at[own, height, p], got_below.at[at], below_sem.at[0, *at], below_sem.at[1, *at], to_up
        )

    def descend(height, p):
        at = (height, p)
        return send(
            acc.at[own, height, p],
            got_above.at[at],
            above_sem.at[0, *at],
            above_sem.at[1, *at],
            to_down,
        )

    def height_of(k):
        return farthest(line, z, k) if line > 1 else 0

    def start(k, carry):
        for q in quarters:
            for p in (0, 1):
                load(q, height_of(k), p).start()
                if paired:
                    hand(q, height_of(k), p).start()
        return carry

    lax.fori_loop(0, line, start, 0)

    def step(k, carry):
        def cores():
            height = height_of(k)
            for q in quarters:
                for p in (0, 1):
                    load(q, height, p).wait()
                    if paired:
                        hand(q, height, p).wait_recv()
                        acc[q, height, p] = acc[q, height, p] + got_pair[q, height, p]
                if square and q is quarters[0]:
                    far_x(height).start()
                    far_y(height).start()

        def sides():
            height = height_of(k - 1)
            along_x(height, 0).start()
            along_y(height, 1).start()
            far_x(height).wait_recv()
            acc[side_y, height, 0] = acc[side_y, height, 0] + got_far_x[height]
            along_y(height, 0).start()
            far_y(height).wait_recv()
            acc[side_x, height, 1] = acc[side_x, height, 1] + got_far_y[height]
            along_x(height, 1).start()

        def column():
            height = height_of(k - 2)
            for p in (0, 1):
                if square:
                    along_x(height, p).wait_recv()
                    along_y(height, p).wait_recv()
                    total = acc[own, height, p].astype(jnp.float32)
                    total = total + got_x[height, p].astype(jnp.float32)
                    total = total + got_y[height, p].astype(jnp.float32)
                    acc[own, height, p] = total.astype(acc.dtype)
                if line > 1:
                    pl.when((z == 0) & (height > z))(lambda: climb(height, p).start())
                    pl.when((z == line - 1) & (height < z))(lambda: descend(height, p).start())

        def pass_on():
            height = height_of(k - 3)
            for p in (0, 1):

                def upwards():
                    climb(height, p).wait_recv()
                    acc[own, height, p] = acc[own, height, p] + got_below[height, p]
                    climb(height, p).start()

                def downwards():
                    descend(height, p).wait_recv()
                    acc[own, height, p] = acc[own, height, p] + got_above[height, p]
                    descend(height, p).start()

                pl.when((height > z) & (z > 0))(upwards)
                pl.when((height < z) & (z < line - 1))(downwards)

        pl.when(k < line)(cores)
        if square:
            pl.when((k >= 1) & (k < line + 1))(sides)
        pl.when((k >= 2) & (k < line + 2))(column)
        if line > 1:
            pl.when(k >= 3)(pass_on)
        return carry

    lax.fori_loop(0, line + (3 if line > 1 else 2), step, 0)
    home = z if line > 1 else 0
    for p in (0, 1):
        out_ref[p] = acc[own, home, p].astype(jnp.float32)
        if line > 1:

            def from_below():
                climb(z, p).wait_recv()
                out_ref[p] = out_ref[p] + got_below[z, p].astype(jnp.float32)

            def from_above():
                descend(z, p).wait_recv()
                out_ref[p] = out_ref[p] + got_above[z, p].astype(jnp.float32)

            pl.when(z > 0)(from_below)
            pl.when(z < line - 1)(from_above)

    def finish(height, carry):
        if square:
            far_x(height).wait_send()
            far_y(height).wait_send()
        for p in (0, 1):
            if paired:
                for q in quarters:
                    hand(q, height, p).wait_send()
            if square:
                along_x(height, p).wait_send()
                along_y(height, p).wait_send()
            if line > 1:
                pl.when(height > z)(lambda: climb(height, p).wait_send())
                pl.when(height < z)(lambda: descend(height, p).wait_send())
        return carry

    lax.fori_loop(0, line, finish, 0)


def reduce_to(parts, square, line, paired, name, number):
    _, rows, width = parts.shape
    quarters, cores, half = (4 if square else 1), (2 if paired else 1), rows // 2

    def space(used, *shape):
        return pltpu.VMEM((*shape, half, width) if used else (*shape, 16, 128), parts.dtype)

    sems = pltpu.SemaphoreType.DMA
    total = pl.pallas_call(
        functools.partial(reduce_kernel, square, line, paired),
        out_shape=jax.ShapeDtypeStruct((2, half, width), jnp.float32),
        in_specs=[pl.BlockSpec(memory_space=pl.ANY)],
        out_specs=pl.BlockSpec(memory_space=pltpu.VMEM),
        scratch_shapes=[
            space(True, quarters, line, 2),
            space(paired, quarters, line, 2),
            space(square, line, 2),
            space(square, line, 2),
            space(square, line),
            space(square, line),
            space(line > 1, line, 2),
            space(line > 1, line, 2),
            sems((quarters, line, 2)),
            sems((2, quarters, line, 2)),
            sems((2, line, 2)),
            sems((2, line, 2)),
            sems((2, line)),
            sems((2, line)),
            sems((2, line, 2)),
            sems((2, line, 2)),
        ],
        compiler_params=pltpu.CompilerParams(
            collective_id=number, has_side_effects=True, vmem_limit_bytes=60 << 20
        ),
        name=name,
    )(parts.reshape(quarters, line, cores, 2, half, width))
    return total.reshape(rows, width)


def scatter_dp(rows):
    return reduce_to(rows.reshape(4, -1, rows.shape[1]), True, 1, False, "scatter_dp", 3)


def visit_others(line, z, visit):
    def turn(k, carry):
        visit((z + k) % line)
        return carry

    lax.fori_loop(1, line, turn, 0)


def greet_line(line, dp, z, c):
    visit_others(line, z, lambda other: greet((dp, 2 * other + c)))
    greet((dp, 2 * z + 1 - c))
    pl.semaphore_wait(pltpu.get_barrier_semaphore(), line)


def columns(z):
    return pl.ds(pl.multiple_of(z * HD, HD), HD)


def to_heads_kernel(line, shared, *refs):
    count = len(shared)
    ins, outs = refs[:count], refs[count : 2 * count]
    sent, arrived, pair_sent, pair_arrived, own_sem = refs[2 * count :]
    dp, place = lax.axis_index("dp"), lax.axis_index("expert")
    z, c = place // 2, place % 2
    pair = (dp, 2 * z + 1 - c)
    greet_line(line, dp, z, c)

    def block(i, origin):
        return outs[i].at[origin, c] if shared[i] else outs[i].at[origin]

    def out(i, other):
        source = ins[i].at[:, columns(other)]
        device = (dp, 2 * other + c)
        return send(source, block(i, z), sent.at[i, other], arrived.at[i, z], device)

    def into(i, origin):
        part = block(i, origin)
        return send(part, part, sent.at[i, origin], arrived.at[i, origin], pair)

    def share(i, origin, source=None):
        part = block(i, origin)
        return send(
            part if source is None else source,
            part,
            pair_sent.at[i, origin],
            pair_arrived.at[i, origin],
            pair,
        )

    def own(i):
        return pltpu.make_async_copy(ins[i].at[:, columns(z)], block(i, z), own_sem.at[i])

    def dispatch(other):
        for i in range(count):
            out(i, other).start()

    visit_others(line, z, dispatch)
    for i in range(count):
        own(i).start()
        if shared[i]:
            share(i, z, ins[i].at[:, columns(z)]).start()

    def receive(origin):
        for i in range(count):
            into(i, origin).wait_recv()
            if shared[i]:
                share(i, origin).start()

    visit_others(line, z, receive)

    def finish(other):
        for i in range(count):
            out(i, other).wait_send()

    visit_others(line, z, finish)
    for i in range(count):
        own(i).wait()
        if shared[i]:

            def settle(origin, carry):
                share(i, origin).wait()
                return carry

            lax.fori_loop(0, line, settle, 0)


def to_heads(arrays, shared, line, name, number):
    rows = arrays[0].shape[0]
    count = len(arrays)
    sems = pltpu.SemaphoreType.DMA
    return pl.pallas_call(
        functools.partial(to_heads_kernel, line, shared),
        out_shape=[
            jax.ShapeDtypeStruct((line, 2, rows, HD) if both else (line, rows, HD), array.dtype)
            for array, both in zip(arrays, shared)
        ],
        in_specs=[pl.BlockSpec(memory_space=pltpu.VMEM)] * count,
        out_specs=[pl.BlockSpec(memory_space=pl.ANY)] * count,
        scratch_shapes=[sems((count, line))] * 4 + [sems((count,))],
        compiler_params=pltpu.CompilerParams(collective_id=number, has_side_effects=True),
        name=name,
    )(*arrays)


def to_tokens_kernel(line, summed, working, *refs):
    count, sums = len(summed), sum(summed)
    if working:
        work_in, work_out, work_refs = refs[count : count + 2], refs[2 * count + 2], refs[-7:]
        refs = (*refs[:count], *refs[count + 2 : 2 * count + 2], *refs[2 * count + 3 : -7])
    ins, outs = refs[:count], refs[count : 2 * count]
    mine, theirs = refs[2 * count : 2 * count + 2]
    sent, arrived, pair_sem, load_sem, own_sem = refs[2 * count + 2 :]
    dp, place = lax.axis_index("dp"), lax.axis_index("expert")
    z, c = place // 2, place % 2
    pair = (dp, 2 * z + 1 - c)
    greet_line(line, dp, z, c)
    at_sum = [sum(summed[:i]) for i in range(count)]

    def load(i, other):
        return pltpu.make_async_copy(
            ins[i].at[other, c], mine.at[at_sum[i], other], load_sem.at[at_sum[i], other]
        )

    def hand(i, other):
        s = at_sum[i]
        return send(
            ins[i].at[other, 1 - c],
            theirs.at[s, other],
            pair_sem.at[0, s, other],
            pair_sem.at[1, s, other],
            pair,
        )

    def source(i, other):
        return mine.at[at_sum[i], other] if summed[i] else ins[i].at[other]

    def out(i, other):
        target = outs[i].at[:, columns(z)]
        device = (dp, 2 * other + c)
        return send(source(i, other), target, sent.at[i, other], arrived.at[i, z], device)

    def into(i, origin):
        part = outs[i].at[:, columns(origin)]
        return send(part, part, sent.at[i, origin], arrived.at[i, origin], pair)

    def own(i):
        return pltpu.make_async_copy(source(i, z), outs[i].at[:, columns(z)], own_sem.at[i])

    def prepare(other):
        for i in range(count):
            if summed[i]:
                load(i, other).start()
                hand(i, other).start()

    def add(i, other):
        if summed[i]:
            load(i, other).wait()
            hand(i, other).wait_recv()
            s = at_sum[i]
            mine[s, other] = mine[s, other] + theirs[s, other]

    def dispatch(other):
        for i in range(count):
            add(i, other)
            out(i, other).start()

    if sums:
        visit_others(line, z, prepare)
        prepare(z)
    visit_others(line, z, dispatch)
    for i in range(count):
        add(i, z)
        own(i).start()
    if working:
        work, work_end, turns = unit_grads(0, *work_in, work_out, *work_refs)

        def turn(n, carry):
            work(n)
            return carry

        lax.fori_loop(0, turns, turn, 0)
        work_end()

    def finish(other):
        for i in range(count):
            into(i, other).wait_recv()
            out(i, other).wait_send()
            if summed[i]:
                hand(i, other).wait_send()

    visit_others(line, z, finish)
    for i in range(count):
        own(i).wait()
        if summed[i]:
            hand(i, z).wait_send()


def to_tokens(arrays, summed, line, name, number, work=None):
    rows = arrays[0].shape[-2]
    count, sums = len(arrays), max(sum(summed), 1)
    sems = pltpu.SemaphoreType.DMA
    dtype = arrays[0].dtype
    held = (sums, line, rows, HD) if sum(summed) else (1, 1, 16, HD)
    work_in, work_shape, work_space = [], [], []
    if work is not None:
        xn, units, shape = work
        work_in, work_space = [xn, units], unit_grads_space(xn, units, shape)
        work_shape = [jax.ShapeDtypeStruct(shape, dtype)]
    return pl.pallas_call(
        functools.partial(to_tokens_kernel, line, summed, work is not None),
        out_shape=[jax.ShapeDtypeStruct((rows, line * HD), dtype)] * count + work_shape,
        in_specs=[pl.BlockSpec(memory_space=pl.ANY)] * (count + len(work_in)),
        out_specs=[pl.BlockSpec(memory_space=pl.ANY)] * (count + len(work_shape)),
        scratch_shapes=[pltpu.VMEM(held, dtype)] * 2
        + [
            sems((count, line)),
            sems((count, line)),
            sems((2, sums, line)),
            sems((sums, line)),
            sems((count,)),
            *work_space,
        ],
        compiler_params=pltpu.CompilerParams(
            collective_id=number, has_side_effects=True, vmem_limit_bytes=40 << 20
        ),
        name=name,
    )(*arrays, *work_in)


KEY_TILE = 512


def masked_scores(keys, queries, tile, first, starts):
    scores = contract(keys, queries, 1, 1) * HD ** (-0.5)
    key_at = tile * KEY_TILE + lax.broadcasted_iota(jnp.int32, scores.shape, 0)
    query_at = first + lax.broadcasted_iota(jnp.int32, (1, scores.shape[1]), 1)
    return jnp.where((key_at >= starts) & (key_at <= query_at), scores, masked_score)


def attend_kernel(bounds, q_ref, k_ref, v_ref, start_ref, o_ref, total_ref):
    i = pl.program_id(0)
    queries, starts = q_ref[0], start_ref[0]
    span = queries.shape[0]

    def tile_step(tile, carry):
        largest, total, acc = carry
        rows = pl.ds(pl.multiple_of(tile * KEY_TILE, KEY_TILE), KEY_TILE)
        scores = masked_scores(k_ref[rows, :], queries, tile, bounds[2, i], starts)
        new = jnp.maximum(largest, jnp.max(scores, axis=0, keepdims=True))
        weights = jnp.exp(scores - new)
        fade = jnp.exp(largest - new)
        total = fade * total + jnp.sum(weights, axis=0, keepdims=True)
        acc = fade * acc + contract(v_ref[rows, :], weights.astype(jnp.bfloat16), 0, 0)
        return new, total, acc

    largest, total, acc = lax.fori_loop(
        bounds[0, i],
        bounds[1, i],
        tile_step,
        (
            jnp.full((1, span), masked_score, jnp.float32),
            jnp.zeros((1, span), jnp.float32),
            jnp.zeros((HD, span), jnp.float32),
        ),
    )
    o_ref[0] = (acc / total).T.astype(o_ref.dtype)
    total_ref[0] = largest + jnp.log(total)


def attend_back_kernel(
    bounds, q_ref, k_ref, v_ref, start_ref, total_ref, delta_ref, d_ref, dq_ref, dk_ref, dv_ref, dk, dv
):
    i = pl.program_id(0)
    queries, starts, grad = q_ref[0], start_ref[0], d_ref[0]
    total, delta = total_ref[0], delta_ref[0]

    @pl.when(i == 0)
    def _():
        dk[...] = jnp.zeros_like(dk)
        dv[...] = jnp.zeros_like(dv)

    def tile_step(tile, acc):
        rows = pl.ds(pl.multiple_of(tile * KEY_TILE, KEY_TILE), KEY_TILE)
        keys = k_ref[rows, :]
        scores = masked_scores(keys, queries, tile, bounds[2, i], starts)
        weights = jnp.exp(scores - total)
        grad_weights = contract(v_ref[rows, :], grad, 1, 1)
        grad_scores = (weights * (grad_weights - delta)).astype(jnp.bfloat16)
        dv[rows, :] += contract(weights.astype(jnp.bfloat16), grad, 1, 0)
        dk[rows, :] += contract(grad_scores, queries, 1, 0)
        return acc + contract(keys, grad_scores, 0, 0)

    acc = jnp.zeros((HD, queries.shape[0]), jnp.float32)
    acc = lax.fori_loop(bounds[0, i], bounds[1, i], tile_step, acc)
    dq_ref[0] = (acc * HD ** (-0.5)).T.astype(dq_ref.dtype)

    @pl.when(i == pl.num_programs(0) - 1)
    def _():
        dk_ref[...] = (dk[...] * HD ** (-0.5)).astype(dk_ref.dtype)
        dv_ref[...] = dv[...].astype(dv_ref.dtype)


def attend(bounds, queries, keys, values, starts):
    line, span, _ = queries.shape
    pack = keys.shape[0]
    block = pl.BlockSpec((1, span, HD), lambda i, _: (i, 0, 0))
    row = pl.BlockSpec((1, 1, span), lambda i, _: (i, 0, 0))
    whole = pl.BlockSpec((pack, HD), lambda i, _: (0, 0))
    return pl.pallas_call(
        attend_kernel,
        grid_spec=pltpu.PrefetchScalarGridSpec(
            num_scalar_prefetch=1,
            grid=(line,),
            in_specs=[block, whole, whole, row],
            out_specs=[block, row],
        ),
        out_shape=[
            jax.ShapeDtypeStruct(queries.shape, jnp.bfloat16),
            jax.ShapeDtypeStruct(starts.shape, jnp.float32),
        ],
        name="attend",
    )(bounds, queries, keys, values, starts)


def attend_back(bounds, queries, keys, values, starts, total, delta, grad):
    line, span, _ = queries.shape
    pack = keys.shape[0]
    block = pl.BlockSpec((1, span, HD), lambda i, _: (i, 0, 0))
    row = pl.BlockSpec((1, 1, span), lambda i, _: (i, 0, 0))
    whole = pl.BlockSpec((pack, HD), lambda i, _: (0, 0))
    return pl.pallas_call(
        attend_back_kernel,
        grid_spec=pltpu.PrefetchScalarGridSpec(
            num_scalar_prefetch=1,
            grid=(line,),
            in_specs=[block, whole, whole, row, row, row, block],
            out_specs=[block, whole, whole],
            scratch_shapes=[pltpu.VMEM((pack, HD), jnp.float32)] * 2,
        ),
        out_shape=[jax.ShapeDtypeStruct(queries.shape, jnp.bfloat16)]
        + [jax.ShapeDtypeStruct((pack, HD), jnp.bfloat16)] * 2,
        name="attend_back",
    )(bounds, queries, keys, values, starts, total, delta, grad)


def out_sum_kernel(
    line,
    o_ref,
    w_ref,
    attended_ref,
    out_ref,
    att,
    made,
    got_x,
    got_y,
    got_far_x,
    got_far_y,
    sent,
    arrived,
    own_sem,
    att_sem,
    x_sem,
    y_sem,
    far_x_sem,
    far_y_sem,
):
    dp, place = lax.axis_index("dp"), lax.axis_index("expert")
    z, c = place // 2, place % 2
    side_x, side_y = corners(dp)
    far = 3 - dp
    to_x, to_y = (side_x, place), (side_y, place)
    visit_others(line, z, lambda other: greet((dp, 2 * other + c)))
    greet(to_x)
    greet(to_y)
    pl.semaphore_wait(pltpu.get_barrier_semaphore(), line + 1)
    rows, half, width = att.shape[1], made.shape[2], made.shape[3]
    chunk = 512
    order = (far, side_x, side_y, dp)

    def block(q):
        return pl.ds(pl.multiple_of(q * rows, rows), rows)

    def out(q, other):
        device = (dp, 2 * other + c)
        source, target = o_ref.at[other, block(q)], att.at[q, :, columns(z)]
        return send(source, target, sent.at[q, other], arrived.at[q, z], device)

    def into(q, origin):
        part = att.at[q, :, columns(origin)]
        return send(part, part, sent.at[q, origin], arrived.at[q, origin], to_x)

    def own(q):
        return pltpu.make_async_copy(
            o_ref.at[z, block(q)], att.at[q, :, columns(z)], own_sem.at[q]
        )

    def att_out(q):
        return pltpu.make_async_copy(att.at[q], attended_ref.at[block(q)], att_sem.at[q])

    def along_x(p):
        return send(made.at[side_x, p], got_x.at[p], x_sem.at[0, p], x_sem.at[1, p], to_x)

    def along_y(p):
        return send(made.at[side_y, p], got_y.at[p], y_sem.at[0, p], y_sem.at[1, p], to_y)

    def far_x():
        return send(made.at[far, 0], got_far_x, far_x_sem.at[0], far_x_sem.at[1], to_x)

    def far_y():
        return send(made.at[far, 1], got_far_y, far_y_sem.at[0], far_y_sem.at[1], to_y)

    for q in order:
        visit_others(line, z, lambda other: out(q, other).start())
        own(q).start()
    for i, q in enumerate(order):
        visit_others(line, z, lambda origin: into(q, origin).wait_recv())
        own(q).wait()
        att_out(q).start()
        for at in range(0, width, chunk):
            part = contract(att[q], w_ref[:, at : at + chunk], 1, 0).astype(made.dtype)
            made[q, :, :, at : at + chunk] = part.reshape(2, half, chunk)
        if i == 0:
            far_x().start()
            far_y().start()
        if i == 1:
            along_x(0).start()
        if i == 2:
            along_y(1).start()
    far_y().wait_recv()
    made[side_x, 1] = made[side_x, 1] + got_far_y[...]
    along_x(1).start()
    far_x().wait_recv()
    made[side_y, 0] = made[side_y, 0] + got_far_x[...]
    along_y(0).start()
    for p in (0, 1):
        along_x(p).wait_recv()
        along_y(p).wait_recv()
        total = made[dp, p].astype(jnp.float32)
        out_ref[p] = total + got_x[p].astype(jnp.float32) + got_y[p].astype(jnp.float32)
    far_x().wait_send()
    far_y().wait_send()
    for p in (0, 1):
        along_x(p).wait_send()
        along_y(p).wait_send()
    for q in order:
        visit_others(line, z, lambda other: out(q, other).wait_send())
        att_out(q).wait()


def out_sum(heads, w_out, line):
    rows = heads.shape[1]
    depth, width = w_out.shape
    quarter, half = rows // 4, rows // 8
    sems = pltpu.SemaphoreType.DMA
    dtype = heads.dtype
    anywhere, inside = pl.BlockSpec(memory_space=pl.ANY), pl.BlockSpec(memory_space=pltpu.VMEM)
    attended, total = pl.pallas_call(
        functools.partial(out_sum_kernel, line),
        out_shape=[
            jax.ShapeDtypeStruct((rows, depth), dtype),
            jax.ShapeDtypeStruct((2, half, width), jnp.float32),
        ],
        in_specs=[anywhere, inside],
        out_specs=[anywhere, inside],
        scratch_shapes=[
            pltpu.VMEM((4, quarter, depth), dtype),
            pltpu.VMEM((4, 2, half, width), dtype),
            pltpu.VMEM((2, half, width), dtype),
            pltpu.VMEM((2, half, width), dtype),
            pltpu.VMEM((half, width), dtype),
            pltpu.VMEM((half, width), dtype),
            sems((4, line)),
            sems((4, line)),
            sems((4,)),
            sems((4,)),
            sems((2, 2)),
            sems((2, 2)),
            sems((2,)),
            sems((2,)),
        ],
        compiler_params=pltpu.CompilerParams(
            collective_id=7, has_side_effects=True, vmem_limit_bytes=40 << 20
        ),
        name="out_sum",
    )(heads, w_out)
    return attended, total.reshape(quarter, width)


def out_back_kernel(
    line, x_ref, w_ref, all_ref, grad_ref, buf, grads, spread_sem, arrive_sem, own_sem, all_sem, sent, arrived, mine_sem
):
    dp, place = lax.axis_index("dp"), lax.axis_index("expert")
    z, c = place // 2, place % 2
    side_x, side_y = corners(dp)
    far = 3 - dp
    devices = ((side_x, place), (side_y, place))
    visit_others(line, z, lambda other: greet((dp, 2 * other + c)))
    for device in devices:
        greet(device)
    pl.semaphore_wait(pltpu.get_barrier_semaphore(), line + 1)
    rows = grads.shape[1]

    def spread(corner, p, way, source=None):
        target = buf.at[corner, p]
        return send(
            target if source is None else source,
            target,
            spread_sem.at[corner, p, way],
            arrive_sem.at[corner, p],
            devices[way],
        )

    def own(p):
        return pltpu.make_async_copy(x_ref.at[p], buf.at[dp, p], own_sem.at[p])

    def all_out(q):
        return pltpu.make_async_copy(buf.at[q], all_ref.at[q], all_sem.at[q])

    def block(q):
        return pl.ds(pl.multiple_of(q * rows, rows), rows)

    def out(q, other):
        device = (dp, 2 * other + c)
        source, target = grads.at[q, :, columns(other)], grad_ref.at[z, block(q)]
        return send(source, target, sent.at[q, other], arrived.at[q, z], device)

    def into(q, origin):
        part = grad_ref.at[origin, block(q)]
        return send(part, part, sent.at[q, origin], arrived.at[q, origin], devices[0])

    def mine(q):
        return pltpu.make_async_copy(
            grads.at[q, :, columns(z)], grad_ref.at[z, block(q)], mine_sem.at[q]
        )

    def product(q):
        all_out(q).start()
        value = contract(buf[q].reshape(rows, buf.shape[3]), w_ref[...], 1, 1)
        grads[q] = value.astype(grads.dtype)
        visit_others(line, z, lambda other: out(q, other).start())
        mine(q).start()

    for p in (0, 1):
        spread(dp, p, 0, x_ref.at[p]).start()
        spread(dp, 1 - p, 1, x_ref.at[1 - p]).start()
        own(p).start()
    for p in (0, 1):
        own(p).wait()
    product(dp)
    spread(side_x, 0, 0).wait_recv()
    spread(side_x, 0, 1).start()
    spread(side_y, 1, 0).wait_recv()
    spread(side_y, 1, 0).start()
    spread(side_x, 1, 0).wait_recv()
    product(side_x)
    spread(side_y, 0, 0).wait_recv()
    product(side_y)
    for p in (0, 1):
        spread(far, p, 0).wait_recv()
    product(far)
    for q in (dp, side_x, side_y, far):
        visit_others(line, z, lambda origin: into(q, origin).wait_recv())
        visit_others(line, z, lambda other: out(q, other).wait_send())
        mine(q).wait()
        all_out(q).wait()
    for p in (0, 1):
        for way in (0, 1):
            spread(dp, p, way).wait_send()
    spread(side_x, 0, 1).wait_send()
    spread(side_y, 1, 0).wait_send()


def out_back(own, w_out, line):
    quarter, width = own.shape
    depth = w_out.shape[0]
    half = quarter // 2
    sems = pltpu.SemaphoreType.DMA
    dtype = own.dtype
    anywhere, inside = pl.BlockSpec(memory_space=pl.ANY), pl.BlockSpec(memory_space=pltpu.VMEM)
    everyone, grad = pl.pallas_call(
        functools.partial(out_back_kernel, line),
        out_shape=[
            jax.ShapeDtypeStruct((4, 2, half, width), dtype),
            jax.ShapeDtypeStruct((line, 4 * quarter, HD), dtype),
        ],
        in_specs=[inside, inside],
        out_specs=[anywhere, anywhere],
        scratch_shapes=[
            pltpu.VMEM((4, 2, half, width), dtype),
            pltpu.VMEM((4, quarter, depth), dtype),
            sems((4, 2, 2)),
            sems((4, 2)),
            sems((2,)),
            sems((4,)),
            sems((4, line)),
            sems((4, line)),
            sems((4,)),
        ],
        compiler_params=pltpu.CompilerParams(
            collective_id=8, has_side_effects=True, vmem_limit_bytes=40 << 20
        ),
        name="out_back",
    )(own.reshape(2, half, width), w_out)
    return everyone.reshape(4 * quarter, width), grad


def by_head(layout, w_out, line):
    positions = layout[1][0]
    pack = positions.shape[0]
    span = pack // (2 * line)
    core = lax.axis_index("expert") % 2
    starts = (jnp.arange(pack, dtype=jnp.int32) - positions).reshape(line, 2, 1, span)
    starts = lax.dynamic_index_in_dim(starts, core, 1, keepdims=False)
    first = (2 * jnp.arange(line, dtype=jnp.int32) + core) * span
    bounds = jnp.stack(
        [starts[:, 0, 0] // KEY_TILE, (first + span - 1) // KEY_TILE + 1, first]
    ).astype(jnp.int32)

    def forward(queries, keys, values):
        q, k, v = to_heads(
            [queries, keys, values], (False, True, True), line, "scatter_heads", 6
        )
        k, v = k.reshape(pack, HD), v.reshape(pack, HD)
        out, total = attend(bounds, q, k, v, starts)
        return *out_sum(out, w_out, line), (q, k, v, out, total)

    def backward(kept, grad_own, work):
        q, k, v, out, total = kept
        grad_all, grad = out_back(grad_own, w_out, line)
        delta = jnp.sum(grad.astype(jnp.float32) * out.astype(jnp.float32), axis=-1)
        dq, dk, dv = attend_back(bounds, q, k, v, starts, total, delta[:, None, :], grad)
        shape = (line, 2, span, HD)
        grads = to_tokens(
            [dq, dk.reshape(shape), dv.reshape(shape)],
            (False, True, True),
            line,
            "gather_grads",
            9,
            work,
        )
        return grad_all, *grads

    return forward, backward


def by_query(layout, w_out, offset_rows):
    segment = layout[0][0]
    pack = segment.shape[0]

    def heads(rows):
        return rows.reshape(rows.shape[0], -1, HD)

    def score_block(queries, keys):
        rows = queries.shape[0]
        scores = jnp.einsum("shd,lhd->hsl", queries, keys, preferred_element_type=jnp.float32)
        own = lax.dynamic_slice_in_dim(segment, offset_rows, rows, 0)
        query_places = offset_rows + jnp.arange(rows, dtype=jnp.int32)
        key_places = jnp.arange(pack, dtype=jnp.int32)
        allowed = (own[:, None] == segment[None, :]) & (
            key_places[None, :] <= query_places[:, None]
        )
        return jnp.where(allowed[None], scores * HD ** (-0.5), masked_score)

    def forward(queries, keys, values):
        q = heads(queries)
        k = heads(lax.all_gather(keys, "expert", axis=0, tiled=True))
        v = heads(lax.all_gather(values, "expert", axis=0, tiled=True))
        scores = score_block(q, k)
        largest = jnp.max(scores, axis=-1, keepdims=True)
        total = largest + jnp.log(jnp.sum(jnp.exp(scores - largest), axis=-1, keepdims=True))
        weights = jnp.exp(scores - total).astype(jnp.bfloat16)
        attended = jnp.einsum("hsl,lhd->shd", weights, v, preferred_element_type=jnp.float32)
        attended = attended.astype(jnp.bfloat16).reshape(queries.shape)
        projected = scatter_dp(contract(attended, w_out, 1, 0).astype(jnp.bfloat16))
        return attended, projected, (q, k, v, total)

    def backward(kept, grad_own, work):
        q, k, v, total = kept
        grad_all = gather_dp(grad_own)
        grad = contract(grad_all, w_out, 1, 1).astype(jnp.bfloat16)
        shape = grad.shape
        grad = heads(grad)
        weights = jnp.exp(score_block(q, k) - total)
        grad_weights = jnp.einsum("shd,lhd->hsl", grad, v, preferred_element_type=jnp.float32)
        delta = jnp.sum(weights * grad_weights, axis=-1, keepdims=True)
        grad_scores = (weights * (grad_weights - delta)).astype(jnp.bfloat16)
        dq = jnp.einsum("hsl,lhd->shd", grad_scores, k, preferred_element_type=jnp.float32)
        dk = jnp.einsum("hsl,shd->lhd", grad_scores, q, preferred_element_type=jnp.float32)
        weights = weights.astype(jnp.bfloat16)
        dv = jnp.einsum("hsl,shd->lhd", weights, grad, preferred_element_type=jnp.float32)

        def to_owner(part):
            part = part.astype(jnp.bfloat16).reshape(pack, shape[1])
            return lax.psum_scatter(part, "expert", scatter_dimension=0, tiled=True)

        scale = HD ** (-0.5)
        dq = (dq * scale).reshape(shape)
        xn, units, (local, _, width) = work
        units = units.reshape(pack, -1)
        gate = [contract(xn, units[:, e * width : (e + 1) * width], 0, 0) for e in range(local)]
        return grad_all, dq, to_owner(dk * scale), to_owner(dv), jnp.stack(gate)

    return forward, backward


def nearest(line, z, k):
    return ranked(line, z, k, lambda place, at: (abs(place - at), place))


def ranked(line, z, k, rank):
    total = jnp.int32(0)
    for at in range(line):
        order = sorted(range(line), key=lambda place: rank(place, at))
        place = sum([jnp.where(k == i, order[i], 0) for i in range(line)])
        total = total + jnp.where(z == at, place, 0)
    return total


def gate_act_kernel(
    line,
    x_ref,
    top_ref,
    wg_ref,
    wu_ref,
    wd_ref,
    xn_ref,
    grads_ref,
    scaled_ref,
    gates_ref,
    xbuf,
    top_buf,
    grads_buf,
    scaled_buf,
    gates_buf,
    sent,
    arrived,
    own_sem,
    top_sem,
    xn_sem,
    grads_sem,
    scaled_sem,
    gates_sem,
):
    dp, place = lax.axis_index("dp"), lax.axis_index("expert")
    z, c = place // 2, place % 2
    side_x, side_y = corners(dp)
    far = 3 - dp
    devices = (
        (dp, place + 2),
        (dp, place - 2),
        (side_x, place),
        (side_y, place),
        (dp, 2 * z + 1 - c),
    )
    up, down, along_x, along_y, pair = range(5)
    has_up, has_down = z < line - 1, z > 0
    for way in (along_x, along_y, pair):
        greet(devices[way])
    pl.when(has_up)(lambda: greet(devices[up]))
    pl.when(has_down)(lambda: greet(devices[down]))
    greeted = 3 + has_up.astype(jnp.int32) + has_down.astype(jnp.int32)
    pl.semaphore_wait(pltpu.get_barrier_semaphore(), greeted)
    local, width, units = wg_ref.shape
    rows = top_buf.shape[1]
    first = place * local

    def slot(corner, height, core):
        return corner * (2 * line) + 2 * height + core

    def copy(s, p, way, source=None):
        target = xbuf.at[s, p]
        return send(
            target if source is None else source,
            target,
            sent.at[s, p, way],
            arrived.at[s, p],
            devices[way],
        )

    def arrive(s, p):
        copy(s, p, pair).wait_recv()

    mine = slot(dp, z, c)
    for p in (0, 1):
        pltpu.make_async_copy(x_ref.at[p], xbuf.at[mine, p], own_sem.at[p]).start()
        pl.when(has_up)(lambda: copy(mine, p, up, x_ref.at[p]).start())
        pl.when(has_down)(lambda: copy(mine, p, down, x_ref.at[p]).start())
        for way in (along_x, along_y, pair):
            copy(mine, p, way, x_ref.at[p]).start()

    def decode(i):
        turn, j = i // 4, i % 4
        k = turn - (j > 0).astype(jnp.int32) - (j == 3).astype(jnp.int32)
        valid = (i >= 0) & (k >= 0) & (k < line)
        corner = jnp.where(j == 0, dp, jnp.where(j == 1, side_x, jnp.where(j == 2, side_y, far)))
        return j, k, valid, corner, nearest(line, z, k)

    def top_load(i, corner, height):
        block = corner * line + height
        return pltpu.make_async_copy(top_ref.at[block], top_buf.at[i % 2], top_sem.at[i % 2])

    def xn_out(block):
        return pltpu.make_async_copy(
            xbuf.at[pl.ds(2 * block, 2), :, :, pl.ds(0, width)],
            xn_ref.at[pl.ds(2 * block, 2)],
            xn_sem.at[block],
        )

    def grads_out(block):
        return pltpu.make_async_copy(grads_buf.at[block], grads_ref.at[block], grads_sem.at[block])

    def scaled_out(block):
        return pltpu.make_async_copy(
            scaled_buf.at[block], scaled_ref.at[block], scaled_sem.at[block]
        )

    def gates_out(block):
        return pltpu.make_async_copy(gates_buf.at[block], gates_ref.at[block], gates_sem.at[block])

    def compute(i):
        j, k, _, corner, height = decode(i)
        block = corner * line + height
        for p in (0, 1):
            arrive(slot(corner, height, 1 - c), p)
        xn_out(block).start()
        top_load(i, corner, height).wait()
        lanes = lax.broadcasted_iota(jnp.int32, (rows, 128), 1)

        def tokens():
            return xbuf[pl.ds(2 * block, 2), :, :, pl.ds(0, width)].reshape(rows, width)

        table = xbuf[pl.ds(2 * block, 2), :, :, pl.ds(width, 128)].reshape(rows, 128)
        table = table.astype(jnp.float32)
        gate_grads = jnp.zeros((rows, 128), jnp.float32)
        for e in range(local):
            at = (lanes == first + e) | (lanes == first + e + 64)
            gate = jnp.sum(jnp.where(at, table, 0.0), axis=1, keepdims=True)
            g = contract(tokens(), wg_ref[e], 1, 0)
            u = contract(tokens(), wu_ref[e], 1, 0)
            h = contract(top_buf[i % 2], wd_ref[e], 1, 1)
            sigmoid = 1.0 / (1.0 + jnp.exp(-g))
            silu = g * sigmoid
            act = silu * u
            gate_grad = jnp.sum(act * h, axis=1, keepdims=True)
            gate_grads = gate_grads + jnp.where(lanes == first + e, gate_grad, 0.0)
            grad_act = h * gate
            dg = grad_act * u * sigmoid * (1.0 + g * (1.0 - sigmoid))
            du = grad_act * silu
            scaled_buf[block, :, e * units : (e + 1) * units] = (act * gate).astype(jnp.bfloat16)
            grads_buf[block, :, e * units : (e + 1) * units] = dg.astype(jnp.bfloat16)
            at = (local + e) * units
            grads_buf[block, :, at : at + units] = du.astype(jnp.bfloat16)
        gates_buf[block] = gate_grads.astype(jnp.bfloat16)
        grads_out(block).start()
        scaled_out(block).start()
        gates_out(block).start()

    def step(i, carry):
        j, k, valid, corner, height = decode(i)
        s = slot(corner, height, c)

        def own():
            for p in (0, 1):
                pltpu.make_async_copy(x_ref.at[p], xbuf.at[mine, p], own_sem.at[p]).wait()

        def column():
            for p in (0, 1):
                arrive(s, p)
                pl.when(has_up & (height < z))(lambda: copy(s, p, up).start())
                pl.when(has_down & (height > z))(lambda: copy(s, p, down).start())
                for way in (along_x, along_y, pair):
                    copy(s, p, way).start()

        def sides():
            for p in (0, 1):
                arrive(s, p)
                copy(s, p, pair).start()
            pl.when(j == 1)(lambda: copy(s, 0, along_y).start())
            pl.when(j == 2)(lambda: copy(s, 1, along_x).start())

        def opposite():
            for p in (0, 1):
                arrive(s, p)
                copy(s, p, pair).start()

        pl.when(valid & (j == 0) & (k == 0))(own)
        pl.when(valid & (j == 0) & (k > 0))(column)
        pl.when(valid & ((j == 1) | (j == 2)))(sides)
        pl.when(valid & (j == 3))(opposite)
        pl.when(valid)(lambda: top_load(i, corner, height).start())
        pl.when(decode(i - 1)[2])(lambda: compute(i - 1))
        return carry

    lax.fori_loop(0, 4 * (line + 2) + 1, step, 0)

    def finish(height, carry):
        for p in (0, 1):
            for corner in range(4):
                copy(slot(corner, height, c), p, pair).wait_send()
            s = slot(dp, height, c)
            copy(s, p, along_x).wait_send()
            copy(s, p, along_y).wait_send()
            pl.when(has_up & (height <= z))(lambda: copy(s, p, up).wait_send())
            pl.when(has_down & (height >= z))(lambda: copy(s, p, down).wait_send())
        copy(slot(side_x, height, c), 0, along_y).wait_send()
        copy(slot(side_y, height, c), 1, along_x).wait_send()
        for corner in range(4):
            block = corner * line + height
            xn_out(block).wait()
            grads_out(block).wait()
            scaled_out(block).wait()
            gates_out(block).wait()
        return carry

    lax.fori_loop(0, line, finish, 0)


def gate_act(own, tops, w_gate, w_up, w_down, line):
    count, wide = own.shape
    local, width, units = w_gate.shape
    slots, blocks, rows, half = 8 * line, 4 * line, 2 * count, count // 2
    sems = pltpu.SemaphoreType.DMA
    dtype = own.dtype
    xn, grads, scaled, gates = pl.pallas_call(
        functools.partial(gate_act_kernel, line),
        out_shape=[
            jax.ShapeDtypeStruct((slots, 2, half, width), dtype),
            jax.ShapeDtypeStruct((blocks, rows, 2 * local * units), dtype),
            jax.ShapeDtypeStruct((blocks, rows, local * units), dtype),
            jax.ShapeDtypeStruct((blocks, rows, 128), dtype),
        ],
        in_specs=[
            pl.BlockSpec(memory_space=pltpu.VMEM),
            pl.BlockSpec(memory_space=pl.ANY),
            pl.BlockSpec(memory_space=pltpu.VMEM),
            pl.BlockSpec(memory_space=pltpu.VMEM),
            pl.BlockSpec(memory_space=pltpu.VMEM),
        ],
        out_specs=[pl.BlockSpec(memory_space=pl.ANY)] * 4,
        scratch_shapes=[
            pltpu.VMEM((slots, 2, half, wide), dtype),
            pltpu.VMEM((2, rows, width), dtype),
            pltpu.VMEM((blocks, rows, 2 * local * units), dtype),
            pltpu.VMEM((blocks, rows, local * units), dtype),
            pltpu.VMEM((blocks, rows, 128), dtype),
            sems((slots, 2, 5)),
            sems((slots, 2)),
            sems((2,)),
            sems((2,)),
            sems((blocks,)),
            sems((blocks,)),
            sems((blocks,)),
            sems((blocks,)),
        ],
        compiler_params=pltpu.CompilerParams(
            collective_id=1, has_side_effects=True, vmem_limit_bytes=60 << 20
        ),
        name="gate_act",
    )(own.reshape(2, half, wide), tops.reshape(blocks, rows, width), w_gate, w_up, w_down)
    return xn.reshape(slots * count, width), grads, scaled, gates


def column_products(left_ref, right_ref, chunk_buf, right_buf, total, chunk_sem, right_sem, store):
    span = chunk_buf.shape[2]
    blocks, rows, _ = right_buf.shape
    joined = max(1, min(blocks, 1024 // rows))
    depth = joined * rows
    turns = left_ref.shape[1] // span

    def at(n):
        return pl.ds(pl.multiple_of(n * span, span), span)

    def chunk(n):
        return pltpu.make_async_copy(
            left_ref.at[:, at(n)], chunk_buf.at[n % 2], chunk_sem.at[n % 2]
        )

    right_load = pltpu.make_async_copy(right_ref, right_buf, right_sem.at[0])
    chunk(0).start()
    right_load.start()

    def turn(n):
        pl.when(n + 1 < turns)(lambda: chunk(n + 1).start())
        chunk(n).wait()
        pl.when(n == 0)(right_load.wait)
        total[...] = jnp.zeros_like(total)

        def part(k, carry):
            left = chunk_buf[n % 2, pl.ds(pl.multiple_of(k * depth, depth), depth), :]
            right = right_buf[pl.ds(k * joined, joined)].reshape(depth, right_buf.shape[2])
            total[...] += contract(left, right, 0, 0)
            return carry

        lax.fori_loop(0, blocks // joined, part, 0)
        store(n, at(n))

    return turn, turns


def unit_grads(
    kind, xn_ref, units_ref, out_ref, chunk_buf, units_buf, total, made, chunk_sem, units_sem, out_sem
):
    local, _, units = out_ref.shape
    span = chunk_buf.shape[2]

    def copies(at):
        return [
            pltpu.make_async_copy(
                made.at[:, pl.ds(e * units, units)], out_ref.at[e, at, :], out_sem.at[e]
            )
            for e in range(local)
        ]

    start = pl.ds(0, span)

    def store(n, at):
        @pl.when(n > 0)
        def _():
            for copy in copies(start):
                copy.wait()

        made[...] = total[...].astype(made.dtype)
        for copy in copies(at):
            copy.start()

    def end():
        for copy in copies(start):
            copy.wait()

    side = units_ref.at[:, :, pl.ds(kind * local * units, local * units)]
    turn, turns = column_products(
        xn_ref, side, chunk_buf, units_buf, total, chunk_sem, units_sem, store
    )
    return turn, end, turns


def unit_grads_space(xn, units, shape):
    local, _, width = shape
    blocks, rows, _ = units.shape
    sems = pltpu.SemaphoreType.DMA
    return [
        pltpu.VMEM((2, xn.shape[0], SPAN), xn.dtype),
        pltpu.VMEM((blocks, rows, local * width), xn.dtype),
        pltpu.VMEM((SPAN, local * width), jnp.float32),
        pltpu.VMEM((SPAN, local * width), xn.dtype),
        sems((2,)),
        sems((1,)),
        sems((local,)),
    ]


def down_grads(
    top_ref, scaled_ref, down_ref, chunk_buf, scaled_buf, total, out, chunk_sem, scaled_sem, out_sem
):
    local, units, _ = down_ref.shape

    def copies(at):
        return [
            pltpu.make_async_copy(out.at[e], down_ref.at[e, :, at], out_sem.at[e])
            for e in range(local)
        ]

    start = pl.ds(0, chunk_buf.shape[2])

    def store(n, at):
        @pl.when(n > 0)
        def _():
            for copy in copies(start):
                copy.wait()

        for e in range(local):
            out[e] = total[:, e * units : (e + 1) * units].T.astype(out.dtype)
        for copy in copies(at):
            copy.start()

    def end():
        for copy in copies(start):
            copy.wait()

    turn, turns = column_products(
        top_ref, scaled_ref, chunk_buf, scaled_buf, total, chunk_sem, scaled_sem, store
    )
    return turn, end, turns


SPAN = 256


def line_sum(
    line,
    parts_ref,
    small_ref,
    summed_ref,
    shared_ref,
    acc,
    got_pair,
    got_below,
    got_above,
    small,
    got_small,
    load_sem,
    pair_sem,
    load_small_sem,
    pair_small_sem,
    below_sem,
    above_sem,
    small_sem,
    summed_sem,
):
    dp, place = lax.axis_index("dp"), lax.axis_index("expert")
    z, c = place // 2, place % 2
    side_x, side_y = corners(dp)
    to_pair, to_up, to_down = (dp, 2 * z + 1 - c), (dp, place + 2), (dp, place - 2)
    large = parts_ref.shape[3]
    top_rows, low_rows = pl.ds(0, large), pl.ds(large, small_ref.shape[3])

    def loads(height, p):
        return (
            pltpu.make_async_copy(
                parts_ref.at[height, c, p], acc.at[height, p, top_rows], load_sem.at[height, p]
            ),
            pltpu.make_async_copy(
                small_ref.at[height, c, p], acc.at[height, p, low_rows], load_small_sem.at[height, p]
            ),
        )

    def hands(height, p):
        at = (height, p)
        return (
            send(
                parts_ref.at[height, 1 - c, p],
                got_pair.at[height, p, top_rows],
                pair_sem.at[0, *at],
                pair_sem.at[1, *at],
                to_pair,
            ),
            send(
                small_ref.at[height, 1 - c, p],
                got_pair.at[height, p, low_rows],
                pair_small_sem.at[0, *at],
                pair_small_sem.at[1, *at],
                to_pair,
            ),
        )

    def climb(height, p):
        at = (height, p)
        return send(
            acc.at[at], got_below.at[at], below_sem.at[0, *at], below_sem.at[1, *at], to_up
        )

    def descend(height, p):
        at = (height, p)
        return send(
            acc.at[at], got_above.at[at], above_sem.at[0, *at], above_sem.at[1, *at], to_down
        )

    def start(k, carry):
        height = farthest(line, z, k)
        for p in (0, 1):
            for copy in (*loads(height, p), *hands(height, p)):
                copy.start()
        return carry

    def pair_sum(k, carry):
        height = farthest(line, z, k)
        for p in (0, 1):
            for copy in loads(height, p):
                copy.wait()
            for copy in hands(height, p):
                copy.wait_recv()
            acc[height, p] = acc[height, p] + got_pair[height, p]
            pl.when((z == 0) & (height > z))(lambda: climb(height, p).start())
            pl.when((z == line - 1) & (height < z))(lambda: descend(height, p).start())
        return carry

    def pass_on(k, carry):
        height = farthest(line, z, k)
        for p in (0, 1):

            def upwards():
                climb(height, p).wait_recv()
                acc[height, p] = acc[height, p] + got_below[height, p]
                climb(height, p).start()

            def downwards():
                descend(height, p).wait_recv()
                acc[height, p] = acc[height, p] + got_above[height, p]
                descend(height, p).start()

            pl.when((height > z) & (z > 0))(upwards)
            pl.when((height < z) & (z < line - 1))(downwards)
        return carry

    def summed_out(p):
        return pltpu.make_async_copy(acc.at[z, p], summed_ref.at[p], summed_sem.at[p])

    def end():
        for p in (0, 1):

            def from_below():
                climb(z, p).wait_recv()
                acc[z, p] = acc[z, p] + got_below[z, p]

            def from_above():
                descend(z, p).wait_recv()
                acc[z, p] = acc[z, p] + got_above[z, p]

            pl.when(z > 0)(from_below)
            pl.when(z < line - 1)(from_above)
        small[0] = acc[z, :, large:, :]

        def finish(height, carry):
            for p in (0, 1):
                for copy in hands(height, p):
                    copy.wait_send()
                pl.when(height > z)(lambda: climb(height, p).wait_send())
                pl.when(height < z)(lambda: descend(height, p).wait_send())
            return carry

        lax.fori_loop(0, line, finish, 0)
        for side, device in enumerate(((side_x, place), (side_y, place))):
            exchange = send(
                small.at[side],
                got_small.at[side],
                small_sem.at[0, side],
                small_sem.at[1, side],
                device,
            )
            exchange.start()
            exchange.wait_recv()
            total = small[side].astype(jnp.float32) + got_small[side].astype(jnp.float32)
            if side == 0:
                small[1] = total.astype(small.dtype)
                for p in (0, 1):
                    summed_out(p).start()
            else:
                shared_ref[...] = total
            exchange.wait_send()
        for p in (0, 1):
            summed_out(p).wait()

    return start, pair_sum, pass_on, end


def line_sum_space(line, rows, small_rows, wide, dtype):
    high = (rows + small_rows) // 2
    sems = pltpu.SemaphoreType.DMA
    return (
        [pltpu.VMEM((line, 2, high, wide), dtype)] * 4
        + [pltpu.VMEM((2, 2, small_rows // 2, wide), dtype)] * 2
        + [sems((line, 2)), sems((2, line, 2))] * 2
        + [sems((2, line, 2))] * 2
        + [sems((2, 2)), sems((2,))]
    )


def product_sum_kernel(
    line,
    flipped,
    extra,
    grads,
    *refs,
):
    a_ref, w_ref = refs[0], refs[1]
    e_ref = refs[2] if extra else None
    refs = refs[3:] if extra else refs[2:]
    w_loads = []
    if flipped:
        up_ref, *refs, w_buf, w_sem = refs
        experts, _, units = w_ref.shape
        for kind, source in enumerate((w_ref, up_ref)):
            for e in range(experts):
                at = kind * experts + e
                target = w_buf.at[:, at * units : (at + 1) * units]
                w_loads.append(pltpu.make_async_copy(source.at[e], target, w_sem.at[at]))
        w_ref = w_buf
        for copy in w_loads:
            copy.start()
    if grads:
        top_ref, parts_ref, small_ref, out_ref, down_ref, summed_ref, shared_ref = refs[:7]
        refs, work_refs, sum_refs = (out_ref, *refs[7:-21]), refs[-21:-14], refs[-14:]
    (
        out_ref,
        made,
        a_buf,
        e_buf,
        got_pair,
        got_x,
        got_y,
        got_far_x,
        got_far_y,
        got_below,
        got_above,
        load_sem,
        extra_sem,
        pair_sem,
        x_sem,
        y_sem,
        far_x_sem,
        far_y_sem,
        below_sem,
        above_sem,
    ) = refs
    dp, place = lax.axis_index("dp"), lax.axis_index("expert")
    z, c = place // 2, place % 2
    side_x, side_y = corners(dp)
    far = 3 - dp
    to_x, to_y, to_pair = (side_x, place), (side_y, place), (dp, 2 * z + 1 - c)
    to_up, to_down = (dp, place + 2), (dp, place - 2)
    for device in (to_x, to_y, to_pair):
        greet(device)
    pl.when(z > 0)(lambda: greet(to_down))
    pl.when(z < line - 1)(lambda: greet(to_up))
    greeted = 3 + (z > 0).astype(jnp.int32) + (z < line - 1).astype(jnp.int32)
    pl.semaphore_wait(pltpu.get_barrier_semaphore(), greeted)
    count = 4 * line
    width = w_ref.shape[0] if flipped else w_ref.shape[1]
    half = made.shape[4]
    chunk = 512

    def mine(q, height, p):
        return made.at[q, height, c, p]

    def hand(q, height, p):
        at = (q, height, p)
        source = made.at[q, height, 1 - c, p]
        return send(source, got_pair.at[at], pair_sem.at[0, *at], pair_sem.at[1, *at], to_pair)

    def along_x(height, p):
        at = (height, p)
        source = mine(side_x, height, p)
        return send(source, got_x.at[at], x_sem.at[0, *at], x_sem.at[1, *at], to_x)

    def along_y(height, p):
        at = (height, p)
        source = mine(side_y, height, p)
        return send(source, got_y.at[at], y_sem.at[0, *at], y_sem.at[1, *at], to_y)

    def far_x(height):
        source = mine(far, height, 0)
        return send(
            source, got_far_x.at[height], far_x_sem.at[0, height], far_x_sem.at[1, height], to_x
        )

    def far_y(height):
        source = mine(far, height, 1)
        return send(
            source, got_far_y.at[height], far_y_sem.at[0, height], far_y_sem.at[1, height], to_y
        )

    def climb(height, p):
        at = (height, p)
        source = mine(dp, height, p)
        return send(source, got_below.at[at], below_sem.at[0, *at], below_sem.at[1, *at], to_up)

    def descend(height, p):
        at = (height, p)
        source = mine(dp, height, p)
        return send(source, got_above.at[at], above_sem.at[0, *at], above_sem.at[1, *at], to_down)

    def decode(i):
        k, j = i // 4, i % 4
        q = jnp.where(j == 0, far, jnp.where(j == 1, side_x, jnp.where(j == 2, side_y, dp)))
        return k, j, q, farthest(line, z, k)

    def load(i):
        _, _, q, height = decode(i)
        return pltpu.make_async_copy(
            a_ref.at[q * line + height], a_buf.at[i % 2], load_sem.at[i % 2]
        )

    def load_extra(i):
        _, _, q, height = decode(i)
        return pltpu.make_async_copy(
            e_ref.at[q * line + height], e_buf.at[i % 2], extra_sem.at[i % 2]
        )

    def start_load(i):
        load(i).start()
        if extra:
            load_extra(i).start()

    def add(q, height, p, other):
        at = (q, height, c, p)
        made[at] = made[at] + other[...]

    def compute(i):
        _, _, q, height = decode(i)
        load(i).wait()
        if extra:
            load_extra(i).wait()
        pl.when(i + 1 < count)(lambda: start_load(i + 1))
        for at in range(0, width, chunk):
            if flipped:
                part = contract(a_buf[i % 2], w_ref[at : at + chunk, :], 1, 1)
            else:
                part = contract(a_buf[i % 2], w_ref[:, at : at + chunk], 1, 0)
            part = part.astype(made.dtype).reshape(2, 2, half, chunk)
            made[q, height, :, :, :, at : at + chunk] = part
        if extra:
            made[q, height, :, :, :, width : width + 128] = e_buf[i % 2].reshape(2, 2, half, 128)
        for p in (0, 1):
            hand(q, height, p).start()

    def settle(i):
        _, j, q, height = decode(i)
        for p in (0, 1):
            hand(q, height, p).wait_recv()
            add(q, height, p, got_pair.at[q, height, p])

        def opposite():
            far_x(height).start()
            far_y(height).start()

        pl.when(j == 0)(opposite)
        pl.when(j == 1)(lambda: along_x(height, 0).start())
        pl.when(j == 2)(lambda: along_y(height, 1).start())

    def settle_far(i):
        _, j, _, height = decode(i)

        def side_of_x():
            far_y(height).wait_recv()
            add(side_x, height, 1, got_far_y.at[height])
            along_x(height, 1).start()

        def side_of_y():
            far_x(height).wait_recv()
            add(side_y, height, 0, got_far_x.at[height])
            along_y(height, 0).start()

        pl.when(j == 1)(side_of_x)
        pl.when(j == 2)(side_of_y)

    def column(height):
        for p in (0, 1):
            along_x(height, p).wait_recv()
            along_y(height, p).wait_recv()
            total = made[dp, height, c, p].astype(jnp.float32)
            total = total + got_x[height, p].astype(jnp.float32)
            total = total + got_y[height, p].astype(jnp.float32)
            made[dp, height, c, p] = total.astype(made.dtype)
            pl.when((z == 0) & (height > z))(lambda: climb(height, p).start())
            pl.when((z == line - 1) & (height < z))(lambda: descend(height, p).start())

    def pass_on(height):
        for p in (0, 1):

            def upwards():
                climb(height, p).wait_recv()
                add(dp, height, p, got_below.at[height, p])
                climb(height, p).start()

            def downwards():
                descend(height, p).wait_recv()
                add(dp, height, p, got_above.at[height, p])
                descend(height, p).start()

            pl.when((height > z) & (z > 0))(upwards)
            pl.when((height < z) & (z < line - 1))(downwards)

    start_load(0)
    for copy in w_loads:
        copy.wait()
    if grads:
        work, work_end, turns = down_grads(top_ref, a_ref, down_ref, *work_refs)
        line_start, line_pair, line_pass, line_end = line_sum(
            line, parts_ref, small_ref, summed_ref, shared_ref, *sum_refs
        )
        lax.fori_loop(0, line, line_start, 0)

    def step(i, carry):
        k, j, _, _ = decode(i)
        pl.when(i < count)(lambda: compute(i))
        pl.when((i >= 1) & (i <= count))(lambda: settle(i - 1))
        if grads:
            every = count // turns
            pl.when((i < count) & (i % every == 0))(lambda: work(i // every))

            @pl.when(i < line)
            def _():
                line_pair(i, 0)

            @pl.when((i >= 6) & (i % 4 == 2) & (i < 6 + 4 * line))
            def _():
                line_pass((i - 6) // 4, 0)

        pl.when((i >= 4) & (i < count + 4))(lambda: settle_far(i - 4))
        pl.when((k >= 3) & (j == 2))(lambda: pass_on(farthest(line, z, k - 3)))
        pl.when((k >= 2) & (j == 3))(lambda: column(farthest(line, z, k - 2)))
        return carry

    lax.fori_loop(0, count + 8, step, 0)
    if grads:
        line_end()
        work_end()
    for p in (0, 1):
        out_ref[p] = made[dp, z, c, p].astype(jnp.float32)

        def from_below():
            climb(z, p).wait_recv()
            out_ref[p] = out_ref[p] + got_below[z, p].astype(jnp.float32)

        def from_above():
            descend(z, p).wait_recv()
            out_ref[p] = out_ref[p] + got_above[z, p].astype(jnp.float32)

        pl.when(z > 0)(from_below)
        pl.when(z < line - 1)(from_above)

    def finish(height, carry):
        far_x(height).wait_send()
        far_y(height).wait_send()
        for p in (0, 1):
            for q in range(4):
                hand(q, height, p).wait_send()
            along_x(height, p).wait_send()
            along_y(height, p).wait_send()
            pl.when(height > z)(lambda: climb(height, p).wait_send())
            pl.when(height < z)(lambda: descend(height, p).wait_send())
        return carry

    lax.fori_loop(0, line, finish, 0)


def product_sum(blocks, weights, flipped, extra, line, name, number, grads=None):
    count, rows, depth = blocks.shape
    width = weights[0].shape[1] if flipped else weights.shape[1]
    wide = width + (0 if extra is None else 128)
    half = rows // 4
    sems = pltpu.SemaphoreType.DMA
    dtype = blocks.dtype

    def space(*shape):
        return pltpu.VMEM((*shape, half, wide), dtype)

    anywhere, inside = pl.BlockSpec(memory_space=pl.ANY), pl.BlockSpec(memory_space=pltpu.VMEM)
    out_shape = [jax.ShapeDtypeStruct((2, half, wide), jnp.float32)]
    work_in, work_space = [], []
    if grads is not None:
        tops, parts, small, shape = grads
        local, units, _ = shape
        _, large, wider = parts.shape
        small_rows = small.shape[1]
        span = SPAN if large >= 8 * small_rows else SPAN // 2
        work_in = [
            tops,
            parts.reshape(line, 2, 2, large // 2, wider),
            small.reshape(line, 2, 2, small_rows // 2, wider),
        ]
        out_shape += [
            jax.ShapeDtypeStruct(shape, dtype),
            jax.ShapeDtypeStruct((2, (large + small_rows) // 2, wider), dtype),
            jax.ShapeDtypeStruct((2, small_rows // 2, wider), jnp.float32),
        ]
        work_space = [
            pltpu.VMEM((2, tops.shape[0], span), dtype),
            pltpu.VMEM(blocks.shape, dtype),
            pltpu.VMEM((span, local * units), jnp.float32),
            pltpu.VMEM((local, units, span), dtype),
            sems((2,)),
            sems((1,)),
            sems((local,)),
            *line_sum_space(line, large, small_rows, wider, dtype),
        ]
    total, *work_out = pl.pallas_call(
        functools.partial(product_sum_kernel, line, flipped, extra is not None, grads is not None),
        out_shape=out_shape,
        in_specs=[anywhere, anywhere if flipped else inside]
        + ([] if extra is None else [anywhere])
        + [anywhere] * (len(work_in) + flipped),
        out_specs=[inside] + ([] if grads is None else [anywhere, anywhere, inside]),
        scratch_shapes=[
            space(4, line, 2, 2),
            pltpu.VMEM((2, rows, depth), dtype),
            pltpu.VMEM((2, rows, 128), dtype),
            space(4, line, 2),
            space(line, 2),
            space(line, 2),
            space(line),
            space(line),
            space(line, 2),
            space(line, 2),
            sems((2,)),
            sems((2,)),
            sems((2, 4, line, 2)),
            sems((2, line, 2)),
            sems((2, line, 2)),
            sems((2, line)),
            sems((2, line)),
            sems((2, line, 2)),
            sems((2, line, 2)),
            *work_space,
            *([pltpu.VMEM((width, depth), dtype), sems((2 * weights[0].shape[0],))] if flipped else []),
        ],
        compiler_params=pltpu.CompilerParams(
            collective_id=number, has_side_effects=True, vmem_limit_bytes=63 << 20
        ),
        name=name,
    )(
        blocks,
        weights[0] if flipped else weights,
        *([] if extra is None else [extra]),
        *([weights[1]] if flipped else []),
        *work_in,
    )
    return total.reshape(2 * half, wide), *work_out


def closing_kernel(
    first_ref,
    grad_ref,
    unit_ref,
    inverse_ref,
    gain_ref,
    output_ref,
    xn_ref,
    units_ref,
    outputs_ref,
    grads_ref,
    up_ref,
    part,
    got_x,
    got_y,
    got_far_x,
    got_far_y,
    grad_own,
    part_sem,
    x_sem,
    y_sem,
    far_x_sem,
    far_y_sem,
    spread_sem,
    arrive_sem,
    own_sem,
    *work_refs,
):
    dp, place = lax.axis_index("dp"), lax.axis_index("expert")
    side_x, side_y = corners(dp)
    far = 3 - dp
    to_x, to_y = meet_square(dp, place)

    def first_load(q, p):
        return pltpu.make_async_copy(first_ref.at[q, p], part.at[q, p], part_sem.at[q, p])

    def along_x(p):
        return send(part.at[side_x, p], got_x.at[p], x_sem.at[0, p], x_sem.at[1, p], to_x)

    def along_y(p):
        return send(part.at[side_y, p], got_y.at[p], y_sem.at[0, p], y_sem.at[1, p], to_y)

    def far_x():
        return send(part.at[far, 0], got_far_x, far_x_sem.at[0], far_x_sem.at[1], to_x)

    def far_y():
        return send(part.at[far, 1], got_far_y, far_y_sem.at[0], far_y_sem.at[1], to_y)

    spreads = ((output_ref, outputs_ref), (grad_own, grads_ref))

    def spread(a, corner, p, way, source=None):
        target = spreads[a][1].at[corner, p]
        return send(
            target if source is None else source,
            target,
            spread_sem.at[a, corner, p, way],
            arrive_sem.at[a, corner, p],
            (to_x, to_y)[way],
        )

    def own_copy(a, p):
        return pltpu.make_async_copy(
            spreads[a][0].at[p], spreads[a][1].at[dp, p], own_sem.at[a, p]
        )

    def spread_own(a, p):
        own_copy(a, p).start()
        for way in (0, 1):
            spread(a, dp, p, way, spreads[a][0].at[p]).start()

    def spread_far(a):
        spread(a, side_x, 0, 0).wait_recv()
        spread(a, side_x, 0, 1).start()
        spread(a, side_y, 1, 0).wait_recv()
        spread(a, side_y, 1, 0).start()

    work, work_end, turns = unit_grads(1, xn_ref, units_ref, up_ref, *work_refs)
    pauses = 4

    def meanwhile(i):
        def turn(n, carry):
            work(n)
            return carry

        lax.fori_loop(turns * i // pauses, turns * (i + 1) // pauses, turn, 0)

    for q in (far, side_x, side_y, dp):
        for p in (0, 1):
            first_load(q, p).start()
    for q in (far, side_x, side_y, dp):
        for p in (0, 1):
            first_load(q, p).wait()
    far_x().start()
    far_y().start()
    along_x(0).start()
    along_y(1).start()
    for p in (0, 1):
        spread_own(0, p)
    far_x().wait_recv()
    part[side_y, 0] = part[side_y, 0] + got_far_x[...]
    along_y(0).start()
    far_y().wait_recv()
    part[side_x, 1] = part[side_x, 1] + got_far_y[...]
    along_x(1).start()
    meanwhile(0)
    spread_far(0)
    for p in (0, 1):
        along_x(p).wait_recv()
        along_y(p).wait_recv()
        total = part[dp, p].astype(jnp.float32)
        total = total + got_x[p].astype(jnp.float32) + got_y[p].astype(jnp.float32)
        total = total * gain_ref[...]
        unit = unit_ref[p]
        mean = jnp.sum(total * unit, axis=1, keepdims=True) * (1.0 / unit.shape[1])
        rows = grad_ref[p] + inverse_ref[p] * (total - unit * mean)
        grad_own[p] = rows.astype(grad_own.dtype)
        spread_own(1, p)
    meanwhile(1)
    meanwhile(2)
    spread_far(1)
    meanwhile(3)
    for a in (0, 1):
        spread(a, side_x, 1, 0).wait_recv()
        spread(a, side_y, 0, 0).wait_recv()
        for p in (0, 1):
            spread(a, far, p, 0).wait_recv()
            for way in (0, 1):
                spread(a, dp, p, way).wait_send()
            own_copy(a, p).wait()
        spread(a, side_x, 0, 1).wait_send()
        spread(a, side_y, 1, 0).wait_send()
    far_x().wait_send()
    far_y().wait_send()
    for p in (0, 1):
        along_x(p).wait_send()
        along_y(p).wait_send()
    work_end()


def closing(first, grad, unit, inverse, gain, output, xn, units, shape):
    own, width = output.shape
    half = own // 2
    sems = pltpu.SemaphoreType.DMA
    dtype = output.dtype
    anywhere, inside = pl.BlockSpec(memory_space=pl.ANY), pl.BlockSpec(memory_space=pltpu.VMEM)
    everyone = jax.ShapeDtypeStruct((4, 2, half, width), dtype)
    weight = jax.ShapeDtypeStruct(shape, dtype)
    outputs, grads, up = pl.pallas_call(
        closing_kernel,
        out_shape=[everyone, everyone, weight],
        in_specs=[anywhere] + [inside] * 5 + [anywhere] * 2,
        out_specs=[anywhere] * 3,
        scratch_shapes=[
            pltpu.VMEM((4, 2, half, width), dtype),
            pltpu.VMEM((2, half, width), dtype),
            pltpu.VMEM((2, half, width), dtype),
            pltpu.VMEM((half, width), dtype),
            pltpu.VMEM((half, width), dtype),
            pltpu.VMEM((2, half, width), dtype),
            sems((4, 2)),
            sems((2, 2)),
            sems((2, 2)),
            sems((2,)),
            sems((2,)),
            sems((2, 4, 2, 2)),
            sems((2, 4, 2)),
            sems((2, 2)),
            *unit_grads_space(xn, units, shape),
        ],
        compiler_params=pltpu.CompilerParams(
            collective_id=5, has_side_effects=True, vmem_limit_bytes=60 << 20
        ),
        name="closing",
    )(
        first.reshape(4, 2, half, width),
        grad.reshape(2, half, width),
        unit.reshape(2, half, width),
        inverse.reshape(2, half, 1),
        gain.reshape(1, width),
        output.reshape(2, half, width),
        xn,
        units,
    )
    return outputs.reshape(4 * own, width), grads.reshape(4 * own, width), up


def square_sum(values, got, sem, side, device):
    copy = send(values.at[side], got.at[side], sem.at[0, side], sem.at[1, side], device)
    copy.start()
    copy.wait()
    return values[side] + got[side]


def as_rows(column):
    return jnp.broadcast_to(column, (column.shape[0], 128)).T[:8]


def as_column(rows):
    return jnp.broadcast_to(rows[:1], (128, rows.shape[1])).T[:, :1]


def meet_square(dp, place):
    side_x, side_y = corners(dp)
    devices = ((side_x, place), (side_y, place))
    for device in devices:
        greet(device)
    pl.semaphore_wait(pltpu.get_barrier_semaphore(), 2)
    return devices


def normed_heads_kernel(
    model_width, q_ref, k_ref, q_gain, k_gain, cos_ref, sin_ref, queries, keys, inverse, sums, got, sem
):
    devices = meet_square(lax.axis_index("dp"), lax.axis_index("expert"))
    raws, gains, outs = (q_ref, k_ref), (q_gain, k_gain), (queries, keys)
    for i, raw in enumerate(raws):
        total = jnp.sum(raw[...] * raw[...], axis=1, keepdims=True)
        sums[0, 8 * i : 8 * i + 8] = as_rows(total)
    sums[1] = square_sum(sums, got, sem, 0, devices[0])
    total = square_sum(sums, got, sem, 1, devices[1])
    inverse[...] = lax.rsqrt(total * (1.0 / model_width) + epsilon)
    for i, raw in enumerate(raws):
        scale = as_column(inverse[8 * i : 8 * i + 8])
        for at in range(0, raw.shape[1], HD):
            head = raw[:, at : at + HD] * scale * gains[i][:, at : at + HD]
            turned = head * cos_ref[...] + pltpu.roll(head, HD // 2, 1) * sin_ref[...]
            outs[i][:, at : at + HD] = turned.astype(outs[i].dtype)


def normed_heads(q_raw, k_raw, q_gain, k_gain, cos, sin, model_width):
    rows, width = q_raw.shape
    head = jax.ShapeDtypeStruct((rows, width), jnp.bfloat16)
    return pl.pallas_call(
        functools.partial(normed_heads_kernel, model_width),
        out_shape=[head, head, jax.ShapeDtypeStruct((16, rows), jnp.float32)],
        in_specs=[pl.BlockSpec(memory_space=pltpu.VMEM)] * 6,
        out_specs=[pl.BlockSpec(memory_space=pltpu.VMEM)] * 3,
        scratch_shapes=[
            pltpu.VMEM((2, 16, rows), jnp.float32),
            pltpu.VMEM((2, 16, rows), jnp.float32),
            pltpu.SemaphoreType.DMA((2, 2)),
        ],
        compiler_params=pltpu.CompilerParams(
            collective_id=11, has_side_effects=True, vmem_limit_bytes=40 << 20
        ),
        name="normed_heads",
    )(q_raw, k_raw, q_gain.reshape(1, width), k_gain.reshape(1, width), cos, sin)


def normed_heads_back_kernel(
    model_width,
    dq_ref,
    dk_ref,
    dv_ref,
    q_ref,
    k_ref,
    q_gain,
    k_gain,
    cos_ref,
    sin_ref,
    inverse,
    grads,
    gain_grads,
    sums,
    got,
    sem,
):
    devices = meet_square(lax.axis_index("dp"), lax.axis_index("expert"))
    raws, gains, news = (q_ref, k_ref), (q_gain, k_gain), (dq_ref, dk_ref)
    rows, width = q_ref.shape

    def parts(i, at):
        cut = slice(at, at + HD)
        new = news[i][:, cut].astype(jnp.float32)
        back = new * cos_ref[...] - pltpu.roll(new, HD // 2, 1) * sin_ref[...]
        unit = raws[i][:, cut] * as_column(inverse[8 * i : 8 * i + 8])
        return back, unit, back * gains[i][:, cut]

    for i in (0, 1):
        total = jnp.zeros((rows, 1), jnp.float32)
        for at in range(0, width, HD):
            back, unit, scaled = parts(i, at)
            gain_grad = jnp.sum(back * unit, axis=0, keepdims=True)
            gain_grads[8 * i : 8 * i + 8, at : at + HD] = jnp.broadcast_to(gain_grad, (8, HD))
            total = total + jnp.sum(scaled * unit, axis=1, keepdims=True)
        sums[0, 8 * i : 8 * i + 8] = as_rows(total)
    sums[1] = square_sum(sums, got, sem, 0, devices[0])
    dots = square_sum(sums, got, sem, 1, devices[1]) * (1.0 / model_width)
    for i in (0, 1):
        dot = as_column(dots[8 * i : 8 * i + 8])
        scale = as_column(inverse[8 * i : 8 * i + 8])
        for at in range(0, width, HD):
            _, unit, scaled = parts(i, at)
            value = scale * (scaled - unit * dot)
            grads[:, i * width + at : i * width + at + HD] = value.astype(grads.dtype)
    grads[:, 2 * width :] = dv_ref[...]


def normed_heads_back(dq, dk, dv, q_raw, k_raw, q_gain, k_gain, cos, sin, inverse, model_width):
    rows, width = q_raw.shape
    return pl.pallas_call(
        functools.partial(normed_heads_back_kernel, model_width),
        out_shape=[
            jax.ShapeDtypeStruct((rows, 3 * width), jnp.bfloat16),
            jax.ShapeDtypeStruct((16, width), jnp.float32),
        ],
        in_specs=[pl.BlockSpec(memory_space=pltpu.VMEM)] * 10,
        out_specs=[pl.BlockSpec(memory_space=pltpu.VMEM)] * 2,
        scratch_shapes=[
            pltpu.VMEM((2, 16, rows), jnp.float32),
            pltpu.VMEM((2, 16, rows), jnp.float32),
            pltpu.SemaphoreType.DMA((2, 2)),
        ],
        compiler_params=pltpu.CompilerParams(
            collective_id=12, has_side_effects=True, vmem_limit_bytes=40 << 20
        ),
        name="normed_heads_back",
    )(
        dq,
        dk,
        dv,
        q_raw,
        k_raw,
        q_gain.reshape(1, width),
        k_gain.reshape(1, width),
        cos,
        sin,
        inverse,
    )


def per_device(
    inputs,
    attention_norm_gain,
    w_query,
    w_key,
    w_value,
    w_out,
    q_gain,
    k_gain,
    expert_norm_gain,
    w_router,
    w_gate,
    w_up,
    w_down,
    routes,
    lengths,
    d_output,
):
    pack_count, seg_rows, model_width = inputs.shape
    local_width = w_query.shape[1]
    local_heads = local_width // HD
    experts = w_router.shape[1]
    groups = lax.axis_size("expert")
    line = groups // 2
    pack_span = seg_rows * groups
    local_experts = w_gate.shape[0]
    offset_rows = lax.axis_index("expert") * seg_rows
    segment, positions = doc_layout(lengths, pack_span)
    pos_query = lax.dynamic_slice_in_dim(positions, offset_rows, seg_rows, 1)
    cos_table, sin_table = rope_tables(pos_query[0], HD)
    inputs_single_float = inputs.astype(jnp.float32)
    first_inverse_norm = lax.rsqrt(
        jnp.mean(inputs_single_float * inputs_single_float, axis=-1, keepdims=True) + epsilon
    )
    first_unit_input = inputs_single_float * first_inverse_norm
    first_normed_input = (first_unit_input * attention_norm_gain).astype(jnp.bfloat16)
    q_raw = jnp.dot(first_normed_input[0], w_query, preferred_element_type=jnp.float32)
    k_raw = jnp.dot(first_normed_input[0], w_key, preferred_element_type=jnp.float32)
    value_rows = jnp.dot(first_normed_input[0], w_value, preferred_element_type=jnp.float32).astype(
        jnp.bfloat16
    )
    queries, keys, head_inverse = normed_heads(
        q_raw, k_raw, q_gain, k_gain, cos_table, sin_table, model_width
    )
    layout = (segment, positions)
    if local_heads == line:
        attention = by_head(layout, w_out, line)
    else:
        attention = by_query(layout, w_out, offset_rows)
    attended, projected, kept = attention[0](queries, keys, value_rows)
    own = lax.axis_index("dp")
    part_rows = seg_rows // lax.axis_size("dp")

    def own_rows(rows):
        return lax.dynamic_slice_in_dim(rows, own * part_rows, part_rows, 0)

    hidden_state = own_rows(inputs_single_float[0]) + projected
    second_inverse_norm = lax.rsqrt(
        jnp.mean(hidden_state * hidden_state, axis=-1, keepdims=True) + epsilon
    )
    second_unit_input = hidden_state * second_inverse_norm
    second_normed_input = second_unit_input * expert_norm_gain
    router = jax.nn.softmax(
        jnp.dot(second_normed_input, w_router, precision=lax.Precision.HIGHEST), axis=-1
    )
    chosen = own_rows(routes[:, 0, :])
    expert_range = jnp.arange(experts, dtype=jnp.int32)
    named = jnp.any(chosen[:, :, None] == expert_range, axis=1)
    top_own = own_rows(d_output[0])
    top_all = lax.all_gather(top_own, ALL, axis=0, tiled=True)
    gate_table = jnp.where(named, router, 0.0)
    gate_high = gate_table.astype(jnp.bfloat16)
    gate_low = (gate_table - gate_high.astype(jnp.float32)).astype(jnp.bfloat16)
    widen = ((0, 0), (0, 64 - experts))
    own_tokens = jnp.concatenate(
        [
            second_normed_input.astype(jnp.bfloat16),
            jnp.pad(gate_high, widen),
            jnp.pad(gate_low, widen),
        ],
        axis=1,
    )
    xn_all, grad_units, scaled, gate_part = gate_act(
        own_tokens, top_all, w_gate, w_up, w_down, line
    )
    (grad_tokens,) = product_sum(
        grad_units, (w_gate, w_up), True, gate_part, line, "grad_tokens", 4)
    grad_xn_exp = grad_tokens[:, :model_width]
    gate_sums = grad_tokens[:, model_width : model_width + experts]
    grad_router_probs = jnp.where(named, gate_sums, 0.0)
    grad_logits = router * (
        grad_router_probs - jnp.sum(router * grad_router_probs, axis=-1, keepdims=True)
    )
    grad_second_normed_input = grad_xn_exp + jnp.einsum(
        "se,de->sd", grad_logits, w_router, precision=lax.Precision.HIGHEST
    )
    grad_router = jnp.einsum(
        "sd,se->de", second_normed_input, grad_logits, precision=lax.Precision.HIGHEST
    )
    grad_expert_norm_gain = jnp.sum(grad_second_normed_input * second_unit_input, axis=0)
    grad_second_unit_input = grad_second_normed_input * expert_norm_gain
    grad_hidden = top_own.astype(jnp.float32) + second_inverse_norm * (
        grad_second_unit_input
        - second_unit_input
        * jnp.mean(grad_second_unit_input * second_unit_input, axis=-1, keepdims=True)
    )
    grad_attn, grad_queries, grad_keys, grad_values, grad_gate = attention[1](
        kept, grad_hidden.astype(jnp.bfloat16), (xn_all, grad_units, w_gate.shape)
    )
    grad_out = jnp.einsum("sk,sd->kd", attended, grad_attn, preferred_element_type=jnp.float32)
    grad_heads_raw, gain_grads = normed_heads_back(
        grad_queries.astype(jnp.bfloat16),
        grad_keys,
        grad_values,
        q_raw,
        k_raw,
        q_gain,
        k_gain,
        cos_table,
        sin_table,
        head_inverse,
        model_width,
    )
    grad_q_gain, grad_k_gain = gain_grads[0], gain_grads[8]
    grad_projections = jnp.einsum(
        "sd,sk->dk", first_normed_input[0], grad_heads_raw, preferred_element_type=jnp.float32
    )
    grad_first_normed_input = sum(
        contract(grad_heads_raw[:, i * local_width : (i + 1) * local_width], weight, 1, 1)
        for i, weight in enumerate((w_query, w_key, w_value))
    )
    grad_attn_gain = jnp.sum(grad_first_normed_input * first_unit_input[0], axis=0)
    wide = grad_projections.shape[1]
    small = jnp.concatenate(
        [
            grad_q_gain.reshape(groups, -1),
            grad_k_gain.reshape(groups, -1),
            grad_attn_gain.reshape(groups, -1),
            grad_expert_norm_gain.reshape(groups, -1),
            grad_router.reshape(groups, -1),
        ],
        axis=1,
    )
    small_rows = 32
    filled = small.shape[1]
    small = jnp.pad(small, ((0, 0), (0, small_rows * wide - filled)))
    moe_out, grad_down, summed, shared = product_sum(
        scaled,
        w_down.reshape(-1, model_width),
        False,
        None,
        line,
        "expert_sum",
        2,
        (
            top_all,
            grad_projections.astype(jnp.bfloat16).reshape(groups, -1, wide),
            small.astype(jnp.bfloat16).reshape(groups, small_rows, wide),
            w_down.shape,
        ),
    )
    large = summed.shape[1] - small_rows // 2
    own_small = summed[:, large:].astype(jnp.float32)
    summed = summed[:, :large].reshape(2 * large, wide).astype(jnp.float32)
    output = (hidden_state + moe_out).astype(jnp.bfloat16)
    outputs, grad_input, grad_up = closing(
        grad_first_normed_input.astype(jnp.bfloat16),
        grad_hidden,
        own_rows(first_unit_input[0]),
        own_rows(first_inverse_norm[0]),
        attention_norm_gain,
        output,
        xn_all,
        grad_units,
        w_gate.shape,
    )
    gain_size, norm_size = local_width // groups, model_width // groups
    own_gains = own_small.reshape(-1)[: 2 * gain_size]
    shared = shared.reshape(-1)[2 * gain_size : filled]
    grad_out = lax.psum_scatter(
        grad_out.astype(jnp.bfloat16), "expert", scatter_dimension=0, tiled=True
    ).astype(jnp.float32)
    return (
        outputs[None],
        grad_input.astype(jnp.float32)[None],
        shared[:norm_size],
        summed[:, :local_width],
        summed[:, local_width : 2 * local_width],
        summed[:, 2 * local_width :],
        grad_out,
        own_gains[:gain_size],
        own_gains[gain_size:],
        shared[norm_size : 2 * norm_size],
        shared[2 * norm_size :].reshape(norm_size, experts),
        grad_gate.astype(jnp.float32),
        grad_up.astype(jnp.float32),
        grad_down.astype(jnp.float32),
    )


def solution(mesh):
    placed = (
        P(None, "expert", None),
        P(),
        P(None, "dp"),
        P(None, "dp"),
        P(None, "dp"),
        P("dp", None),
        P("dp"),
        P("dp"),
        P(),
        P(),
        P("expert", None, "dp"),
        P("expert", None, "dp"),
        P("expert", "dp", None),
        P("expert", None, None),
        P(),
        P(None, "expert", None),
    )
    return jax.shard_map(
        per_device,
        mesh=mesh,
        in_specs=placed,
        out_specs=(
            P(None, "expert", None),
            P(None, "expert", None),
            P("expert"),
            P("expert", "dp"),
            P("expert", "dp"),
            P("expert", "dp"),
            P(("dp", "expert"), None),
            P(("dp", "expert")),
            P(("dp", "expert")),
            P("expert"),
            P("expert", None),
            P("expert", None, "dp"),
            P("expert", None, "dp"),
            P("expert", "dp", None),
        ),
        check_vma=False,
    )
```

```python
import functools

import jax
import jax.numpy as jnp
from jax import lax
from jax.experimental import pallas as pl
from jax.experimental.pallas import tpu as pltpu
from jax.sharding import PartitionSpec as P

HD = 128


epsilon = 1e-05
rope_base = 10000.0
masked_score = -1e30


def doc_layout(lengths, pack_span):
    doc_ends = jnp.cumsum(lengths, axis=1)
    starts = doc_ends - lengths
    places = jnp.arange(pack_span, dtype=jnp.int32)
    segment = jnp.sum((places[None, :, None] >= doc_ends[:, None, :]).astype(jnp.int32), axis=2)
    member = segment[:, :, None] == jnp.arange(lengths.shape[1], dtype=jnp.int32)[None, None, :]
    begins = jnp.sum(jnp.where(member, starts[:, None, :], 0), axis=2)
    return (segment, places[None, :] - begins)


def rope_tables(positions, head_size):
    half_size = head_size // 2
    frequency = rope_base ** (-2.0 * jnp.arange(half_size, dtype=jnp.float32) / head_size)
    angles = positions.astype(jnp.float32)[..., None] * frequency
    cos, sin = jnp.cos(angles), jnp.sin(angles)
    return jnp.concatenate([cos, cos], axis=-1), jnp.concatenate([-sin, sin], axis=-1)


ALL = ("dp", "expert")


DEVICES = pl.DeviceIdType.MESH


def greet(device):
    pl.semaphore_signal(
        pltpu.get_barrier_semaphore(), inc=1, device_id=device, device_id_type=DEVICES
    )


def send(source, target, send_sem, arrive_sem, device):
    return pltpu.make_async_remote_copy(
        src_ref=source,
        dst_ref=target,
        send_sem=send_sem,
        recv_sem=arrive_sem,
        device_id=device,
        device_id_type=DEVICES,
    )


def contract(a, b, a_dim, b_dim):
    return lax.dot_general(
        a, b, (((a_dim,), (b_dim,)), ((), ())), preferred_element_type=jnp.float32
    )


def corners(dp):
    return dp + 1 - 2 * (dp % 2), (dp + 2) % 4


def gather_square_kernel(x_ref, out_ref, sent, arrived, own_sem):
    dp, place = lax.axis_index("dp"), lax.axis_index("expert")
    side_x, side_y = corners(dp)
    devices = ((side_x, place), (side_y, place))
    for device in devices:
        greet(device)
    pl.semaphore_wait(pltpu.get_barrier_semaphore(), 2)

    def copy(corner, p, way, source=None):
        target = out_ref.at[corner, p]
        return send(
            target if source is None else source,
            target,
            sent.at[corner, p, way],
            arrived.at[corner, p],
            devices[way],
        )

    for p in (0, 1):
        pltpu.make_async_copy(x_ref.at[p], out_ref.at[dp, p], own_sem.at[p]).start()
        for way in (0, 1):
            copy(dp, p, way, x_ref.at[p]).start()
    copy(side_x, 0, 0).wait_recv()
    copy(side_x, 0, 1).start()
    copy(side_y, 0, 0).wait_recv()
    copy(side_x, 1, 0).wait_recv()
    copy(side_y, 1, 0).wait_recv()
    copy(side_y, 1, 0).start()
    for p in (0, 1):
        copy(3 - dp, p, 0).wait_recv()
        for way in (0, 1):
            copy(dp, p, way).wait_send()
        pltpu.make_async_copy(x_ref.at[p], out_ref.at[dp, p], own_sem.at[p]).wait()
    copy(side_x, 0, 1).wait_send()
    copy(side_y, 1, 0).wait_send()


def gather_dp(rows):
    count, width = rows.shape
    gathered = pl.pallas_call(
        gather_square_kernel,
        out_shape=jax.ShapeDtypeStruct((4, 2, count // 2, width), rows.dtype),
        in_specs=[pl.BlockSpec(memory_space=pltpu.VMEM)],
        out_specs=pl.BlockSpec(memory_space=pl.ANY),
        scratch_shapes=[
            pltpu.SemaphoreType.DMA((4, 2, 2)),
            pltpu.SemaphoreType.DMA((4, 2)),
            pltpu.SemaphoreType.DMA((2,)),
        ],
        compiler_params=pltpu.CompilerParams(collective_id=10, has_side_effects=True),
        name="gather_dp",
    )(rows.reshape(2, count // 2, width))
    return gathered.reshape(4 * count, width)


def farthest(line, z, k):
    return ranked(line, z, k, lambda place, at: (-abs(place - at), place))


def reduce_kernel(
    square,
    line,
    paired,
    x_ref,
    out_ref,
    acc,
    got_pair,
    got_x,
    got_y,
    got_far_x,
    got_far_y,
    got_below,
    got_above,
    load_sem,
    pair_sem,
    x_sem,
    y_sem,
    far_x_sem,
    far_y_sem,
    below_sem,
    above_sem,
):
    dp, place = lax.axis_index("dp"), lax.axis_index("expert")
    z, c = place // 2, place % 2
    side_x, side_y = corners(dp)
    core = c if paired else 0
    own = dp if square else 0
    quarters = (3 - dp, side_x, side_y, dp) if square else (0,)
    to_x, to_y = (side_x, place), (side_y, place)
    to_pair, to_up, to_down = (dp, 2 * z + 1 - c), (dp, place + 2), (dp, place - 2)
    greeted = 0
    if square:
        greet(to_x)
        greet(to_y)
        greeted += 2
    if paired:
        greet(to_pair)
        greeted += 1
    if line > 1:
        pl.when(z > 0)(lambda: greet(to_down))
        pl.when(z < line - 1)(lambda: greet(to_up))
        greeted = greeted + (z > 0).astype(jnp.int32) + (z < line - 1).astype(jnp.int32)
    pl.semaphore_wait(pltpu.get_barrier_semaphore(), greeted)

    def load(q, height, p):
        return pltpu.make_async_copy(
            x_ref.at[q, height, core, p], acc.at[q, height, p], load_sem.at[q, height, p]
        )

    def hand(q, height, p):
        at = (q, height, p)
        source = x_ref.at[q, height, 1 - core, p]
        return send(source, got_pair.at[at], pair_sem.at[0, *at], pair_sem.at[1, *at], to_pair)

    def along_x(height, p):
        at = (height, p)
        return send(
            acc.at[side_x, height, p], got_x.at[at], x_sem.at[0, *at], x_sem.at[1, *at], to_x
        )

    def along_y(height, p):
        at = (height, p)
        return send(
            acc.at[side_y, height, p], got_y.at[at], y_sem.at[0, *at], y_sem.at[1, *at], to_y
        )

    def far_x(height):
        return send(
            acc.at[3 - dp, height, 0],
            got_far_x.at[height],
            far_x_sem.at[0, height],
            far_x_sem.at[1, height],
            to_x,
        )

    def far_y(height):
        return send(
            acc.at[3 - dp, height, 1],
            got_far_y.at[height],
            far_y_sem.at[0, height],
            far_y_sem.at[1, height],
            to_y,
        )

    def climb(height, p):
        at = (height, p)
        return send(
            acc.at[own, height, p], got_below.at[at], below_sem.at[0, *at], below_sem.at[1, *at], to_up
        )

    def descend(height, p):
        at = (height, p)
        return send(
            acc.at[own, height, p],
            got_above.at[at],
            above_sem.at[0, *at],
            above_sem.at[1, *at],
            to_down,
        )

    def height_of(k):
        return farthest(line, z, k) if line > 1 else 0

    def start(k, carry):
        for q in quarters:
            for p in (0, 1):
                load(q, height_of(k), p).start()
                if paired:
                    hand(q, height_of(k), p).start()
        return carry

    lax.fori_loop(0, line, start, 0)

    def step(k, carry):
        def cores():
            height = height_of(k)
            for q in quarters:
                for p in (0, 1):
                    load(q, height, p).wait()
                    if paired:
                        hand(q, height, p).wait_recv()
                        acc[q, height, p] = acc[q, height, p] + got_pair[q, height, p]
                if square and q is quarters[0]:
                    far_x(height).start()
                    far_y(height).start()

        def sides():
            height = height_of(k - 1)
            along_x(height, 0).start()
            along_y(height, 1).start()
            far_x(height).wait_recv()
            acc[side_y, height, 0] = acc[side_y, height, 0] + got_far_x[height]
            along_y(height, 0).start()
            far_y(height).wait_recv()
            acc[side_x, height, 1] = acc[side_x, height, 1] + got_far_y[height]
            along_x(height, 1).start()

        def column():
            height = height_of(k - 2)
            for p in (0, 1):
                if square:
                    along_x(height, p).wait_recv()
                    along_y(height, p).wait_recv()
                    total = acc[own, height, p].astype(jnp.float32)
                    total = total + got_x[height, p].astype(jnp.float32)
                    total = total + got_y[height, p].astype(jnp.float32)
                    acc[own, height, p] = total.astype(acc.dtype)
                if line > 1:
                    pl.when((z == 0) & (height > z))(lambda: climb(height, p).start())
                    pl.when((z == line - 1) & (height < z))(lambda: descend(height, p).start())

        def pass_on():
            height = height_of(k - 3)
            for p in (0, 1):

                def upwards():
                    climb(height, p).wait_recv()
                    acc[own, height, p] = acc[own, height, p] + got_below[height, p]
                    climb(height, p).start()

                def downwards():
                    descend(height, p).wait_recv()
                    acc[own, height, p] = acc[own, height, p] + got_above[height, p]
                    descend(height, p).start()

                pl.when((height > z) & (z > 0))(upwards)
                pl.when((height < z) & (z < line - 1))(downwards)

        pl.when(k < line)(cores)
        if square:
            pl.when((k >= 1) & (k < line + 1))(sides)
        pl.when((k >= 2) & (k < line + 2))(column)
        if line > 1:
            pl.when(k >= 3)(pass_on)
        return carry

    lax.fori_loop(0, line + (3 if line > 1 else 2), step, 0)
    home = z if line > 1 else 0
    for p in (0, 1):
        out_ref[p] = acc[own, home, p].astype(jnp.float32)
        if line > 1:

            def from_below():
                climb(z, p).wait_recv()
                out_ref[p] = out_ref[p] + got_below[z, p].astype(jnp.float32)

            def from_above():
                descend(z, p).wait_recv()
                out_ref[p] = out_ref[p] + got_above[z, p].astype(jnp.float32)

            pl.when(z > 0)(from_below)
            pl.when(z < line - 1)(from_above)

    def finish(height, carry):
        if square:
            far_x(height).wait_send()
            far_y(height).wait_send()
        for p in (0, 1):
            if paired:
                for q in quarters:
                    hand(q, height, p).wait_send()
            if square:
                along_x(height, p).wait_send()
                along_y(height, p).wait_send()
            if line > 1:
                pl.when(height > z)(lambda: climb(height, p).wait_send())
                pl.when(height < z)(lambda: descend(height, p).wait_send())
        return carry

    lax.fori_loop(0, line, finish, 0)


def reduce_to(parts, square, line, paired, name, number):
    _, rows, width = parts.shape
    quarters, cores, half = (4 if square else 1), (2 if paired else 1), rows // 2

    def space(used, *shape):
        return pltpu.VMEM((*shape, half, width) if used else (*shape, 16, 128), parts.dtype)

    sems = pltpu.SemaphoreType.DMA
    total = pl.pallas_call(
        functools.partial(reduce_kernel, square, line, paired),
        out_shape=jax.ShapeDtypeStruct((2, half, width), jnp.float32),
        in_specs=[pl.BlockSpec(memory_space=pl.ANY)],
        out_specs=pl.BlockSpec(memory_space=pltpu.VMEM),
        scratch_shapes=[
            space(True, quarters, line, 2),
            space(paired, quarters, line, 2),
            space(square, line, 2),
            space(square, line, 2),
            space(square, line),
            space(square, line),
            space(line > 1, line, 2),
            space(line > 1, line, 2),
            sems((quarters, line, 2)),
            sems((2, quarters, line, 2)),
            sems((2, line, 2)),
            sems((2, line, 2)),
            sems((2, line)),
            sems((2, line)),
            sems((2, line, 2)),
            sems((2, line, 2)),
        ],
        compiler_params=pltpu.CompilerParams(
            collective_id=number, has_side_effects=True, vmem_limit_bytes=60 << 20
        ),
        name=name,
    )(parts.reshape(quarters, line, cores, 2, half, width))
    return total.reshape(rows, width)


def scatter_dp(rows):
    return reduce_to(rows.reshape(4, -1, rows.shape[1]), True, 1, False, "scatter_dp", 3)


def visit_others(line, z, visit):
    def turn(k, carry):
        visit((z + k) % line)
        return carry

    lax.fori_loop(1, line, turn, 0)


def greet_line(line, dp, z, c):
    visit_others(line, z, lambda other: greet((dp, 2 * other + c)))
    greet((dp, 2 * z + 1 - c))
    pl.semaphore_wait(pltpu.get_barrier_semaphore(), line)


def columns(z):
    return pl.ds(pl.multiple_of(z * HD, HD), HD)


def to_heads_kernel(line, shared, *refs):
    count = len(shared)
    ins, outs = refs[:count], refs[count : 2 * count]
    sent, arrived, pair_sent, pair_arrived, own_sem = refs[2 * count :]
    dp, place = lax.axis_index("dp"), lax.axis_index("expert")
    z, c = place // 2, place % 2
    pair = (dp, 2 * z + 1 - c)
    greet_line(line, dp, z, c)

    def block(i, origin):
        return outs[i].at[origin, c] if shared[i] else outs[i].at[origin]

    def out(i, other):
        source = ins[i].at[:, columns(other)]
        device = (dp, 2 * other + c)
        return send(source, block(i, z), sent.at[i, other], arrived.at[i, z], device)

    def into(i, origin):
        part = block(i, origin)
        return send(part, part, sent.at[i, origin], arrived.at[i, origin], pair)

    def share(i, origin, source=None):
        part = block(i, origin)
        return send(
            part if source is None else source,
            part,
            pair_sent.at[i, origin],
            pair_arrived.at[i, origin],
            pair,
        )

    def own(i):
        return pltpu.make_async_copy(ins[i].at[:, columns(z)], block(i, z), own_sem.at[i])

    def dispatch(other):
        for i in range(count):
            out(i, other).start()

    visit_others(line, z, dispatch)
    for i in range(count):
        own(i).start()
        if shared[i]:
            share(i, z, ins[i].at[:, columns(z)]).start()

    def receive(origin):
        for i in range(count):
            into(i, origin).wait_recv()
            if shared[i]:
                share(i, origin).start()

    visit_others(line, z, receive)

    def finish(other):
        for i in range(count):
            out(i, other).wait_send()

    visit_others(line, z, finish)
    for i in range(count):
        own(i).wait()
        if shared[i]:

            def settle(origin, carry):
                share(i, origin).wait()
                return carry

            lax.fori_loop(0, line, settle, 0)


def to_heads(arrays, shared, line, name, number):
    rows = arrays[0].shape[0]
    count = len(arrays)
    sems = pltpu.SemaphoreType.DMA
    return pl.pallas_call(
        functools.partial(to_heads_kernel, line, shared),
        out_shape=[
            jax.ShapeDtypeStruct((line, 2, rows, HD) if both else (line, rows, HD), array.dtype)
            for array, both in zip(arrays, shared)
        ],
        in_specs=[pl.BlockSpec(memory_space=pltpu.VMEM)] * count,
        out_specs=[pl.BlockSpec(memory_space=pl.ANY)] * count,
        scratch_shapes=[sems((count, line))] * 4 + [sems((count,))],
        compiler_params=pltpu.CompilerParams(collective_id=number, has_side_effects=True),
        name=name,
    )(*arrays)


def head_return(
    line, summed, ins, outs, mine, theirs, sent, arrived, pair_sem, load_sem, own_sem
):
    count = len(summed)
    dp, place = lax.axis_index("dp"), lax.axis_index("expert")
    z, c = place // 2, place % 2
    pair = (dp, 2 * z + 1 - c)
    at_sum = [sum(summed[:i]) for i in range(count)]

    def load(i, other):
        return pltpu.make_async_copy(
            ins[i].at[other, c], mine.at[at_sum[i], other], load_sem.at[at_sum[i], other]
        )

    def hand(i, other):
        s = at_sum[i]
        return send(
            ins[i].at[other, 1 - c],
            theirs.at[s, other],
            pair_sem.at[0, s, other],
            pair_sem.at[1, s, other],
            pair,
        )

    def source(i, other):
        return mine.at[at_sum[i], other] if summed[i] else ins[i].at[other]

    def out(i, other):
        target = outs[i].at[:, columns(z)]
        device = (dp, 2 * other + c)
        return send(source(i, other), target, sent.at[i, other], arrived.at[i, z], device)

    def into(i, origin):
        part = outs[i].at[:, columns(origin)]
        return send(part, part, sent.at[i, origin], arrived.at[i, origin], pair)

    def own(i):
        return pltpu.make_async_copy(source(i, z), outs[i].at[:, columns(z)], own_sem.at[i])

    def prepare(other):
        for i in range(count):
            if summed[i]:
                load(i, other).start()
                hand(i, other).start()

    def add(i, other):
        if summed[i]:
            load(i, other).wait()
            hand(i, other).wait_recv()
            s = at_sum[i]
            mine[s, other] = mine[s, other] + theirs[s, other]

    def begin():
        visit_others(line, z, prepare)
        prepare(z)

    def dispatch(k):
        other = (z + 1 + k) % line
        for i in range(count):
            add(i, other)

            @pl.when(k < line - 1)
            def _():
                out(i, other).start()

            @pl.when(k == line - 1)
            def _():
                own(i).start()

    def finish(other):
        for i in range(count):
            into(i, other).wait_recv()
            out(i, other).wait_send()
            if summed[i]:
                hand(i, other).wait_send()

    def end():
        visit_others(line, z, finish)
        for i in range(count):
            own(i).wait()
            if summed[i]:
                hand(i, z).wait_send()

    return begin, dispatch, end


def head_return_space(arrays, summed, line):
    rows, dtype = arrays[0].shape[-2], arrays[0].dtype
    count, sums = len(arrays), sum(summed)
    sems = pltpu.SemaphoreType.DMA
    return [pltpu.VMEM((sums, line, rows, HD), dtype)] * 2 + [
        sems((count, line)),
        sems((count, line)),
        sems((2, sums, line)),
        sems((sums, line)),
        sems((count,)),
    ]


KEY_TILE = 512


def masked_scores(keys, queries, tile, first, starts):
    scores = contract(keys, queries, 1, 1) * HD ** (-0.5)
    key_at = tile * KEY_TILE + lax.broadcasted_iota(jnp.int32, scores.shape, 0)
    query_at = first + lax.broadcasted_iota(jnp.int32, (1, scores.shape[1]), 1)
    return jnp.where((key_at >= starts) & (key_at <= query_at), scores, masked_score)


def attend_kernel(bounds, q_ref, k_ref, v_ref, start_ref, o_ref, total_ref):
    i = pl.program_id(0)
    queries, starts = q_ref[0], start_ref[0]
    span = queries.shape[0]

    def tile_step(tile, carry):
        largest, total, acc = carry
        rows = pl.ds(pl.multiple_of(tile * KEY_TILE, KEY_TILE), KEY_TILE)
        scores = masked_scores(k_ref[rows, :], queries, tile, bounds[2, i], starts)
        new = jnp.maximum(largest, jnp.max(scores, axis=0, keepdims=True))
        weights = jnp.exp(scores - new)
        fade = jnp.exp(largest - new)
        total = fade * total + jnp.sum(weights, axis=0, keepdims=True)
        acc = fade * acc + contract(v_ref[rows, :], weights.astype(jnp.bfloat16), 0, 0)
        return new, total, acc

    largest, total, acc = lax.fori_loop(
        bounds[0, i],
        bounds[1, i],
        tile_step,
        (
            jnp.full((1, span), masked_score, jnp.float32),
            jnp.zeros((1, span), jnp.float32),
            jnp.zeros((HD, span), jnp.float32),
        ),
    )
    o_ref[0] = (acc / total).T.astype(o_ref.dtype)
    total_ref[0] = largest + jnp.log(total)


def attend_back_kernel(
    bounds, q_ref, k_ref, v_ref, start_ref, total_ref, delta_ref, d_ref, dq_ref, dk_ref, dv_ref, dk, dv
):
    i = pl.program_id(0)
    queries, starts, grad = q_ref[0], start_ref[0], d_ref[0]
    total, delta = total_ref[0], delta_ref[0]

    @pl.when(i == 0)
    def _():
        dk[...] = jnp.zeros_like(dk)
        dv[...] = jnp.zeros_like(dv)

    def tile_step(tile, acc):
        rows = pl.ds(pl.multiple_of(tile * KEY_TILE, KEY_TILE), KEY_TILE)
        keys = k_ref[rows, :]
        scores = masked_scores(keys, queries, tile, bounds[2, i], starts)
        weights = jnp.exp(scores - total)
        grad_weights = contract(v_ref[rows, :], grad, 1, 1)
        grad_scores = (weights * (grad_weights - delta)).astype(jnp.bfloat16)
        dv[rows, :] += contract(weights.astype(jnp.bfloat16), grad, 1, 0)
        dk[rows, :] += contract(grad_scores, queries, 1, 0)
        return acc + contract(keys, grad_scores, 0, 0)

    acc = jnp.zeros((HD, queries.shape[0]), jnp.float32)
    acc = lax.fori_loop(bounds[0, i], bounds[1, i], tile_step, acc)
    dq_ref[0] = (acc * HD ** (-0.5)).T.astype(dq_ref.dtype)

    @pl.when(i == pl.num_programs(0) - 1)
    def _():
        dk_ref[...] = (dk[...] * HD ** (-0.5)).astype(dk_ref.dtype)
        dv_ref[...] = dv[...].astype(dv_ref.dtype)


def attend(bounds, queries, keys, values, starts):
    line, span, _ = queries.shape
    pack = keys.shape[0]
    block = pl.BlockSpec((1, span, HD), lambda i, _: (i, 0, 0))
    row = pl.BlockSpec((1, 1, span), lambda i, _: (i, 0, 0))
    whole = pl.BlockSpec((pack, HD), lambda i, _: (0, 0))
    return pl.pallas_call(
        attend_kernel,
        grid_spec=pltpu.PrefetchScalarGridSpec(
            num_scalar_prefetch=1,
            grid=(line,),
            in_specs=[block, whole, whole, row],
            out_specs=[block, row],
        ),
        out_shape=[
            jax.ShapeDtypeStruct(queries.shape, jnp.bfloat16),
            jax.ShapeDtypeStruct(starts.shape, jnp.float32),
        ],
        name="attend",
    )(bounds, queries, keys, values, starts)


def attend_back(bounds, queries, keys, values, starts, total, delta, grad):
    line, span, _ = queries.shape
    pack = keys.shape[0]
    block = pl.BlockSpec((1, span, HD), lambda i, _: (i, 0, 0))
    row = pl.BlockSpec((1, 1, span), lambda i, _: (i, 0, 0))
    whole = pl.BlockSpec((pack, HD), lambda i, _: (0, 0))
    return pl.pallas_call(
        attend_back_kernel,
        grid_spec=pltpu.PrefetchScalarGridSpec(
            num_scalar_prefetch=1,
            grid=(line,),
            in_specs=[block, whole, whole, row, row, row, block],
            out_specs=[block, whole, whole],
            scratch_shapes=[pltpu.VMEM((pack, HD), jnp.float32)] * 2,
        ),
        out_shape=[jax.ShapeDtypeStruct(queries.shape, jnp.bfloat16)]
        + [jax.ShapeDtypeStruct((pack, HD), jnp.bfloat16)] * 2,
        name="attend_back",
    )(bounds, queries, keys, values, starts, total, delta, grad)


def out_sum_kernel(
    line,
    o_ref,
    w_ref,
    attended_ref,
    out_ref,
    att,
    made,
    got_x,
    got_y,
    got_far_x,
    got_far_y,
    sent,
    arrived,
    own_sem,
    att_sem,
    x_sem,
    y_sem,
    far_x_sem,
    far_y_sem,
):
    dp, place = lax.axis_index("dp"), lax.axis_index("expert")
    z, c = place // 2, place % 2
    side_x, side_y = corners(dp)
    far = 3 - dp
    to_x, to_y = (side_x, place), (side_y, place)
    visit_others(line, z, lambda other: greet((dp, 2 * other + c)))
    greet(to_x)
    greet(to_y)
    pl.semaphore_wait(pltpu.get_barrier_semaphore(), line + 1)
    rows, half, width = att.shape[1], made.shape[2], made.shape[3]
    chunk = 512
    order = (far, side_x, side_y, dp)

    def block(q):
        return pl.ds(pl.multiple_of(q * rows, rows), rows)

    def out(q, other):
        device = (dp, 2 * other + c)
        source, target = o_ref.at[other, block(q)], att.at[q, :, columns(z)]
        return send(source, target, sent.at[q, other], arrived.at[q, z], device)

    def into(q, origin):
        part = att.at[q, :, columns(origin)]
        return send(part, part, sent.at[q, origin], arrived.at[q, origin], to_x)

    def own(q):
        return pltpu.make_async_copy(
            o_ref.at[z, block(q)], att.at[q, :, columns(z)], own_sem.at[q]
        )

    def att_out(q):
        return pltpu.make_async_copy(att.at[q], attended_ref.at[block(q)], att_sem.at[q])

    def along_x(p):
        return send(made.at[side_x, p], got_x.at[p], x_sem.at[0, p], x_sem.at[1, p], to_x)

    def along_y(p):
        return send(made.at[side_y, p], got_y.at[p], y_sem.at[0, p], y_sem.at[1, p], to_y)

    def far_x():
        return send(made.at[far, 0], got_far_x, far_x_sem.at[0], far_x_sem.at[1], to_x)

    def far_y():
        return send(made.at[far, 1], got_far_y, far_y_sem.at[0], far_y_sem.at[1], to_y)

    for q in order:
        visit_others(line, z, lambda other: out(q, other).start())
        own(q).start()
    for i, q in enumerate(order):
        visit_others(line, z, lambda origin: into(q, origin).wait_recv())
        own(q).wait()
        att_out(q).start()
        for at in range(0, width, chunk):
            part = contract(att[q], w_ref[:, at : at + chunk], 1, 0).astype(made.dtype)
            made[q, :, :, at : at + chunk] = part.reshape(2, half, chunk)
        if i == 0:
            far_x().start()
            far_y().start()
        if i == 1:
            along_x(0).start()
        if i == 2:
            along_y(1).start()
    far_y().wait_recv()
    made[side_x, 1] = made[side_x, 1] + got_far_y[...]
    along_x(1).start()
    far_x().wait_recv()
    made[side_y, 0] = made[side_y, 0] + got_far_x[...]
    along_y(0).start()
    for p in (0, 1):
        along_x(p).wait_recv()
        along_y(p).wait_recv()
        total = made[dp, p].astype(jnp.float32)
        out_ref[p] = total + got_x[p].astype(jnp.float32) + got_y[p].astype(jnp.float32)
    far_x().wait_send()
    far_y().wait_send()
    for p in (0, 1):
        along_x(p).wait_send()
        along_y(p).wait_send()
    for q in order:
        visit_others(line, z, lambda other: out(q, other).wait_send())
        att_out(q).wait()


def out_sum(heads, w_out, line):
    rows = heads.shape[1]
    depth, width = w_out.shape
    quarter, half = rows // 4, rows // 8
    sems = pltpu.SemaphoreType.DMA
    dtype = heads.dtype
    anywhere, inside = pl.BlockSpec(memory_space=pl.ANY), pl.BlockSpec(memory_space=pltpu.VMEM)
    attended, total = pl.pallas_call(
        functools.partial(out_sum_kernel, line),
        out_shape=[
            jax.ShapeDtypeStruct((rows, depth), dtype),
            jax.ShapeDtypeStruct((2, half, width), jnp.float32),
        ],
        in_specs=[anywhere, inside],
        out_specs=[anywhere, inside],
        scratch_shapes=[
            pltpu.VMEM((4, quarter, depth), dtype),
            pltpu.VMEM((4, 2, half, width), dtype),
            pltpu.VMEM((2, half, width), dtype),
            pltpu.VMEM((2, half, width), dtype),
            pltpu.VMEM((half, width), dtype),
            pltpu.VMEM((half, width), dtype),
            sems((4, line)),
            sems((4, line)),
            sems((4,)),
            sems((4,)),
            sems((2, 2)),
            sems((2, 2)),
            sems((2,)),
            sems((2,)),
        ],
        compiler_params=pltpu.CompilerParams(
            collective_id=7, has_side_effects=True, vmem_limit_bytes=40 << 20
        ),
        name="out_sum",
    )(heads, w_out)
    return attended, total.reshape(quarter, width)


def out_back_kernel(
    line, x_ref, w_ref, all_ref, grad_ref, buf, grads, spread_sem, arrive_sem, own_sem, all_sem, sent, arrived, mine_sem
):
    dp, place = lax.axis_index("dp"), lax.axis_index("expert")
    z, c = place // 2, place % 2
    side_x, side_y = corners(dp)
    far = 3 - dp
    devices = ((side_x, place), (side_y, place))
    visit_others(line, z, lambda other: greet((dp, 2 * other + c)))
    for device in devices:
        greet(device)
    pl.semaphore_wait(pltpu.get_barrier_semaphore(), line + 1)
    rows = grads.shape[1]

    def spread(corner, p, way, source=None):
        target = buf.at[corner, p]
        return send(
            target if source is None else source,
            target,
            spread_sem.at[corner, p, way],
            arrive_sem.at[corner, p],
            devices[way],
        )

    def own(p):
        return pltpu.make_async_copy(x_ref.at[p], buf.at[dp, p], own_sem.at[p])

    def all_out(q):
        return pltpu.make_async_copy(buf.at[q], all_ref.at[q], all_sem.at[q])

    def block(q):
        return pl.ds(pl.multiple_of(q * rows, rows), rows)

    def out(q, other):
        device = (dp, 2 * other + c)
        source, target = grads.at[q, :, columns(other)], grad_ref.at[z, block(q)]
        return send(source, target, sent.at[q, other], arrived.at[q, z], device)

    def into(q, origin):
        part = grad_ref.at[origin, block(q)]
        return send(part, part, sent.at[q, origin], arrived.at[q, origin], devices[0])

    def mine(q):
        return pltpu.make_async_copy(
            grads.at[q, :, columns(z)], grad_ref.at[z, block(q)], mine_sem.at[q]
        )

    def product(q):
        all_out(q).start()
        value = contract(buf[q].reshape(rows, buf.shape[3]), w_ref[...], 1, 1)
        grads[q] = value.astype(grads.dtype)
        visit_others(line, z, lambda other: out(q, other).start())
        mine(q).start()

    for p in (0, 1):
        spread(dp, p, 0, x_ref.at[p]).start()
        spread(dp, 1 - p, 1, x_ref.at[1 - p]).start()
        own(p).start()
    for p in (0, 1):
        own(p).wait()
    product(dp)
    spread(side_x, 0, 0).wait_recv()
    spread(side_x, 0, 1).start()
    spread(side_y, 1, 0).wait_recv()
    spread(side_y, 1, 0).start()
    spread(side_x, 1, 0).wait_recv()
    product(side_x)
    spread(side_y, 0, 0).wait_recv()
    product(side_y)
    for p in (0, 1):
        spread(far, p, 0).wait_recv()
    product(far)
    for q in (dp, side_x, side_y, far):
        visit_others(line, z, lambda origin: into(q, origin).wait_recv())
        visit_others(line, z, lambda other: out(q, other).wait_send())
        mine(q).wait()
        all_out(q).wait()
    for p in (0, 1):
        for way in (0, 1):
            spread(dp, p, way).wait_send()
    spread(side_x, 0, 1).wait_send()
    spread(side_y, 1, 0).wait_send()


def out_back(own, w_out, line):
    quarter, width = own.shape
    depth = w_out.shape[0]
    half = quarter // 2
    sems = pltpu.SemaphoreType.DMA
    dtype = own.dtype
    anywhere, inside = pl.BlockSpec(memory_space=pl.ANY), pl.BlockSpec(memory_space=pltpu.VMEM)
    everyone, grad = pl.pallas_call(
        functools.partial(out_back_kernel, line),
        out_shape=[
            jax.ShapeDtypeStruct((4, 2, half, width), dtype),
            jax.ShapeDtypeStruct((line, 4 * quarter, HD), dtype),
        ],
        in_specs=[inside, inside],
        out_specs=[anywhere, anywhere],
        scratch_shapes=[
            pltpu.VMEM((4, 2, half, width), dtype),
            pltpu.VMEM((4, quarter, depth), dtype),
            sems((4, 2, 2)),
            sems((4, 2)),
            sems((2,)),
            sems((4,)),
            sems((4, line)),
            sems((4, line)),
            sems((4,)),
        ],
        compiler_params=pltpu.CompilerParams(
            collective_id=8, has_side_effects=True, vmem_limit_bytes=40 << 20
        ),
        name="out_back",
    )(own.reshape(2, half, width), w_out)
    return everyone.reshape(4 * quarter, width), grad


def by_head(layout, w_out, line):
    positions = layout[1][0]
    pack = positions.shape[0]
    span = pack // (2 * line)
    core = lax.axis_index("expert") % 2
    starts = (jnp.arange(pack, dtype=jnp.int32) - positions).reshape(line, 2, 1, span)
    starts = lax.dynamic_index_in_dim(starts, core, 1, keepdims=False)
    first = (2 * jnp.arange(line, dtype=jnp.int32) + core) * span
    bounds = jnp.stack(
        [starts[:, 0, 0] // KEY_TILE, (first + span - 1) // KEY_TILE + 1, first]
    ).astype(jnp.int32)

    def forward(queries, keys, values):
        q, k, v = to_heads(
            [queries, keys, values], (False, True, True), line, "scatter_heads", 6
        )
        k, v = k.reshape(pack, HD), v.reshape(pack, HD)
        out, total = attend(bounds, q, k, v, starts)
        return *out_sum(out, w_out, line), (q, k, v, out, total)

    def backward(kept, grad_own):
        q, k, v, out, total = kept
        grad_all, grad = out_back(grad_own, w_out, line)
        delta = jnp.sum(grad.astype(jnp.float32) * out.astype(jnp.float32), axis=-1)
        dq, dk, dv = attend_back(bounds, q, k, v, starts, total, delta[:, None, :], grad)
        shape = (line, 2, span, HD)
        return grad_all, [dq, dk.reshape(shape), dv.reshape(shape)], []

    return forward, backward


def by_query(layout, w_out, offset_rows):
    segment = layout[0][0]
    pack = segment.shape[0]

    def heads(rows):
        return rows.reshape(rows.shape[0], -1, HD)

    def score_block(queries, keys):
        rows = queries.shape[0]
        scores = jnp.einsum("shd,lhd->hsl", queries, keys, preferred_element_type=jnp.float32)
        own = lax.dynamic_slice_in_dim(segment, offset_rows, rows, 0)
        query_places = offset_rows + jnp.arange(rows, dtype=jnp.int32)
        key_places = jnp.arange(pack, dtype=jnp.int32)
        allowed = (own[:, None] == segment[None, :]) & (
            key_places[None, :] <= query_places[:, None]
        )
        return jnp.where(allowed[None], scores * HD ** (-0.5), masked_score)

    def forward(queries, keys, values):
        q = heads(queries)
        k = heads(lax.all_gather(keys, "expert", axis=0, tiled=True))
        v = heads(lax.all_gather(values, "expert", axis=0, tiled=True))
        scores = score_block(q, k)
        largest = jnp.max(scores, axis=-1, keepdims=True)
        total = largest + jnp.log(jnp.sum(jnp.exp(scores - largest), axis=-1, keepdims=True))
        weights = jnp.exp(scores - total).astype(jnp.bfloat16)
        attended = jnp.einsum("hsl,lhd->shd", weights, v, preferred_element_type=jnp.float32)
        attended = attended.astype(jnp.bfloat16).reshape(queries.shape)
        projected = scatter_dp(contract(attended, w_out, 1, 0).astype(jnp.bfloat16))
        return attended, projected, (q, k, v, total)

    def backward(kept, grad_own):
        q, k, v, total = kept
        grad_all = gather_dp(grad_own)
        grad = contract(grad_all, w_out, 1, 1).astype(jnp.bfloat16)
        shape = grad.shape
        grad = heads(grad)
        weights = jnp.exp(score_block(q, k) - total)
        grad_weights = jnp.einsum("shd,lhd->hsl", grad, v, preferred_element_type=jnp.float32)
        delta = jnp.sum(weights * grad_weights, axis=-1, keepdims=True)
        grad_scores = (weights * (grad_weights - delta)).astype(jnp.bfloat16)
        dq = jnp.einsum("hsl,lhd->shd", grad_scores, k, preferred_element_type=jnp.float32)
        dk = jnp.einsum("hsl,shd->lhd", grad_scores, q, preferred_element_type=jnp.float32)
        weights = weights.astype(jnp.bfloat16)
        dv = jnp.einsum("hsl,shd->lhd", weights, grad, preferred_element_type=jnp.float32)

        def to_owner(part):
            part = part.astype(jnp.bfloat16).reshape(pack, shape[1])
            return lax.psum_scatter(part, "expert", scatter_dimension=0, tiled=True)

        scale = HD ** (-0.5)
        dq = (dq * scale).reshape(shape)
        dq = dq.astype(jnp.bfloat16)
        return grad_all, [], [dq, to_owner(dk * scale), to_owner(dv)]

    return forward, backward


def nearest(line, z, k):
    return ranked(line, z, k, lambda place, at: (abs(place - at), place))


def ranked(line, z, k, rank):
    total = jnp.int32(0)
    for at in range(line):
        order = sorted(range(line), key=lambda place: rank(place, at))
        place = sum([jnp.where(k == i, order[i], 0) for i in range(line)])
        total = total + jnp.where(z == at, place, 0)
    return total


def gate_act_kernel(
    line,
    x_ref,
    top_ref,
    wg_ref,
    wu_ref,
    wd_ref,
    xn_ref,
    grads_ref,
    scaled_ref,
    gates_ref,
    xbuf,
    top_buf,
    grads_buf,
    scaled_buf,
    gates_buf,
    sent,
    arrived,
    own_sem,
    top_sem,
    xn_sem,
    grads_sem,
    scaled_sem,
    gates_sem,
):
    dp, place = lax.axis_index("dp"), lax.axis_index("expert")
    z, c = place // 2, place % 2
    side_x, side_y = corners(dp)
    far = 3 - dp
    devices = (
        (dp, place + 2),
        (dp, place - 2),
        (side_x, place),
        (side_y, place),
        (dp, 2 * z + 1 - c),
    )
    up, down, along_x, along_y, pair = range(5)
    has_up, has_down = z < line - 1, z > 0
    for way in (along_x, along_y, pair):
        greet(devices[way])
    pl.when(has_up)(lambda: greet(devices[up]))
    pl.when(has_down)(lambda: greet(devices[down]))
    greeted = 3 + has_up.astype(jnp.int32) + has_down.astype(jnp.int32)
    pl.semaphore_wait(pltpu.get_barrier_semaphore(), greeted)
    local, width, units = wg_ref.shape
    rows = top_buf.shape[1]
    first = place * local

    def slot(corner, height, core):
        return corner * (2 * line) + 2 * height + core

    def copy(s, p, way, source=None):
        target = xbuf.at[s, p]
        return send(
            target if source is None else source,
            target,
            sent.at[s, p, way],
            arrived.at[s, p],
            devices[way],
        )

    def arrive(s, p):
        copy(s, p, pair).wait_recv()

    mine = slot(dp, z, c)
    for p in (0, 1):
        pltpu.make_async_copy(x_ref.at[p], xbuf.at[mine, p], own_sem.at[p]).start()
        pl.when(has_up)(lambda: copy(mine, p, up, x_ref.at[p]).start())
        pl.when(has_down)(lambda: copy(mine, p, down, x_ref.at[p]).start())
        for way in (along_x, along_y, pair):
            copy(mine, p, way, x_ref.at[p]).start()

    def decode(i):
        turn, j = i // 4, i % 4
        k = turn - (j > 0).astype(jnp.int32) - (j == 3).astype(jnp.int32)
        valid = (i >= 0) & (k >= 0) & (k < line)
        corner = jnp.where(j == 0, dp, jnp.where(j == 1, side_x, jnp.where(j == 2, side_y, far)))
        return j, k, valid, corner, nearest(line, z, k)

    def top_load(i, corner, height):
        block = corner * line + height
        return pltpu.make_async_copy(top_ref.at[block], top_buf.at[i % 2], top_sem.at[i % 2])

    def xn_out(block):
        return pltpu.make_async_copy(
            xbuf.at[pl.ds(2 * block, 2), :, :, pl.ds(0, width)],
            xn_ref.at[pl.ds(2 * block, 2)],
            xn_sem.at[block],
        )

    def grads_out(block):
        return pltpu.make_async_copy(grads_buf.at[block], grads_ref.at[block], grads_sem.at[block])

    def scaled_out(block):
        return pltpu.make_async_copy(
            scaled_buf.at[block], scaled_ref.at[block], scaled_sem.at[block]
        )

    def gates_out(block):
        return pltpu.make_async_copy(gates_buf.at[block], gates_ref.at[block], gates_sem.at[block])

    def compute(i):
        j, k, _, corner, height = decode(i)
        block = corner * line + height
        for p in (0, 1):
            arrive(slot(corner, height, 1 - c), p)
        xn_out(block).start()
        top_load(i, corner, height).wait()
        lanes = lax.broadcasted_iota(jnp.int32, (rows, 128), 1)

        def tokens():
            return xbuf[pl.ds(2 * block, 2), :, :, pl.ds(0, width)].reshape(rows, width)

        table = xbuf[pl.ds(2 * block, 2), :, :, pl.ds(width, 128)].reshape(rows, 128)
        table = table.astype(jnp.float32)
        gate_grads = jnp.zeros((rows, 128), jnp.float32)
        for e in range(local):
            at = (lanes == first + e) | (lanes == first + e + 64)
            gate = jnp.sum(jnp.where(at, table, 0.0), axis=1, keepdims=True)
            g = contract(tokens(), wg_ref[e], 1, 0)
            u = contract(tokens(), wu_ref[e], 1, 0)
            h = contract(top_buf[i % 2], wd_ref[e], 1, 1)
            sigmoid = 1.0 / (1.0 + jnp.exp(-g))
            silu = g * sigmoid
            act = silu * u
            gate_grad = jnp.sum(act * h, axis=1, keepdims=True)
            gate_grads = gate_grads + jnp.where(lanes == first + e, gate_grad, 0.0)
            grad_act = h * gate
            dg = grad_act * u * sigmoid * (1.0 + g * (1.0 - sigmoid))
            du = grad_act * silu
            scaled_buf[block, :, e * units : (e + 1) * units] = (act * gate).astype(jnp.bfloat16)
            grads_buf[block, :, e * units : (e + 1) * units] = dg.astype(jnp.bfloat16)
            at = (local + e) * units
            grads_buf[block, :, at : at + units] = du.astype(jnp.bfloat16)
        gates_buf[block] = gate_grads.astype(jnp.bfloat16)
        grads_out(block).start()
        scaled_out(block).start()
        gates_out(block).start()

    def step(i, carry):
        j, k, valid, corner, height = decode(i)
        s = slot(corner, height, c)

        def own():
            for p in (0, 1):
                pltpu.make_async_copy(x_ref.at[p], xbuf.at[mine, p], own_sem.at[p]).wait()

        def column():
            for p in (0, 1):
                arrive(s, p)
                pl.when(has_up & (height < z))(lambda: copy(s, p, up).start())
                pl.when(has_down & (height > z))(lambda: copy(s, p, down).start())
                for way in (along_x, along_y, pair):
                    copy(s, p, way).start()

        def sides():
            for p in (0, 1):
                arrive(s, p)
                copy(s, p, pair).start()
            pl.when(j == 1)(lambda: copy(s, 0, along_y).start())
            pl.when(j == 2)(lambda: copy(s, 1, along_x).start())

        def opposite():
            for p in (0, 1):
                arrive(s, p)
                copy(s, p, pair).start()

        pl.when(valid & (j == 0) & (k == 0))(own)
        pl.when(valid & (j == 0) & (k > 0))(column)
        pl.when(valid & ((j == 1) | (j == 2)))(sides)
        pl.when(valid & (j == 3))(opposite)
        pl.when(valid)(lambda: top_load(i, corner, height).start())
        pl.when(decode(i - 1)[2])(lambda: compute(i - 1))
        return carry

    lax.fori_loop(0, 4 * (line + 2) + 1, step, 0)

    def finish(height, carry):
        for p in (0, 1):
            for corner in range(4):
                copy(slot(corner, height, c), p, pair).wait_send()
            s = slot(dp, height, c)
            copy(s, p, along_x).wait_send()
            copy(s, p, along_y).wait_send()
            pl.when(has_up & (height <= z))(lambda: copy(s, p, up).wait_send())
            pl.when(has_down & (height >= z))(lambda: copy(s, p, down).wait_send())
        copy(slot(side_x, height, c), 0, along_y).wait_send()
        copy(slot(side_y, height, c), 1, along_x).wait_send()
        for corner in range(4):
            block = corner * line + height
            xn_out(block).wait()
            grads_out(block).wait()
            scaled_out(block).wait()
            gates_out(block).wait()
        return carry

    lax.fori_loop(0, line, finish, 0)


def gate_act(own, tops, w_gate, w_up, w_down, line):
    count, wide = own.shape
    local, width, units = w_gate.shape
    slots, blocks, rows, half = 8 * line, 4 * line, 2 * count, count // 2
    sems = pltpu.SemaphoreType.DMA
    dtype = own.dtype
    xn, grads, scaled, gates = pl.pallas_call(
        functools.partial(gate_act_kernel, line),
        out_shape=[
            jax.ShapeDtypeStruct((slots, 2, half, width), dtype),
            jax.ShapeDtypeStruct((blocks, rows, 2 * local * units), dtype),
            jax.ShapeDtypeStruct((blocks, rows, local * units), dtype),
            jax.ShapeDtypeStruct((blocks, rows, 128), dtype),
        ],
        in_specs=[
            pl.BlockSpec(memory_space=pltpu.VMEM),
            pl.BlockSpec(memory_space=pl.ANY),
            pl.BlockSpec(memory_space=pltpu.VMEM),
            pl.BlockSpec(memory_space=pltpu.VMEM),
            pl.BlockSpec(memory_space=pltpu.VMEM),
        ],
        out_specs=[pl.BlockSpec(memory_space=pl.ANY)] * 4,
        scratch_shapes=[
            pltpu.VMEM((slots, 2, half, wide), dtype),
            pltpu.VMEM((2, rows, width), dtype),
            pltpu.VMEM((blocks, rows, 2 * local * units), dtype),
            pltpu.VMEM((blocks, rows, local * units), dtype),
            pltpu.VMEM((blocks, rows, 128), dtype),
            sems((slots, 2, 5)),
            sems((slots, 2)),
            sems((2,)),
            sems((2,)),
            sems((blocks,)),
            sems((blocks,)),
            sems((blocks,)),
            sems((blocks,)),
        ],
        compiler_params=pltpu.CompilerParams(
            collective_id=1, has_side_effects=True, vmem_limit_bytes=60 << 20
        ),
        name="gate_act",
    )(own.reshape(2, half, wide), tops.reshape(blocks, rows, width), w_gate, w_up, w_down)
    return xn.reshape(slots * count, width), grads, scaled, gates


def column_products(left_ref, right_ref, chunk_buf, right_buf, total, chunk_sem, right_sem, store):
    span = chunk_buf.shape[2]
    blocks, rows, _ = right_buf.shape
    joined = max(1, min(blocks, 1024 // rows))
    depth = joined * rows
    turns = left_ref.shape[1] // span

    def at(n):
        return pl.ds(pl.multiple_of(n * span, span), span)

    def chunk(n):
        return pltpu.make_async_copy(
            left_ref.at[:, at(n)], chunk_buf.at[n % 2], chunk_sem.at[n % 2]
        )

    right_load = pltpu.make_async_copy(right_ref, right_buf, right_sem.at[0])
    chunk(0).start()
    right_load.start()

    def turn(n):
        pl.when(n + 1 < turns)(lambda: chunk(n + 1).start())
        chunk(n).wait()
        pl.when(n == 0)(right_load.wait)
        total[...] = jnp.zeros_like(total)

        def part(k, carry):
            left = chunk_buf[n % 2, pl.ds(pl.multiple_of(k * depth, depth), depth), :]
            right = right_buf[pl.ds(k * joined, joined)].reshape(depth, right_buf.shape[2])
            total[...] += contract(left, right, 0, 0)
            return carry

        lax.fori_loop(0, blocks // joined, part, 0)
        store(n, at(n))

    return turn, turns


def gate_up_grads(
    xn_ref, units_ref, gate_ref, up_ref, chunk_buf, units_buf, total, both, chunk_sem, units_sem, out_sem
):
    local, _, units = gate_ref.shape
    outs = (gate_ref, up_ref)

    def copies(at):
        return [
            pltpu.make_async_copy(
                both.at[:, pl.ds((kind * local + e) * units, units)],
                outs[kind].at[e, at, :],
                out_sem.at[kind, e],
            )
            for kind in (0, 1)
            for e in range(local)
        ]

    start = pl.ds(0, chunk_buf.shape[2])

    def store(n, at):
        @pl.when(n > 0)
        def _():
            for copy in copies(start):
                copy.wait()

        both[...] = total[...].astype(both.dtype)
        for copy in copies(at):
            copy.start()

    def end():
        for copy in copies(start):
            copy.wait()

    turn, turns = column_products(
        xn_ref, units_ref, chunk_buf, units_buf, total, chunk_sem, units_sem, store
    )
    return turn, end, turns


def down_grads(
    top_ref, scaled_ref, down_ref, chunk_buf, scaled_buf, total, out, chunk_sem, scaled_sem, out_sem
):
    local, units, _ = down_ref.shape

    def copies(at):
        return [
            pltpu.make_async_copy(out.at[e], down_ref.at[e, :, at], out_sem.at[e])
            for e in range(local)
        ]

    start = pl.ds(0, chunk_buf.shape[2])

    def store(n, at):
        @pl.when(n > 0)
        def _():
            for copy in copies(start):
                copy.wait()

        for e in range(local):
            out[e] = total[:, e * units : (e + 1) * units].T.astype(out.dtype)
        for copy in copies(at):
            copy.start()

    def end():
        for copy in copies(start):
            copy.wait()

    turn, turns = column_products(
        top_ref, scaled_ref, chunk_buf, scaled_buf, total, chunk_sem, scaled_sem, store
    )
    return turn, end, turns


SPAN = 256


def product_sum_kernel(
    line,
    flipped,
    extra,
    grads,
    summed,
    *refs,
):
    a_ref, w_ref = refs[0], refs[1]
    e_ref = refs[2] if extra else None
    refs = refs[3:] if extra else refs[2:]
    w_loads = []
    if flipped:
        up_ref, *refs, w_buf, w_sem = refs
        experts, _, units = w_ref.shape
        for kind, source in enumerate((w_ref, up_ref)):
            for e in range(experts):
                at = kind * experts + e
                target = w_buf.at[:, at * units : (at + 1) * units]
                w_loads.append(pltpu.make_async_copy(source.at[e], target, w_sem.at[at]))
        w_ref = w_buf
        for copy in w_loads:
            copy.start()
    heads = len(summed)
    if heads:
        head_ins, head_refs = refs[2 : 2 + heads], refs[-7:]
        head_outs = refs[5 + heads : 5 + 2 * heads]
        refs = (*refs[:2], *refs[2 + heads : 5 + heads], *refs[5 + 2 * heads : -7])
    if grads:
        work_refs, refs = (*refs[:2], *refs[3:5], *refs[-7:]), (refs[2], *refs[5:-7])
    (
        out_ref,
        made,
        a_buf,
        e_buf,
        got_pair,
        got_x,
        got_y,
        got_far_x,
        got_far_y,
        got_below,
        got_above,
        load_sem,
        extra_sem,
        pair_sem,
        x_sem,
        y_sem,
        far_x_sem,
        far_y_sem,
        below_sem,
        above_sem,
    ) = refs
    dp, place = lax.axis_index("dp"), lax.axis_index("expert")
    z, c = place // 2, place % 2
    side_x, side_y = corners(dp)
    far = 3 - dp
    to_x, to_y, to_pair = (side_x, place), (side_y, place), (dp, 2 * z + 1 - c)
    to_up, to_down = (dp, place + 2), (dp, place - 2)
    for device in (to_x, to_y, to_pair):
        greet(device)
    if heads:
        visit_others(line, z, lambda other: greet((dp, 2 * other + c)))
        greeted = 2 + line
    else:
        pl.when(z > 0)(lambda: greet(to_down))
        pl.when(z < line - 1)(lambda: greet(to_up))
        greeted = 3 + (z > 0).astype(jnp.int32) + (z < line - 1).astype(jnp.int32)
    pl.semaphore_wait(pltpu.get_barrier_semaphore(), greeted)
    count = 4 * line
    width = w_ref.shape[0] if flipped else w_ref.shape[1]
    half = made.shape[4]
    chunk = 512

    def mine(q, height, p):
        return made.at[q, height, c, p]

    def hand(q, height, p):
        at = (q, height, p)
        source = made.at[q, height, 1 - c, p]
        return send(source, got_pair.at[at], pair_sem.at[0, *at], pair_sem.at[1, *at], to_pair)

    def along_x(height, p):
        at = (height, p)
        source = mine(side_x, height, p)
        return send(source, got_x.at[at], x_sem.at[0, *at], x_sem.at[1, *at], to_x)

    def along_y(height, p):
        at = (height, p)
        source = mine(side_y, height, p)
        return send(source, got_y.at[at], y_sem.at[0, *at], y_sem.at[1, *at], to_y)

    def far_x(height):
        source = mine(far, height, 0)
        return send(
            source, got_far_x.at[height], far_x_sem.at[0, height], far_x_sem.at[1, height], to_x
        )

    def far_y(height):
        source = mine(far, height, 1)
        return send(
            source, got_far_y.at[height], far_y_sem.at[0, height], far_y_sem.at[1, height], to_y
        )

    def climb(height, p):
        at = (height, p)
        source = mine(dp, height, p)
        return send(source, got_below.at[at], below_sem.at[0, *at], below_sem.at[1, *at], to_up)

    def descend(height, p):
        at = (height, p)
        source = mine(dp, height, p)
        return send(source, got_above.at[at], above_sem.at[0, *at], above_sem.at[1, *at], to_down)

    def decode(i):
        k, j = i // 4, i % 4
        q = jnp.where(j == 0, far, jnp.where(j == 1, side_x, jnp.where(j == 2, side_y, dp)))
        return k, j, q, farthest(line, z, k)

    def load(i):
        _, _, q, height = decode(i)
        return pltpu.make_async_copy(
            a_ref.at[q * line + height], a_buf.at[i % 2], load_sem.at[i % 2]
        )

    def load_extra(i):
        _, _, q, height = decode(i)
        return pltpu.make_async_copy(
            e_ref.at[q * line + height], e_buf.at[i % 2], extra_sem.at[i % 2]
        )

    def start_load(i):
        load(i).start()
        if extra:
            load_extra(i).start()

    def add(q, height, p, other):
        at = (q, height, c, p)
        made[at] = made[at] + other[...]

    def compute(i):
        _, _, q, height = decode(i)
        load(i).wait()
        if extra:
            load_extra(i).wait()
        pl.when(i + 1 < count)(lambda: start_load(i + 1))
        for at in range(0, width, chunk):
            if flipped:
                part = contract(a_buf[i % 2], w_ref[at : at + chunk, :], 1, 1)
            else:
                part = contract(a_buf[i % 2], w_ref[:, at : at + chunk], 1, 0)
            part = part.astype(made.dtype).reshape(2, 2, half, chunk)
            made[q, height, :, :, :, at : at + chunk] = part
        if extra:
            made[q, height, :, :, :, width : width + 128] = e_buf[i % 2].reshape(2, 2, half, 128)
        for p in (0, 1):
            hand(q, height, p).start()

    def settle(i):
        _, j, q, height = decode(i)
        for p in (0, 1):
            hand(q, height, p).wait_recv()
            add(q, height, p, got_pair.at[q, height, p])

        def opposite():
            far_x(height).start()
            far_y(height).start()

        pl.when(j == 0)(opposite)
        pl.when(j == 1)(lambda: along_x(height, 0).start())
        pl.when(j == 2)(lambda: along_y(height, 1).start())

    def settle_far(i):
        _, j, _, height = decode(i)

        def side_of_x():
            far_y(height).wait_recv()
            add(side_x, height, 1, got_far_y.at[height])
            along_x(height, 1).start()

        def side_of_y():
            far_x(height).wait_recv()
            add(side_y, height, 0, got_far_x.at[height])
            along_y(height, 0).start()

        pl.when(j == 1)(side_of_x)
        pl.when(j == 2)(side_of_y)

    def column(height):
        for p in (0, 1):
            along_x(height, p).wait_recv()
            along_y(height, p).wait_recv()
            total = made[dp, height, c, p].astype(jnp.float32)
            total = total + got_x[height, p].astype(jnp.float32)
            total = total + got_y[height, p].astype(jnp.float32)
            made[dp, height, c, p] = total.astype(made.dtype)
            pl.when((z == 0) & (height > z))(lambda: climb(height, p).start())
            pl.when((z == line - 1) & (height < z))(lambda: descend(height, p).start())

    def pass_on(height):
        for p in (0, 1):

            def upwards():
                climb(height, p).wait_recv()
                add(dp, height, p, got_below.at[height, p])
                climb(height, p).start()

            def downwards():
                descend(height, p).wait_recv()
                add(dp, height, p, got_above.at[height, p])
                descend(height, p).start()

            pl.when((height > z) & (z > 0))(upwards)
            pl.when((height < z) & (z < line - 1))(downwards)

    start_load(0)
    for copy in w_loads:
        copy.wait()
    if heads:
        begin, dispatch, heads_end = head_return(line, summed, head_ins, head_outs, *head_refs)
        begin()
    work, work_end, turns = gate_up_grads(*work_refs) if grads else (None, None, 1)

    def step(i, carry):
        k, j, _, _ = decode(i)
        pl.when(i < count)(lambda: compute(i))
        pl.when((i >= 1) & (i <= count))(lambda: settle(i - 1))
        if grads:
            every = count // turns
            pl.when((i < count) & (i % every == 0))(lambda: work(i // every))
        if heads:
            pl.when(i < line)(lambda: dispatch(i))
        pl.when((i >= 4) & (i < count + 4))(lambda: settle_far(i - 4))
        pl.when((k >= 3) & (j == 2))(lambda: pass_on(farthest(line, z, k - 3)))
        pl.when((k >= 2) & (j == 3))(lambda: column(farthest(line, z, k - 2)))
        return carry

    lax.fori_loop(0, count + 8, step, 0)
    if heads:
        heads_end()
    if grads:
        work_end()
    for p in (0, 1):
        out_ref[p] = made[dp, z, c, p].astype(jnp.float32)

        def from_below():
            climb(z, p).wait_recv()
            out_ref[p] = out_ref[p] + got_below[z, p].astype(jnp.float32)

        def from_above():
            descend(z, p).wait_recv()
            out_ref[p] = out_ref[p] + got_above[z, p].astype(jnp.float32)

        pl.when(z > 0)(from_below)
        pl.when(z < line - 1)(from_above)

    def finish(height, carry):
        far_x(height).wait_send()
        far_y(height).wait_send()
        for p in (0, 1):
            for q in range(4):
                hand(q, height, p).wait_send()
            along_x(height, p).wait_send()
            along_y(height, p).wait_send()
            pl.when(height > z)(lambda: climb(height, p).wait_send())
            pl.when(height < z)(lambda: descend(height, p).wait_send())
        return carry

    lax.fori_loop(0, line, finish, 0)


def product_sum(
    blocks, weights, flipped, extra, line, name, number, grads=None, heads=(), summed=()
):
    count, rows, depth = blocks.shape
    width = weights[0].shape[1] if flipped else weights.shape[1]
    wide = width + (0 if extra is None else 128)
    half = rows // 4
    sems = pltpu.SemaphoreType.DMA
    dtype = blocks.dtype

    def space(*shape):
        return pltpu.VMEM((*shape, half, wide), dtype)

    anywhere, inside = pl.BlockSpec(memory_space=pl.ANY), pl.BlockSpec(memory_space=pltpu.VMEM)
    out_shape = [jax.ShapeDtypeStruct((2, half, wide), jnp.float32)]
    work_in, work_space = [], []
    if grads is not None:
        xn, both, shape = grads
        work_in = [xn, both]
        out_shape += [jax.ShapeDtypeStruct(shape, dtype)] * 2
        work_space = [
            pltpu.VMEM((2, xn.shape[0], SPAN), dtype),
            pltpu.VMEM(both.shape, dtype),
            pltpu.VMEM((SPAN, both.shape[2]), jnp.float32),
            pltpu.VMEM((SPAN, both.shape[2]), dtype),
            sems((2,)),
            sems((1,)),
            sems((2, shape[0])),
        ]
    if heads:
        tokens = jax.ShapeDtypeStruct((heads[0].shape[-2], line * HD), dtype)
        work_in += heads
        out_shape += [tokens] * len(heads)
        work_space += head_return_space(heads, summed, line)
    total, *work_out = pl.pallas_call(
        functools.partial(
            product_sum_kernel, line, flipped, extra is not None, grads is not None, summed
        ),
        out_shape=out_shape,
        in_specs=[anywhere, anywhere if flipped else inside]
        + ([] if extra is None else [anywhere])
        + [anywhere] * (len(work_in) + flipped),
        out_specs=[inside] + [anywhere] * (len(out_shape) - 1),
        scratch_shapes=[
            space(4, line, 2, 2),
            pltpu.VMEM((2, rows, depth), dtype),
            pltpu.VMEM((2, rows, 128), dtype),
            space(4, line, 2),
            space(line, 2),
            space(line, 2),
            space(line),
            space(line),
            space(line, 2),
            space(line, 2),
            sems((2,)),
            sems((2,)),
            sems((2, 4, line, 2)),
            sems((2, line, 2)),
            sems((2, line, 2)),
            sems((2, line)),
            sems((2, line)),
            sems((2, line, 2)),
            sems((2, line, 2)),
            *work_space,
            *(
                [pltpu.VMEM((width, depth), dtype), sems((2 * weights[0].shape[0],))]
                if flipped
                else []
            ),
        ],
        compiler_params=pltpu.CompilerParams(
            collective_id=number, has_side_effects=True, vmem_limit_bytes=63 << 20
        ),
        name=name,
    )(
        blocks,
        weights[0] if flipped else weights,
        *([] if extra is None else [extra]),
        *([weights[1]] if flipped else []),
        *work_in,
    )
    return total.reshape(2 * half, wide), *work_out


def closing_kernel(
    line,
    shared_rows,
    parts_ref,
    small_ref,
    first_ref,
    grad_ref,
    unit_ref,
    inverse_ref,
    gain_ref,
    output_ref,
    top_ref,
    scaled_ref,
    summed_ref,
    shared_ref,
    outputs_ref,
    grads_ref,
    down_ref,
    acc,
    got_pair,
    got_below,
    got_above,
    part,
    got_x,
    got_y,
    got_far_x,
    got_far_y,
    grad_own,
    small,
    got_small,
    load_sem,
    pair_sem,
    load_small_sem,
    pair_small_sem,
    below_sem,
    above_sem,
    part_sem,
    x_sem,
    y_sem,
    far_x_sem,
    far_y_sem,
    spread_sem,
    arrive_sem,
    own_sem,
    small_sem,
    *work_refs,
):
    dp, place = lax.axis_index("dp"), lax.axis_index("expert")
    z, c = place // 2, place % 2
    side_x, side_y = corners(dp)
    far = 3 - dp
    to_x, to_y, to_pair = (side_x, place), (side_y, place), (dp, 2 * z + 1 - c)
    to_up, to_down = (dp, place + 2), (dp, place - 2)
    for device in (to_x, to_y, to_pair):
        greet(device)
    pl.when(z > 0)(lambda: greet(to_down))
    pl.when(z < line - 1)(lambda: greet(to_up))
    greeted = 3 + (z > 0).astype(jnp.int32) + (z < line - 1).astype(jnp.int32)
    pl.semaphore_wait(pltpu.get_barrier_semaphore(), greeted)

    large = parts_ref.shape[3]
    top_rows, low_rows = pl.ds(0, large), pl.ds(large, shared_rows // 2)

    def loads(height, p):
        return (
            pltpu.make_async_copy(
                parts_ref.at[height, c, p], acc.at[height, p, top_rows], load_sem.at[height, p]
            ),
            pltpu.make_async_copy(
                small_ref.at[height, c, p], acc.at[height, p, low_rows], load_small_sem.at[height, p]
            ),
        )

    def hands(height, p):
        at = (height, p)
        return (
            send(
                parts_ref.at[height, 1 - c, p],
                got_pair.at[height, p, top_rows],
                pair_sem.at[0, *at],
                pair_sem.at[1, *at],
                to_pair,
            ),
            send(
                small_ref.at[height, 1 - c, p],
                got_pair.at[height, p, low_rows],
                pair_small_sem.at[0, *at],
                pair_small_sem.at[1, *at],
                to_pair,
            ),
        )

    def climb(height, p):
        at = (height, p)
        return send(
            acc.at[at], got_below.at[at], below_sem.at[0, *at], below_sem.at[1, *at], to_up
        )

    def descend(height, p):
        at = (height, p)
        return send(
            acc.at[at], got_above.at[at], above_sem.at[0, *at], above_sem.at[1, *at], to_down
        )

    def start(k, carry):
        height = farthest(line, z, k)
        for p in (0, 1):
            for copy in (*loads(height, p), *hands(height, p)):
                copy.start()
        return carry

    def pair_sum(k, carry):
        height = farthest(line, z, k)
        for p in (0, 1):
            for copy in loads(height, p):
                copy.wait()
            for copy in hands(height, p):
                copy.wait_recv()
            acc[height, p] = acc[height, p] + got_pair[height, p]
            pl.when((z == 0) & (height > z))(lambda: climb(height, p).start())
            pl.when((z == line - 1) & (height < z))(lambda: descend(height, p).start())
        return carry

    def pass_on(k, carry):
        height = farthest(line, z, k)
        for p in (0, 1):

            def upwards():
                climb(height, p).wait_recv()
                acc[height, p] = acc[height, p] + got_below[height, p]
                climb(height, p).start()

            def downwards():
                descend(height, p).wait_recv()
                acc[height, p] = acc[height, p] + got_above[height, p]
                descend(height, p).start()

            pl.when((height > z) & (z > 0))(upwards)
            pl.when((height < z) & (z < line - 1))(downwards)
        return carry

    def first_load(q, p):
        return pltpu.make_async_copy(first_ref.at[q, p], part.at[q, p], part_sem.at[q, p])

    def along_x(p):
        return send(part.at[side_x, p], got_x.at[p], x_sem.at[0, p], x_sem.at[1, p], to_x)

    def along_y(p):
        return send(part.at[side_y, p], got_y.at[p], y_sem.at[0, p], y_sem.at[1, p], to_y)

    def far_x():
        return send(part.at[far, 0], got_far_x, far_x_sem.at[0], far_x_sem.at[1], to_x)

    def far_y():
        return send(part.at[far, 1], got_far_y, far_y_sem.at[0], far_y_sem.at[1], to_y)

    spreads = ((output_ref, outputs_ref), (grad_own, grads_ref))

    def spread(a, corner, p, way, source=None):
        target = spreads[a][1].at[corner, p]
        return send(
            target if source is None else source,
            target,
            spread_sem.at[a, corner, p, way],
            arrive_sem.at[a, corner, p],
            (to_x, to_y)[way],
        )

    def own_copy(a, p):
        return pltpu.make_async_copy(
            spreads[a][0].at[p], spreads[a][1].at[dp, p], own_sem.at[a, p]
        )

    def spread_own(a, p):
        own_copy(a, p).start()
        for way in (0, 1):
            spread(a, dp, p, way, spreads[a][0].at[p]).start()

    def spread_far(a):
        spread(a, side_x, 0, 0).wait_recv()
        spread(a, side_x, 0, 1).start()
        spread(a, side_y, 1, 0).wait_recv()
        spread(a, side_y, 1, 0).start()

    work, work_end, turns = down_grads(top_ref, scaled_ref, down_ref, *work_refs)
    pauses = 4

    def meanwhile(i):
        def turn(n, carry):
            work(n)
            return carry

        lax.fori_loop(turns * i // pauses, turns * (i + 1) // pauses, turn, 0)

    lax.fori_loop(0, 1, start, 0)
    for q in (far, side_x, side_y, dp):
        for p in (0, 1):
            first_load(q, p).start()
    lax.fori_loop(1, line, start, 0)
    for q in (far, side_x, side_y, dp):
        for p in (0, 1):
            first_load(q, p).wait()
    far_x().start()
    far_y().start()
    along_x(0).start()
    along_y(1).start()
    lax.fori_loop(0, 1, pair_sum, 0)
    far_x().wait_recv()
    part[side_y, 0] = part[side_y, 0] + got_far_x[...]
    along_y(0).start()
    far_y().wait_recv()
    part[side_x, 1] = part[side_x, 1] + got_far_y[...]
    along_x(1).start()
    for p in (0, 1):
        spread_own(0, p)
    lax.fori_loop(1, line, pair_sum, 0)
    meanwhile(0)
    lax.fori_loop(0, 1, pass_on, 0)
    for p in (0, 1):
        along_x(p).wait_recv()
        along_y(p).wait_recv()
        total = part[dp, p].astype(jnp.float32)
        total = total + got_x[p].astype(jnp.float32) + got_y[p].astype(jnp.float32)
        total = total * gain_ref[...]
        unit = unit_ref[p]
        mean = jnp.sum(total * unit, axis=1, keepdims=True) * (1.0 / unit.shape[1])
        rows = grad_ref[p] + inverse_ref[p] * (total - unit * mean)
        grad_own[p] = rows.astype(grad_own.dtype)
        spread_own(1, p)
    meanwhile(1)
    spread_far(0)
    lax.fori_loop(1, 2, pass_on, 0)
    spread_far(1)
    meanwhile(2)
    lax.fori_loop(2, line, pass_on, 0)
    meanwhile(3)
    for p in (0, 1):
        summed_ref[p] = acc[z, p].astype(jnp.float32)

        def from_below():
            climb(z, p).wait_recv()
            summed_ref[p] = summed_ref[p] + got_below[z, p].astype(jnp.float32)

        def from_above():
            descend(z, p).wait_recv()
            summed_ref[p] = summed_ref[p] + got_above[z, p].astype(jnp.float32)

        pl.when(z > 0)(from_below)
        pl.when(z < line - 1)(from_above)

    for side, device in enumerate((to_x, to_y)):
        value = summed_ref[:, large:, :] if side == 0 else shared_ref[...]
        small[side] = value.astype(small.dtype)
        spread(side, side_x, 1, 0).wait_recv()
        spread(side, side_y, 0, 0).wait_recv()
        for p in (0, 1):
            spread(side, far, p, 0).wait_recv()
            for way in (0, 1):
                spread(side, dp, p, way).wait_send()
            own_copy(side, p).wait()
        spread(side, side_x, 0, 1).wait_send()
        spread(side, side_y, 1, 0).wait_send()
        exchange = send(
            small.at[side], got_small.at[side], small_sem.at[0, side], small_sem.at[1, side], device
        )
        exchange.start()
        exchange.wait_recv()
        shared_ref[...] = small[side].astype(jnp.float32) + got_small[side].astype(jnp.float32)
        exchange.wait_send()

    far_x().wait_send()
    far_y().wait_send()
    for p in (0, 1):
        along_x(p).wait_send()
        along_y(p).wait_send()

    def finish(height, carry):
        for p in (0, 1):
            for copy in hands(height, p):
                copy.wait_send()
            pl.when(height > z)(lambda: climb(height, p).wait_send())
            pl.when(height < z)(lambda: descend(height, p).wait_send())
        return carry

    lax.fori_loop(0, line, finish, 0)
    work_end()


def closing(parts, small, first, grad, unit, inverse, gain, output, tops, scaled, shape, line):
    _, rows, wide = parts.shape
    shared_rows = small.shape[1]
    own, width = output.shape
    high, half = (rows + shared_rows) // 2, own // 2
    local, units, _ = shape
    sems = pltpu.SemaphoreType.DMA
    dtype = parts.dtype
    single = jnp.float32
    anywhere, inside = pl.BlockSpec(memory_space=pl.ANY), pl.BlockSpec(memory_space=pltpu.VMEM)
    everyone = jax.ShapeDtypeStruct((4, 2, half, width), dtype)
    summed, shared, outputs, grads, down = pl.pallas_call(
        functools.partial(closing_kernel, line, shared_rows),
        out_shape=[
            jax.ShapeDtypeStruct((2, high, wide), single),
            jax.ShapeDtypeStruct((2, shared_rows // 2, wide), single),
            everyone,
            everyone,
            jax.ShapeDtypeStruct(shape, dtype),
        ],
        in_specs=[anywhere] * 3 + [inside] * 5 + [anywhere] * 2,
        out_specs=[inside, inside, anywhere, anywhere, anywhere],
        scratch_shapes=[
            pltpu.VMEM((line, 2, high, wide), dtype),
            pltpu.VMEM((line, 2, high, wide), dtype),
            pltpu.VMEM((line, 2, high, wide), dtype),
            pltpu.VMEM((line, 2, high, wide), dtype),
            pltpu.VMEM((4, 2, half, width), dtype),
            pltpu.VMEM((2, half, width), dtype),
            pltpu.VMEM((2, half, width), dtype),
            pltpu.VMEM((half, width), dtype),
            pltpu.VMEM((half, width), dtype),
            pltpu.VMEM((2, half, width), dtype),
            pltpu.VMEM((2, 2, shared_rows // 2, wide), dtype),
            pltpu.VMEM((2, 2, shared_rows // 2, wide), dtype),
            sems((line, 2)),
            sems((2, line, 2)),
            sems((line, 2)),
            sems((2, line, 2)),
            sems((2, line, 2)),
            sems((2, line, 2)),
            sems((4, 2)),
            sems((2, 2)),
            sems((2, 2)),
            sems((2,)),
            sems((2,)),
            sems((2, 4, 2, 2)),
            sems((2, 4, 2)),
            sems((2, 2)),
            sems((2, 2)),
            pltpu.VMEM((2, tops.shape[0], SPAN), dtype),
            pltpu.VMEM(scaled.shape, dtype),
            pltpu.VMEM((SPAN, local * units), single),
            pltpu.VMEM((local, units, SPAN), dtype),
            sems((2,)),
            sems((1,)),
            sems((local,)),
        ],
        compiler_params=pltpu.CompilerParams(
            collective_id=5, has_side_effects=True, vmem_limit_bytes=60 << 20
        ),
        name="closing",
    )(
        parts.reshape(line, 2, 2, rows // 2, wide),
        small.reshape(line, 2, 2, shared_rows // 2, wide),
        first.reshape(4, 2, half, width),
        grad.reshape(2, half, width),
        unit.reshape(2, half, width),
        inverse.reshape(2, half, 1),
        gain.reshape(1, width),
        output.reshape(2, half, width),
        tops,
        scaled,
    )
    return (
        summed[:, : rows // 2].reshape(rows, wide),
        summed[:, rows // 2 :],
        shared,
        outputs.reshape(4 * own, width),
        grads.reshape(4 * own, width),
        down,
    )


def square_sum(values, got, sem, side, device):
    copy = send(values.at[side], got.at[side], sem.at[0, side], sem.at[1, side], device)
    copy.start()
    copy.wait()
    return values[side] + got[side]


def as_rows(column):
    return jnp.broadcast_to(column, (column.shape[0], 128)).T[:8]


def as_column(rows):
    return jnp.broadcast_to(rows[:1], (128, rows.shape[1])).T[:, :1]


def meet_square(dp, place):
    side_x, side_y = corners(dp)
    devices = ((side_x, place), (side_y, place))
    for device in devices:
        greet(device)
    pl.semaphore_wait(pltpu.get_barrier_semaphore(), 2)
    return devices


def normed_heads_kernel(
    model_width, q_ref, k_ref, q_gain, k_gain, cos_ref, sin_ref, queries, keys, inverse, sums, got, sem
):
    devices = meet_square(lax.axis_index("dp"), lax.axis_index("expert"))
    raws, gains, outs = (q_ref, k_ref), (q_gain, k_gain), (queries, keys)
    for i, raw in enumerate(raws):
        total = jnp.sum(raw[...] * raw[...], axis=1, keepdims=True)
        sums[0, 8 * i : 8 * i + 8] = as_rows(total)
    sums[1] = square_sum(sums, got, sem, 0, devices[0])
    total = square_sum(sums, got, sem, 1, devices[1])
    inverse[...] = lax.rsqrt(total * (1.0 / model_width) + epsilon)
    for i, raw in enumerate(raws):
        scale = as_column(inverse[8 * i : 8 * i + 8])
        for at in range(0, raw.shape[1], HD):
            head = raw[:, at : at + HD] * scale * gains[i][:, at : at + HD]
            turned = head * cos_ref[...] + pltpu.roll(head, HD // 2, 1) * sin_ref[...]
            outs[i][:, at : at + HD] = turned.astype(outs[i].dtype)


def normed_heads(q_raw, k_raw, q_gain, k_gain, cos, sin, model_width):
    rows, width = q_raw.shape
    head = jax.ShapeDtypeStruct((rows, width), jnp.bfloat16)
    return pl.pallas_call(
        functools.partial(normed_heads_kernel, model_width),
        out_shape=[head, head, jax.ShapeDtypeStruct((16, rows), jnp.float32)],
        in_specs=[pl.BlockSpec(memory_space=pltpu.VMEM)] * 6,
        out_specs=[pl.BlockSpec(memory_space=pltpu.VMEM)] * 3,
        scratch_shapes=[
            pltpu.VMEM((2, 16, rows), jnp.float32),
            pltpu.VMEM((2, 16, rows), jnp.float32),
            pltpu.SemaphoreType.DMA((2, 2)),
        ],
        compiler_params=pltpu.CompilerParams(
            collective_id=11, has_side_effects=True, vmem_limit_bytes=40 << 20
        ),
        name="normed_heads",
    )(q_raw, k_raw, q_gain.reshape(1, width), k_gain.reshape(1, width), cos, sin)


def normed_heads_back_kernel(
    model_width,
    dq_ref,
    dk_ref,
    dv_ref,
    q_ref,
    k_ref,
    q_gain,
    k_gain,
    cos_ref,
    sin_ref,
    inverse,
    grads,
    gain_grads,
    sums,
    got,
    sem,
):
    devices = meet_square(lax.axis_index("dp"), lax.axis_index("expert"))
    raws, gains, news = (q_ref, k_ref), (q_gain, k_gain), (dq_ref, dk_ref)
    rows, width = q_ref.shape

    def parts(i, at):
        cut = slice(at, at + HD)
        new = news[i][:, cut].astype(jnp.float32)
        back = new * cos_ref[...] - pltpu.roll(new, HD // 2, 1) * sin_ref[...]
        unit = raws[i][:, cut] * as_column(inverse[8 * i : 8 * i + 8])
        return back, unit, back * gains[i][:, cut]

    for i in (0, 1):
        total = jnp.zeros((rows, 1), jnp.float32)
        for at in range(0, width, HD):
            back, unit, scaled = parts(i, at)
            gain_grad = jnp.sum(back * unit, axis=0, keepdims=True)
            gain_grads[8 * i : 8 * i + 8, at : at + HD] = jnp.broadcast_to(gain_grad, (8, HD))
            total = total + jnp.sum(scaled * unit, axis=1, keepdims=True)
        sums[0, 8 * i : 8 * i + 8] = as_rows(total)
    sums[1] = square_sum(sums, got, sem, 0, devices[0])
    dots = square_sum(sums, got, sem, 1, devices[1]) * (1.0 / model_width)
    for i in (0, 1):
        dot = as_column(dots[8 * i : 8 * i + 8])
        scale = as_column(inverse[8 * i : 8 * i + 8])
        for at in range(0, width, HD):
            _, unit, scaled = parts(i, at)
            value = scale * (scaled - unit * dot)
            grads[:, i * width + at : i * width + at + HD] = value.astype(grads.dtype)
    grads[:, 2 * width :] = dv_ref[...]


def normed_heads_back(dq, dk, dv, q_raw, k_raw, q_gain, k_gain, cos, sin, inverse, model_width):
    rows, width = q_raw.shape
    return pl.pallas_call(
        functools.partial(normed_heads_back_kernel, model_width),
        out_shape=[
            jax.ShapeDtypeStruct((rows, 3 * width), jnp.bfloat16),
            jax.ShapeDtypeStruct((16, width), jnp.float32),
        ],
        in_specs=[pl.BlockSpec(memory_space=pltpu.VMEM)] * 10,
        out_specs=[pl.BlockSpec(memory_space=pltpu.VMEM)] * 2,
        scratch_shapes=[
            pltpu.VMEM((2, 16, rows), jnp.float32),
            pltpu.VMEM((2, 16, rows), jnp.float32),
            pltpu.SemaphoreType.DMA((2, 2)),
        ],
        compiler_params=pltpu.CompilerParams(
            collective_id=12, has_side_effects=True, vmem_limit_bytes=40 << 20
        ),
        name="normed_heads_back",
    )(
        dq,
        dk,
        dv,
        q_raw,
        k_raw,
        q_gain.reshape(1, width),
        k_gain.reshape(1, width),
        cos,
        sin,
        inverse,
    )


def per_device(
    inputs,
    attention_norm_gain,
    w_query,
    w_key,
    w_value,
    w_out,
    q_gain,
    k_gain,
    expert_norm_gain,
    w_router,
    w_gate,
    w_up,
    w_down,
    routes,
    lengths,
    d_output,
):
    pack_count, seg_rows, model_width = inputs.shape
    local_width = w_query.shape[1]
    local_heads = local_width // HD
    experts = w_router.shape[1]
    groups = lax.axis_size("expert")
    line = groups // 2
    pack_span = seg_rows * groups
    local_experts = w_gate.shape[0]
    offset_rows = lax.axis_index("expert") * seg_rows
    segment, positions = doc_layout(lengths, pack_span)
    pos_query = lax.dynamic_slice_in_dim(positions, offset_rows, seg_rows, 1)
    cos_table, sin_table = rope_tables(pos_query[0], HD)
    inputs_single_float = inputs.astype(jnp.float32)
    first_inverse_norm = lax.rsqrt(
        jnp.mean(inputs_single_float * inputs_single_float, axis=-1, keepdims=True) + epsilon
    )
    first_unit_input = inputs_single_float * first_inverse_norm
    first_normed_input = (first_unit_input * attention_norm_gain).astype(jnp.bfloat16)
    q_raw = jnp.dot(first_normed_input[0], w_query, preferred_element_type=jnp.float32)
    k_raw = jnp.dot(first_normed_input[0], w_key, preferred_element_type=jnp.float32)
    value_rows = jnp.dot(first_normed_input[0], w_value, preferred_element_type=jnp.float32).astype(
        jnp.bfloat16
    )
    queries, keys, head_inverse = normed_heads(
        q_raw, k_raw, q_gain, k_gain, cos_table, sin_table, model_width
    )
    layout = (segment, positions)
    if local_heads == line:
        attention = by_head(layout, w_out, line)
    else:
        attention = by_query(layout, w_out, offset_rows)
    attended, projected, kept = attention[0](queries, keys, value_rows)
    own = lax.axis_index("dp")
    part_rows = seg_rows // lax.axis_size("dp")

    def own_rows(rows):
        return lax.dynamic_slice_in_dim(rows, own * part_rows, part_rows, 0)

    hidden_state = own_rows(inputs_single_float[0]) + projected
    second_inverse_norm = lax.rsqrt(
        jnp.mean(hidden_state * hidden_state, axis=-1, keepdims=True) + epsilon
    )
    second_unit_input = hidden_state * second_inverse_norm
    second_normed_input = second_unit_input * expert_norm_gain
    router = jax.nn.softmax(
        jnp.dot(second_normed_input, w_router, precision=lax.Precision.HIGHEST), axis=-1
    )
    chosen = own_rows(routes[:, 0, :])
    expert_range = jnp.arange(experts, dtype=jnp.int32)
    named = jnp.any(chosen[:, :, None] == expert_range, axis=1)
    top_own = own_rows(d_output[0])
    top_all = lax.all_gather(top_own, ALL, axis=0, tiled=True)
    gate_table = jnp.where(named, router, 0.0)
    gate_high = gate_table.astype(jnp.bfloat16)
    gate_low = (gate_table - gate_high.astype(jnp.float32)).astype(jnp.bfloat16)
    widen = ((0, 0), (0, 64 - experts))
    own_tokens = jnp.concatenate(
        [
            second_normed_input.astype(jnp.bfloat16),
            jnp.pad(gate_high, widen),
            jnp.pad(gate_low, widen),
        ],
        axis=1,
    )
    xn_all, grad_units, scaled, gate_part = gate_act(
        own_tokens, top_all, w_gate, w_up, w_down, line
    )
    (grad_tokens,) = product_sum(
        grad_units, (w_gate, w_up), True, gate_part, line, "grad_tokens", 4)
    grad_xn_exp = grad_tokens[:, :model_width]
    gate_sums = grad_tokens[:, model_width : model_width + experts]
    grad_router_probs = jnp.where(named, gate_sums, 0.0)
    grad_logits = router * (
        grad_router_probs - jnp.sum(router * grad_router_probs, axis=-1, keepdims=True)
    )
    grad_second_normed_input = grad_xn_exp + jnp.einsum(
        "se,de->sd", grad_logits, w_router, precision=lax.Precision.HIGHEST
    )
    grad_router = jnp.einsum(
        "sd,se->de", second_normed_input, grad_logits, precision=lax.Precision.HIGHEST
    )
    grad_expert_norm_gain = jnp.sum(grad_second_normed_input * second_unit_input, axis=0)
    grad_second_unit_input = grad_second_normed_input * expert_norm_gain
    grad_hidden = top_own.astype(jnp.float32) + second_inverse_norm * (
        grad_second_unit_input
        - second_unit_input
        * jnp.mean(grad_second_unit_input * second_unit_input, axis=-1, keepdims=True)
    )
    grad_attn, by_heads, by_tokens = attention[1](kept, grad_hidden.astype(jnp.bfloat16))
    moe_out, grad_gate, grad_up, *returned = product_sum(
        scaled,
        w_down.reshape(-1, model_width),
        False,
        None,
        line,
        "expert_sum",
        2,
        (xn_all, grad_units, w_gate.shape),
        by_heads,
        (False, True, True) if by_heads else (),
    )
    grad_queries, grad_keys, grad_values = returned or by_tokens
    output = (hidden_state + moe_out).astype(jnp.bfloat16)
    grad_out = jnp.einsum("sk,sd->kd", attended, grad_attn, preferred_element_type=jnp.float32)
    grad_heads_raw, gain_grads = normed_heads_back(
        grad_queries,
        grad_keys,
        grad_values,
        q_raw,
        k_raw,
        q_gain,
        k_gain,
        cos_table,
        sin_table,
        head_inverse,
        model_width,
    )
    grad_q_gain, grad_k_gain = gain_grads[0], gain_grads[8]
    grad_projections = jnp.einsum(
        "sd,sk->dk", first_normed_input[0], grad_heads_raw, preferred_element_type=jnp.float32
    )
    grad_first_normed_input = sum(
        contract(grad_heads_raw[:, i * local_width : (i + 1) * local_width], weight, 1, 1)
        for i, weight in enumerate((w_query, w_key, w_value))
    )
    grad_attn_gain = jnp.sum(grad_first_normed_input * first_unit_input[0], axis=0)
    wide = grad_projections.shape[1]
    small = jnp.concatenate(
        [
            grad_q_gain.reshape(groups, -1),
            grad_k_gain.reshape(groups, -1),
            grad_attn_gain.reshape(groups, -1),
            grad_expert_norm_gain.reshape(groups, -1),
            grad_router.reshape(groups, -1),
        ],
        axis=1,
    )
    small_rows = 32
    filled = small.shape[1]
    small = jnp.pad(small, ((0, 0), (0, small_rows * wide - filled)))
    summed, own_small, shared, outputs, grad_input, grad_down = closing(
        grad_projections.astype(jnp.bfloat16).reshape(groups, -1, wide),
        small.astype(jnp.bfloat16).reshape(groups, small_rows, wide),
        grad_first_normed_input.astype(jnp.bfloat16),
        grad_hidden,
        own_rows(first_unit_input[0]),
        own_rows(first_inverse_norm[0]),
        attention_norm_gain,
        output,
        top_all,
        scaled,
        w_down.shape,
        line,
    )
    gain_size, norm_size = local_width // groups, model_width // groups
    own_gains = own_small.reshape(-1)[: 2 * gain_size]
    shared = shared.reshape(-1)[2 * gain_size : filled]
    grad_out = lax.psum_scatter(
        grad_out.astype(jnp.bfloat16), "expert", scatter_dimension=0, tiled=True
    ).astype(jnp.float32)
    return (
        outputs[None],
        grad_input.astype(jnp.float32)[None],
        shared[:norm_size],
        summed[:, :local_width],
        summed[:, local_width : 2 * local_width],
        summed[:, 2 * local_width :],
        grad_out,
        own_gains[:gain_size],
        own_gains[gain_size:],
        shared[norm_size : 2 * norm_size],
        shared[2 * norm_size :].reshape(norm_size, experts),
        grad_gate.astype(jnp.float32),
        grad_up.astype(jnp.float32),
        grad_down.astype(jnp.float32),
    )


def solution(mesh):
    placed = (
        P(None, "expert", None),
        P(),
        P(None, "dp"),
        P(None, "dp"),
        P(None, "dp"),
        P("dp", None),
        P("dp"),
        P("dp"),
        P(),
        P(),
        P("expert", None, "dp"),
        P("expert", None, "dp"),
        P("expert", "dp", None),
        P("expert", None, None),
        P(),
        P(None, "expert", None),
    )
    return jax.shard_map(
        per_device,
        mesh=mesh,
        in_specs=placed,
        out_specs=(
            P(None, "expert", None),
            P(None, "expert", None),
            P("expert"),
            P("expert", "dp"),
            P("expert", "dp"),
            P("expert", "dp"),
            P(("dp", "expert"), None),
            P(("dp", "expert")),
            P(("dp", "expert")),
            P("expert"),
            P("expert", None),
            P("expert", None, "dp"),
            P("expert", None, "dp"),
            P("expert", "dp", None),
        ),
        check_vma=False,
    )
```
